32 devices in a mesh: dp: 1 (over z), tp: 32 (over y, x, core).
Axes of the slice: x: 4, y: 4, z: 1, core: 2. Of those that a mesh axis runs over, the one named last changes fastest.
The devices are a block of a 4x4x8 slice.
Arguments:
- hidden: bfloat16 [3, 768, 5120], P('dp')
- grad_out: bfloat16 [3, 768, 5120], P('dp')
- norm_gain: bfloat16 [5120], replicated
- w_query: bfloat16 [5120, 4096], P(None, 'tp')
- w_key: bfloat16 [5120, 1024], replicated
- w_value: bfloat16 [5120, 1024], replicated
- w_out: bfloat16 [4096, 5120], P('tp')
Outputs:
- output 1: bfloat16 [3, 768, 5120], P('dp')
- output 2: bfloat16 [3, 768, 5120], P('dp')
- output 3: float32 [5120], P('dp')
- output 4: float32 [5120, 4096], P('dp', 'tp')
- output 5: float32 [5120, 4096], P('dp', 'tp')
- output 6: float32 [5120, 4096], P('dp', 'tp')
- output 7: float32 [4096, 5120], P(('dp', 'tp'))
All inputs are finite; a program needn't handle non-finite values.
Results may differ from the reference program's by a relative error of at most 0.00989727.
Values sent between devices are 32-bit elements.
A program may use at most 768 MiB of HBM per device.

```python
import math
import jax
import jax.numpy as jnp
from jax import lax

BATCH_SIZE = 3
SEQ_LEN = 768
D_MODEL = 5120
Q_HEADS = 32
KV_HEADS = 8
HEAD_DIM = 128
TP_SIZE = 32
NORM_EPS = 1.0e-5
ROPE_BASE = 10000.0
MASK_VALUE = -1.0e30


def setup_inputs(seed: int = 0, part: int = 0) -> dict:
    root_key = jax.random.key(seed)
    shared_key, local_key = jax.random.split(root_key)
    part_key = jax.random.fold_in(local_key, part)
    key_hidden, key_grad = jax.random.split(part_key)
    key_gain, key_query, key_key, key_value, key_out = jax.random.split(shared_key, 5)
    inner_width = Q_HEADS * HEAD_DIM
    kv_width = KV_HEADS * HEAD_DIM
    score_gain = math.sqrt(0.5 * math.log(SEQ_LEN))
    act_shape = (BATCH_SIZE, SEQ_LEN, D_MODEL)
    hidden = jax.random.normal(key_hidden, act_shape, jnp.float32)
    grad_out = jax.random.normal(key_grad, act_shape, jnp.float32)
    norm_gain = 1.0 + 0.3 * jax.random.normal(key_gain, (D_MODEL,), jnp.float32)
    w_query = jax.random.normal(key_query, (D_MODEL, inner_width), jnp.float32) * (score_gain / math.sqrt(D_MODEL))
    w_key = jax.random.normal(key_key, (D_MODEL, kv_width), jnp.float32) / math.sqrt(D_MODEL)
    w_value = jax.random.normal(key_value, (D_MODEL, kv_width), jnp.float32) / math.sqrt(D_MODEL)
    w_out = jax.random.normal(key_out, (inner_width, D_MODEL), jnp.float32) * (3.0 / math.sqrt(inner_width))
    return {
        'hidden': hidden.astype(jnp.bfloat16),
        'grad_out': grad_out.astype(jnp.bfloat16),
        'norm_gain': norm_gain.astype(jnp.bfloat16),
        'w_query': w_query.astype(jnp.bfloat16),
        'w_key': w_key.astype(jnp.bfloat16),
        'w_value': w_value.astype(jnp.bfloat16),
        'w_out': w_out.astype(jnp.bfloat16),
    }


def to_bf16(tensor):
    return tensor + lax.stop_gradient(tensor.astype(jnp.bfloat16).astype(tensor.dtype) - tensor)


def rope_tables():
    positions = jnp.arange(SEQ_LEN, dtype=jnp.float32)
    inv_freq = ROPE_BASE ** (-jnp.arange(0, HEAD_DIM, 2, dtype=jnp.float32) / HEAD_DIM)
    angles = positions[:, None] * inv_freq[None, :]
    return jnp.cos(angles), jnp.sin(angles)


def rotate_pairs(tensor, cos_t, sin_t):
    pair_view = tensor.reshape(tensor.shape[:-1] + (HEAD_DIM // 2, 2))
    even_part = pair_view[..., 0]
    odd_part = pair_view[..., 1]
    cos_b = cos_t[:, None, :]
    sin_b = sin_t[:, None, :]
    rotated = jnp.stack([even_part * cos_b - odd_part * sin_b, even_part * sin_b + odd_part * cos_b], axis=-1)
    return rotated.reshape(tensor.shape)


def group_attention(blocks):
    q_block, k_block, v_block = blocks
    scores = jnp.einsum('bqjh,bkh->bjqk', q_block, k_block) / math.sqrt(HEAD_DIM)
    causal = jnp.arange(SEQ_LEN)[:, None] >= jnp.arange(SEQ_LEN)[None, :]
    scores = jnp.where(causal, scores, MASK_VALUE)
    attn_probs = to_bf16(jax.nn.softmax(scores, axis=-1))
    return to_bf16(jnp.einsum('bjqk,bkh->bqjh', attn_probs, v_block))


def forward(hidden, norm_gain, w_query, w_key, w_value, w_out):
    heads_per_kv = Q_HEADS // KV_HEADS
    mean_sq = jnp.mean(hidden * hidden, axis=-1, keepdims=True)
    normed = to_bf16(hidden * lax.rsqrt(mean_sq + NORM_EPS) * norm_gain)
    cos_t, sin_t = rope_tables()
    q_proj = jnp.einsum('bsd,de->bse', normed, w_query).reshape(BATCH_SIZE, SEQ_LEN, Q_HEADS, HEAD_DIM)
    k_proj = jnp.einsum('bsd,de->bse', normed, w_key).reshape(BATCH_SIZE, SEQ_LEN, KV_HEADS, HEAD_DIM)
    v_proj = jnp.einsum('bsd,de->bse', normed, w_value).reshape(BATCH_SIZE, SEQ_LEN, KV_HEADS, HEAD_DIM)
    q_rot = to_bf16(rotate_pairs(q_proj, cos_t, sin_t)).reshape(BATCH_SIZE, SEQ_LEN, KV_HEADS, heads_per_kv, HEAD_DIM)
    k_rot = to_bf16(rotate_pairs(k_proj, cos_t, sin_t))
    v_heads = to_bf16(v_proj)
    attn_heads = lax.map(jax.checkpoint(group_attention), (jnp.moveaxis(q_rot, 2, 0), jnp.moveaxis(k_rot, 2, 0), jnp.moveaxis(v_heads, 2, 0)))
    attn_flat = jnp.moveaxis(attn_heads, 0, 2).reshape(BATCH_SIZE, SEQ_LEN, Q_HEADS * HEAD_DIM)
    attn_sum = jnp.einsum('bse,ed->bsd', attn_flat, w_out)
    return to_bf16(hidden + attn_sum)


def reference(hidden, grad_out, norm_gain, w_query, w_key, w_value, w_out):
    block_out, pullback = jax.vjp(forward, hidden.astype(jnp.float32), norm_gain.astype(jnp.float32), w_query.astype(jnp.float32), w_key.astype(jnp.float32), w_value.astype(jnp.float32), w_out.astype(jnp.float32))
    grad_hidden, grad_gain, grad_w_query, grad_w_key, grad_w_value, grad_w_out = pullback(grad_out.astype(jnp.float32))
    sharers = TP_SIZE // KV_HEADS
    grad_w_key_rep = jnp.repeat(grad_w_key.reshape(D_MODEL, KV_HEADS, HEAD_DIM), sharers, axis=1).reshape(D_MODEL, TP_SIZE * HEAD_DIM)
    grad_w_value_rep = jnp.repeat(grad_w_value.reshape(D_MODEL, KV_HEADS, HEAD_DIM), sharers, axis=1).reshape(D_MODEL, TP_SIZE * HEAD_DIM)
    return (block_out.astype(jnp.bfloat16), grad_hidden.astype(jnp.bfloat16), grad_gain.astype(jnp.float32), grad_w_query.astype(jnp.float32), grad_w_key_rep.astype(jnp.float32), grad_w_value_rep.astype(jnp.float32), grad_w_out.astype(jnp.float32))
```

```python
import math
import jax
import jax.numpy as jnp
from jax import lax
from jax.sharding import PartitionSpec as P

HEAD_DIM = 128
NORM_EPS = 1.0e-5
ROPE_BASE = 10000.0
MASK_VALUE = -1.0e30
SCORE_SCALE = 1.0 / math.sqrt(HEAD_DIM)


def rope_tables(seq_len):
    positions = jnp.arange(seq_len, dtype=jnp.float32)
    inv_freq = ROPE_BASE ** (-jnp.arange(0, HEAD_DIM, 2, dtype=jnp.float32) / HEAD_DIM)
    angles = positions[:, None] * inv_freq[None, :]
    return jnp.cos(angles), jnp.sin(angles)


def rotate_pairs(tensor, cos_t, sin_t):
    pair_view = tensor.reshape(tensor.shape[:-1] + (HEAD_DIM // 2, 2))
    even_part = pair_view[..., 0]
    odd_part = pair_view[..., 1]
    cos_b = cos_t[:, None, :]
    sin_b = sin_t[:, None, :]
    rotated = jnp.stack([even_part * cos_b - odd_part * sin_b, even_part * sin_b + odd_part * cos_b], axis=-1)
    return rotated.reshape(tensor.shape)


def group_sum(tensor, tp_size, group_size):
    total = tensor
    for level in range(group_size.bit_length() - 1):
        distance = 2 ** level
        partner_pairs = [(source, source ^ distance) for source in range(tp_size)]
        total = total + lax.ppermute(total, 'tp', perm=partner_pairs)
    return total


def solution(mesh):
    tp_size = mesh.shape['tp']

    def block_fn(hidden, grad_out, norm_gain, w_query, w_key, w_value, w_out):
        kv_heads = w_key.shape[1] // HEAD_DIM
        group_size = tp_size // kv_heads
        q_heads_local = w_query.shape[1] // HEAD_DIM
        batch_local, seq_len, d_model = hidden.shape
        kv_index = lax.axis_index('tp') // group_size
        w_kv = jnp.concatenate([
            lax.dynamic_slice_in_dim(w_key, kv_index * HEAD_DIM, HEAD_DIM, axis=1),
            lax.dynamic_slice_in_dim(w_value, kv_index * HEAD_DIM, HEAD_DIM, axis=1)], axis=1)
        cos_t, sin_t = rope_tables(seq_len)

        hidden_f32 = hidden.astype(jnp.float32)
        inv_rms = lax.rsqrt(jnp.mean(hidden_f32 * hidden_f32, axis=-1, keepdims=True) + NORM_EPS)
        unit_rows = hidden_f32 * inv_rms
        gain_f32 = norm_gain.astype(jnp.float32)
        normed = (unit_rows * gain_f32).astype(jnp.bfloat16)
        q_proj = jnp.einsum('bsd,de->bse', normed, w_query, preferred_element_type=jnp.float32)
        q_rot = rotate_pairs(q_proj.reshape(batch_local, seq_len, q_heads_local, HEAD_DIM), cos_t, sin_t).astype(jnp.bfloat16)
        kv_proj = jnp.einsum('bsd,de->bse', normed, w_kv, preferred_element_type=jnp.float32)
        k_rot = rotate_pairs(kv_proj[:, :, None, :HEAD_DIM], cos_t, sin_t)[:, :, 0, :].astype(jnp.bfloat16)
        v_head = kv_proj[:, :, HEAD_DIM:].astype(jnp.bfloat16)
        scores = jnp.einsum('bqjh,bkh->bjqk', q_rot, k_rot, preferred_element_type=jnp.float32) * SCORE_SCALE
        causal = jnp.arange(seq_len)[:, None] >= jnp.arange(seq_len)[None, :]
        attn_probs = jax.nn.softmax(jnp.where(causal, scores, MASK_VALUE), axis=-1)
        probs_bf16 = attn_probs.astype(jnp.bfloat16)
        attn_heads = jnp.einsum('bjqk,bkh->bqjh', probs_bf16, v_head, preferred_element_type=jnp.float32).astype(jnp.bfloat16)
        attn_flat = attn_heads.reshape(batch_local, seq_len, q_heads_local * HEAD_DIM)
        out_part = jnp.einsum('bse,ed->bsd', attn_flat, w_out, preferred_element_type=jnp.float32)
        attn_rows = lax.psum_scatter(out_part.reshape(batch_local * seq_len, d_model), 'tp', scatter_dimension=0, tiled=True)
        attn_sum = lax.all_gather(attn_rows, 'tp', axis=0, tiled=True).reshape(batch_local, seq_len, d_model)
        block_out = (hidden_f32 + attn_sum).astype(jnp.bfloat16)

        grad_w_out = jnp.einsum('bse,bsd->ed', attn_flat, grad_out, preferred_element_type=jnp.float32)
        grad_heads = jnp.einsum('bsd,ed->bse', grad_out, w_out, preferred_element_type=jnp.float32).astype(jnp.bfloat16).reshape(batch_local, seq_len, q_heads_local, HEAD_DIM)
        grad_probs = jnp.einsum('bqjh,bkh->bjqk', grad_heads, v_head, preferred_element_type=jnp.float32)
        grad_v = jnp.einsum('bjqk,bqjh->bkh', probs_bf16, grad_heads, preferred_element_type=jnp.float32)
        row_dot = jnp.sum(attn_probs * grad_probs, axis=-1, keepdims=True)
        grad_scores = (attn_probs * (grad_probs - row_dot) * SCORE_SCALE).astype(jnp.bfloat16)
        grad_q_rot = jnp.einsum('bjqk,bkh->bqjh', grad_scores, k_rot, preferred_element_type=jnp.float32)
        grad_k_rot = jnp.einsum('bjqk,bqjh->bkh', grad_scores, q_rot, preferred_element_type=jnp.float32)
        grad_q = rotate_pairs(grad_q_rot, cos_t, -sin_t).astype(jnp.bfloat16).reshape(batch_local, seq_len, q_heads_local * HEAD_DIM)
        grad_k = rotate_pairs(grad_k_rot[:, :, None, :], cos_t, -sin_t)[:, :, 0, :]
        grad_kv_f32 = jnp.concatenate([grad_k, grad_v], axis=-1)
        grad_kv = grad_kv_f32.astype(jnp.bfloat16)
        grad_normed_part = (jnp.einsum('bse,de->bsd', grad_q, w_query, preferred_element_type=jnp.float32)
                            + jnp.einsum('bse,de->bsd', grad_kv, w_kv, preferred_element_type=jnp.float32))
        rows = batch_local * seq_len // tp_size
        grad_rows = lax.psum_scatter(grad_normed_part.reshape(batch_local * seq_len, d_model), 'tp', scatter_dimension=0, tiled=True)
        first = lax.axis_index('tp') * rows
        unit_own = lax.dynamic_slice_in_dim(unit_rows.reshape(batch_local * seq_len, d_model), first, rows, axis=0)
        inv_own = lax.dynamic_slice_in_dim(inv_rms.reshape(batch_local * seq_len, 1), first, rows, axis=0)
        gain_own = grad_rows * gain_f32
        delta = inv_own * (gain_own - unit_own * jnp.mean(gain_own * unit_own, axis=-1, keepdims=True))
        grad_gain = lax.psum(jnp.sum(grad_rows * unit_own, axis=0), 'tp')
        delta_all = lax.all_gather(delta, 'tp', axis=0, tiled=True).reshape(batch_local, seq_len, d_model)
        grad_hidden = (grad_out.astype(jnp.float32) + delta_all).astype(jnp.bfloat16)
        grad_kv_sum = group_sum(grad_kv_f32, tp_size, group_size).astype(jnp.bfloat16)
        grad_w_query = jnp.einsum('bsd,bse->de', normed, grad_q, preferred_element_type=jnp.float32)
        grad_w_kv = jnp.einsum('bsd,bse->de', normed, grad_kv_sum, preferred_element_type=jnp.float32)
        return block_out, grad_hidden, grad_gain, grad_w_query, grad_w_kv[:, :HEAD_DIM], grad_w_kv[:, HEAD_DIM:], grad_w_out

    act_spec = P('dp', None, None)
    return jax.shard_map(
        block_fn, mesh=mesh,
        in_specs=(act_spec, act_spec, P(None), P(None, 'tp'), P(None, None), P(None, None), P('tp', None)),
        out_specs=(act_spec, act_spec, P('dp'), P('dp', 'tp'), P('dp', 'tp'), P('dp', 'tp'), P(('dp', 'tp'), None)),
        check_vma=False)
```

```python
import functools
import math
import jax
import jax.numpy as jnp
from jax import lax
from jax.experimental import pallas as pl
from jax.experimental.pallas import tpu as pltpu
from jax.sharding import PartitionSpec as P

HEAD_DIM = 128
NORM_EPS = 1.0e-5
ROPE_BASE = 10000.0
MASK_VALUE = -1.0e30
SCORE_SCALE = 1.0 / math.sqrt(HEAD_DIM)
RING = 4
CORES = 2
ROW_DEVICES = RING * CORES
CHUNKS = 6
VMEM_BYTES = 56 * 1024 * 1024


def rope_tables(seq_len):
    positions = jnp.arange(seq_len, dtype=jnp.float32)
    inv_freq = ROPE_BASE ** (-jnp.arange(0, HEAD_DIM, 2, dtype=jnp.float32) / HEAD_DIM)
    angles = positions[:, None] * inv_freq[None, :]
    return jnp.cos(angles), jnp.sin(angles)


def rotate_pairs(tensor, cos_t, sin_t):
    pair_view = tensor.reshape(tensor.shape[:-1] + (HEAD_DIM // 2, 2))
    even_part = pair_view[..., 0]
    odd_part = pair_view[..., 1]
    cos_b = cos_t[:, None, :]
    sin_b = sin_t[:, None, :]
    rotated = jnp.stack([even_part * cos_b - odd_part * sin_b, even_part * sin_b + odd_part * cos_b], axis=-1)
    return rotated.reshape(tensor.shape)


class Place:
    def __init__(self):
        index = lax.axis_index('tp')
        self.c = lax.rem(index, CORES)
        self.x = lax.rem(index // CORES, RING)
        self.y = index // ROW_DEVICES

    def at(self, y, x, c):
        return {'tp': (y * RING + x) * CORES + c}


def turn(position, by):
    return lax.rem(position + (by % RING), RING)


def exchange_kernel(backward, chunks, *refs):
    if backward:
        (act_hbm, kv_hbm, wt_ref, wkv_ref, x_ref, dout_ref, inv_ref, gain_ref, out_ref, kv_out,
         gath, wb, part, ring, kvp, kv_core, kv_send, kv_chip, rowpart, rowall,
         gs_sem, gr_sem, rs_sem, rr_sem, ks_sem, kr_sem, ms_sem, mr_sem, loc_sem) = refs
    else:
        act_hbm, wt_ref, x_ref, out_ref, gath, wb, part, ring, gs_sem, gr_sem, rs_sem, rr_sem, loc_sem = refs
    me = Place()
    x, y, c = me.x, me.y, me.c
    xr, xl, xo = turn(x, 1), turn(x, -1), turn(x, 2)
    yu, yd = turn(y, 1), turn(y, -1)
    other = 1 - c
    own = CORES * x + c
    left, right, far = CORES * xl + c, CORES * xr + c, CORES * xo + c
    parts = gath.shape[1]
    half = parts // 2
    rows_y, width = out_ref.shape[0] if not backward else x_ref.shape[0], out_ref.shape[1]
    r = rows_y // chunks
    h = r // 2

    barrier = pltpu.get_barrier_semaphore()
    peers = [me.at(yu, x, c), me.at(yd, x, c), me.at(y, xr, c), me.at(y, xl, c), me.at(y, x, other)]
    if backward:
        peers += [me.at(y, xo, c), me.at(y, xr, other), me.at(y, xl, other), me.at(y, xo, other)]
    for peer in peers:
        pl.semaphore_signal(barrier, inc=1, device_id=peer, device_id_type=pl.DeviceIdType.MESH)

    load = pltpu.make_async_copy(act_hbm, gath.at[own, pl.ds(0, RING)], loc_sem.at[0])
    load.start()
    if backward:
        load_kv = pltpu.make_async_copy(kv_hbm, kvp, loc_sem.at[1])
        load_kv.start()
    wb[pl.ds(0, wt_ref.shape[0]), :] = wt_ref[...].astype(jnp.bfloat16)
    if backward:
        wb[pl.ds(wt_ref.shape[0], wkv_ref.shape[0]), :] = wkv_ref[...]
        load_kv.wait()
    load.wait()
    pl.semaphore_wait(barrier, len(peers))

    def remote(src, dst, send_sem, recv_sem, peer):
        return pltpu.make_async_remote_copy(src_ref=src, dst_ref=dst, send_sem=send_sem, recv_sem=recv_sem,
                                            device_id=peer, device_id_type=pl.DeviceIdType.MESH)

    def block(source, k, first=0, count=parts):
        return gath.at[source, pl.ds(first, count), pl.ds(k * r, r)]

    def gather(event, k, source, peer, first=0, count=parts):
        return remote(block(source, k, first, count), block(source, k, first, count),
                      gs_sem.at[event, k], gr_sem.at[event, k], peer)

    to_right, to_left, to_partner = me.at(y, xr, c), me.at(y, xl, c), me.at(y, x, other)

    def sends(k):
        return [gather(0, k, own, to_right), gather(1, k, own, to_left), gather(2, k, own, to_partner),
                gather(3, k, left, to_right, 0, half), gather(4, k, right, to_left, half, parts - half),
                gather(5, k, left, to_partner), gather(6, k, right, to_partner), gather(7, k, far, to_partner)]

    p_own, p_left, p_right, p_far = [CORES * pos + other for pos in (x, xl, xr, xo)]

    def receives(k):
        return [gather(0, k, left, to_right), gather(1, k, right, to_left), gather(2, k, p_own, to_partner),
                gather(3, k, far, to_right, 0, half), gather(4, k, far, to_left, half, parts - half),
                gather(5, k, p_left, to_partner), gather(6, k, p_right, to_partner), gather(7, k, p_far, to_partner)]

    def rows_of(way, k):
        return pl.ds(k * r + way * h, h)

    def sum_copy(way, step, k):
        d = turn(y, -(1 + step) if way == 0 else 1 + step)
        return remote(part.at[d, rows_of(way, k)], ring.at[way, step, k], rs_sem.at[way, step, k],
                      rr_sem.at[way, step, k], me.at(yu if way == 0 else yd, x, c))

    def multiply(d, k):
        rows = pl.ds(k * r, r)
        pieces = [gath[j, d, rows, :] for j in range(ROW_DEVICES)]
        if backward:
            j = CORES * lax.rem(d, 2) + d // 2
            pieces += [gath[j, RING, rows, :], gath[j, RING + 1, rows, :],
                       gath[j + RING, RING, rows, :], gath[j + RING, RING + 1, rows, :]]
        lhs = jnp.concatenate([piece.astype(jnp.bfloat16) for piece in pieces], axis=1)
        part[d, rows, :] = jnp.dot(lhs, wb[...], preferred_element_type=jnp.float32)

    def advance(k, step):
        for way in (0, 1):
            sum_copy(way, step, k).wait_recv()
            d = turn(y, -(2 + step) if way == 0 else 2 + step)
            part[d, rows_of(way, k), :] += ring[way, step, k]
            if step < RING - 2:
                sum_copy(way, step + 1, k).start()
        if step == RING - 2:
            finish(k)

    def finish(k):
        rows = pl.ds(k * r, r)
        total = part[y, rows, :]
        if not backward:
            out_ref[rows, :] = (x_ref[rows, :].astype(jnp.float32) + total).astype(jnp.bfloat16).astype(jnp.float32)
            return
        unit = x_ref[rows, :].astype(jnp.float32) * inv_ref[rows, :]
        row_sum = jnp.sum(total * gain_ref[...] * unit, axis=1, keepdims=True)
        square = jnp.concatenate([jnp.broadcast_to(row_sum, (r, 128)), jnp.zeros((128 - r, 128), jnp.float32)], axis=0)
        rowpart[k] = jnp.transpose(square)[0:8, :]
        gain_row = jnp.sum(total * unit, axis=0, keepdims=True)
        tail = pl.ds(rows_y, 8)
        row_id = lax.broadcasted_iota(jnp.int32, (8, width), 0)
        addend = jnp.where(row_id == 0, jnp.broadcast_to(gain_row, (8, width)), 0.0)
        out_ref[tail, :] = addend if k == 0 else out_ref[tail, :] + addend

    if backward:
        p = lax.rem(x, 2)
        xn = x + 1 - 2 * p
        mine, theirs = CORES * c + p, CORES * c + 1 - p
        core_copy = remote(kvp.at[pl.ds(CORES * other, CORES)], kv_core, ks_sem.at[0], kr_sem.at[0], to_partner)
        core_copy.start()
        core_copy.wait_recv()

        def chip_copy(k):
            return remote(kv_send.at[:, pl.ds(k * r, r)], kv_chip.at[:, pl.ds(k * r, r)], ks_sem.at[1 + k],
                          kr_sem.at[1 + k], me.at(y, xn, c))

        for k in range(chunks):
            rows = pl.ds(k * r, r)
            kv_send[:, rows, :] = kvp[theirs, :, rows, :] + kv_core[1 - p, :, rows, :]
            chip_copy(k).start()

        def settle_kv(k):
            chip_copy(k).wait_recv()
            rows = pl.ds(k * r, r)
            total = kvp[mine, :, rows, :] + kv_core[p, :, rows, :] + kv_chip[:, rows, :]
            gath[own, pl.ds(RING, 2), rows, :] = total.astype(jnp.bfloat16).astype(jnp.float32)

    def begin(k):
        if backward:
            settle_kv(k)
        for copy in sends(k)[:3]:
            copy.start()

    begin(0)
    if chunks > 1:
        begin(1)
    for k in range(chunks + RING - 1):
        if k < chunks:
            out_going, incoming = sends(k), receives(k)
            incoming[0].wait_recv()
            out_going[3].start()
            out_going[5].start()
            incoming[1].wait_recv()
            out_going[4].start()
            out_going[6].start()
            if k + 2 < chunks:
                begin(k + 2)
        for step in range(RING - 1):
            if 0 <= k - 1 - step < chunks:
                advance(k - 1 - step, step)
        if k < chunks:
            incoming[3].wait_recv()
            incoming[4].wait_recv()
            out_going[7].start()
            for event in (2, 5, 6, 7):
                incoming[event].wait_recv()
            multiply(yd, k)
            sum_copy(0, 0, k).start()
            multiply(yu, k)
            sum_copy(1, 0, k).start()
            multiply(turn(y, 2), k)
            multiply(y, k)

    if backward:
        members = [(pos, core) for pos in (xr, xl, xo) for core in (c, other)] + [(x, other)]

        def mean_copy(n, m):
            pos, core = members[n]
            return remote(rowpart, rowall.at[m], ms_sem.at[n], mr_sem.at[m], me.at(y, pos, core))

        slots = [2, 3, 0, 1, 4, 5, 6]
        copies = [mean_copy(n, slots[n]) for n in range(7)]
        for copy in copies:
            copy.start()
        kv_head = x // 2
        kv_copies = [pltpu.make_async_copy(gath.at[CORES * (2 * kv_head + d % 2) + d // 2, pl.ds(RING, 2)], kv_out.at[d],
                                           loc_sem.at[d]) for d in range(RING)]
        for copy in kv_copies:
            copy.start()
        for copy in copies:
            copy.wait_recv()
        sums = rowpart[...]
        for m in range(7):
            sums = sums + rowall[m]
        d_model = width * ROW_DEVICES
        for k in range(chunks):
            rows = pl.ds(k * r, r)
            mean = jnp.transpose(sums[k])[0:r, 0:1] * (1.0 / d_model)
            inv = inv_ref[rows, :]
            unit = x_ref[rows, :].astype(jnp.float32) * inv
            delta = inv * (part[y, rows, :] * gain_ref[...] - unit * mean)
            out_ref[rows, :] = (dout_ref[rows, :].astype(jnp.float32) + delta).astype(jnp.bfloat16).astype(jnp.float32)
        for copy in kv_copies:
            copy.wait()
        for copy in copies:
            copy.wait_send()
        core_copy.wait_send()
        for k in range(chunks):
            chip_copy(k).wait_send()
    for k in range(chunks):
        for copy in sends(k):
            copy.wait_send()
        for way in (0, 1):
            for step in range(RING - 1):
                sum_copy(way, step, k).wait_send()


def exchange(act, weights, x_block, extra=None, collective_id=0):
    backward = extra is not None
    rows_y, width = x_block.shape
    chunks = CHUNKS
    h = rows_y // chunks // 2
    parts = RING + (2 if backward else 0)
    any_spec = pl.BlockSpec(memory_space=pl.ANY)
    vmem_spec = pl.BlockSpec(memory_space=pltpu.VMEM)
    depth = weights.shape[0] + (extra[1].shape[0] if backward else 0)
    dma = pltpu.SemaphoreType.DMA
    scratch = [
        pltpu.VMEM((ROW_DEVICES, parts, rows_y, HEAD_DIM), jnp.float32),
        pltpu.VMEM((depth, width), jnp.bfloat16),
        pltpu.VMEM((RING, rows_y, width), jnp.float32),
        pltpu.VMEM((2, RING - 1, chunks, h, width), jnp.float32),
    ]
    sems = [dma((8, chunks)), dma((8, chunks)), dma((2, RING - 1, chunks)), dma((2, RING - 1, chunks))]
    if backward:
        kv, w_kv, dout_block, inv_block, gain_block = extra
        args = (act, kv, weights, w_kv, x_block, dout_block, inv_block, gain_block)
        in_specs = [any_spec, any_spec] + [vmem_spec] * 6
        out_shape = (jax.ShapeDtypeStruct((rows_y + 8, width), jnp.float32),
                     jax.ShapeDtypeStruct((RING, 2, rows_y, HEAD_DIM), jnp.float32))
        out_specs = (vmem_spec, any_spec)
        scratch += [
            pltpu.VMEM((RING, 2, rows_y, HEAD_DIM), jnp.float32),
            pltpu.VMEM((CORES, 2, rows_y, HEAD_DIM), jnp.float32),
            pltpu.VMEM((2, rows_y, HEAD_DIM), jnp.float32),
            pltpu.VMEM((2, rows_y, HEAD_DIM), jnp.float32),
            pltpu.VMEM((chunks, 8, 128), jnp.float32),
            pltpu.VMEM((ROW_DEVICES - 1, chunks, 8, 128), jnp.float32),
        ]
        sems += [dma((1 + chunks,)), dma((1 + chunks,)), dma((ROW_DEVICES - 1,)), dma((ROW_DEVICES - 1,))]
    else:
        args = (act, weights, x_block)
        in_specs = [any_spec] + [vmem_spec] * 2
        out_shape = jax.ShapeDtypeStruct((rows_y, width), jnp.float32)
        out_specs = vmem_spec
    sems += [dma((RING,))]
    flops = 2 * RING * rows_y * depth * width
    return pl.pallas_call(
        functools.partial(exchange_kernel, backward, chunks),
        out_shape=out_shape, in_specs=in_specs, out_specs=out_specs, scratch_shapes=scratch + sems,
        compiler_params=pltpu.CompilerParams(collective_id=collective_id, has_side_effects=True, vmem_limit_bytes=VMEM_BYTES),
        cost_estimate=pl.CostEstimate(flops=flops, bytes_accessed=4 * RING * rows_y * width, transcendentals=0),
        name='exchange_bwd' if backward else 'exchange_fwd',
    )(*args)


def narrow(gathered, pad, d_model):
    rows_y, width = gathered.shape[0] // (RING * ROW_DEVICES) - pad, gathered.shape[1]

    def kernel(in_ref, out_ref):
        out_ref[...] = in_ref[pl.ds(0, rows_y), :].astype(jnp.bfloat16)

    return pl.pallas_call(
        kernel, grid=(RING, ROW_DEVICES),
        in_specs=[pl.BlockSpec((rows_y + pad, width), lambda y, i: (y * ROW_DEVICES + i, 0))],
        out_specs=pl.BlockSpec((rows_y, width), lambda y, i: (y, i)),
        out_shape=jax.ShapeDtypeStruct((RING * rows_y, d_model), jnp.bfloat16),
        compiler_params=pltpu.CompilerParams(vmem_limit_bytes=16 * 1024 * 1024),
        cost_estimate=pl.CostEstimate(flops=RING * rows_y * d_model, bytes_accessed=6 * RING * rows_y * d_model, transcendentals=0),
        name='narrow',
    )(gathered)


def solution(mesh):
    tp_size = mesh.shape['tp']
    row_groups = [list(range(first, first + ROW_DEVICES)) for first in range(0, tp_size, ROW_DEVICES)]

    def block_fn(hidden, grad_out, norm_gain, w_query, w_key, w_value, w_out):
        batch, seq_len, d_model = hidden.shape
        kv_heads = w_key.shape[1] // HEAD_DIM
        group_size = tp_size // kv_heads
        index = lax.axis_index('tp')
        y, column = index // ROW_DEVICES, index % ROW_DEVICES
        tokens, width = batch * seq_len, d_model // ROW_DEVICES
        rows_y = tokens // RING
        kv_pair = ROW_DEVICES // group_size * HEAD_DIM

        def spread(weight):
            blocks = weight.astype(jnp.float32).reshape(HEAD_DIM, ROW_DEVICES, width).transpose(1, 0, 2)
            got = lax.all_to_all(blocks, 'tp', 0, 0, axis_index_groups=row_groups, tiled=True)
            return got.reshape(ROW_DEVICES * HEAD_DIM, width)

        def own_block(array):
            return lax.dynamic_slice(array.reshape(tokens, d_model), (y * rows_y, column * width), (rows_y, width))

        def kv_block(weight):
            block = lax.dynamic_slice(weight, (column * width, y * kv_pair), (width, kv_pair))
            return block.T.reshape(-1, 1, HEAD_DIM, width)

        w_out_block = spread(w_out)
        w_query_block = spread(w_query.T)
        w_kv_block = jnp.concatenate([kv_block(w_key), kv_block(w_value)], axis=1).reshape(-1, width)

        kv_index = index // group_size
        w_kv = jnp.concatenate([
            lax.dynamic_slice_in_dim(w_key, kv_index * HEAD_DIM, HEAD_DIM, axis=1),
            lax.dynamic_slice_in_dim(w_value, kv_index * HEAD_DIM, HEAD_DIM, axis=1)], axis=1)
        cos_t, sin_t = rope_tables(seq_len)

        hidden_f32 = hidden.astype(jnp.float32)
        inv_rms = lax.rsqrt(jnp.mean(hidden_f32 * hidden_f32, axis=-1, keepdims=True) + NORM_EPS)
        gain_f32 = norm_gain.astype(jnp.float32)
        normed = (hidden_f32 * inv_rms * gain_f32).astype(jnp.bfloat16)
        q_proj = jnp.einsum('bsd,de->bse', normed, w_query, preferred_element_type=jnp.float32)
        q_rot = rotate_pairs(q_proj[:, :, None, :], cos_t, sin_t).astype(jnp.bfloat16)
        kv_proj = jnp.einsum('bsd,de->bse', normed, w_kv, preferred_element_type=jnp.float32)
        k_rot = rotate_pairs(kv_proj[:, :, None, :HEAD_DIM], cos_t, sin_t)[:, :, 0, :].astype(jnp.bfloat16)
        v_head = kv_proj[:, :, HEAD_DIM:].astype(jnp.bfloat16)
        scores = jnp.einsum('bqjh,bkh->bjqk', q_rot, k_rot, preferred_element_type=jnp.float32) * SCORE_SCALE
        causal = jnp.arange(seq_len)[:, None] >= jnp.arange(seq_len)[None, :]
        attn_probs = jax.nn.softmax(jnp.where(causal, scores, MASK_VALUE), axis=-1)
        probs_bf16 = attn_probs.astype(jnp.bfloat16)
        attn_heads = jnp.einsum('bjqk,bkh->bqjh', probs_bf16, v_head, preferred_element_type=jnp.float32).astype(jnp.bfloat16)
        attn_flat = attn_heads.reshape(batch, seq_len, HEAD_DIM)
        attn_send = lax.optimization_barrier(attn_flat).astype(jnp.float32).reshape(RING, rows_y, HEAD_DIM)
        x_block = own_block(hidden)
        out_block = exchange(attn_send, w_out_block, x_block, collective_id=1)
        out_all = lax.all_gather(out_block, 'tp', axis=0, tiled=True)
        block_out = narrow(out_all, 0, d_model).reshape(batch, seq_len, d_model)

        grad_w_out = jnp.einsum('bse,bsd->ed', attn_flat, grad_out, preferred_element_type=jnp.float32)
        grad_heads = jnp.einsum('bsd,ed->bse', grad_out, w_out, preferred_element_type=jnp.float32).astype(jnp.bfloat16)[:, :, None, :]
        grad_probs = jnp.einsum('bqjh,bkh->bjqk', grad_heads, v_head, preferred_element_type=jnp.float32)
        grad_v = jnp.einsum('bjqk,bqjh->bkh', probs_bf16, grad_heads, preferred_element_type=jnp.float32)
        row_dot = jnp.sum(attn_probs * grad_probs, axis=-1, keepdims=True)
        grad_scores = (attn_probs * (grad_probs - row_dot) * SCORE_SCALE).astype(jnp.bfloat16)
        grad_q_rot = jnp.einsum('bjqk,bkh->bqjh', grad_scores, k_rot, preferred_element_type=jnp.float32)
        grad_k_rot = jnp.einsum('bjqk,bqjh->bkh', grad_scores, q_rot, preferred_element_type=jnp.float32)
        grad_q = rotate_pairs(grad_q_rot, cos_t, -sin_t).astype(jnp.bfloat16).reshape(batch, seq_len, HEAD_DIM)
        grad_k = rotate_pairs(grad_k_rot[:, :, None, :], cos_t, -sin_t)[:, :, 0, :]
        grad_q_send = lax.optimization_barrier(grad_q).astype(jnp.float32).reshape(RING, rows_y, HEAD_DIM)
        grad_kv_send = jnp.stack([grad_k.reshape(RING, rows_y, HEAD_DIM), grad_v.reshape(RING, rows_y, HEAD_DIM)], axis=1)
        inv_block = lax.dynamic_slice(inv_rms.reshape(tokens, 1), (y * rows_y, 0), (rows_y, 1))
        gain_block = lax.dynamic_slice(gain_f32.reshape(1, d_model), (0, column * width), (1, width))
        grad_block, grad_kv = exchange(grad_q_send, w_query_block, x_block,
                                       (grad_kv_send, w_kv_block, own_block(grad_out), inv_block, gain_block), collective_id=2)
        grad_all = lax.all_gather(grad_block, 'tp', axis=0, tiled=True)
        grad_hidden = narrow(grad_all, 8, d_model).reshape(batch, seq_len, d_model)
        gain_rows = grad_all.reshape(RING, ROW_DEVICES, rows_y + 8, width)[:, :, rows_y, :]
        grad_gain = jnp.sum(gain_rows, axis=0).reshape(d_model)

        grad_w_query = jnp.einsum('bsd,bse->de', normed, grad_q, preferred_element_type=jnp.float32)
        normed_flat = normed.reshape(tokens, d_model)
        grad_kv = grad_kv.astype(jnp.bfloat16)
        grad_w_key = jnp.einsum('sd,se->de', normed_flat, grad_kv[:, 0].reshape(tokens, HEAD_DIM), preferred_element_type=jnp.float32)
        grad_w_value = jnp.einsum('sd,se->de', normed_flat, grad_kv[:, 1].reshape(tokens, HEAD_DIM), preferred_element_type=jnp.float32)
        return block_out, grad_hidden, grad_gain, grad_w_query, grad_w_key, grad_w_value, grad_w_out

    act_spec = P('dp', None, None)
    return jax.shard_map(
        block_fn, mesh=mesh,
        in_specs=(act_spec, act_spec, P(None), P(None, 'tp'), P(None, None), P(None, None), P('tp', None)),
        out_specs=(act_spec, act_spec, P('dp'), P('dp', 'tp'), P('dp', 'tp'), P('dp', 'tp'), P(('dp', 'tp'), None)),
        check_vma=False)
```

```python
import functools
import math
import jax
import jax.numpy as jnp
from jax import lax
from jax.experimental import pallas as pl
from jax.experimental.pallas import tpu as pltpu
from jax.sharding import PartitionSpec as P

HEAD_DIM = 128
NORM_EPS = 1.0e-5
ROPE_BASE = 10000.0
MASK_VALUE = -1.0e30
SCORE_SCALE = 1.0 / math.sqrt(HEAD_DIM)
RING = 4
CORES = 2
ROW_DEVICES = RING * CORES
CHUNKS = 6
VMEM_BYTES = 56 * 1024 * 1024


def rope_lanes(seq_len):
    lane = lax.broadcasted_iota(jnp.int32, (1, HEAD_DIM), 1)
    inv_freq = ROPE_BASE ** (-(lane - lane % 2).astype(jnp.float32) / HEAD_DIM)
    angles = jnp.arange(seq_len, dtype=jnp.float32)[:, None] * inv_freq
    return jnp.cos(angles), jnp.where(lane % 2 == 0, -jnp.sin(angles), jnp.sin(angles))


def rotate(tensor, cos_l, sin_l):
    lane = lax.broadcasted_iota(jnp.int32, tensor.shape, 1)
    swapped = jnp.where(lane % 2 == 0, pltpu.roll(tensor, HEAD_DIM - 1, 1), pltpu.roll(tensor, 1, 1))
    return tensor * cos_l + swapped * sin_l


def project(hidden, gain, weights, cos_l, sin_l):
    tokens, d_model = hidden.shape
    seq_len = cos_l.shape[0]
    rows = 256

    def kernel(x_ref, gain_ref, w_ref, cos_ref, sin_ref, normed_ref, inv_ref, q_ref, k_ref, v_ref):
        values = x_ref[...].astype(jnp.float32)
        inv = lax.rsqrt(jnp.mean(values * values, axis=1, keepdims=True) + NORM_EPS)
        inv_ref[...] = inv
        normed = (values * inv * gain_ref[...]).astype(jnp.bfloat16)
        normed_ref[...] = normed
        heads = jnp.dot(normed, w_ref[...], preferred_element_type=jnp.float32)
        q_ref[...] = rotate(heads[:, :HEAD_DIM], cos_ref[...], sin_ref[...]).astype(jnp.bfloat16)
        k_ref[...] = rotate(heads[:, HEAD_DIM:2 * HEAD_DIM], cos_ref[...], sin_ref[...]).astype(jnp.bfloat16)
        v_ref[...] = heads[:, 2 * HEAD_DIM:].astype(jnp.bfloat16)

    row_spec = pl.BlockSpec((rows, d_model), lambda i: (i, 0))
    head_spec = pl.BlockSpec((rows, HEAD_DIM), lambda i: (i, 0))
    table_spec = pl.BlockSpec((rows, HEAD_DIM), lambda i: (i % (seq_len // rows), 0))
    head = jax.ShapeDtypeStruct((tokens, HEAD_DIM), jnp.bfloat16)
    return pl.pallas_call(
        kernel, grid=(tokens // rows,),
        in_specs=[row_spec, pl.BlockSpec((1, d_model), lambda i: (0, 0)), pl.BlockSpec(weights.shape, lambda i: (0, 0)),
                  table_spec, table_spec],
        out_specs=(row_spec, pl.BlockSpec((rows, 1), lambda i: (i, 0)), head_spec, head_spec, head_spec),
        out_shape=(jax.ShapeDtypeStruct((tokens, d_model), jnp.bfloat16), jax.ShapeDtypeStruct((tokens, 1), jnp.float32),
                   head, head, head),
        compiler_params=pltpu.CompilerParams(vmem_limit_bytes=40 * 1024 * 1024),
        cost_estimate=pl.CostEstimate(flops=2 * tokens * d_model * weights.shape[1], bytes_accessed=4 * tokens * d_model,
                                      transcendentals=0),
        name='project',
    )(hidden, gain, weights, cos_l, sin_l)


NT = (((1,), (1,)), ((), ()))
TN = (((0,), (0,)), ((), ()))


def softmax_rows(q, k):
    scores = lax.dot_general(q, k, NT, preferred_element_type=jnp.float32) * SCORE_SCALE
    row = lax.broadcasted_iota(jnp.int32, scores.shape, 0)
    col = lax.broadcasted_iota(jnp.int32, scores.shape, 1)
    scores = jnp.where(row >= col, scores, MASK_VALUE)
    weight = jnp.exp(scores - jnp.max(scores, axis=1, keepdims=True))
    return weight * (1.0 / jnp.sum(weight, axis=1, keepdims=True))


def attend(q, k, v, seq_len):
    def kernel(q_ref, k_ref, v_ref, o_ref, send_ref):
        probs = softmax_rows(q_ref[...], k_ref[...]).astype(jnp.bfloat16)
        heads = jnp.dot(probs, v_ref[...], preferred_element_type=jnp.float32).astype(jnp.bfloat16)
        o_ref[...] = heads
        send_ref[...] = heads.astype(jnp.float32)

    spec = pl.BlockSpec((seq_len, HEAD_DIM), lambda b: (b, 0))
    tokens = q.shape[0]
    return pl.pallas_call(
        kernel, grid=(tokens // seq_len,), in_specs=[spec] * 3, out_specs=(spec, spec),
        out_shape=(jax.ShapeDtypeStruct(q.shape, jnp.bfloat16), jax.ShapeDtypeStruct(q.shape, jnp.float32)),
        compiler_params=pltpu.CompilerParams(vmem_limit_bytes=32 * 1024 * 1024),
        cost_estimate=pl.CostEstimate(flops=4 * tokens * seq_len * HEAD_DIM, bytes_accessed=10 * tokens * HEAD_DIM,
                                      transcendentals=tokens * seq_len),
        name='attend',
    )(q, k, v)


def attend_back(q, k, v, grad_heads, cos_l, sin_l, seq_len):
    def kernel(q_ref, k_ref, v_ref, do_ref, cos_ref, sin_ref, dq_ref, send_ref, dkv_ref):
        q_rows, k_rows, v_rows, grad = q_ref[...], k_ref[...], v_ref[...], do_ref[...]
        probs = softmax_rows(q_rows, k_rows)
        grad_probs = lax.dot_general(grad, v_rows, NT, preferred_element_type=jnp.float32)
        dkv_ref[1] = lax.dot_general(probs.astype(jnp.bfloat16), grad, TN, preferred_element_type=jnp.float32)
        row_dot = jnp.sum(probs * grad_probs, axis=1, keepdims=True)
        grad_scores = (probs * (grad_probs - row_dot) * SCORE_SCALE).astype(jnp.bfloat16)
        grad_q = jnp.dot(grad_scores, k_rows, preferred_element_type=jnp.float32)
        grad_k = lax.dot_general(grad_scores, q_rows, TN, preferred_element_type=jnp.float32)
        cos_t, sin_t = cos_ref[...], -sin_ref[...]
        grad_q = rotate(grad_q, cos_t, sin_t).astype(jnp.bfloat16)
        dq_ref[...] = grad_q
        send_ref[...] = grad_q.astype(jnp.float32)
        dkv_ref[0] = rotate(grad_k, cos_t, sin_t)

    spec = pl.BlockSpec((seq_len, HEAD_DIM), lambda b: (b, 0))
    table = pl.BlockSpec((seq_len, HEAD_DIM), lambda b: (0, 0))
    tokens = q.shape[0]
    return pl.pallas_call(
        kernel, grid=(tokens // seq_len,), in_specs=[spec] * 4 + [table] * 2,
        out_specs=(spec, spec, pl.BlockSpec((2, seq_len, HEAD_DIM), lambda b: (0, b, 0))),
        out_shape=(jax.ShapeDtypeStruct(q.shape, jnp.bfloat16), jax.ShapeDtypeStruct(q.shape, jnp.float32),
                   jax.ShapeDtypeStruct((2,) + q.shape, jnp.float32)),
        compiler_params=pltpu.CompilerParams(vmem_limit_bytes=40 * 1024 * 1024),
        cost_estimate=pl.CostEstimate(flops=10 * tokens * seq_len * HEAD_DIM, bytes_accessed=20 * tokens * HEAD_DIM,
                                      transcendentals=tokens * seq_len),
        name='attend_back',
    )(q, k, v, grad_heads, cos_l, sin_l)


class Place:
    def __init__(self):
        index = lax.axis_index('tp')
        self.c = lax.rem(index, CORES)
        self.x = lax.rem(index // CORES, RING)
        self.y = index // ROW_DEVICES

    def at(self, y, x, c):
        return {'tp': (y * RING + x) * CORES + c}


def turn(position, by):
    return lax.rem(position + (by % RING), RING)


def exchange_kernel(backward, chunks, *refs):
    if backward:
        (act_hbm, kv_hbm, wt_ref, wkv_ref, x_ref, dout_ref, inv_ref, gain_ref, out_ref, out_tail, kv_out,
         gath, wb, part, ring, kvp, kv_core, kv_send, kv_chip, rowpart, rowall,
         gs_sem, gr_sem, rs_sem, rr_sem, ks_sem, kr_sem, ms_sem, mr_sem, loc_sem) = refs
    else:
        act_hbm, wt_ref, x_ref, out_ref, gath, wb, part, ring, gs_sem, gr_sem, rs_sem, rr_sem, loc_sem = refs
    me = Place()
    x, y, c = me.x, me.y, me.c
    xr, xl, xo = turn(x, 1), turn(x, -1), turn(x, 2)
    yu, yd = turn(y, 1), turn(y, -1)
    other = 1 - c
    own = CORES * x + c
    left, right, far = CORES * xl + c, CORES * xr + c, CORES * xo + c
    parts = gath.shape[1]
    half = parts // 2
    rows_y, width = x_ref.shape
    r = rows_y // chunks
    h = r // 2

    barrier = pltpu.get_barrier_semaphore()
    peers = [me.at(yu, x, c), me.at(yd, x, c), me.at(y, xr, c), me.at(y, xl, c), me.at(y, x, other)]
    if backward:
        peers += [me.at(y, xo, c), me.at(y, xr, other), me.at(y, xl, other), me.at(y, xo, other)]
    for peer in peers:
        pl.semaphore_signal(barrier, inc=1, device_id=peer, device_id_type=pl.DeviceIdType.MESH)

    load = pltpu.make_async_copy(act_hbm, gath.at[own, pl.ds(0, RING)], loc_sem.at[0])
    load.start()
    if backward:
        load_kv = [pltpu.make_async_copy(kv_hbm.at[s], kvp.at[:, s], loc_sem.at[1 + s]) for s in (0, 1)]
        for copy in load_kv:
            copy.start()
    wb[pl.ds(0, wt_ref.shape[0]), :] = wt_ref[...].astype(jnp.bfloat16)
    if backward:
        wb[pl.ds(wt_ref.shape[0], wkv_ref.shape[0]), :] = wkv_ref[...]
        for copy in load_kv:
            copy.wait()
    load.wait()
    pl.semaphore_wait(barrier, len(peers))

    def remote(src, dst, send_sem, recv_sem, peer):
        return pltpu.make_async_remote_copy(src_ref=src, dst_ref=dst, send_sem=send_sem, recv_sem=recv_sem,
                                            device_id=peer, device_id_type=pl.DeviceIdType.MESH)

    def block(source, k, first=0, count=parts):
        return gath.at[source, pl.ds(first, count), pl.ds(k * r, r)]

    def gather(event, k, source, peer, first=0, count=parts):
        return remote(block(source, k, first, count), block(source, k, first, count),
                      gs_sem.at[event, k], gr_sem.at[event, k], peer)

    to_right, to_left, to_partner = me.at(y, xr, c), me.at(y, xl, c), me.at(y, x, other)

    def sends(k):
        return [gather(0, k, own, to_right), gather(1, k, own, to_left), gather(2, k, own, to_partner),
                gather(3, k, left, to_right, 0, half), gather(4, k, right, to_left, half, parts - half),
                gather(5, k, left, to_partner), gather(6, k, right, to_partner), gather(7, k, far, to_partner)]

    p_own, p_left, p_right, p_far = [CORES * pos + other for pos in (x, xl, xr, xo)]

    def receives(k):
        return [gather(0, k, left, to_right), gather(1, k, right, to_left), gather(2, k, p_own, to_partner),
                gather(3, k, far, to_right, 0, half), gather(4, k, far, to_left, half, parts - half),
                gather(5, k, p_left, to_partner), gather(6, k, p_right, to_partner), gather(7, k, p_far, to_partner)]

    def rows_of(way, k):
        return pl.ds(k * r + way * h, h)

    def sum_copy(way, step, k):
        d = turn(y, -(1 + step) if way == 0 else 1 + step)
        return remote(part.at[d, rows_of(way, k)], ring.at[way, step, k], rs_sem.at[way, step, k],
                      rr_sem.at[way, step, k], me.at(yu if way == 0 else yd, x, c))

    def multiply(d, k):
        rows = pl.ds(k * r, r)
        pieces = [gath[j, d, rows, :] for j in range(ROW_DEVICES)]
        if backward:
            j = CORES * lax.rem(d, 2) + d // 2
            pieces += [gath[j, RING, rows, :], gath[j, RING + 1, rows, :],
                       gath[j + RING, RING, rows, :], gath[j + RING, RING + 1, rows, :]]
        lhs = jnp.concatenate([piece.astype(jnp.bfloat16) for piece in pieces], axis=1)
        part[d, rows, :] = jnp.dot(lhs, wb[...], preferred_element_type=jnp.float32)

    def advance(k, step):
        for way in (0, 1):
            sum_copy(way, step, k).wait_recv()
            d = turn(y, -(2 + step) if way == 0 else 2 + step)
            part[d, rows_of(way, k), :] += ring[way, step, k]
            if step < RING - 2:
                sum_copy(way, step + 1, k).start()
        if step == RING - 2:
            finish(k)

    def finish(k):
        rows = pl.ds(k * r, r)
        total = part[y, rows, :]
        if not backward:
            out_ref[rows, :] = (x_ref[rows, :].astype(jnp.float32) + total).astype(jnp.bfloat16).astype(jnp.float32)
            return
        unit = x_ref[rows, :].astype(jnp.float32) * inv_ref[rows, :]
        row_sum = jnp.sum(total * gain_ref[...] * unit, axis=1, keepdims=True)
        square = jnp.concatenate([jnp.broadcast_to(row_sum, (r, 128)), jnp.zeros((128 - r, 128), jnp.float32)], axis=0)
        rowpart[k] = jnp.transpose(square)[0:8, :]
        gain_row = jnp.sum(total * unit, axis=0, keepdims=True)
        tail = pl.ds(rows_y // 2, 8)
        row_id = lax.broadcasted_iota(jnp.int32, (8, width), 0)
        addend = jnp.where(row_id == 0, jnp.broadcast_to(gain_row, (8, width)), 0.0)
        out_tail[tail, :] = addend if k == 0 else out_tail[tail, :] + addend

    if backward:
        p = lax.rem(x, 2)
        xn = x + 1 - 2 * p
        mine, theirs = CORES * c + p, CORES * c + 1 - p
        core_copy = remote(kvp.at[pl.ds(CORES * other, CORES)], kv_core, ks_sem.at[0], kr_sem.at[0], to_partner)
        core_copy.start()
        core_copy.wait_recv()

        def chip_copy(k):
            return remote(kv_send.at[:, pl.ds(k * r, r)], kv_chip.at[:, pl.ds(k * r, r)], ks_sem.at[1 + k],
                          kr_sem.at[1 + k], me.at(y, xn, c))

        for k in range(chunks):
            rows = pl.ds(k * r, r)
            kv_send[:, rows, :] = kvp[theirs, :, rows, :] + kv_core[1 - p, :, rows, :]
            chip_copy(k).start()

        def settle_kv(k):
            chip_copy(k).wait_recv()
            rows = pl.ds(k * r, r)
            total = kvp[mine, :, rows, :] + kv_core[p, :, rows, :] + kv_chip[:, rows, :]
            gath[own, pl.ds(RING, 2), rows, :] = total.astype(jnp.bfloat16).astype(jnp.float32)

    def begin(k):
        if backward:
            settle_kv(k)
        for copy in sends(k)[:3]:
            copy.start()

    begin(0)
    if chunks > 1:
        begin(1)
    for k in range(chunks + RING - 1):
        if k < chunks:
            out_going, incoming = sends(k), receives(k)
            incoming[0].wait_recv()
            out_going[3].start()
            out_going[5].start()
            incoming[1].wait_recv()
            out_going[4].start()
            out_going[6].start()
            if k + 2 < chunks:
                begin(k + 2)
        for step in range(RING - 1):
            if 0 <= k - 1 - step < chunks:
                advance(k - 1 - step, step)
        if k < chunks:
            incoming[3].wait_recv()
            incoming[4].wait_recv()
            out_going[7].start()
            for event in (2, 5, 6, 7):
                incoming[event].wait_recv()
            multiply(yd, k)
            sum_copy(0, 0, k).start()
            multiply(yu, k)
            sum_copy(1, 0, k).start()
            multiply(turn(y, 2), k)
            multiply(y, k)

    if backward:
        members = [(pos, core) for pos in (xr, xl, xo) for core in (c, other)] + [(x, other)]

        def mean_copy(n, m):
            pos, core = members[n]
            return remote(rowpart, rowall.at[m], ms_sem.at[n], mr_sem.at[m], me.at(y, pos, core))

        slots = [2, 3, 0, 1, 4, 5, 6]
        copies = [mean_copy(n, slots[n]) for n in range(7)]
        for copy in copies:
            copy.start()
        kv_head = x // 2
        kv_copies = [pltpu.make_async_copy(gath.at[CORES * (2 * kv_head + d % 2) + d // 2, pl.ds(RING, 2)], kv_out.at[:, d],
                                           loc_sem.at[d]) for d in range(RING)]
        for copy in kv_copies:
            copy.start()
        for copy in copies:
            copy.wait_recv()
        sums = rowpart[...]
        for m in range(7):
            sums = sums + rowall[m]
        d_model = width * ROW_DEVICES
        for k in range(chunks):
            rows = pl.ds(k * r, r)
            mean = jnp.transpose(sums[k])[0:r, 0:1] * (1.0 / d_model)
            inv = inv_ref[rows, :]
            unit = x_ref[rows, :].astype(jnp.float32) * inv
            delta = inv * (part[y, rows, :] * gain_ref[...] - unit * mean)
            target, first = (out_ref, 0) if 2 * k < chunks else (out_tail, rows_y // 2)
            target[pl.ds(k * r - first, r), :] = (dout_ref[rows, :].astype(jnp.float32) + delta).astype(jnp.bfloat16).astype(jnp.float32)
        for copy in kv_copies:
            copy.wait()
        for copy in copies:
            copy.wait_send()
        core_copy.wait_send()
        for k in range(chunks):
            chip_copy(k).wait_send()
    for k in range(chunks):
        for copy in sends(k):
            copy.wait_send()
        for way in (0, 1):
            for step in range(RING - 1):
                sum_copy(way, step, k).wait_send()


def exchange(act, weights, x_block, extra=None, collective_id=0):
    backward = extra is not None
    rows_y, width = x_block.shape
    chunks = CHUNKS
    h = rows_y // chunks // 2
    parts = RING + (2 if backward else 0)
    any_spec = pl.BlockSpec(memory_space=pl.ANY)
    vmem_spec = pl.BlockSpec(memory_space=pltpu.VMEM)
    depth = weights.shape[0] + (extra[1].shape[0] if backward else 0)
    dma = pltpu.SemaphoreType.DMA
    scratch = [
        pltpu.VMEM((ROW_DEVICES, parts, rows_y, HEAD_DIM), jnp.float32),
        pltpu.VMEM((depth, width), jnp.bfloat16),
        pltpu.VMEM((RING, rows_y, width), jnp.float32),
        pltpu.VMEM((2, RING - 1, chunks, h, width), jnp.float32),
    ]
    sems = [dma((8, chunks)), dma((8, chunks)), dma((2, RING - 1, chunks)), dma((2, RING - 1, chunks))]
    if backward:
        kv, w_kv, dout_block, inv_block, gain_block = extra
        args = (act, kv, weights, w_kv, x_block, dout_block, inv_block, gain_block)
        in_specs = [any_spec, any_spec] + [vmem_spec] * 6
        out_shape = (jax.ShapeDtypeStruct((rows_y // 2, width), jnp.float32),
                     jax.ShapeDtypeStruct((rows_y // 2 + 8, width), jnp.float32),
                     jax.ShapeDtypeStruct((2, RING, rows_y, HEAD_DIM), jnp.float32))
        out_specs = (vmem_spec, vmem_spec, any_spec)
        scratch += [
            pltpu.VMEM((RING, 2, rows_y, HEAD_DIM), jnp.float32),
            pltpu.VMEM((CORES, 2, rows_y, HEAD_DIM), jnp.float32),
            pltpu.VMEM((2, rows_y, HEAD_DIM), jnp.float32),
            pltpu.VMEM((2, rows_y, HEAD_DIM), jnp.float32),
            pltpu.VMEM((chunks, 8, 128), jnp.float32),
            pltpu.VMEM((ROW_DEVICES - 1, chunks, 8, 128), jnp.float32),
        ]
        sems += [dma((1 + chunks,)), dma((1 + chunks,)), dma((ROW_DEVICES - 1,)), dma((ROW_DEVICES - 1,))]
    else:
        args = (act, weights, x_block)
        in_specs = [any_spec] + [vmem_spec] * 2
        out_shape = jax.ShapeDtypeStruct((rows_y, width), jnp.float32)
        out_specs = vmem_spec
    sems += [dma((RING,))]
    flops = 2 * RING * rows_y * depth * width
    return pl.pallas_call(
        functools.partial(exchange_kernel, backward, chunks),
        out_shape=out_shape, in_specs=in_specs, out_specs=out_specs, scratch_shapes=scratch + sems,
        compiler_params=pltpu.CompilerParams(collective_id=collective_id, has_side_effects=True, vmem_limit_bytes=VMEM_BYTES),
        cost_estimate=pl.CostEstimate(flops=flops, bytes_accessed=4 * RING * rows_y * width, transcendentals=0),
        name='exchange_bwd' if backward else 'exchange_fwd',
    )(*args)


def narrow(gathered, pad, piece, pieces, so_far=None):
    rows, width = gathered.shape[0] // (RING * ROW_DEVICES) - pad, gathered.shape[1]
    group = 2 if pieces == 1 else 4
    out = jax.ShapeDtypeStruct((RING * pieces * rows, ROW_DEVICES * width), jnp.bfloat16)

    def kernel(in_ref, *rest):
        for n in range(group):
            rest[-1][:, pl.ds(n * width, width)] = in_ref[pl.ds(n * (rows + pad), rows), :].astype(jnp.bfloat16)

    groups = ROW_DEVICES // group
    return pl.pallas_call(
        kernel, grid=(RING, groups),
        in_specs=[pl.BlockSpec((group * (rows + pad), width), lambda y, i: (y * groups + i, 0))]
        + ([pl.BlockSpec(memory_space=pl.ANY)] if so_far is not None else []),
        out_specs=pl.BlockSpec((rows, group * width), lambda y, i: (y * pieces + piece, i)),
        out_shape=out, input_output_aliases={1: 0} if so_far is not None else {},
        compiler_params=pltpu.CompilerParams(vmem_limit_bytes=VMEM_BYTES),
        cost_estimate=pl.CostEstimate(flops=out.size // pieces, bytes_accessed=6 * out.size // pieces, transcendentals=0),
        name='narrow',
    )(*((gathered,) if so_far is None else (gathered, so_far)))


def solution(mesh):
    tp_size = mesh.shape['tp']
    row_groups = [list(range(first, first + ROW_DEVICES)) for first in range(0, tp_size, ROW_DEVICES)]

    def block_fn(hidden, grad_out, norm_gain, w_query, w_key, w_value, w_out):
        batch, seq_len, d_model = hidden.shape
        kv_heads = w_key.shape[1] // HEAD_DIM
        group_size = tp_size // kv_heads
        index = lax.axis_index('tp')
        y, column = index // ROW_DEVICES, index % ROW_DEVICES
        tokens, width = batch * seq_len, d_model // ROW_DEVICES
        rows_y = tokens // RING
        kv_pair = ROW_DEVICES // group_size * HEAD_DIM

        def spread(weight):
            blocks = weight.astype(jnp.float32).reshape(HEAD_DIM, ROW_DEVICES, width).transpose(1, 0, 2)
            got = lax.all_to_all(blocks, 'tp', 0, 0, axis_index_groups=row_groups, tiled=True)
            return got.reshape(ROW_DEVICES * HEAD_DIM, width)

        def own_block(array):
            return lax.dynamic_slice(array.reshape(tokens, d_model), (y * rows_y, column * width), (rows_y, width))

        def kv_block(weight):
            block = lax.dynamic_slice(weight, (column * width, y * kv_pair), (width, kv_pair))
            return block.T.reshape(-1, 1, HEAD_DIM, width)

        w_out_block = spread(w_out)
        w_query_block = spread(w_query.T)
        w_kv_block = jnp.concatenate([kv_block(w_key), kv_block(w_value)], axis=1).reshape(-1, width)

        kv_index = index // group_size
        w_local = jnp.concatenate([
            w_query,
            lax.dynamic_slice_in_dim(w_key, kv_index * HEAD_DIM, HEAD_DIM, axis=1),
            lax.dynamic_slice_in_dim(w_value, kv_index * HEAD_DIM, HEAD_DIM, axis=1)], axis=1)
        cos_l, sin_l = rope_lanes(seq_len)
        gain_row = norm_gain.astype(jnp.float32).reshape(1, d_model)
        grad_rows = grad_out.reshape(tokens, d_model)

        normed, inv_rms, q_rot, k_rot, v_head = project(hidden.reshape(tokens, d_model), gain_row, w_local, cos_l, sin_l)
        heads, heads_send = attend(q_rot, k_rot, v_head, seq_len)
        x_block = own_block(hidden)
        out_block = exchange(heads_send.reshape(RING, rows_y, HEAD_DIM), w_out_block, x_block, collective_id=1)
        w_out_late, out_block = lax.optimization_barrier((w_out, out_block))
        out_all = lax.all_gather(out_block, 'tp', axis=0, tiled=True)

        grad_heads = jnp.einsum('sd,ed->se', grad_rows, w_out_late, preferred_element_type=jnp.float32).astype(jnp.bfloat16)
        grad_q, grad_q_send, grad_kv_send = attend_back(q_rot, k_rot, v_head, grad_heads, cos_l, sin_l, seq_len)
        inv_block = lax.dynamic_slice(inv_rms, (y * rows_y, 0), (rows_y, 1))
        gain_block = lax.dynamic_slice(gain_row, (0, column * width), (1, width))
        grad_first, grad_second, grad_kv = exchange(
            grad_q_send.reshape(RING, rows_y, HEAD_DIM), w_query_block, x_block,
            (grad_kv_send.reshape(2, RING, rows_y, HEAD_DIM), w_kv_block, own_block(grad_out), inv_block, gain_block), collective_id=2)
        grad_first, out_all = lax.optimization_barrier((grad_first, out_all))
        block_out = narrow(out_all, 0, 0, 1).reshape(batch, seq_len, d_model)
        first_all = lax.all_gather(grad_first, 'tp', axis=0, tiled=True)
        second_all = lax.all_gather(grad_second, 'tp', axis=0, tiled=True)
        grad_hidden = narrow(first_all, 0, 0, 2, narrow(second_all, 8, 1, 2)).reshape(batch, seq_len, d_model)
        gain_rows = second_all.reshape(RING, ROW_DEVICES, rows_y // 2 + 8, width)[:, :, rows_y // 2, :]
        grad_gain = jnp.sum(gain_rows, axis=0).reshape(d_model)

        def weight_grad(grad):
            return jnp.einsum('sd,se->de', normed, grad, preferred_element_type=jnp.float32)

        grad_w_out = jnp.einsum('se,sd->ed', heads, grad_rows, preferred_element_type=jnp.float32)
        grad_w_query = weight_grad(grad_q)
        grad_w_key = weight_grad(grad_kv[0].reshape(tokens, HEAD_DIM).astype(jnp.bfloat16))
        grad_w_value = weight_grad(grad_kv[1].reshape(tokens, HEAD_DIM).astype(jnp.bfloat16))
        return block_out, grad_hidden, grad_gain, grad_w_query, grad_w_key, grad_w_value, grad_w_out

    act_spec = P('dp', None, None)
    return jax.shard_map(
        block_fn, mesh=mesh,
        in_specs=(act_spec, act_spec, P(None), P(None, 'tp'), P(None, None), P(None, None), P('tp', None)),
        out_specs=(act_spec, act_spec, P('dp'), P('dp', 'tp'), P('dp', 'tp'), P('dp', 'tp'), P(('dp', 'tp'), None)),
        check_vma=False)
```

```python
import functools
import math
import jax
import jax.numpy as jnp
from jax import lax
from jax.experimental import pallas as pl
from jax.experimental.pallas import tpu as pltpu
from jax.sharding import PartitionSpec as P

HEAD_DIM = 128
NORM_EPS = 1.0e-5
ROPE_BASE = 10000.0
MASK_VALUE = -1.0e30
SCORE_SCALE = 1.0 / math.sqrt(HEAD_DIM)
RING = 4
CORES = 2
ROW_DEVICES = RING * CORES
CHUNKS = 6
AHEAD = 2
SPREAD_FORWARD = 2
SPREAD_BACKWARD = 4
EARLY_WEIGHTS = True
VMEM_BYTES = 56 * 1024 * 1024


def rope_lanes(seq_len):
    lane = lax.broadcasted_iota(jnp.int32, (1, HEAD_DIM), 1)
    inv_freq = ROPE_BASE ** (-(lane - lane % 2).astype(jnp.float32) / HEAD_DIM)
    angles = jnp.arange(seq_len, dtype=jnp.float32)[:, None] * inv_freq
    return jnp.cos(angles), jnp.where(lane % 2 == 0, -jnp.sin(angles), jnp.sin(angles))


def rotate(tensor, cos_l, sin_l):
    lane = lax.broadcasted_iota(jnp.int32, tensor.shape, 1)
    swapped = jnp.where(lane % 2 == 0, pltpu.roll(tensor, HEAD_DIM - 1, 1), pltpu.roll(tensor, 1, 1))
    return tensor * cos_l + swapped * sin_l


def project(hidden, gain, weights, cos_l, sin_l):
    tokens, d_model = hidden.shape
    seq_len = cos_l.shape[0]
    rows = 256

    def kernel(x_ref, gain_ref, w_ref, cos_ref, sin_ref, normed_ref, inv_ref, q_ref, k_ref, v_ref):
        values = x_ref[...].astype(jnp.float32)
        inv = lax.rsqrt(jnp.mean(values * values, axis=1, keepdims=True) + NORM_EPS)
        inv_ref[...] = inv
        normed = (values * inv * gain_ref[...]).astype(jnp.bfloat16)
        normed_ref[...] = normed
        heads = jnp.dot(normed, w_ref[...], preferred_element_type=jnp.float32)
        q_ref[...] = rotate(heads[:, :HEAD_DIM], cos_ref[...], sin_ref[...]).astype(jnp.bfloat16)
        k_ref[...] = rotate(heads[:, HEAD_DIM:2 * HEAD_DIM], cos_ref[...], sin_ref[...]).astype(jnp.bfloat16)
        v_ref[...] = heads[:, 2 * HEAD_DIM:].astype(jnp.bfloat16)

    row_spec = pl.BlockSpec((rows, d_model), lambda i: (i, 0))
    head_spec = pl.BlockSpec((rows, HEAD_DIM), lambda i: (i, 0))
    table_spec = pl.BlockSpec((rows, HEAD_DIM), lambda i: (i % (seq_len // rows), 0))
    head = jax.ShapeDtypeStruct((tokens, HEAD_DIM), jnp.bfloat16)
    return pl.pallas_call(
        kernel, grid=(tokens // rows,),
        in_specs=[row_spec, pl.BlockSpec((1, d_model), lambda i: (0, 0)), pl.BlockSpec(weights.shape, lambda i: (0, 0)),
                  table_spec, table_spec],
        out_specs=(row_spec, pl.BlockSpec((rows, 1), lambda i: (i, 0)), head_spec, head_spec, head_spec),
        out_shape=(jax.ShapeDtypeStruct((tokens, d_model), jnp.bfloat16), jax.ShapeDtypeStruct((tokens, 1), jnp.float32),
                   head, head, head),
        compiler_params=pltpu.CompilerParams(vmem_limit_bytes=40 * 1024 * 1024),
        cost_estimate=pl.CostEstimate(flops=2 * tokens * d_model * weights.shape[1], bytes_accessed=4 * tokens * d_model,
                                      transcendentals=0),
        name='project',
    )(hidden, gain, weights, cos_l, sin_l)


NT = (((1,), (1,)), ((), ()))
TN = (((0,), (0,)), ((), ()))


def softmax_rows(q, k):
    scores = lax.dot_general(q, k, NT, preferred_element_type=jnp.float32) * SCORE_SCALE
    row = lax.broadcasted_iota(jnp.int32, scores.shape, 0)
    col = lax.broadcasted_iota(jnp.int32, scores.shape, 1)
    scores = jnp.where(row >= col, scores, MASK_VALUE)
    weight = jnp.exp(scores - jnp.max(scores, axis=1, keepdims=True))
    return weight * (1.0 / jnp.sum(weight, axis=1, keepdims=True))


def attend(q, k, v, seq_len):
    def kernel(q_ref, k_ref, v_ref, o_ref, send_ref):
        probs = softmax_rows(q_ref[...], k_ref[...]).astype(jnp.bfloat16)
        heads = jnp.dot(probs, v_ref[...], preferred_element_type=jnp.float32).astype(jnp.bfloat16)
        o_ref[...] = heads
        send_ref[...] = heads.astype(jnp.float32)

    spec = pl.BlockSpec((seq_len, HEAD_DIM), lambda b: (b, 0))
    tokens = q.shape[0]
    return pl.pallas_call(
        kernel, grid=(tokens // seq_len,), in_specs=[spec] * 3, out_specs=(spec, spec),
        out_shape=(jax.ShapeDtypeStruct(q.shape, jnp.bfloat16), jax.ShapeDtypeStruct(q.shape, jnp.float32)),
        compiler_params=pltpu.CompilerParams(vmem_limit_bytes=32 * 1024 * 1024),
        cost_estimate=pl.CostEstimate(flops=4 * tokens * seq_len * HEAD_DIM, bytes_accessed=10 * tokens * HEAD_DIM,
                                      transcendentals=tokens * seq_len),
        name='attend',
    )(q, k, v)


def attend_back(q, k, v, grad_heads, cos_l, sin_l, seq_len):
    def kernel(q_ref, k_ref, v_ref, do_ref, cos_ref, sin_ref, dq_ref, send_ref, dkv_ref):
        q_rows, k_rows, v_rows, grad = q_ref[...], k_ref[...], v_ref[...], do_ref[...]
        probs = softmax_rows(q_rows, k_rows)
        grad_probs = lax.dot_general(grad, v_rows, NT, preferred_element_type=jnp.float32)
        dkv_ref[1] = lax.dot_general(probs.astype(jnp.bfloat16), grad, TN, preferred_element_type=jnp.float32)
        row_dot = jnp.sum(probs * grad_probs, axis=1, keepdims=True)
        grad_scores = (probs * (grad_probs - row_dot) * SCORE_SCALE).astype(jnp.bfloat16)
        grad_q = jnp.dot(grad_scores, k_rows, preferred_element_type=jnp.float32)
        grad_k = lax.dot_general(grad_scores, q_rows, TN, preferred_element_type=jnp.float32)
        cos_t, sin_t = cos_ref[...], -sin_ref[...]
        grad_q = rotate(grad_q, cos_t, sin_t).astype(jnp.bfloat16)
        dq_ref[...] = grad_q
        send_ref[...] = grad_q.astype(jnp.float32)
        dkv_ref[0] = rotate(grad_k, cos_t, sin_t)

    spec = pl.BlockSpec((seq_len, HEAD_DIM), lambda b: (b, 0))
    table = pl.BlockSpec((seq_len, HEAD_DIM), lambda b: (0, 0))
    tokens = q.shape[0]
    return pl.pallas_call(
        kernel, grid=(tokens // seq_len,), in_specs=[spec] * 4 + [table] * 2,
        out_specs=(spec, spec, pl.BlockSpec((2, seq_len, HEAD_DIM), lambda b: (0, b, 0))),
        out_shape=(jax.ShapeDtypeStruct(q.shape, jnp.bfloat16), jax.ShapeDtypeStruct(q.shape, jnp.float32),
                   jax.ShapeDtypeStruct((2,) + q.shape, jnp.float32)),
        compiler_params=pltpu.CompilerParams(vmem_limit_bytes=40 * 1024 * 1024),
        cost_estimate=pl.CostEstimate(flops=10 * tokens * seq_len * HEAD_DIM, bytes_accessed=20 * tokens * HEAD_DIM,
                                      transcendentals=tokens * seq_len),
        name='attend_back',
    )(q, k, v, grad_heads, cos_l, sin_l)


class Place:
    def __init__(self):
        index = lax.axis_index('tp')
        self.c = lax.rem(index, CORES)
        self.x = lax.rem(index // CORES, RING)
        self.y = index // ROW_DEVICES

    def at(self, y, x, c):
        return {'tp': (y * RING + x) * CORES + c}


def turn(position, by):
    return lax.rem(position + (by % RING), RING)


class Transfer:
    def __init__(self, link, size, outgoing, incoming=None):
        self.link, self.size, self.outgoing, self.incoming = link, size, outgoing, incoming or outgoing


class Step:
    def __init__(self, waits=(), work=None, sends=(), after=(), cost=0.05, bulk=False):
        self.waits, self.work, self.sends, self.after, self.cost, self.bulk = waits, work, sends, after, cost, bulk


LINK_RATE = 46.6e3
CORE_RATE = 200e3
HOP = 2.0
QUEUE = 4.0


def in_order(threads):
    now, busy, arrival, finished, order = 0.0, {}, {}, set(), []
    position = [0] * len(threads)
    while any(position[i] < len(threads[i]) for i in range(len(threads))):
        chosen, soonest = None, math.inf
        for i, steps in enumerate(threads):
            if position[i] == len(steps) or any(step not in finished for step in steps[position[i]].after):
                continue
            step = steps[position[i]]
            ready = max([arrival.get(copy, math.inf) for copy in step.waits], default=0.0)
            if step.bulk:
                ready = max([ready] + [busy.get(copy.link, 0.0) - QUEUE for copy in step.sends if copy.link != 'core'])
            if ready <= now:
                chosen = i
                break
            soonest = min(soonest, ready)
        if chosen is None:
            now = soonest
            continue
        step = threads[chosen][position[chosen]]
        position[chosen] += 1
        now += step.cost
        for copy in step.sends:
            rate = CORE_RATE if copy.link == 'core' else LINK_RATE
            busy[copy.link] = max(now, busy.get(copy.link, 0.0)) + copy.size / rate
            arrival[copy] = busy[copy.link] + HOP
        finished.add(step)
        order.append(step)
    return order


def exchange_kernel(backward, chunks, spread, *refs):
    refs = list(refs)
    if backward:
        act_hbm, kv_hbm, wt_ref, wkv_ref, x_ref, dout_ref, inv_ref, gain_ref = refs[:8]
        rest_ref, all_hbm, kv_out, gath, wb, part, ring, fin, kvp, kv_core, kv_send, kv_chip, rowpart, rowall = refs[8:22]
        sems = refs[22:]
    else:
        act_hbm, wt_ref, x_ref, rest_ref, all_hbm, gath, wb, part, ring, fin = refs[:10]
        sems = refs[10:]
    send_sem, recv_sem, loc_sem = sems
    me = Place()
    x, y, c = me.x, me.y, me.c
    xr, xl, xo = turn(x, 1), turn(x, -1), turn(x, 2)
    yu, yd, yo = turn(y, 1), turn(y, -1), turn(y, 2)
    other = 1 - c
    own = CORES * x + c
    left, right, far = CORES * xl + c, CORES * xr + c, CORES * xo + c
    p_own, p_left, p_right, p_far = [CORES * pos + other for pos in (x, xl, xr, xo)]
    parts = gath.shape[1]
    half = parts // 2
    rows_y, width = x_ref.shape
    r = rows_y // chunks
    h = r // 2
    to_right, to_left, to_partner = me.at(y, xr, c), me.at(y, xl, c), me.at(y, x, other)
    to_up, to_down = me.at(yu, x, c), me.at(yd, x, c)

    barrier = pltpu.get_barrier_semaphore()
    peers = [to_up, to_down, to_right, to_left, to_partner]
    if backward:
        peers += [me.at(y, xo, c), me.at(y, xr, other), me.at(y, xl, other), me.at(y, xo, other)]
    for peer in peers:
        pl.semaphore_signal(barrier, inc=1, device_id=peer, device_id_type=pl.DeviceIdType.MESH)
    loads = [pltpu.make_async_copy(act_hbm, gath.at[own, pl.ds(0, RING)], loc_sem.at[0])]
    if backward:
        loads += [pltpu.make_async_copy(kv_hbm.at[s], kvp.at[:, s], loc_sem.at[1 + s]) for s in (0, 1)]
    for copy in loads:
        copy.start()
    depth = wt_ref.shape[0]
    wb[pl.ds(0, depth), :] = wt_ref[...].astype(jnp.bfloat16)
    if backward:
        wb[pl.ds(depth, wkv_ref.shape[0]), :] = wkv_ref[...]
        rest_ref[pl.ds((chunks - spread) * r, 8), :] = jnp.zeros((8, width), jnp.float32)
    for copy in loads:
        copy.wait()
    pl.semaphore_wait(barrier, len(peers))

    transfers = []

    def transfer(link, peer, src, dst, came_from=None, came_to=None):
        n = len(transfers)

        def copy(a, b):
            return lambda: pltpu.make_async_remote_copy(
                src_ref=a, dst_ref=b, send_sem=send_sem.at[n], recv_sem=recv_sem.at[n], device_id=peer,
                device_id_type=pl.DeviceIdType.MESH)
        size = 4 * math.prod(dst.shape)
        made = Transfer(link, size, copy(src, dst), copy(came_from, came_to) if came_to is not None else None)
        transfers.append(made)
        return made

    def moved(link, peer, sent, came):
        return transfer(link, peer, sent, sent, came, came)

    threads, settle, settled = [], [lambda: None] * chunks, [()] * chunks
    if backward:
        p = lax.rem(x, 2)
        xn = x + 1 - 2 * p
        mine, theirs = CORES * c + p, CORES * c + 1 - p
        core_copy = transfer('core', to_partner, kvp.at[pl.ds(CORES * other, CORES)], kv_core)
        steps = [Step(sends=[core_copy])]
        for k in range(chunks):
            rows = pl.ds(k * r, r)
            chip_copy = transfer('right', me.at(y, xn, c), kv_send.at[:, rows], kv_chip.at[:, rows])

            def add_core(rows=rows):
                kv_send[:, rows, :] = kvp[theirs, :, rows, :] + kv_core[1 - p, :, rows, :]

            def add_chip(rows=rows):
                total = kvp[mine, :, rows, :] + kv_core[p, :, rows, :] + kv_chip[:, rows, :]
                gath[own, pl.ds(RING, 2), rows, :] = total.astype(jnp.bfloat16).astype(jnp.float32)

            steps.append(Step([core_copy] if k == 0 else [], add_core, [chip_copy], cost=0.1))
            settle[k], settled[k] = add_chip, (chip_copy,)
        threads.append(steps)

    def multiply(d, k):
        rows = pl.ds(k * r, r)
        pieces = [gath[j, d, rows, :] for j in range(ROW_DEVICES)]
        if backward:
            j = CORES * lax.rem(d, 2) + d // 2
            pieces += [gath[j, RING, rows, :], gath[j, RING + 1, rows, :],
                       gath[j + RING, RING, rows, :], gath[j + RING, RING + 1, rows, :]]
        lhs = jnp.concatenate([piece.astype(jnp.bfloat16) for piece in pieces], axis=1)
        part[d, rows, :] = jnp.dot(lhs, wb[...], preferred_element_type=jnp.float32)

    def add_ring(way, step, k):
        d = turn(y, -(2 + step) if way == 0 else 2 + step)
        part[d, pl.ds(k * r + way * h, h), :] += ring[way, step, k]

    def store(k, values):
        if k < spread:
            fin[pl.ds(k * r, r), :] = values
        else:
            rest_ref[pl.ds((k - spread) * r, r), :] = values

    def finish_forward(k):
        rows = pl.ds(k * r, r)
        store(k, (x_ref[rows, :].astype(jnp.float32) + part[y, rows, :]).astype(jnp.bfloat16).astype(jnp.float32))

    def row_sums(k):
        rows = pl.ds(k * r, r)
        total = part[y, rows, :]
        unit = x_ref[rows, :].astype(jnp.float32) * inv_ref[rows, :]
        row_sum = jnp.sum(total * gain_ref[...] * unit, axis=1, keepdims=True)
        square = jnp.concatenate([jnp.broadcast_to(row_sum, (r, 128)), jnp.zeros((128 - r, 128), jnp.float32)], axis=0)
        rowpart[k] = jnp.transpose(square)[0:8, :]
        gain_row = jnp.sum(total * unit, axis=0, keepdims=True)
        tail = pl.ds((chunks - spread) * r, 8)
        row_id = lax.broadcasted_iota(jnp.int32, (8, width), 0)
        addend = jnp.where(row_id == 0, jnp.broadcast_to(gain_row, (8, width)), 0.0)
        rest_ref[tail, :] += addend

    def finish_backward(k):
        rows = pl.ds(k * r, r)
        sums = rowpart[k]
        for m in range(ROW_DEVICES - 1):
            sums = sums + rowall[m, k]
        mean = jnp.transpose(sums)[0:r, 0:1] * (1.0 / (width * ROW_DEVICES))
        inv = inv_ref[rows, :]
        unit = x_ref[rows, :].astype(jnp.float32) * inv
        delta = inv * (part[y, rows, :] * gain_ref[...] - unit * mean)
        store(k, (dout_ref[rows, :].astype(jnp.float32) + delta).astype(jnp.bfloat16).astype(jnp.float32))

    passed, done = [], []
    for k in range(chunks):
        rows = pl.ds(k * r, r)

        def block(source, first=0, count=parts, rows=rows):
            return gath.at[source, pl.ds(first, count), rows]

        s_right = moved('right', to_right, block(own), block(left))
        s_left = moved('left', to_left, block(own), block(right))
        s_core = moved('core', to_partner, block(own), block(p_own))
        f_right = moved('right', to_right, block(left, 0, half), block(far, 0, half))
        f_left = moved('left', to_left, block(right, half, parts - half), block(far, half, parts - half))
        c_left = moved('core', to_partner, block(left), block(p_left))
        c_right = moved('core', to_partner, block(right), block(p_right))
        c_far = moved('core', to_partner, block(far), block(p_far))
        sums = [[transfer(link, peer, part.at[turn(y, -(1 + step) if way == 0 else 1 + step), pl.ds(k * r + way * h, h)],
                          ring.at[way, step, k]) for step in range(RING - 1)]
                for way, (link, peer) in enumerate((('up', to_up), ('down', to_down)))]
        wait_for = (passed[k - AHEAD],) if k >= AHEAD else ()
        steps = [Step(settled[k], settle[k], [s_right, s_left, s_core], wait_for, 0.1),
                 Step([s_right], None, [f_right, c_left]), Step([s_left], None, [f_left, c_right])]
        passed.append(steps[-1])
        cost = 0.6 * r / 96 * wb.shape[0] / 1024
        steps += [Step([f_right, f_left], None, [c_far]),
                  Step([s_core, c_left, c_right, c_far], functools.partial(multiply, yd, k), [sums[0][0]], cost=cost),
                  Step((), functools.partial(multiply, yu, k), [sums[1][0]], cost=cost),
                  Step((), functools.partial(multiply, yo, k), cost=cost),
                  Step((), functools.partial(multiply, y, k), cost=cost)]
        for step in range(RING - 1):
            for way in (0, 1):
                steps.append(Step([sums[way][step]], functools.partial(add_ring, way, step, k),
                                  [sums[way][step + 1]] if step < RING - 2 else [], cost=0.15))
        if backward:
            members = [(pos, core) for pos in (xr, xl, xo) for core in (c, other)] + [(x, other)]
            notes = [transfer('note', me.at(y, pos, core), rowpart.at[k], rowall.at[m, k])
                     for (pos, core), m in zip(members, (2, 3, 0, 1, 4, 5, 6))]
            steps.append(Step((), functools.partial(row_sums, k), notes, cost=0.4))
            steps.append(Step(notes, functools.partial(finish_backward, k), cost=0.5))
        else:
            steps.append(Step((), functools.partial(finish_forward, k), cost=0.3))
        done.append(steps[-1])
        threads.append(steps)

    for k in range(spread):
        along_x = k % 2 == 0
        (a_plus, a_minus, a, a_up, a_down, a_far), (b_plus, b_minus, b, b_up, b_down, b_far) = [
            (('right', to_right), ('left', to_left), x, xr, xl, xo), (('up', to_up), ('down', to_down), y, yu, yd, yo)
        ][::1 if along_x else -1]

        def place(core, b_pos, a_pos, part_rows=None, k=k, along_x=along_x):
            spot = (k, core, b_pos, a_pos) if along_x else (k, core, a_pos, b_pos)
            return all_hbm.at[spot + (() if part_rows is None else (pl.ds(*part_rows),))]

        def bundle(core, b_pos, first=0, count=RING, k=k, along_x=along_x):
            return all_hbm.at[(k, core, b_pos, pl.ds(first, count)) if along_x else (k, core, pl.ds(first, count), b_pos)]

        source = fin.at[pl.ds(k * r, r)]
        keep = pltpu.make_async_copy(source, place(c, b, a), loc_sem.at[RING + k])
        top, low = (0, h), (h, h)
        a0 = transfer(*a_plus, source, place(c, b, a), source, place(c, b, a_down))
        a1 = transfer(*a_minus, source, place(c, b, a), source, place(c, b, a_up))
        h0 = moved(*a_plus, place(c, b, a_down, top), place(c, b, a_far, top))
        h1 = moved(*a_minus, place(c, b, a_up, low), place(c, b, a_far, low))
        b0 = moved(*b_plus, bundle(c, b, 0, 2), bundle(c, b_down, 0, 2))
        b1 = moved(*b_minus, bundle(c, b, 2, 2), bundle(c, b_up, 2, 2))
        b2 = moved(*b_plus, bundle(c, b, 2, 2), bundle(c, b_down, 2, 2))
        b3 = moved(*b_minus, bundle(c, b, 0, 2), bundle(c, b_up, 0, 2))
        g0 = moved(*b_plus, bundle(c, b_down, 0, 2), bundle(c, b_far, 0, 2))
        g1 = moved(*b_minus, bundle(c, b_up, 2, 2), bundle(c, b_far, 2, 2))
        cores = [moved('core', to_partner, bundle(c, pos), bundle(other, pos)) for pos in (b, b_down, b_up, b_far)]
        threads.append([
            Step((), keep.start, [a0, a1], (done[k],), 0.1, True),
            Step([a0], None, [h0], bulk=True), Step([a1], None, [h1], bulk=True),
            Step([h0, h1], keep.wait, [b0, b1, b2, b3, cores[0]], cost=0.1, bulk=True),
            Step([b0], None, [g0], bulk=True), Step([b1], None, [g1], bulk=True),
            Step([b2], None, [cores[1]]), Step([b3], None, [cores[2]]),
            Step([g0, g1], None, [cores[3]]), Step(cores)])

    for step in in_order(threads):
        for copy in step.waits:
            copy.incoming().wait_recv()
        if step.work is not None:
            step.work()
        for copy in step.sends:
            copy.outgoing().start()

    if backward:
        kv_copies = [pltpu.make_async_copy(gath.at[CORES * (2 * (x // 2) + d % 2) + d // 2, pl.ds(RING, 2)],
                                           kv_out.at[:, d], loc_sem.at[d]) for d in range(RING)]
        for copy in kv_copies:
            copy.start()
        for copy in kv_copies:
            copy.wait()
    for copy in transfers:
        copy.outgoing().wait_send()


def exchange(act, weights, x_block, extra=None, collective_id=0, spread=0):
    backward = extra is not None
    rows_y, width = x_block.shape
    chunks = CHUNKS
    r = rows_y // chunks
    parts = RING + (2 if backward else 0)
    any_spec = pl.BlockSpec(memory_space=pl.ANY)
    vmem_spec = pl.BlockSpec(memory_space=pltpu.VMEM)
    depth = weights.shape[0] + (extra[1].shape[0] if backward else 0)
    rest = (chunks - spread) * r + (8 if backward else 0)
    out_shape = [jax.ShapeDtypeStruct((rest, width), jnp.float32),
                 jax.ShapeDtypeStruct((max(spread, 1), CORES, RING, RING, r, width), jnp.float32)]
    out_specs = [vmem_spec, any_spec]
    scratch = [
        pltpu.VMEM((ROW_DEVICES, parts, rows_y, HEAD_DIM), jnp.float32),
        pltpu.VMEM((depth, width), jnp.bfloat16),
        pltpu.VMEM((RING, rows_y, width), jnp.float32),
        pltpu.VMEM((2, RING - 1, chunks, r // 2, width), jnp.float32),
        pltpu.VMEM((max(spread, 1) * r, width), jnp.float32),
    ]
    if backward:
        kv, w_kv, dout_block, inv_block, gain_block = extra
        args = (act, kv, weights, w_kv, x_block, dout_block, inv_block, gain_block)
        in_specs = [any_spec, any_spec] + [vmem_spec] * 6
        out_shape.append(jax.ShapeDtypeStruct((2, RING, rows_y, HEAD_DIM), jnp.float32))
        out_specs.append(any_spec)
        scratch += [
            pltpu.VMEM((RING, 2, rows_y, HEAD_DIM), jnp.float32),
            pltpu.VMEM((CORES, 2, rows_y, HEAD_DIM), jnp.float32),
            pltpu.VMEM((2, rows_y, HEAD_DIM), jnp.float32),
            pltpu.VMEM((2, rows_y, HEAD_DIM), jnp.float32),
            pltpu.VMEM((chunks, 8, 128), jnp.float32),
            pltpu.VMEM((ROW_DEVICES - 1, chunks, 8, 128), jnp.float32),
        ]
    else:
        args = (act, weights, x_block)
        in_specs = [any_spec] + [vmem_spec] * 2
    per_chunk = 8 + 2 * (RING - 1) + (ROW_DEVICES if backward else 0)
    copies = chunks * per_chunk + 14 * spread + (1 if backward else 0)
    dma = pltpu.SemaphoreType.DMA
    flops = 2 * RING * rows_y * depth * width
    return pl.pallas_call(
        functools.partial(exchange_kernel, backward, chunks, spread),
        out_shape=out_shape, in_specs=in_specs, out_specs=out_specs,
        scratch_shapes=scratch + [dma((copies,)), dma((copies,)), dma((RING + max(spread, 1),))],
        compiler_params=pltpu.CompilerParams(collective_id=collective_id, has_side_effects=True, vmem_limit_bytes=VMEM_BYTES),
        cost_estimate=pl.CostEstimate(flops=flops, bytes_accessed=4 * RING * rows_y * width, transcendentals=0),
        name='exchange_bwd' if backward else 'exchange_fwd',
    )(*args)


def rounded(kernel, gathered, grid, block, index_map, out_rows, place_of, rows, so_far):
    d_model = ROW_DEVICES * gathered.shape[-1]
    moved_rows = math.prod(grid) * out_rows
    return pl.pallas_call(
        kernel, grid=grid,
        in_specs=[pl.BlockSpec(block, index_map)] + ([pl.BlockSpec(memory_space=pl.ANY)] if so_far is not None else []),
        out_specs=pl.BlockSpec((out_rows, d_model), lambda *at: (place_of(*at), 0)),
        out_shape=jax.ShapeDtypeStruct((rows, d_model), jnp.bfloat16),
        input_output_aliases={1: 0} if so_far is not None else {},
        compiler_params=pltpu.CompilerParams(vmem_limit_bytes=VMEM_BYTES),
        cost_estimate=pl.CostEstimate(flops=moved_rows * d_model, bytes_accessed=6 * moved_rows * d_model, transcendentals=0),
        name='narrow',
    )(*((gathered,) if so_far is None else (gathered, so_far)))


def narrow_spread(gathered, spread, rows, so_far=None):
    r, width = gathered.shape[-2:]
    chunks = rows // RING // r

    def kernel(in_ref, *rest):
        for n in range(ROW_DEVICES):
            rest[-1][:, pl.ds(n * width, width)] = in_ref[0, n % CORES, 0, n // CORES].astype(jnp.bfloat16)

    return rounded(kernel, gathered, (spread, RING), (1, CORES, 1, RING, r, width), lambda k, y: (k, 0, y, 0, 0, 0), r,
                   lambda k, y: y * chunks + k, rows, so_far)


def narrow_rest(gathered, pad, spread, r, rows, so_far=None):
    width = gathered.shape[-1]
    chunks = rows // RING // r
    count = chunks - spread
    step = count if chunks % count == 0 and spread % count == 0 else 1
    assert step == count or pad == 0
    blocks = gathered.reshape(RING * ROW_DEVICES, count * r + pad, width)

    def kernel(in_ref, *rest):
        for n in range(ROW_DEVICES):
            rest[-1][:, pl.ds(n * width, width)] = in_ref[n, pl.ds(0, step * r), :].astype(jnp.bfloat16)

    return rounded(kernel, blocks, (RING, count // step), (ROW_DEVICES, step * r + pad, width), lambda y, j: (y, j, 0), step * r,
                   lambda y, j: (y * chunks + spread) // step + j, rows, so_far)


def solution(mesh):
    tp_size = mesh.shape['tp']
    row_groups = [list(range(first, first + ROW_DEVICES)) for first in range(0, tp_size, ROW_DEVICES)]

    def block_fn(hidden, grad_out, norm_gain, w_query, w_key, w_value, w_out):
        batch, seq_len, d_model = hidden.shape
        kv_heads = w_key.shape[1] // HEAD_DIM
        group_size = tp_size // kv_heads
        index = lax.axis_index('tp')
        y, column = index // ROW_DEVICES, index % ROW_DEVICES
        tokens, width = batch * seq_len, d_model // ROW_DEVICES
        rows_y = tokens // RING
        kv_pair = ROW_DEVICES // group_size * HEAD_DIM

        def spread(weight):
            blocks = weight.astype(jnp.float32).reshape(HEAD_DIM, ROW_DEVICES, width).transpose(1, 0, 2)
            got = lax.all_to_all(blocks, 'tp', 0, 0, axis_index_groups=row_groups, tiled=True)
            return got.reshape(ROW_DEVICES * HEAD_DIM, width)

        def own_block(array):
            return lax.dynamic_slice(array.reshape(tokens, d_model), (y * rows_y, column * width), (rows_y, width))

        def kv_block(weight):
            block = lax.dynamic_slice(weight, (column * width, y * kv_pair), (width, kv_pair))
            return block.T.reshape(-1, 1, HEAD_DIM, width)

        w_out_block = spread(w_out)
        w_query_block = spread(w_query.T)
        w_kv_block = jnp.concatenate([kv_block(w_key), kv_block(w_value)], axis=1).reshape(-1, width)

        kv_index = index // group_size
        w_local = jnp.concatenate([
            w_query,
            lax.dynamic_slice_in_dim(w_key, kv_index * HEAD_DIM, HEAD_DIM, axis=1),
            lax.dynamic_slice_in_dim(w_value, kv_index * HEAD_DIM, HEAD_DIM, axis=1)], axis=1)
        cos_l, sin_l = rope_lanes(seq_len)
        gain_row = norm_gain.astype(jnp.float32).reshape(1, d_model)
        grad_rows = grad_out.reshape(tokens, d_model)

        normed, inv_rms, q_rot, k_rot, v_head = project(hidden.reshape(tokens, d_model), gain_row, w_local, cos_l, sin_l)
        def weight_grad(grad):
            return jnp.einsum('sd,se->de', normed, grad, preferred_element_type=jnp.float32)

        heads, heads_send = attend(q_rot, k_rot, v_head, seq_len)
        x_block = own_block(hidden)
        rest_block, out_spread = exchange(heads_send.reshape(RING, rows_y, HEAD_DIM), w_out_block, x_block,
                                          collective_id=1, spread=SPREAD_FORWARD)
        w_out_late, rest_block = lax.optimization_barrier((w_out, rest_block))
        out_rest = lax.all_gather(rest_block, 'tp', axis=0, tiled=True)
        grad_heads = jnp.einsum('sd,ed->se', grad_rows, w_out_late, preferred_element_type=jnp.float32).astype(jnp.bfloat16)
        grad_q, grad_q_send, grad_kv_send = attend_back(q_rot, k_rot, v_head, grad_heads, cos_l, sin_l, seq_len)
        grad_w_out = jnp.einsum('se,sd->ed', heads, grad_rows, preferred_element_type=jnp.float32)
        grad_w_query = weight_grad(grad_q)
        inv_block = lax.dynamic_slice(inv_rms, (y * rows_y, 0), (rows_y, 1))
        gain_block = lax.dynamic_slice(gain_row, (0, column * width), (1, width))
        if EARLY_WEIGHTS:
            grad_q_send, grad_w_out, grad_w_query = lax.optimization_barrier((grad_q_send, grad_w_out, grad_w_query))
        grad_block, grad_spread, grad_kv = exchange(
            grad_q_send.reshape(RING, rows_y, HEAD_DIM), w_query_block, x_block,
            (grad_kv_send.reshape(2, RING, rows_y, HEAD_DIM), w_kv_block, own_block(grad_out), inv_block, gain_block),
            collective_id=2, spread=SPREAD_BACKWARD)
        grad_block, out_rest = lax.optimization_barrier((grad_block, out_rest))
        grad_rest = lax.all_gather(grad_block, 'tp', axis=0, tiled=True)
        r = rows_y // CHUNKS
        block_out = narrow_rest(out_rest, 0, SPREAD_FORWARD, r, tokens,
                                narrow_spread(out_spread, SPREAD_FORWARD, tokens) if SPREAD_FORWARD else None)
        grad_hidden = narrow_rest(grad_rest, 8, SPREAD_BACKWARD, r, tokens, narrow_spread(grad_spread, SPREAD_BACKWARD, tokens))
        grad_gain = jnp.sum(grad_rest.reshape(RING, ROW_DEVICES, -1, width)[:, :, (CHUNKS - SPREAD_BACKWARD) * r, :], axis=0).reshape(d_model)
        block_out, grad_hidden = block_out.reshape(hidden.shape), grad_hidden.reshape(hidden.shape)

        grad_w_key = weight_grad(grad_kv[0].reshape(tokens, HEAD_DIM).astype(jnp.bfloat16))
        grad_w_value = weight_grad(grad_kv[1].reshape(tokens, HEAD_DIM).astype(jnp.bfloat16))
        return block_out, grad_hidden, grad_gain, grad_w_query, grad_w_key, grad_w_value, grad_w_out

    act_spec = P('dp', None, None)
    return jax.shard_map(
        block_fn, mesh=mesh,
        in_specs=(act_spec, act_spec, P(None), P(None, 'tp'), P(None, None), P(None, None), P('tp', None)),
        out_specs=(act_spec, act_spec, P('dp'), P('dp', 'tp'), P('dp', 'tp'), P('dp', 'tp'), P(('dp', 'tp'), None)),
        check_vma=False)
```

```python
import functools
import math
import jax
import jax.numpy as jnp
from jax import lax
from jax.experimental import pallas as pl
from jax.experimental.pallas import tpu as pltpu
from jax.sharding import PartitionSpec as P

HEAD_DIM = 128
NORM_EPS = 1.0e-5
ROPE_BASE = 10000.0
MASK_VALUE = -1.0e30
SCORE_SCALE = 1.0 / math.sqrt(HEAD_DIM)
RING = 4
CORES = 2
ROW_DEVICES = RING * CORES
CHUNKS = 9
AHEAD = 2
SPREAD = 6
VMEM_BYTES = 62 * 1024 * 1024


def rope_lanes(seq_len):
    lane = lax.broadcasted_iota(jnp.int32, (1, HEAD_DIM), 1)
    inv_freq = ROPE_BASE ** (-(lane - lane % 2).astype(jnp.float32) / HEAD_DIM)
    angles = jnp.arange(seq_len, dtype=jnp.float32)[:, None] * inv_freq
    return jnp.cos(angles), jnp.where(lane % 2 == 0, -jnp.sin(angles), jnp.sin(angles))


def rotate(tensor, cos_l, sin_l):
    lane = lax.broadcasted_iota(jnp.int32, tensor.shape, 1)
    swapped = jnp.where(lane % 2 == 0, pltpu.roll(tensor, HEAD_DIM - 1, 1), pltpu.roll(tensor, 1, 1))
    return tensor * cos_l + swapped * sin_l


def project(hidden, grad_out, gain, weights, w_out, cos_l, sin_l):
    tokens, d_model = hidden.shape
    seq_len = cos_l.shape[0]
    rows = 256

    def kernel(x_ref, dout_ref, gain_ref, w_ref, w_out_ref, cos_ref, sin_ref, normed_ref, inv_ref, q_ref, k_ref, v_ref, do_ref):
        values = x_ref[...].astype(jnp.float32)
        inv = lax.rsqrt(jnp.mean(values * values, axis=1, keepdims=True) + NORM_EPS)
        inv_ref[...] = inv
        normed = (values * inv * gain_ref[...]).astype(jnp.bfloat16)
        normed_ref[...] = normed
        heads = jnp.dot(normed, w_ref[...], preferred_element_type=jnp.float32)
        q_ref[...] = rotate(heads[:, :HEAD_DIM], cos_ref[...], sin_ref[...]).astype(jnp.bfloat16)
        k_ref[...] = rotate(heads[:, HEAD_DIM:2 * HEAD_DIM], cos_ref[...], sin_ref[...]).astype(jnp.bfloat16)
        v_ref[...] = heads[:, 2 * HEAD_DIM:].astype(jnp.bfloat16)
        do_ref[...] = lax.dot_general(dout_ref[...], w_out_ref[...], NT, preferred_element_type=jnp.float32).astype(jnp.bfloat16)

    row_spec = pl.BlockSpec((rows, d_model), lambda i: (i, 0))
    head_spec = pl.BlockSpec((rows, HEAD_DIM), lambda i: (i, 0))
    table_spec = pl.BlockSpec((rows, HEAD_DIM), lambda i: (i % (seq_len // rows), 0))
    head = jax.ShapeDtypeStruct((tokens, HEAD_DIM), jnp.bfloat16)

    def whole(array):
        return pl.BlockSpec(array.shape, lambda i: (0, 0))

    return pl.pallas_call(
        kernel, grid=(tokens // rows,),
        in_specs=[row_spec, row_spec, whole(gain), whole(weights), whole(w_out), table_spec, table_spec],
        out_specs=(row_spec, pl.BlockSpec((rows, 1), lambda i: (i, 0)), head_spec, head_spec, head_spec, head_spec),
        out_shape=(jax.ShapeDtypeStruct((tokens, d_model), jnp.bfloat16), jax.ShapeDtypeStruct((tokens, 1), jnp.float32),
                   head, head, head, head),
        compiler_params=pltpu.CompilerParams(vmem_limit_bytes=VMEM_BYTES),
        cost_estimate=pl.CostEstimate(flops=2 * tokens * d_model * (weights.shape[1] + HEAD_DIM), bytes_accessed=6 * tokens * d_model,
                                      transcendentals=0),
        name='project',
    )(hidden, grad_out, gain, weights, w_out, cos_l, sin_l)


NT = (((1,), (1,)), ((), ()))
TN = (((0,), (0,)), ((), ()))


def softmax_rows(q, k):
    scores = lax.dot_general(q, k, NT, preferred_element_type=jnp.float32) * SCORE_SCALE
    row = lax.broadcasted_iota(jnp.int32, scores.shape, 0)
    col = lax.broadcasted_iota(jnp.int32, scores.shape, 1)
    scores = jnp.where(row >= col, scores, MASK_VALUE)
    weight = jnp.exp(scores - jnp.max(scores, axis=1, keepdims=True))
    return weight * (1.0 / jnp.sum(weight, axis=1, keepdims=True))


def attend(q, k, v, grad_heads, cos_l, sin_l, seq_len):
    def kernel(q_ref, k_ref, v_ref, do_ref, cos_ref, sin_ref, o_ref, o_send, dq_ref, dq_send, dkv_ref):
        q_rows, k_rows, v_rows, grad = q_ref[...], k_ref[...], v_ref[...], do_ref[...]
        probs = softmax_rows(q_rows, k_rows)
        probs_bf16 = probs.astype(jnp.bfloat16)
        heads = jnp.dot(probs_bf16, v_rows, preferred_element_type=jnp.float32).astype(jnp.bfloat16)
        o_ref[...] = heads
        o_send[...] = heads.astype(jnp.float32)
        grad_probs = lax.dot_general(grad, v_rows, NT, preferred_element_type=jnp.float32)
        dkv_ref[1] = lax.dot_general(probs_bf16, grad, TN, preferred_element_type=jnp.float32)
        row_dot = jnp.sum(probs * grad_probs, axis=1, keepdims=True)
        grad_scores = (probs * (grad_probs - row_dot) * SCORE_SCALE).astype(jnp.bfloat16)
        grad_q = jnp.dot(grad_scores, k_rows, preferred_element_type=jnp.float32)
        grad_k = lax.dot_general(grad_scores, q_rows, TN, preferred_element_type=jnp.float32)
        cos_t, sin_t = cos_ref[...], -sin_ref[...]
        grad_q = rotate(grad_q, cos_t, sin_t).astype(jnp.bfloat16)
        dq_ref[...] = grad_q
        dq_send[...] = grad_q.astype(jnp.float32)
        dkv_ref[0] = rotate(grad_k, cos_t, sin_t)

    spec = pl.BlockSpec((seq_len, HEAD_DIM), lambda b: (b, 0))
    table = pl.BlockSpec((seq_len, HEAD_DIM), lambda b: (0, 0))
    tokens = q.shape[0]
    rounded, wide = jax.ShapeDtypeStruct(q.shape, jnp.bfloat16), jax.ShapeDtypeStruct(q.shape, jnp.float32)
    return pl.pallas_call(
        kernel, grid=(tokens // seq_len,), in_specs=[spec] * 4 + [table] * 2,
        out_specs=(spec, spec, spec, spec, pl.BlockSpec((2, seq_len, HEAD_DIM), lambda b: (0, b, 0))),
        out_shape=(rounded, wide, rounded, wide, jax.ShapeDtypeStruct((2,) + q.shape, jnp.float32)),
        compiler_params=pltpu.CompilerParams(vmem_limit_bytes=40 * 1024 * 1024),
        cost_estimate=pl.CostEstimate(flops=14 * tokens * seq_len * HEAD_DIM, bytes_accessed=28 * tokens * HEAD_DIM,
                                      transcendentals=tokens * seq_len),
        name='attend',
    )(q, k, v, grad_heads, cos_l, sin_l)


def weight_grads(normed, grad_out, grad_q, grad_kv, heads):
    tokens, d_model = normed.shape
    columns = 512

    def kernel(n_ref, dout_ref, dq_ref, dkv_ref, o_ref, wq_ref, wk_ref, wv_ref, wo_ref, left_ref):
        @pl.when(pl.program_id(0) == 0)
        def _():
            pieces = (dq_ref[...].astype(jnp.float32), dkv_ref[0], dkv_ref[1], o_ref[...].astype(jnp.float32))
            for n, piece in enumerate(pieces):
                left_ref[pl.ds(n * HEAD_DIM, HEAD_DIM), :] = jnp.transpose(piece).astype(jnp.bfloat16)

        grads = jnp.dot(left_ref[pl.ds(0, 3 * HEAD_DIM), :], n_ref[...], preferred_element_type=jnp.float32)
        for n, ref in enumerate((wq_ref, wk_ref, wv_ref)):
            ref[...] = jnp.transpose(grads[n * HEAD_DIM:(n + 1) * HEAD_DIM])
        wo_ref[...] = jnp.dot(left_ref[pl.ds(3 * HEAD_DIM, HEAD_DIM), :], dout_ref[...], preferred_element_type=jnp.float32)

    wide = pl.BlockSpec((tokens, columns), lambda i: (0, i))
    tall = pl.BlockSpec((columns, HEAD_DIM), lambda i: (i, 0))
    head = pl.BlockSpec((tokens, HEAD_DIM), lambda i: (0, 0))
    tall_out = jax.ShapeDtypeStruct((d_model, HEAD_DIM), jnp.float32)
    return pl.pallas_call(
        kernel, grid=(d_model // columns,),
        in_specs=[wide, wide, head, pl.BlockSpec((2, tokens, HEAD_DIM), lambda i: (0, 0, 0)), head],
        out_specs=(tall, tall, tall, pl.BlockSpec((HEAD_DIM, columns), lambda i: (0, i))),
        out_shape=(tall_out, tall_out, tall_out, jax.ShapeDtypeStruct((HEAD_DIM, d_model), jnp.float32)),
        scratch_shapes=[pltpu.VMEM((4 * HEAD_DIM, tokens), jnp.bfloat16)],
        compiler_params=pltpu.CompilerParams(vmem_limit_bytes=VMEM_BYTES),
        cost_estimate=pl.CostEstimate(flops=8 * tokens * d_model * HEAD_DIM, bytes_accessed=4 * tokens * d_model, transcendentals=0),
        name='weight_grads',
    )(normed, grad_out, grad_q, grad_kv, heads)


class Place:
    def __init__(self):
        index = lax.axis_index('tp')
        self.c = lax.rem(index, CORES)
        self.x = lax.rem(index // CORES, RING)
        self.y = index // ROW_DEVICES

    def at(self, y, x, c):
        return {'tp': (y * RING + x) * CORES + c}


def turn(position, by):
    return lax.rem(position + (by % RING), RING)


class Transfer:
    def __init__(self, link, size, outgoing, incoming=None):
        self.link, self.size, self.outgoing, self.incoming = link, size, outgoing, incoming or outgoing
        self.left = False


class Step:
    def __init__(self, waits=(), work=None, sends=(), after=(), cost=0.05, bulk=False):
        self.waits, self.work, self.sends, self.after, self.cost, self.bulk = waits, work, sends, after, cost, bulk


LINK_RATE = 46.6e3
CORE_RATE = 200e3
HOP = 2.0
CORE_HOP = 1.5
QUEUE = 8.0


def in_order(threads):
    now, busy, arrival, finished, order = 4.0, {}, {}, set(), []
    position = [0] * len(threads)
    while any(position[i] < len(threads[i]) for i in range(len(threads))):
        chosen, soonest = None, math.inf
        for i, steps in enumerate(threads):
            if position[i] == len(steps) or any(step not in finished for step in steps[position[i]].after):
                continue
            step = steps[position[i]]
            ready = max([arrival.get(copy, math.inf) for copy in step.waits], default=0.0)
            if step.bulk:
                ready = max([ready] + [busy.get(copy.link, 0.0) - QUEUE for copy in step.sends if copy.link != 'core'])
            if ready <= now:
                chosen = i
                break
            soonest = min(soonest, ready)
        if chosen is None:
            now = soonest
            continue
        step = threads[chosen][position[chosen]]
        position[chosen] += 1
        now += step.cost
        for copy in step.sends:
            rate, hop = (CORE_RATE, CORE_HOP) if copy.link == 'core' else (LINK_RATE, HOP)
            busy[copy.link] = max(now, busy.get(copy.link, 0.0)) + copy.size / rate
            arrival[copy] = busy[copy.link] + hop
        finished.add(step)
        order.append(step)
    return order


def exchange_kernel(chunks, spreads, *refs):
    (heads_hbm, grad_q_hbm, kv_hbm, w_hbm, w_kv_hbm, x_hbm, dout_hbm, inv_hbm, gain_ref,
     rest_ref, out_all, grad_all, kv_out,
     gath_f, gath_b, wb_f, wb_b, part, ring_f, ring_b, fin_f, fin_b, x_ref, dout_ref, inv_ref,
     kvp, kv_core, kv_send, kv_chip, rowpart, rowall, send_sem, recv_sem, loc_sem) = refs
    me = Place()
    x, y, c = me.x, me.y, me.c
    xr, xl, xo = turn(x, 1), turn(x, -1), turn(x, 2)
    yu, yd, yo = turn(y, 1), turn(y, -1), turn(y, 2)
    other = 1 - c
    own = CORES * x + c
    left, right, far = CORES * xl + c, CORES * xr + c, CORES * xo + c
    p_own, p_left, p_right, p_far = [CORES * pos + other for pos in (x, xl, xr, xo)]
    rows_y, width = x_ref.shape
    r = rows_y // chunks
    h = r // 2
    to_right, to_left, to_partner = me.at(y, xr, c), me.at(y, xl, c), me.at(y, x, other)
    to_up, to_down = me.at(yu, x, c), me.at(yd, x, c)

    barrier = pltpu.get_barrier_semaphore()
    peers = [to_up, to_down, to_right, to_left, to_partner,
             me.at(y, xo, c), me.at(y, xr, other), me.at(y, xl, other), me.at(y, xo, other)]
    for peer in peers:
        pl.semaphore_signal(barrier, inc=1, device_id=peer, device_id_type=pl.DeviceIdType.MESH)

    depth = w_hbm.shape[1]
    n_kv = w_kv_hbm.shape[0]
    own_rows = pl.ds(pl.multiple_of(y * rows_y, rows_y), rows_y)
    own_columns = pl.ds(pl.multiple_of(own * width, width), width)
    copies = [
        (heads_hbm, gath_f.at[own, pl.ds(0, RING)]), (grad_q_hbm, gath_b.at[own, pl.ds(0, RING)]),
        (kv_hbm.at[0], kvp.at[:, 0]), (kv_hbm.at[1], kvp.at[:, 1]),
        (w_hbm.at[0, pl.ds(0, rows_y)], part.at[0]),
        (w_hbm.at[0, pl.ds(rows_y, depth - rows_y)], part.at[1, pl.ds(0, depth - rows_y)]),
        (w_hbm.at[1, pl.ds(0, rows_y)], part.at[2]),
        (w_hbm.at[1, pl.ds(rows_y, depth - rows_y)], part.at[3, pl.ds(0, depth - rows_y)]),
        (w_kv_hbm, wb_b.at[pl.ds(depth, n_kv)]),
        (x_hbm.at[own_rows, own_columns], x_ref), (dout_hbm.at[own_rows, own_columns], dout_ref),
        (inv_hbm.at[own_rows], inv_ref)]
    loads = [pltpu.make_async_copy(src, dst, loc_sem.at[n]) for n, (src, dst) in enumerate(copies)]
    keep_sem = len(loads)
    for copy in loads:
        copy.start()
    first_rest = (chunks - spreads[1]) * r
    rest_ref[pl.ds(first_rest, 8), :] = jnp.zeros((8, width), jnp.float32)
    for copy in loads:
        copy.wait()
    wb_f[pl.ds(0, rows_y), :] = part[0].astype(jnp.bfloat16)
    wb_f[pl.ds(rows_y, depth - rows_y), :] = part[1, pl.ds(0, depth - rows_y), :].astype(jnp.bfloat16)
    wb_b[pl.ds(0, rows_y), :] = part[2].astype(jnp.bfloat16)
    wb_b[pl.ds(rows_y, depth - rows_y), :] = part[3, pl.ds(0, depth - rows_y), :].astype(jnp.bfloat16)
    pl.semaphore_wait(barrier, len(peers))

    transfers = []

    def transfer(link, peer, src, dst, came_from=None, came_to=None):
        n = len(transfers)

        def copy(a, b):
            return lambda: pltpu.make_async_remote_copy(
                src_ref=a, dst_ref=b, send_sem=send_sem.at[n], recv_sem=recv_sem.at[n], device_id=peer,
                device_id_type=pl.DeviceIdType.MESH)
        made = Transfer(link, 4 * math.prod(dst.shape), copy(src, dst), copy(came_from, came_to) if came_to is not None else None)
        transfers.append(made)
        return made

    def moved(link, peer, sent, came):
        return transfer(link, peer, sent, sent, came, came)

    def gone(sent):
        for copy in sent:
            copy.outgoing().wait_send()
            copy.left = True

    p = lax.rem(x, 2)
    xn = x + 1 - 2 * p
    mine, theirs = CORES * c + p, CORES * c + 1 - p
    kv_threads, settle, settled = [], [], []
    for k in range(chunks):
        rows = pl.ds(k * r, r)
        core_copy = transfer('core', to_partner, kvp.at[pl.ds(CORES * other, CORES), :, rows], kv_core.at[:, :, rows])
        chip_copy = transfer('right', me.at(y, xn, c), kv_send.at[:, rows], kv_chip.at[:, rows])

        def add_core(rows=rows):
            kv_send[:, rows, :] = kvp[theirs, :, rows, :] + kv_core[1 - p, :, rows, :]

        def add_chip(rows=rows):
            total = kvp[mine, :, rows, :] + kv_core[p, :, rows, :] + kv_chip[:, rows, :]
            gath_b[own, pl.ds(RING, 2), rows, :] = total.astype(jnp.bfloat16).astype(jnp.float32)

        kv_threads.append([Step(sends=[core_copy]), Step([core_copy], add_core, [chip_copy], cost=0.1)])
        settle.append(add_chip)
        settled.append(chip_copy)

    def add_pass(backward, gath, wb, ring, fin, spread, ahead_of):
        parts = gath.shape[1]
        half = parts // 2
        threads, passed, done, ring_sums = [], [], [], []

        def multiply(d, k, before=()):
            gone(before)
            rows = pl.ds(k * r, r)
            pieces = [gath[j, d, rows, :] for j in range(ROW_DEVICES)]
            if backward:
                j = CORES * lax.rem(d, 2) + d // 2
                pieces += [gath[j, RING, rows, :], gath[j, RING + 1, rows, :],
                           gath[j + RING, RING, rows, :], gath[j + RING, RING + 1, rows, :]]
            lhs = jnp.concatenate([piece.astype(jnp.bfloat16) for piece in pieces], axis=1)
            part[d, rows, :] = jnp.dot(lhs, wb[...], preferred_element_type=jnp.float32)

        def add_ring(way, step, k):
            d = turn(y, -(2 + step) if way == 0 else 2 + step)
            part[d, pl.ds(k * r + way * h, h), :] += ring[way, step, k]

        def store(k, values):
            if k < spread:
                fin[pl.ds(k * r, r), :] = values
            else:
                rest_ref[pl.ds((k - spread) * r, r), :] = values

        def finish_forward(k):
            rows = pl.ds(k * r, r)
            store(k, (x_ref[rows, :].astype(jnp.float32) + part[y, rows, :]).astype(jnp.bfloat16).astype(jnp.float32))

        def row_sums(k):
            rows = pl.ds(k * r, r)
            total = part[y, rows, :]
            unit = x_ref[rows, :].astype(jnp.float32) * inv_ref[rows, :]
            row_sum = jnp.sum(total * gain_ref[...] * unit, axis=1, keepdims=True)
            square = jnp.concatenate([jnp.broadcast_to(row_sum, (r, 128)), jnp.zeros((128 - r, 128), jnp.float32)], axis=0)
            rowpart[k] = jnp.transpose(square)[0:8, :]
            gain_row = jnp.sum(total * unit, axis=0, keepdims=True)
            row_id = lax.broadcasted_iota(jnp.int32, (8, width), 0)
            rest_ref[pl.ds(first_rest, 8), :] += jnp.where(row_id == 0, jnp.broadcast_to(gain_row, (8, width)), 0.0)

        def finish_backward(k):
            rows = pl.ds(k * r, r)
            sums = rowpart[k]
            for m in range(ROW_DEVICES - 1):
                sums = sums + rowall[m, k]
            mean = jnp.transpose(sums)[0:r, 0:1] * (1.0 / (width * ROW_DEVICES))
            inv = inv_ref[rows, :]
            unit = x_ref[rows, :].astype(jnp.float32) * inv
            delta = inv * (part[y, rows, :] * gain_ref[...] - unit * mean)
            store(k, (dout_ref[rows, :].astype(jnp.float32) + delta).astype(jnp.bfloat16).astype(jnp.float32))

        for k in range(chunks):
            rows = pl.ds(k * r, r)

            def block(source, first=0, count=parts, rows=rows):
                return gath.at[source, pl.ds(first, count), rows]

            s_right = moved('right', to_right, block(own), block(left))
            s_left = moved('left', to_left, block(own), block(right))
            s_core = moved('core', to_partner, block(own), block(p_own))
            f_right = moved('right', to_right, block(left, 0, half), block(far, 0, half))
            f_left = moved('left', to_left, block(right, half, parts - half), block(far, half, parts - half))
            c_left = moved('core', to_partner, block(left), block(p_left))
            c_right = moved('core', to_partner, block(right), block(p_right))
            c_far = moved('core', to_partner, block(far), block(p_far))
            sums = [[transfer(link, peer, part.at[turn(y, -(1 + step) if way == 0 else 1 + step), pl.ds(k * r + way * h, h)],
                              ring.at[way, step, k]) for step in range(RING - 1)]
                    for way, (link, peer) in enumerate((('up', to_up), ('down', to_down)))]
            ring_sums.append(sums[0] + sums[1])
            after = [passed[k - AHEAD]] if k >= AHEAD else []
            before = ()
            if ahead_of is not None:
                after.append(ahead_of[0][k])
                before = ahead_of[1][k]
            steps = [Step([settled[k]] if backward else (), settle[k] if backward else None, [s_right, s_left, s_core], after, 0.1),
                     Step([s_right], None, [f_right, c_left]), Step([s_left], None, [f_left, c_right])]
            passed.append(steps[-1])
            cost = 0.6 * r / 96 * wb.shape[0] / 1024
            steps += [Step([f_right, f_left], None, [c_far]),
                      Step([s_core, c_left, c_right, c_far], functools.partial(multiply, yd, k, before), [sums[0][0]], cost=cost),
                      Step((), functools.partial(multiply, yu, k), [sums[1][0]], cost=cost),
                      Step((), functools.partial(multiply, yo, k), cost=cost),
                      Step((), functools.partial(multiply, y, k), cost=cost)]
            for step in range(RING - 1):
                for way in (0, 1):
                    steps.append(Step([sums[way][step]], functools.partial(add_ring, way, step, k),
                                      [sums[way][step + 1]] if step < RING - 2 else [], cost=0.15))
            if backward:
                members = [(pos, core) for pos in (xr, xl, xo) for core in (c, other)] + [(x, other)]
                notes = [transfer('note', me.at(y, pos, core), rowpart.at[k], rowall.at[m, k])
                         for (pos, core), m in zip(members, (2, 3, 0, 1, 4, 5, 6))]
                steps.append(Step((), functools.partial(row_sums, k), notes, cost=0.4))
                steps.append(Step(notes, functools.partial(finish_backward, k), cost=0.5))
            else:
                steps.append(Step((), functools.partial(finish_forward, k), cost=0.3))
            done.append(steps[-1])
            threads.append(steps)
        return threads, done, ring_sums

    def add_spread(all_hbm, fin, spread, done, first_sem):
        threads = []
        for k in range(spread):
            along_x = k % 2 == 0
            (a_plus, a_minus, a, a_up, a_down, a_far), (b_plus, b_minus, b, b_up, b_down, b_far) = [
                (('right', to_right), ('left', to_left), x, xr, xl, xo), (('up', to_up), ('down', to_down), y, yu, yd, yo)
            ][::1 if along_x else -1]

            def place(core, b_pos, a_pos, part_rows=None, k=k, along_x=along_x):
                spot = (k, core, b_pos, a_pos) if along_x else (k, core, a_pos, b_pos)
                return all_hbm.at[spot + (() if part_rows is None else (pl.ds(*part_rows),))]

            def bundle(core, b_pos, first=0, count=RING, k=k, along_x=along_x):
                return all_hbm.at[(k, core, b_pos, pl.ds(first, count)) if along_x else (k, core, pl.ds(first, count), b_pos)]

            source = fin.at[pl.ds(k * r, r)]
            keep = pltpu.make_async_copy(source, place(c, b, a), loc_sem.at[first_sem + k])
            top, low = (0, h), (h, h)
            a0 = transfer(*a_plus, source, place(c, b, a), source, place(c, b, a_down))
            a1 = transfer(*a_minus, source, place(c, b, a), source, place(c, b, a_up))
            h0 = moved(*a_plus, place(c, b, a_down, top), place(c, b, a_far, top))
            h1 = moved(*a_minus, place(c, b, a_up, low), place(c, b, a_far, low))
            b0 = moved(*b_plus, bundle(c, b, 0, 2), bundle(c, b_down, 0, 2))
            b1 = moved(*b_minus, bundle(c, b, 2, 2), bundle(c, b_up, 2, 2))
            b2 = moved(*b_plus, bundle(c, b, 2, 2), bundle(c, b_down, 2, 2))
            b3 = moved(*b_minus, bundle(c, b, 0, 2), bundle(c, b_up, 0, 2))
            g0 = moved(*b_plus, bundle(c, b_down, 0, 2), bundle(c, b_far, 0, 2))
            g1 = moved(*b_minus, bundle(c, b_up, 2, 2), bundle(c, b_far, 2, 2))
            cores = [moved('core', to_partner, bundle(c, pos), bundle(other, pos)) for pos in (b, b_down, b_up, b_far)]
            threads.append([
                Step((), keep.start, [a0, a1], (done[k],), 0.1, True),
                Step([a0], None, [h0], bulk=True), Step([a1], None, [h1], bulk=True),
                Step([h0, h1], keep.wait, [b0, b1, b2, b3, cores[0]], cost=0.1, bulk=True),
                Step([b0], None, [g0], bulk=True), Step([b1], None, [g1], bulk=True),
                Step([b2], None, [cores[1]]), Step([b3], None, [cores[2]]),
                Step([g0, g1], None, [cores[3]]), Step(cores)])
        return threads

    forward, done_f, sums_f = add_pass(False, gath_f, wb_f, ring_f, fin_f, spreads[0], None)
    backward, done_b, _ = add_pass(True, gath_b, wb_b, ring_b, fin_b, spreads[1], (done_f, sums_f))
    spread_f = add_spread(out_all, fin_f, spreads[0], done_f, keep_sem)
    spread_b = add_spread(grad_all, fin_b, spreads[1], done_b, keep_sem + spreads[0])
    for step in in_order(forward + kv_threads + backward + spread_f + spread_b):
        for copy in step.waits:
            copy.incoming().wait_recv()
        if step.work is not None:
            step.work()
        for copy in step.sends:
            copy.outgoing().start()

    kv_copies = [pltpu.make_async_copy(gath_b.at[CORES * (2 * (x // 2) + d % 2) + d // 2, pl.ds(RING, 2)],
                                       kv_out.at[:, d], loc_sem.at[d]) for d in range(RING)]
    for copy in kv_copies:
        copy.start()
    for copy in kv_copies:
        copy.wait()
    gone([copy for copy in transfers if not copy.left])


def exchange(heads, grad_q, kv, w_blocks, w_kv_block, x_rows, dout_rows, inv, gain_block, spread=None):
    tokens, d_model = x_rows.shape
    rows_y, width = tokens // RING, d_model // ROW_DEVICES
    chunks = CHUNKS
    spreads = (chunks, SPREAD if spread is None else spread)
    r = rows_y // chunks
    any_spec = pl.BlockSpec(memory_space=pl.ANY)
    vmem_spec = pl.BlockSpec(memory_space=pltpu.VMEM)
    depth, n_kv = w_blocks.shape[1], w_kv_block.shape[0]
    f32, bf16 = jnp.float32, jnp.bfloat16

    def gathered(count):
        return jax.ShapeDtypeStruct((count, CORES, RING, RING, r, width), f32)

    passes = chunks * (8 + 2 * (RING - 1))
    copies = 2 * passes + chunks * (2 + ROW_DEVICES - 1) + 14 * sum(spreads)
    dma = pltpu.SemaphoreType.DMA
    sums = pltpu.VMEM((2, RING - 1, chunks, r // 2, width), f32)
    return pl.pallas_call(
        functools.partial(exchange_kernel, chunks, spreads),
        out_shape=[jax.ShapeDtypeStruct(((chunks - spreads[1]) * r + 8, width), f32), gathered(spreads[0]), gathered(spreads[1]),
                   jax.ShapeDtypeStruct((2, RING, rows_y, HEAD_DIM), f32)],
        in_specs=[any_spec] * 8 + [vmem_spec],
        out_specs=[vmem_spec, any_spec, any_spec, any_spec],
        scratch_shapes=[
            pltpu.VMEM((ROW_DEVICES, RING, rows_y, HEAD_DIM), f32),
            pltpu.VMEM((ROW_DEVICES, RING + 2, rows_y, HEAD_DIM), f32),
            pltpu.VMEM((depth, width), bf16), pltpu.VMEM((depth + n_kv, width), bf16),
            pltpu.VMEM((RING, rows_y, width), f32), sums, sums,
            pltpu.VMEM((spreads[0] * r, width), f32), pltpu.VMEM((spreads[1] * r, width), f32),
            pltpu.VMEM((rows_y, width), bf16), pltpu.VMEM((rows_y, width), bf16), pltpu.VMEM((rows_y, 1), f32),
            pltpu.VMEM((RING, 2, rows_y, HEAD_DIM), f32), pltpu.VMEM((CORES, 2, rows_y, HEAD_DIM), f32),
            pltpu.VMEM((2, rows_y, HEAD_DIM), f32), pltpu.VMEM((2, rows_y, HEAD_DIM), f32),
            pltpu.VMEM((chunks, 8, 128), f32), pltpu.VMEM((ROW_DEVICES - 1, chunks, 8, 128), f32),
            dma((copies,)), dma((copies,)), dma((12 + sum(spreads),))],
        compiler_params=pltpu.CompilerParams(collective_id=1, has_side_effects=True, vmem_limit_bytes=VMEM_BYTES),
        cost_estimate=pl.CostEstimate(flops=2 * tokens * (2 * depth + n_kv) * width, bytes_accessed=16 * tokens * width, transcendentals=0),
        name='exchange',
    )(heads, grad_q, kv, w_blocks, w_kv_block, x_rows, dout_rows, inv, gain_block)


def rounded(kernel, gathered, grid, block, index_map, out_rows, place_of, rows, so_far):
    d_model = ROW_DEVICES * gathered.shape[-1]
    moved_rows = math.prod(grid) * out_rows
    return pl.pallas_call(
        kernel, grid=grid,
        in_specs=[pl.BlockSpec(block, index_map)] + ([pl.BlockSpec(memory_space=pl.ANY)] if so_far is not None else []),
        out_specs=pl.BlockSpec((out_rows, d_model), lambda *at: (place_of(*at), 0)),
        out_shape=jax.ShapeDtypeStruct((rows, d_model), jnp.bfloat16),
        input_output_aliases={1: 0} if so_far is not None else {},
        compiler_params=pltpu.CompilerParams(vmem_limit_bytes=VMEM_BYTES),
        cost_estimate=pl.CostEstimate(flops=moved_rows * d_model, bytes_accessed=6 * moved_rows * d_model, transcendentals=0),
        name='narrow',
    )(*((gathered,) if so_far is None else (gathered, so_far)))


def narrow_spread(gathered, spread, rows, so_far=None):
    r, width = gathered.shape[-2:]
    chunks = rows // RING // r

    def kernel(in_ref, *rest):
        for n in range(ROW_DEVICES):
            rest[-1][:, pl.ds(n * width, width)] = in_ref[0, n % CORES, 0, n // CORES].astype(jnp.bfloat16)

    return rounded(kernel, gathered, (spread, RING), (1, CORES, 1, RING, r, width), lambda k, y: (k, 0, y, 0, 0, 0), r,
                   lambda k, y: y * chunks + k, rows, so_far)


def narrow_rest(gathered, pad, spread, r, rows, so_far=None):
    width = gathered.shape[-1]
    chunks = rows // RING // r
    count = chunks - spread
    step = count if chunks % count == 0 and spread % count == 0 else 1
    assert step == count or pad == 0
    blocks = gathered.reshape(RING * ROW_DEVICES, count * r + pad, width)

    def kernel(in_ref, *rest):
        for n in range(ROW_DEVICES):
            rest[-1][:, pl.ds(n * width, width)] = in_ref[n, pl.ds(0, step * r), :].astype(jnp.bfloat16)

    return rounded(kernel, blocks, (RING, count // step), (ROW_DEVICES, step * r + pad, width), lambda y, j: (y, j, 0), step * r,
                   lambda y, j: (y * chunks + spread) // step + j, rows, so_far)


def solution(mesh):
    tp_size = mesh.shape['tp']
    row_groups = [list(range(first, first + ROW_DEVICES)) for first in range(0, tp_size, ROW_DEVICES)]

    def block_fn(hidden, grad_out, norm_gain, w_query, w_key, w_value, w_out):
        batch, seq_len, d_model = hidden.shape
        kv_heads = w_key.shape[1] // HEAD_DIM
        group_size = tp_size // kv_heads
        index = lax.axis_index('tp')
        y, column = index // ROW_DEVICES, index % ROW_DEVICES
        tokens, width = batch * seq_len, d_model // ROW_DEVICES
        rows_y = tokens // RING
        kv_pair = ROW_DEVICES // group_size * HEAD_DIM

        blocks = jnp.stack([w_out, w_query.T]).astype(jnp.float32).reshape(2, HEAD_DIM, ROW_DEVICES, width)
        w_blocks = lax.all_to_all(blocks.transpose(0, 2, 1, 3), 'tp', 1, 1, axis_index_groups=row_groups, tiled=True)
        w_blocks = w_blocks.reshape(2, ROW_DEVICES * HEAD_DIM, width)

        def kv_block(weight):
            block = lax.dynamic_slice(weight, (column * width, y * kv_pair), (width, kv_pair))
            return block.T.reshape(-1, 1, HEAD_DIM, width)

        w_kv_block = jnp.concatenate([kv_block(w_key), kv_block(w_value)], axis=1).reshape(-1, width)

        kv_index = index // group_size
        w_local = jnp.concatenate([
            w_query,
            lax.dynamic_slice_in_dim(w_key, kv_index * HEAD_DIM, HEAD_DIM, axis=1),
            lax.dynamic_slice_in_dim(w_value, kv_index * HEAD_DIM, HEAD_DIM, axis=1)], axis=1)
        cos_l, sin_l = rope_lanes(seq_len)
        gain_row = norm_gain.astype(jnp.float32).reshape(1, d_model)
        grad_rows = grad_out.reshape(tokens, d_model)

        normed, inv_rms, q_rot, k_rot, v_head, grad_heads = project(
            hidden.reshape(tokens, d_model), grad_rows, gain_row, w_local, w_out, cos_l, sin_l)
        heads, heads_send, grad_q, grad_q_send, grad_kv_send = attend(q_rot, k_rot, v_head, grad_heads, cos_l, sin_l, seq_len)
        gain_block = lax.dynamic_slice(gain_row, (0, column * width), (1, width))
        by_rows = (RING, rows_y, HEAD_DIM)
        rest_block, out_spread, grad_spread, grad_kv = exchange(
            heads_send.reshape(by_rows), grad_q_send.reshape(by_rows), grad_kv_send.reshape((2,) + by_rows),
            w_blocks, w_kv_block, hidden.reshape(tokens, d_model), grad_rows, inv_rms, gain_block)
        grad_rest = lax.all_gather(rest_block, 'tp', axis=0, tiled=True)
        r = rows_y // CHUNKS
        block_out = narrow_spread(out_spread, CHUNKS, tokens).reshape(hidden.shape)
        grad_hidden = narrow_rest(grad_rest, 8, SPREAD, r, tokens, narrow_spread(grad_spread, SPREAD, tokens)).reshape(hidden.shape)
        grad_gain = jnp.sum(grad_rest.reshape(RING, ROW_DEVICES, -1, width)[:, :, (CHUNKS - SPREAD) * r, :], axis=0).reshape(d_model)
        grad_w_query, grad_w_key, grad_w_value, grad_w_out = weight_grads(
            normed, grad_rows, grad_q, grad_kv.reshape(2, tokens, HEAD_DIM), heads)
        return block_out, grad_hidden, grad_gain, grad_w_query, grad_w_key, grad_w_value, grad_w_out

    act_spec = P('dp', None, None)
    return jax.shard_map(
        block_fn, mesh=mesh,
        in_specs=(act_spec, act_spec, P(None), P(None, 'tp'), P(None, None), P(None, None), P('tp', None)),
        out_specs=(act_spec, act_spec, P('dp'), P('dp', 'tp'), P('dp', 'tp'), P('dp', 'tp'), P(('dp', 'tp'), None)),
        check_vma=False)
```

```python
import functools
import math
import jax
import jax.numpy as jnp
from jax import lax
from jax.experimental import pallas as pl
from jax.experimental.pallas import tpu as pltpu
from jax.sharding import PartitionSpec as P

HEAD_DIM = 128
NORM_EPS = 1.0e-5
ROPE_BASE = 10000.0
MASK_VALUE = -1.0e30
SCORE_SCALE = 1.0 / math.sqrt(HEAD_DIM)
RING = 4
CORES = 2
ROW_DEVICES = RING * CORES
CHUNKS = 9
AHEAD = 2
SPREAD = 6
VMEM_BYTES = 62 * 1024 * 1024


def rope_lanes(seq_len):
    lane = lax.broadcasted_iota(jnp.int32, (1, HEAD_DIM), 1)
    inv_freq = ROPE_BASE ** (-(lane - lane % 2).astype(jnp.float32) / HEAD_DIM)
    angles = jnp.arange(seq_len, dtype=jnp.float32)[:, None] * inv_freq
    return jnp.cos(angles), jnp.where(lane % 2 == 0, -jnp.sin(angles), jnp.sin(angles))


def rotate(tensor, cos_l, sin_l):
    lane = lax.broadcasted_iota(jnp.int32, tensor.shape, 1)
    swapped = jnp.where(lane % 2 == 0, pltpu.roll(tensor, HEAD_DIM - 1, 1), pltpu.roll(tensor, 1, 1))
    return tensor * cos_l + swapped * sin_l


def project(hidden, grad_out, gain, kv_index, w_query, w_key, w_value, w_out, cos_l, sin_l):
    tokens, d_model = hidden.shape
    seq_len = cos_l.shape[0]
    rows = 384

    def kernel(kv_ref, x_ref, dout_ref, gain_ref, wq_ref, wk_ref, wv_ref, w_out_ref, cos_ref, sin_ref,
               normed_ref, inv_ref, q_ref, k_ref, v_ref, do_ref, w_ref):
        @pl.when(pl.program_id(0) == 0)
        def _():
            for n, ref in enumerate((wq_ref, wk_ref, wv_ref)):
                w_ref[:, pl.ds(n * HEAD_DIM, HEAD_DIM)] = ref[...]

        values = x_ref[...].astype(jnp.float32)
        inv = lax.rsqrt(jnp.mean(values * values, axis=1, keepdims=True) + NORM_EPS)
        inv_ref[...] = inv
        normed = (values * inv * gain_ref[...]).astype(jnp.bfloat16)
        normed_ref[...] = normed
        heads = jnp.dot(normed, w_ref[...], preferred_element_type=jnp.float32)
        q_ref[...] = rotate(heads[:, :HEAD_DIM], cos_ref[...], sin_ref[...]).astype(jnp.bfloat16)
        k_ref[...] = rotate(heads[:, HEAD_DIM:2 * HEAD_DIM], cos_ref[...], sin_ref[...]).astype(jnp.bfloat16)
        v_ref[...] = heads[:, 2 * HEAD_DIM:].astype(jnp.bfloat16)
        do_ref[...] = lax.dot_general(dout_ref[...], w_out_ref[...], NT, preferred_element_type=jnp.float32).astype(jnp.bfloat16)

    row_spec = pl.BlockSpec((rows, d_model), lambda i, kv: (i, 0))
    head_spec = pl.BlockSpec((rows, HEAD_DIM), lambda i, kv: (i, 0))
    table_spec = pl.BlockSpec((rows, HEAD_DIM), lambda i, kv: (i % (seq_len // rows), 0))
    kv_spec = pl.BlockSpec((d_model, HEAD_DIM), lambda i, kv: (0, kv[0]))
    head = jax.ShapeDtypeStruct((tokens, HEAD_DIM), jnp.bfloat16)

    def whole(array):
        return pl.BlockSpec(array.shape, lambda i, kv: (0, 0))

    return pl.pallas_call(
        kernel,
        grid_spec=pltpu.PrefetchScalarGridSpec(
            num_scalar_prefetch=1, grid=(tokens // rows,),
            in_specs=[row_spec, row_spec, whole(gain), whole(w_query), kv_spec, kv_spec, whole(w_out), table_spec, table_spec],
            out_specs=(row_spec, pl.BlockSpec((rows, 1), lambda i, kv: (i, 0)), head_spec, head_spec, head_spec, head_spec),
            scratch_shapes=[pltpu.VMEM((d_model, 3 * HEAD_DIM), jnp.bfloat16)]),
        out_shape=(jax.ShapeDtypeStruct((tokens, d_model), jnp.bfloat16), jax.ShapeDtypeStruct((tokens, 1), jnp.float32),
                   head, head, head, head),
        compiler_params=pltpu.CompilerParams(vmem_limit_bytes=VMEM_BYTES),
        cost_estimate=pl.CostEstimate(flops=8 * tokens * d_model * HEAD_DIM, bytes_accessed=6 * tokens * d_model, transcendentals=0),
        name='project',
    )(kv_index, hidden, grad_out, gain, w_query, w_key, w_value, w_out, cos_l, sin_l)


NT = (((1,), (1,)), ((), ()))
TN = (((0,), (0,)), ((), ()))


def softmax_rows(q, k):
    scores = lax.dot_general(q, k, NT, preferred_element_type=jnp.float32) * SCORE_SCALE
    row = lax.broadcasted_iota(jnp.int32, scores.shape, 0)
    col = lax.broadcasted_iota(jnp.int32, scores.shape, 1)
    scores = jnp.where(row >= col, scores, MASK_VALUE)
    weight = jnp.exp(scores - jnp.max(scores, axis=1, keepdims=True))
    return weight * (1.0 / jnp.sum(weight, axis=1, keepdims=True))


def attend(q, k, v, grad_heads, cos_l, sin_l, seq_len):
    def kernel(q_ref, k_ref, v_ref, do_ref, cos_ref, sin_ref, o_ref, o_send, dq_ref, dq_send, dkv_ref):
        q_rows, k_rows, v_rows, grad = q_ref[...], k_ref[...], v_ref[...], do_ref[...]
        probs = softmax_rows(q_rows, k_rows)
        probs_bf16 = probs.astype(jnp.bfloat16)
        heads = jnp.dot(probs_bf16, v_rows, preferred_element_type=jnp.float32).astype(jnp.bfloat16)
        o_ref[...] = heads
        o_send[...] = heads.astype(jnp.float32)
        grad_probs = lax.dot_general(grad, v_rows, NT, preferred_element_type=jnp.float32)
        dkv_ref[1] = lax.dot_general(probs_bf16, grad, TN, preferred_element_type=jnp.float32)
        row_dot = jnp.sum(probs * grad_probs, axis=1, keepdims=True)
        grad_scores = (probs * (grad_probs - row_dot) * SCORE_SCALE).astype(jnp.bfloat16)
        grad_q = jnp.dot(grad_scores, k_rows, preferred_element_type=jnp.float32)
        grad_k = lax.dot_general(grad_scores, q_rows, TN, preferred_element_type=jnp.float32)
        cos_t, sin_t = cos_ref[...], -sin_ref[...]
        grad_q = rotate(grad_q, cos_t, sin_t).astype(jnp.bfloat16)
        dq_ref[...] = grad_q
        dq_send[...] = grad_q.astype(jnp.float32)
        dkv_ref[0] = rotate(grad_k, cos_t, sin_t)

    spec = pl.BlockSpec((seq_len, HEAD_DIM), lambda b: (b, 0))
    table = pl.BlockSpec((seq_len, HEAD_DIM), lambda b: (0, 0))
    tokens = q.shape[0]
    rounded, wide = jax.ShapeDtypeStruct(q.shape, jnp.bfloat16), jax.ShapeDtypeStruct(q.shape, jnp.float32)
    return pl.pallas_call(
        kernel, grid=(tokens // seq_len,), in_specs=[spec] * 4 + [table] * 2,
        out_specs=(spec, spec, spec, spec, pl.BlockSpec((2, seq_len, HEAD_DIM), lambda b: (0, b, 0))),
        out_shape=(rounded, wide, rounded, wide, jax.ShapeDtypeStruct((2,) + q.shape, jnp.float32)),
        compiler_params=pltpu.CompilerParams(vmem_limit_bytes=VMEM_BYTES),
        cost_estimate=pl.CostEstimate(flops=14 * tokens * seq_len * HEAD_DIM, bytes_accessed=28 * tokens * HEAD_DIM,
                                      transcendentals=tokens * seq_len),
        name='attend',
    )(q, k, v, grad_heads, cos_l, sin_l)


def weight_grads(normed, grad_out, grad_q, grad_kv, heads):
    tokens, d_model = normed.shape
    columns = 512

    def kernel(n_ref, dout_ref, dq_ref, dkv_ref, o_ref, wq_ref, wk_ref, wv_ref, wo_ref, left_ref):
        @pl.when(pl.program_id(0) == 0)
        def _():
            pieces = (dq_ref[...].astype(jnp.float32), dkv_ref[0], dkv_ref[1], o_ref[...].astype(jnp.float32))
            for n, piece in enumerate(pieces):
                left_ref[pl.ds(n * HEAD_DIM, HEAD_DIM), :] = jnp.transpose(piece).astype(jnp.bfloat16)

        grads = jnp.dot(left_ref[pl.ds(0, 3 * HEAD_DIM), :], n_ref[...], preferred_element_type=jnp.float32)
        for n, ref in enumerate((wq_ref, wk_ref, wv_ref)):
            ref[...] = jnp.transpose(grads[n * HEAD_DIM:(n + 1) * HEAD_DIM])
        wo_ref[...] = jnp.dot(left_ref[pl.ds(3 * HEAD_DIM, HEAD_DIM), :], dout_ref[...], preferred_element_type=jnp.float32)

    wide = pl.BlockSpec((tokens, columns), lambda i: (0, i))
    tall = pl.BlockSpec((columns, HEAD_DIM), lambda i: (i, 0))
    head = pl.BlockSpec((tokens, HEAD_DIM), lambda i: (0, 0))
    tall_out = jax.ShapeDtypeStruct((d_model, HEAD_DIM), jnp.float32)
    return pl.pallas_call(
        kernel, grid=(d_model // columns,),
        in_specs=[wide, wide, head, pl.BlockSpec((2, tokens, HEAD_DIM), lambda i: (0, 0, 0)), head],
        out_specs=(tall, tall, tall, pl.BlockSpec((HEAD_DIM, columns), lambda i: (0, i))),
        out_shape=(tall_out, tall_out, tall_out, jax.ShapeDtypeStruct((HEAD_DIM, d_model), jnp.float32)),
        scratch_shapes=[pltpu.VMEM((4 * HEAD_DIM, tokens), jnp.bfloat16)],
        compiler_params=pltpu.CompilerParams(vmem_limit_bytes=VMEM_BYTES),
        cost_estimate=pl.CostEstimate(flops=8 * tokens * d_model * HEAD_DIM, bytes_accessed=4 * tokens * d_model, transcendentals=0),
        name='weight_grads',
    )(normed, grad_out, grad_q, grad_kv, heads)


def column_blocks(w_out, w_query):
    d_model = w_out.shape[1]
    width = d_model // ROW_DEVICES

    def kernel(w_out_ref, w_query_ref, out_ref):
        out_ref[0, 0] = w_out_ref[...].astype(jnp.float32)
        out_ref[0, 1] = jnp.transpose(w_query_ref[...].astype(jnp.float32))

    return pl.pallas_call(
        kernel, grid=(ROW_DEVICES,),
        in_specs=[pl.BlockSpec((HEAD_DIM, width), lambda j: (0, j)), pl.BlockSpec((width, HEAD_DIM), lambda j: (j, 0))],
        out_specs=pl.BlockSpec((1, 2, HEAD_DIM, width), lambda j: (j, 0, 0, 0)),
        out_shape=jax.ShapeDtypeStruct((ROW_DEVICES, 2, HEAD_DIM, width), jnp.float32),
        cost_estimate=pl.CostEstimate(flops=2 * HEAD_DIM * d_model, bytes_accessed=12 * HEAD_DIM * d_model, transcendentals=0),
        name='column_blocks',
    )(w_out, w_query)


class Place:
    def __init__(self):
        index = lax.axis_index('tp')
        self.c = lax.rem(index, CORES)
        self.x = lax.rem(index // CORES, RING)
        self.y = index // ROW_DEVICES

    def at(self, y, x, c):
        return {'tp': (y * RING + x) * CORES + c}


def turn(position, by):
    return lax.rem(position + (by % RING), RING)


class Transfer:
    def __init__(self, link, size, outgoing, incoming=None):
        self.link, self.size, self.outgoing, self.incoming = link, size, outgoing, incoming or outgoing
        self.left = False


class Step:
    def __init__(self, waits=(), work=None, sends=(), after=(), cost=0.05, bulk=False):
        self.waits, self.work, self.sends, self.after, self.cost, self.bulk = waits, work, sends, after, cost, bulk


LINK_RATE = 46.6e3
CORE_RATE = 200e3
HOP = 2.0
CORE_HOP = 1.5
QUEUE = 8.0


def in_order(threads):
    now, busy, arrival, finished, order = 4.0, {}, {}, set(), []
    position = [0] * len(threads)
    while any(position[i] < len(threads[i]) for i in range(len(threads))):
        chosen, soonest = None, math.inf
        for i, steps in enumerate(threads):
            if position[i] == len(steps) or any(step not in finished for step in steps[position[i]].after):
                continue
            step = steps[position[i]]
            ready = max([arrival.get(copy, math.inf) for copy in step.waits], default=0.0)
            if step.bulk:
                ready = max([ready] + [busy.get(copy.link, 0.0) - QUEUE for copy in step.sends if copy.link != 'core'])
            if ready <= now:
                chosen = i
                break
            soonest = min(soonest, ready)
        if chosen is None:
            now = soonest
            continue
        step = threads[chosen][position[chosen]]
        position[chosen] += 1
        now += step.cost
        for copy in step.sends:
            rate, hop = (CORE_RATE, CORE_HOP) if copy.link == 'core' else (LINK_RATE, HOP)
            busy[copy.link] = max(now, busy.get(copy.link, 0.0)) + copy.size / rate
            arrival[copy] = busy[copy.link] + hop
        finished.add(step)
        order.append(step)
    return order


def exchange_kernel(chunks, spreads, *refs):
    (heads_hbm, grad_q_hbm, kv_hbm, w_hbm, w_key_hbm, w_value_hbm, x_hbm, dout_hbm, inv_hbm, gain_ref,
     rest_ref, out_all, grad_all, kv_out,
     gath_f, gath_b, wb_f, wb_b, part, ring_f, ring_b, fin_f, fin_b, x_ref, dout_ref, inv_ref,
     kvp, kv_core, kv_send, kv_chip, rowpart, rowall, w_kv, send_sem, recv_sem, loc_sem) = refs
    me = Place()
    x, y, c = me.x, me.y, me.c
    xr, xl, xo = turn(x, 1), turn(x, -1), turn(x, 2)
    yu, yd, yo = turn(y, 1), turn(y, -1), turn(y, 2)
    other = 1 - c
    own = CORES * x + c
    left, right, far = CORES * xl + c, CORES * xr + c, CORES * xo + c
    p_own, p_left, p_right, p_far = [CORES * pos + other for pos in (x, xl, xr, xo)]
    rows_y, width = x_ref.shape
    r = rows_y // chunks
    h = r // 2
    to_right, to_left, to_partner = me.at(y, xr, c), me.at(y, xl, c), me.at(y, x, other)
    to_up, to_down = me.at(yu, x, c), me.at(yd, x, c)

    barrier = pltpu.get_barrier_semaphore()
    peers = [to_up, to_down, to_right, to_left, to_partner,
             me.at(y, xo, c), me.at(y, xr, other), me.at(y, xl, other), me.at(y, xo, other)]
    for peer in peers:
        pl.semaphore_signal(barrier, inc=1, device_id=peer, device_id_type=pl.DeviceIdType.MESH)

    depth = ROW_DEVICES * HEAD_DIM
    n_pair = w_kv.shape[2]
    own_rows = pl.ds(pl.multiple_of(y * rows_y, rows_y), rows_y)
    own_columns = pl.ds(pl.multiple_of(own * width, width), width)
    own_pair = pl.ds(pl.multiple_of(y * n_pair, n_pair), n_pair)
    per_slot = rows_y // HEAD_DIM

    def stage(which, j):
        return part.at[2 * which + j // per_slot, pl.ds(j % per_slot * HEAD_DIM, HEAD_DIM)]

    copies = [(w_hbm.at[j, which], stage(which, j)) for which in (0, 1) for j in range(ROW_DEVICES)]
    copies += [
        (heads_hbm, gath_f.at[own, pl.ds(0, RING)]), (grad_q_hbm, gath_b.at[own, pl.ds(0, RING)]),
        (kv_hbm.at[0], kvp.at[:, 0]), (kv_hbm.at[1], kvp.at[:, 1]),
        (w_key_hbm.at[own_columns, own_pair], w_kv.at[0]), (w_value_hbm.at[own_columns, own_pair], w_kv.at[1]),
        (x_hbm.at[own_rows, own_columns], x_ref), (dout_hbm.at[own_rows, own_columns], dout_ref),
        (inv_hbm.at[own_rows], inv_ref)]
    loads = [pltpu.make_async_copy(src, dst, loc_sem.at[n]) for n, (src, dst) in enumerate(copies)]
    keep_sem = len(loads)
    for copy in loads:
        copy.start()
    first_rest = (chunks - spreads[1]) * r
    rest_ref[pl.ds(first_rest, 8), :] = jnp.zeros((8, width), jnp.float32)
    for copy in loads:
        copy.wait()
    for which, weights in enumerate((wb_f, wb_b)):
        for j in range(ROW_DEVICES):
            weights[pl.ds(j * HEAD_DIM, HEAD_DIM), :] = stage(which, j)[...].astype(jnp.bfloat16)
    for j in range(n_pair // HEAD_DIM):
        for s in (0, 1):
            block = w_kv[s, :, pl.ds(j * HEAD_DIM, HEAD_DIM)].astype(jnp.float32)
            wb_b[pl.ds(depth + (2 * j + s) * HEAD_DIM, HEAD_DIM), :] = jnp.transpose(block).astype(jnp.bfloat16)
    pl.semaphore_wait(barrier, len(peers))

    transfers = []

    def transfer(link, peer, src, dst, came_from=None, came_to=None):
        n = len(transfers)

        def copy(a, b):
            return lambda: pltpu.make_async_remote_copy(
                src_ref=a, dst_ref=b, send_sem=send_sem.at[n], recv_sem=recv_sem.at[n], device_id=peer,
                device_id_type=pl.DeviceIdType.MESH)
        made = Transfer(link, 4 * math.prod(dst.shape), copy(src, dst), copy(came_from, came_to) if came_to is not None else None)
        transfers.append(made)
        return made

    def moved(link, peer, sent, came):
        return transfer(link, peer, sent, sent, came, came)

    def gone(sent):
        for copy in sent:
            copy.outgoing().wait_send()
            copy.left = True

    p = lax.rem(x, 2)
    xn = x + 1 - 2 * p
    mine, theirs = CORES * c + p, CORES * c + 1 - p
    kv_threads, settle, settled = [], [], []
    for k in range(chunks):
        rows = pl.ds(k * r, r)
        core_copy = transfer('core', to_partner, kvp.at[pl.ds(CORES * other, CORES), :, rows], kv_core.at[:, :, rows])
        chip_copy = transfer('right', me.at(y, xn, c), kv_send.at[:, rows], kv_chip.at[:, rows])

        def add_core(rows=rows):
            kv_send[:, rows, :] = kvp[theirs, :, rows, :] + kv_core[1 - p, :, rows, :]

        def add_chip(rows=rows):
            total = kvp[mine, :, rows, :] + kv_core[p, :, rows, :] + kv_chip[:, rows, :]
            gath_b[own, pl.ds(RING, 2), rows, :] = total.astype(jnp.bfloat16).astype(jnp.float32)

        kv_threads.append([Step(sends=[core_copy]), Step([core_copy], add_core, [chip_copy], cost=0.1)])
        settle.append(add_chip)
        settled.append(chip_copy)

    def add_pass(backward, gath, wb, ring, fin, spread, ahead_of):
        parts = gath.shape[1]
        half = parts // 2
        threads, passed, done, ring_sums = [], [], [], []

        def multiply(d, k, before=()):
            gone(before)
            rows = pl.ds(k * r, r)
            pieces = [gath[j, d, rows, :] for j in range(ROW_DEVICES)]
            if backward:
                j = CORES * lax.rem(d, 2) + d // 2
                pieces += [gath[j, RING, rows, :], gath[j, RING + 1, rows, :],
                           gath[j + RING, RING, rows, :], gath[j + RING, RING + 1, rows, :]]
            lhs = jnp.concatenate([piece.astype(jnp.bfloat16) for piece in pieces], axis=1)
            part[d, rows, :] = jnp.dot(lhs, wb[...], preferred_element_type=jnp.float32)

        def add_ring(way, step, k):
            d = turn(y, -(2 + step) if way == 0 else 2 + step)
            part[d, pl.ds(k * r + way * h, h), :] += ring[way, step, k]

        def store(k, values):
            if k < spread:
                fin[pl.ds(k * r, r), :] = values
            else:
                rest_ref[pl.ds((k - spread) * r, r), :] = values

        def finish_forward(k):
            rows = pl.ds(k * r, r)
            store(k, (x_ref[rows, :].astype(jnp.float32) + part[y, rows, :]).astype(jnp.bfloat16).astype(jnp.float32))

        def row_sums(k):
            rows = pl.ds(k * r, r)
            total = part[y, rows, :]
            unit = x_ref[rows, :].astype(jnp.float32) * inv_ref[rows, :]
            row_sum = jnp.sum(total * gain_ref[...] * unit, axis=1, keepdims=True)
            square = jnp.concatenate([jnp.broadcast_to(row_sum, (r, 128)), jnp.zeros((128 - r, 128), jnp.float32)], axis=0)
            rowpart[k] = jnp.transpose(square)[0:8, :]
            gain_row = jnp.sum(total * unit, axis=0, keepdims=True)
            row_id = lax.broadcasted_iota(jnp.int32, (8, width), 0)
            rest_ref[pl.ds(first_rest, 8), :] += jnp.where(row_id == 0, jnp.broadcast_to(gain_row, (8, width)), 0.0)

        def finish_backward(k):
            rows = pl.ds(k * r, r)
            sums = rowpart[k]
            for m in range(ROW_DEVICES - 1):
                sums = sums + rowall[m, k]
            mean = jnp.transpose(sums)[0:r, 0:1] * (1.0 / (width * ROW_DEVICES))
            inv = inv_ref[rows, :]
            unit = x_ref[rows, :].astype(jnp.float32) * inv
            delta = inv * (part[y, rows, :] * gain_ref[...] - unit * mean)
            store(k, (dout_ref[rows, :].astype(jnp.float32) + delta).astype(jnp.bfloat16).astype(jnp.float32))

        for k in range(chunks):
            rows = pl.ds(k * r, r)

            def block(source, first=0, count=parts, rows=rows):
                return gath.at[source, pl.ds(first, count), rows]

            s_right = moved('right', to_right, block(own), block(left))
            s_left = moved('left', to_left, block(own), block(right))
            s_core = moved('core', to_partner, block(own), block(p_own))
            f_right = moved('right', to_right, block(left, 0, half), block(far, 0, half))
            f_left = moved('left', to_left, block(right, half, parts - half), block(far, half, parts - half))
            c_left = moved('core', to_partner, block(left), block(p_left))
            c_right = moved('core', to_partner, block(right), block(p_right))
            c_far = moved('core', to_partner, block(far), block(p_far))
            sums = [[transfer(link, peer, part.at[turn(y, -(1 + step) if way == 0 else 1 + step), pl.ds(k * r + way * h, h)],
                              ring.at[way, step, k]) for step in range(RING - 1)]
                    for way, (link, peer) in enumerate((('up', to_up), ('down', to_down)))]
            ring_sums.append(sums[0] + sums[1])
            after = [passed[k - AHEAD]] if k >= AHEAD else []
            before = ()
            if ahead_of is not None:
                after.append(ahead_of[0][k])
                before = ahead_of[1][k]
            steps = [Step([settled[k]] if backward else (), settle[k] if backward else None, [s_right, s_left, s_core], after, 0.1),
                     Step([s_right], None, [f_right, c_left]), Step([s_left], None, [f_left, c_right])]
            passed.append(steps[-1])
            cost = 0.6 * r / 96 * wb.shape[0] / 1024
            steps += [Step([f_right, f_left], None, [c_far]),
                      Step([s_core, c_left, c_right, c_far], functools.partial(multiply, yd, k, before), [sums[0][0]], cost=cost),
                      Step((), functools.partial(multiply, yu, k), [sums[1][0]], cost=cost),
                      Step((), functools.partial(multiply, yo, k), cost=cost),
                      Step((), functools.partial(multiply, y, k), cost=cost)]
            for step in range(RING - 1):
                for way in (0, 1):
                    steps.append(Step([sums[way][step]], functools.partial(add_ring, way, step, k),
                                      [sums[way][step + 1]] if step < RING - 2 else [], cost=0.15))
            if backward:
                members = [(pos, core) for pos in (xr, xl, xo) for core in (c, other)] + [(x, other)]
                notes = [transfer('note', me.at(y, pos, core), rowpart.at[k], rowall.at[m, k])
                         for (pos, core), m in zip(members, (2, 3, 0, 1, 4, 5, 6))]
                steps.append(Step((), functools.partial(row_sums, k), notes, cost=0.4))
                steps.append(Step(notes, functools.partial(finish_backward, k), cost=0.5))
            else:
                steps.append(Step((), functools.partial(finish_forward, k), cost=0.3))
            done.append(steps[-1])
            threads.append(steps)
        return threads, done, ring_sums

    def add_spread(all_hbm, fin, spread, done, first_sem):
        threads = []
        for k in range(spread):
            along_x = k % 2 == 0
            (a_plus, a_minus, a, a_up, a_down, a_far), (b_plus, b_minus, b, b_up, b_down, b_far) = [
                (('right', to_right), ('left', to_left), x, xr, xl, xo), (('up', to_up), ('down', to_down), y, yu, yd, yo)
            ][::1 if along_x else -1]

            def place(core, b_pos, a_pos, part_rows=None, k=k, along_x=along_x):
                spot = (k, core, b_pos, a_pos) if along_x else (k, core, a_pos, b_pos)
                return all_hbm.at[spot + (() if part_rows is None else (pl.ds(*part_rows),))]

            def bundle(core, b_pos, first=0, count=RING, k=k, along_x=along_x):
                return all_hbm.at[(k, core, b_pos, pl.ds(first, count)) if along_x else (k, core, pl.ds(first, count), b_pos)]

            source = fin.at[pl.ds(k * r, r)]
            keep = pltpu.make_async_copy(source, place(c, b, a), loc_sem.at[first_sem + k])
            top, low = (0, h), (h, h)
            a0 = transfer(*a_plus, source, place(c, b, a), source, place(c, b, a_down))
            a1 = transfer(*a_minus, source, place(c, b, a), source, place(c, b, a_up))
            h0 = moved(*a_plus, place(c, b, a_down, top), place(c, b, a_far, top))
            h1 = moved(*a_minus, place(c, b, a_up, low), place(c, b, a_far, low))
            b0 = moved(*b_plus, bundle(c, b, 0, 2), bundle(c, b_down, 0, 2))
            b1 = moved(*b_minus, bundle(c, b, 2, 2), bundle(c, b_up, 2, 2))
            b2 = moved(*b_plus, bundle(c, b, 2, 2), bundle(c, b_down, 2, 2))
            b3 = moved(*b_minus, bundle(c, b, 0, 2), bundle(c, b_up, 0, 2))
            g0 = moved(*b_plus, bundle(c, b_down, 0, 2), bundle(c, b_far, 0, 2))
            g1 = moved(*b_minus, bundle(c, b_up, 2, 2), bundle(c, b_far, 2, 2))
            cores = [moved('core', to_partner, bundle(c, pos), bundle(other, pos)) for pos in (b, b_down, b_up, b_far)]
            threads.append([
                Step((), keep.start, [a0, a1], (done[k],), 0.1, True),
                Step([a0], None, [h0], bulk=True), Step([a1], None, [h1], bulk=True),
                Step([h0, h1], keep.wait, [b0, b1, b2, b3, cores[0]], cost=0.1, bulk=True),
                Step([b0], None, [g0], bulk=True), Step([b1], None, [g1], bulk=True),
                Step([b2], None, [cores[1]]), Step([b3], None, [cores[2]]),
                Step([g0, g1], None, [cores[3]]), Step(cores)])
        return threads

    forward, done_f, sums_f = add_pass(False, gath_f, wb_f, ring_f, fin_f, spreads[0], None)
    backward, done_b, _ = add_pass(True, gath_b, wb_b, ring_b, fin_b, spreads[1], (done_f, sums_f))
    spread_f = add_spread(out_all, fin_f, spreads[0], done_f, keep_sem)
    spread_b = add_spread(grad_all, fin_b, spreads[1], done_b, keep_sem + spreads[0])
    for step in in_order(forward + kv_threads + backward + spread_f + spread_b):
        for copy in step.waits:
            copy.incoming().wait_recv()
        if step.work is not None:
            step.work()
        for copy in step.sends:
            copy.outgoing().start()

    kv_copies = [pltpu.make_async_copy(gath_b.at[CORES * (2 * (x // 2) + d % 2) + d // 2, pl.ds(RING, 2)],
                                       kv_out.at[:, d], loc_sem.at[d]) for d in range(RING)]
    for copy in kv_copies:
        copy.start()
    for copy in kv_copies:
        copy.wait()
    gone([copy for copy in transfers if not copy.left])


def exchange(heads, grad_q, kv, w_blocks, w_key, w_value, x_rows, dout_rows, inv, gain_block, spread=None):
    tokens, d_model = x_rows.shape
    rows_y, width = tokens // RING, d_model // ROW_DEVICES
    chunks = CHUNKS
    spreads = (chunks, SPREAD if spread is None else spread)
    r = rows_y // chunks
    any_spec = pl.BlockSpec(memory_space=pl.ANY)
    vmem_spec = pl.BlockSpec(memory_space=pltpu.VMEM)
    depth, n_kv = ROW_DEVICES * HEAD_DIM, 2 * w_key.shape[1] // RING
    f32, bf16 = jnp.float32, jnp.bfloat16

    def gathered(count):
        return jax.ShapeDtypeStruct((count, CORES, RING, RING, r, width), f32)

    passes = chunks * (8 + 2 * (RING - 1))
    copies = 2 * passes + chunks * (2 + ROW_DEVICES - 1) + 14 * sum(spreads)
    dma = pltpu.SemaphoreType.DMA
    sums = pltpu.VMEM((2, RING - 1, chunks, r // 2, width), f32)
    return pl.pallas_call(
        functools.partial(exchange_kernel, chunks, spreads),
        out_shape=[jax.ShapeDtypeStruct(((chunks - spreads[1]) * r + 8, width), f32), gathered(spreads[0]), gathered(spreads[1]),
                   jax.ShapeDtypeStruct((2, RING, rows_y, HEAD_DIM), f32)],
        in_specs=[any_spec] * 9 + [vmem_spec],
        out_specs=[vmem_spec, any_spec, any_spec, any_spec],
        scratch_shapes=[
            pltpu.VMEM((ROW_DEVICES, RING, rows_y, HEAD_DIM), f32),
            pltpu.VMEM((ROW_DEVICES, RING + 2, rows_y, HEAD_DIM), f32),
            pltpu.VMEM((depth, width), bf16), pltpu.VMEM((depth + n_kv, width), bf16),
            pltpu.VMEM((RING, rows_y, width), f32), sums, sums,
            pltpu.VMEM((spreads[0] * r, width), f32), pltpu.VMEM((spreads[1] * r, width), f32),
            pltpu.VMEM((rows_y, width), bf16), pltpu.VMEM((rows_y, width), bf16), pltpu.VMEM((rows_y, 1), f32),
            pltpu.VMEM((RING, 2, rows_y, HEAD_DIM), f32), pltpu.VMEM((CORES, 2, rows_y, HEAD_DIM), f32),
            pltpu.VMEM((2, rows_y, HEAD_DIM), f32), pltpu.VMEM((2, rows_y, HEAD_DIM), f32),
            pltpu.VMEM((chunks, 8, 128), f32), pltpu.VMEM((ROW_DEVICES - 1, chunks, 8, 128), f32),
            pltpu.VMEM((2, width, n_kv // 2), bf16),
            dma((copies,)), dma((copies,)), dma((2 * ROW_DEVICES + 9 + sum(spreads),))],
        compiler_params=pltpu.CompilerParams(collective_id=1, has_side_effects=True, vmem_limit_bytes=VMEM_BYTES),
        cost_estimate=pl.CostEstimate(flops=2 * tokens * (2 * depth + n_kv) * width, bytes_accessed=16 * tokens * width, transcendentals=0),
        name='exchange',
    )(heads, grad_q, kv, w_blocks, w_key, w_value, x_rows, dout_rows, inv, gain_block)


def rounded(kernel, gathered, grid, block, index_map, out_rows, place_of, rows, so_far):
    d_model = ROW_DEVICES * gathered.shape[-1]
    moved_rows = math.prod(grid) * out_rows
    return pl.pallas_call(
        kernel, grid=grid,
        in_specs=[pl.BlockSpec(block, index_map)] + ([pl.BlockSpec(memory_space=pl.ANY)] if so_far is not None else []),
        out_specs=pl.BlockSpec((out_rows, d_model), lambda *at: (place_of(*at), 0)),
        out_shape=jax.ShapeDtypeStruct((rows, d_model), jnp.bfloat16),
        input_output_aliases={1: 0} if so_far is not None else {},
        compiler_params=pltpu.CompilerParams(vmem_limit_bytes=VMEM_BYTES),
        cost_estimate=pl.CostEstimate(flops=moved_rows * d_model, bytes_accessed=6 * moved_rows * d_model, transcendentals=0),
        name='narrow',
    )(*((gathered,) if so_far is None else (gathered, so_far)))


def narrow_spread(gathered, spread, rows, so_far=None):
    r, width = gathered.shape[-2:]
    chunks = rows // RING // r
    group = max(n for n in range(1, 5) if math.gcd(spread, chunks) % n == 0)

    def kernel(in_ref, *rest):
        for k in range(group):
            for n in range(ROW_DEVICES):
                rest[-1][pl.ds(k * r, r), pl.ds(n * width, width)] = in_ref[k, n % CORES, 0, n // CORES].astype(jnp.bfloat16)

    return rounded(kernel, gathered, (spread // group, RING), (group, CORES, 1, RING, r, width), lambda k, y: (k, 0, y, 0, 0, 0),
                   group * r, lambda k, y: y * chunks // group + k, rows, so_far)


def narrow_rest(gathered, pad, spread, r, rows, so_far=None):
    width = gathered.shape[-1]
    chunks = rows // RING // r
    count = chunks - spread
    step = count if chunks % count == 0 and spread % count == 0 else 1
    assert step == count or pad == 0
    blocks = gathered.reshape(RING * ROW_DEVICES, count * r + pad, width)

    def kernel(in_ref, *rest):
        for n in range(ROW_DEVICES):
            rest[-1][:, pl.ds(n * width, width)] = in_ref[n, pl.ds(0, step * r), :].astype(jnp.bfloat16)

    return rounded(kernel, blocks, (RING, count // step), (ROW_DEVICES, step * r + pad, width), lambda y, j: (y, j, 0), step * r,
                   lambda y, j: (y * chunks + spread) // step + j, rows, so_far)


def solution(mesh):
    tp_size = mesh.shape['tp']
    row_groups = [list(range(first, first + ROW_DEVICES)) for first in range(0, tp_size, ROW_DEVICES)]

    def block_fn(hidden, grad_out, norm_gain, w_query, w_key, w_value, w_out):
        batch, seq_len, d_model = hidden.shape
        kv_heads = w_key.shape[1] // HEAD_DIM
        group_size = tp_size // kv_heads
        index = lax.axis_index('tp')
        column = index % ROW_DEVICES
        tokens, width = batch * seq_len, d_model // ROW_DEVICES
        rows_y = tokens // RING

        w_blocks = lax.all_to_all(column_blocks(w_out, w_query), 'tp', 0, 0, axis_index_groups=row_groups, tiled=True)
        kv_index = index // group_size
        cos_l, sin_l = rope_lanes(seq_len)
        gain_row = norm_gain.astype(jnp.float32).reshape(1, d_model)
        grad_rows = grad_out.reshape(tokens, d_model)

        normed, inv_rms, q_rot, k_rot, v_head, grad_heads = project(
            hidden.reshape(tokens, d_model), grad_rows, gain_row, kv_index.reshape(1), w_query, w_key, w_value, w_out, cos_l, sin_l)
        heads, heads_send, grad_q, grad_q_send, grad_kv_send = attend(q_rot, k_rot, v_head, grad_heads, cos_l, sin_l, seq_len)
        gain_block = lax.dynamic_slice(gain_row, (0, column * width), (1, width))
        by_rows = (RING, rows_y, HEAD_DIM)
        rest_block, out_spread, grad_spread, grad_kv = exchange(
            heads_send.reshape(by_rows), grad_q_send.reshape(by_rows), grad_kv_send.reshape((2,) + by_rows),
            w_blocks, w_key, w_value, hidden.reshape(tokens, d_model), grad_rows, inv_rms, gain_block)
        grad_rest = lax.all_gather(rest_block, 'tp', axis=0, tiled=True)
        r = rows_y // CHUNKS
        block_out = narrow_spread(out_spread, CHUNKS, tokens).reshape(hidden.shape)
        grad_hidden = narrow_rest(grad_rest, 8, SPREAD, r, tokens, narrow_spread(grad_spread, SPREAD, tokens)).reshape(hidden.shape)
        grad_gain = jnp.sum(grad_rest.reshape(RING, ROW_DEVICES, -1, width)[:, :, (CHUNKS - SPREAD) * r, :], axis=0).reshape(d_model)
        grad_w_query, grad_w_key, grad_w_value, grad_w_out = weight_grads(
            normed, grad_rows, grad_q, grad_kv.reshape(2, tokens, HEAD_DIM), heads)
        return block_out, grad_hidden, grad_gain, grad_w_query, grad_w_key, grad_w_value, grad_w_out

    act_spec = P('dp', None, None)
    return jax.shard_map(
        block_fn, mesh=mesh,
        in_specs=(act_spec, act_spec, P(None), P(None, 'tp'), P(None, None), P(None, None), P('tp', None)),
        out_specs=(act_spec, act_spec, P('dp'), P('dp', 'tp'), P('dp', 'tp'), P('dp', 'tp'), P(('dp', 'tp'), None)),
        check_vma=False)
```

```python
import functools
import math
import jax
import jax.numpy as jnp
from jax import lax
from jax.experimental import pallas as pl
from jax.experimental.pallas import tpu as pltpu
from jax.sharding import PartitionSpec as P

HEAD_DIM = 128
NORM_EPS = 1.0e-5
ROPE_BASE = 10000.0
MASK_VALUE = -1.0e30
SCORE_SCALE = 1.0 / math.sqrt(HEAD_DIM)
RING = 4
CORES = 2
ROW_DEVICES = RING * CORES
CHUNKS = 9
AHEAD = 2
SPREAD = 6
VMEM_BYTES = 62 * 1024 * 1024


def rope_lanes(seq_len):
    lane = lax.broadcasted_iota(jnp.int32, (1, HEAD_DIM), 1)
    inv_freq = ROPE_BASE ** (-(lane - lane % 2).astype(jnp.float32) / HEAD_DIM)
    angles = jnp.arange(seq_len, dtype=jnp.float32)[:, None] * inv_freq
    return jnp.cos(angles), jnp.where(lane % 2 == 0, -jnp.sin(angles), jnp.sin(angles))


def rotate(tensor, cos_l, sin_l):
    lane = lax.broadcasted_iota(jnp.int32, tensor.shape, 1)
    swapped = jnp.where(lane % 2 == 0, pltpu.roll(tensor, HEAD_DIM - 1, 1), pltpu.roll(tensor, 1, 1))
    return tensor * cos_l + swapped * sin_l


NT = (((1,), (1,)), ((), ()))
TN = (((0,), (0,)), ((), ()))


def softmax_rows(q, k):
    scores = lax.dot_general(q, k, NT, preferred_element_type=jnp.float32) * SCORE_SCALE
    row = lax.broadcasted_iota(jnp.int32, scores.shape, 0)
    col = lax.broadcasted_iota(jnp.int32, scores.shape, 1)
    scores = jnp.where(row >= col, scores, MASK_VALUE)
    weight = jnp.exp(scores - jnp.max(scores, axis=1, keepdims=True))
    return weight * (1.0 / jnp.sum(weight, axis=1, keepdims=True))


def attend(q, k, v, grad_heads, cos_l, sin_l, seq_len):
    def kernel(q_ref, k_ref, v_ref, do_ref, cos_ref, sin_ref, o_ref, o_send, dq_ref, dq_send, dkv_ref):
        q_rows, k_rows, v_rows, grad = q_ref[...], k_ref[...], v_ref[...], do_ref[...]
        probs = softmax_rows(q_rows, k_rows)
        probs_bf16 = probs.astype(jnp.bfloat16)
        heads = jnp.dot(probs_bf16, v_rows, preferred_element_type=jnp.float32).astype(jnp.bfloat16)
        o_ref[...] = heads
        o_send[...] = heads.astype(jnp.float32)
        grad_probs = lax.dot_general(grad, v_rows, NT, preferred_element_type=jnp.float32)
        dkv_ref[1] = lax.dot_general(probs_bf16, grad, TN, preferred_element_type=jnp.float32)
        row_dot = jnp.sum(probs * grad_probs, axis=1, keepdims=True)
        grad_scores = (probs * (grad_probs - row_dot) * SCORE_SCALE).astype(jnp.bfloat16)
        grad_q = jnp.dot(grad_scores, k_rows, preferred_element_type=jnp.float32)
        grad_k = lax.dot_general(grad_scores, q_rows, TN, preferred_element_type=jnp.float32)
        cos_t, sin_t = cos_ref[...], -sin_ref[...]
        grad_q = rotate(grad_q, cos_t, sin_t).astype(jnp.bfloat16)
        dq_ref[...] = grad_q
        dq_send[...] = grad_q.astype(jnp.float32)
        dkv_ref[0] = rotate(grad_k, cos_t, sin_t)

    spec = pl.BlockSpec((seq_len, HEAD_DIM), lambda b: (b, 0))
    table = pl.BlockSpec((seq_len, HEAD_DIM), lambda b: (0, 0))
    tokens = q.shape[0]
    rounded, wide = jax.ShapeDtypeStruct(q.shape, jnp.bfloat16), jax.ShapeDtypeStruct(q.shape, jnp.float32)
    return pl.pallas_call(
        kernel, grid=(tokens // seq_len,), in_specs=[spec] * 4 + [table] * 2,
        out_specs=(spec, spec, spec, spec, pl.BlockSpec((2, seq_len, HEAD_DIM), lambda b: (0, b, 0))),
        out_shape=(rounded, wide, rounded, wide, jax.ShapeDtypeStruct((2,) + q.shape, jnp.float32)),
        compiler_params=pltpu.CompilerParams(vmem_limit_bytes=VMEM_BYTES),
        cost_estimate=pl.CostEstimate(flops=14 * tokens * seq_len * HEAD_DIM, bytes_accessed=28 * tokens * HEAD_DIM,
                                      transcendentals=tokens * seq_len),
        name='attend',
    )(q, k, v, grad_heads, cos_l, sin_l)


def weight_grads(normed, grad_out, grad_q, grad_kv, heads):
    tokens, d_model = normed.shape
    columns = 512

    def kernel(n_ref, dout_ref, dq_ref, dkv_ref, o_ref, wq_ref, wk_ref, wv_ref, wo_ref, left_ref):
        @pl.when(pl.program_id(0) == 0)
        def _():
            pieces = (dq_ref[...].astype(jnp.float32), dkv_ref[0], dkv_ref[1], o_ref[...].astype(jnp.float32))
            for n, piece in enumerate(pieces):
                left_ref[pl.ds(n * HEAD_DIM, HEAD_DIM), :] = jnp.transpose(piece).astype(jnp.bfloat16)

        grads = jnp.dot(left_ref[pl.ds(0, 3 * HEAD_DIM), :], n_ref[...], preferred_element_type=jnp.float32)
        for n, ref in enumerate((wq_ref, wk_ref, wv_ref)):
            ref[...] = jnp.transpose(grads[n * HEAD_DIM:(n + 1) * HEAD_DIM])
        wo_ref[...] = jnp.dot(left_ref[pl.ds(3 * HEAD_DIM, HEAD_DIM), :], dout_ref[...], preferred_element_type=jnp.float32)

    wide = pl.BlockSpec((tokens, columns), lambda i: (0, i))
    tall = pl.BlockSpec((columns, HEAD_DIM), lambda i: (i, 0))
    head = pl.BlockSpec((tokens, HEAD_DIM), lambda i: (0, 0))
    tall_out = jax.ShapeDtypeStruct((d_model, HEAD_DIM), jnp.float32)
    return pl.pallas_call(
        kernel, grid=(d_model // columns,),
        in_specs=[wide, wide, head, pl.BlockSpec((2, tokens, HEAD_DIM), lambda i: (0, 0, 0)), head],
        out_specs=(tall, tall, tall, pl.BlockSpec((HEAD_DIM, columns), lambda i: (0, i))),
        out_shape=(tall_out, tall_out, tall_out, jax.ShapeDtypeStruct((HEAD_DIM, d_model), jnp.float32)),
        scratch_shapes=[pltpu.VMEM((4 * HEAD_DIM, tokens), jnp.bfloat16)],
        compiler_params=pltpu.CompilerParams(vmem_limit_bytes=VMEM_BYTES),
        cost_estimate=pl.CostEstimate(flops=8 * tokens * d_model * HEAD_DIM, bytes_accessed=4 * tokens * d_model, transcendentals=0),
        name='weight_grads',
    )(normed, grad_out, grad_q, grad_kv, heads)


class Place:
    def __init__(self):
        index = lax.axis_index('tp')
        self.c = lax.rem(index, CORES)
        self.x = lax.rem(index // CORES, RING)
        self.y = index // ROW_DEVICES

    def at(self, y, x, c):
        return {'tp': (y * RING + x) * CORES + c}


def turn(position, by):
    return lax.rem(position + (by % RING), RING)


def project(hidden, grad_out, gain, w_query, w_key, w_value, w_out, cos_l, sin_l):
    tokens, d_model = hidden.shape
    seq_len = cos_l.shape[0]
    rows = 384
    steps = tokens // rows
    width = d_model // ROW_DEVICES
    sharers = RING * ROW_DEVICES // (w_key.shape[1] // HEAD_DIM)

    def kernel(x_ref, dout_ref, gain_ref, cos_ref, sin_ref, wq_hbm, wk_hbm, wv_hbm, wo_hbm,
               normed_ref, inv_ref, q_ref, k_ref, v_ref, do_ref, got_hbm, w_ref, wo_ref, blocks, loc_sem, send_sem, recv_sem):
        me = Place()
        others = [(by, flip) for by in (1, 2, 3) for flip in (0, 1)] + [(0, 1)]

        def exchanges(which):
            here = me.x if which == 0 else me.y
            for n, (by, flip) in enumerate(others):
                core = 1 - me.c if flip else me.c
                there, origin = turn(here, by), turn(here, -by)
                peer = me.at(me.y, there, core) if which == 0 else me.at(there, me.x, core)

                def copy(dst, which=which, n=n, peer=peer, src=CORES * there + core):
                    return pltpu.make_async_remote_copy(
                        src_ref=blocks.at[which, src], dst_ref=got_hbm.at[which, dst], send_sem=send_sem.at[which, n],
                        recv_sem=recv_sem.at[which, n], device_id=peer, device_id_type=pl.DeviceIdType.MESH)
                yield copy(CORES * here + me.c), copy(CORES * origin + core)

        def kept(which):
            own = CORES * (me.x if which == 0 else me.y) + me.c
            return pltpu.make_async_copy(blocks.at[which, own], got_hbm.at[which, own], loc_sem.at[which])

        @pl.when(pl.program_id(0) == 0)
        def _():
            barrier = pltpu.get_barrier_semaphore()
            peers = [me.at(me.y, turn(me.x, by), 1 - me.c if flip else me.c) for by, flip in others]
            peers += [me.at(turn(me.y, by), me.x, 1 - me.c if flip else me.c) for by, flip in others[:-1]]
            for peer in peers:
                pl.semaphore_signal(barrier, inc=1, device_id=peer, device_id_type=pl.DeviceIdType.MESH)
            head = lax.axis_index('tp') // sharers
            kv_columns = pl.ds(pl.multiple_of(head * HEAD_DIM, HEAD_DIM), HEAD_DIM)
            loads = [pltpu.make_async_copy(src, dst, loc_sem.at[n]) for n, (src, dst) in enumerate((
                (wo_hbm, wo_ref), (wq_hbm, w_ref.at[:, pl.ds(0, HEAD_DIM)]),
                (wk_hbm.at[:, kv_columns], w_ref.at[:, pl.ds(HEAD_DIM, HEAD_DIM)]),
                (wv_hbm.at[:, kv_columns], w_ref.at[:, pl.ds(2 * HEAD_DIM, HEAD_DIM)])))]
            for load in loads:
                load.start()
            for load in loads:
                load.wait()
            for j in range(ROW_DEVICES):
                columns = pl.ds(j * width, width)
                blocks[0, j] = wo_ref[:, columns].astype(jnp.float32)
                blocks[1, j] = jnp.transpose(w_ref[columns, pl.ds(0, HEAD_DIM)].astype(jnp.float32))
            pl.semaphore_wait(barrier, len(peers))
            for which in (0, 1):
                for out, _ in exchanges(which):
                    out.start()
                kept(which).start()

        values = x_ref[...].astype(jnp.float32)
        inv = lax.rsqrt(jnp.mean(values * values, axis=1, keepdims=True) + NORM_EPS)
        inv_ref[...] = inv
        normed = (values * inv * gain_ref[...]).astype(jnp.bfloat16)
        normed_ref[...] = normed
        heads = jnp.dot(normed, w_ref[...], preferred_element_type=jnp.float32)
        q_ref[...] = rotate(heads[:, :HEAD_DIM], cos_ref[...], sin_ref[...]).astype(jnp.bfloat16)
        k_ref[...] = rotate(heads[:, HEAD_DIM:2 * HEAD_DIM], cos_ref[...], sin_ref[...]).astype(jnp.bfloat16)
        v_ref[...] = heads[:, 2 * HEAD_DIM:].astype(jnp.bfloat16)
        do_ref[...] = lax.dot_general(dout_ref[...], wo_ref[...], NT, preferred_element_type=jnp.float32).astype(jnp.bfloat16)

        @pl.when(pl.program_id(0) == steps - 1)
        def _():
            for which in (0, 1):
                for out, came in exchanges(which):
                    came.wait_recv()
                    out.wait_send()
                kept(which).wait()

    row_spec = pl.BlockSpec((rows, d_model), lambda i: (i, 0))
    head_spec = pl.BlockSpec((rows, HEAD_DIM), lambda i: (i, 0))
    table_spec = pl.BlockSpec((rows, HEAD_DIM), lambda i: (i % (seq_len // rows), 0))
    any_spec = pl.BlockSpec(memory_space=pl.ANY)
    head = jax.ShapeDtypeStruct((tokens, HEAD_DIM), jnp.bfloat16)
    blocks = (2, ROW_DEVICES, HEAD_DIM, width)
    dma = pltpu.SemaphoreType.DMA
    return pl.pallas_call(
        kernel, grid=(steps,),
        in_specs=[row_spec, row_spec, pl.BlockSpec((1, d_model), lambda i: (0, 0)), table_spec, table_spec] + [any_spec] * 4,
        out_specs=(row_spec, pl.BlockSpec((rows, 1), lambda i: (i, 0)), head_spec, head_spec, head_spec, head_spec, any_spec),
        out_shape=(jax.ShapeDtypeStruct((tokens, d_model), jnp.bfloat16), jax.ShapeDtypeStruct((tokens, 1), jnp.float32),
                   head, head, head, head, jax.ShapeDtypeStruct(blocks, jnp.float32)),
        scratch_shapes=[pltpu.VMEM((d_model, 3 * HEAD_DIM), jnp.bfloat16), pltpu.VMEM((HEAD_DIM, d_model), jnp.bfloat16),
                        pltpu.VMEM(blocks, jnp.float32), dma((4,)), dma((2, 7)), dma((2, 7))],
        compiler_params=pltpu.CompilerParams(collective_id=2, has_side_effects=True, vmem_limit_bytes=VMEM_BYTES),
        cost_estimate=pl.CostEstimate(flops=8 * tokens * d_model * HEAD_DIM, bytes_accessed=6 * tokens * d_model, transcendentals=0),
        name='project',
    )(hidden, grad_out, gain, cos_l, sin_l, w_query, w_key, w_value, w_out)


class Transfer:
    def __init__(self, link, size, outgoing, incoming=None):
        self.link, self.size, self.outgoing, self.incoming = link, size, outgoing, incoming or outgoing
        self.left = False


class Step:
    def __init__(self, waits=(), work=None, sends=(), after=(), cost=0.05, bulk=False):
        self.waits, self.work, self.sends, self.after, self.cost, self.bulk = waits, work, sends, after, cost, bulk


LINK_RATE = 46.6e3
CORE_RATE = 200e3
HOP = 2.0
CORE_HOP = 1.5
QUEUE = 8.0


def in_order(threads):
    now, busy, arrival, finished, order = 4.0, {}, {}, set(), []
    position = [0] * len(threads)
    while any(position[i] < len(threads[i]) for i in range(len(threads))):
        chosen, soonest = None, math.inf
        for i, steps in enumerate(threads):
            if position[i] == len(steps) or any(step not in finished for step in steps[position[i]].after):
                continue
            step = steps[position[i]]
            ready = max([arrival.get(copy, math.inf) for copy in step.waits], default=0.0)
            if step.bulk:
                ready = max([ready] + [busy.get(copy.link, 0.0) - QUEUE for copy in step.sends if copy.link != 'core'])
            if ready <= now:
                chosen = i
                break
            soonest = min(soonest, ready)
        if chosen is None:
            now = soonest
            continue
        step = threads[chosen][position[chosen]]
        position[chosen] += 1
        now += step.cost
        for copy in step.sends:
            rate, hop = (CORE_RATE, CORE_HOP) if copy.link == 'core' else (LINK_RATE, HOP)
            busy[copy.link] = max(now, busy.get(copy.link, 0.0)) + copy.size / rate
            arrival[copy] = busy[copy.link] + hop
        finished.add(step)
        order.append(step)
    return order


def exchange_kernel(chunks, spreads, *refs):
    (heads_hbm, grad_q_hbm, kv_hbm, w_hbm, w_key_hbm, w_value_hbm, x_hbm, dout_hbm, inv_hbm, gain_ref,
     rest_ref, out_all, grad_all, kv_out,
     gath_f, gath_b, wb_f, wb_b, part, ring_f, ring_b, fin_f, fin_b, x_ref, dout_ref, inv_ref,
     kvp, kv_core, kv_send, kv_chip, kv_far, rowpart, rowall, w_kv, send_sem, recv_sem, loc_sem) = refs
    me = Place()
    x, y, c = me.x, me.y, me.c
    xr, xl, xo = turn(x, 1), turn(x, -1), turn(x, 2)
    yu, yd, yo = turn(y, 1), turn(y, -1), turn(y, 2)
    other = 1 - c
    rows_y, width = x_ref.shape[1:]
    r = rows_y // chunks
    h = r // 2
    to_right, to_left, to_partner = me.at(y, xr, c), me.at(y, xl, c), me.at(y, x, other)
    to_up, to_down = me.at(yu, x, c), me.at(yd, x, c)
    along_x = (('right', to_right), ('left', to_left), x, xr, xl, xo)
    along_y = (('up', to_up), ('down', to_down), y, yu, yd, yo)

    barrier = pltpu.get_barrier_semaphore()
    peers = [to_up, to_down, to_right, to_left, to_partner,
             me.at(yo, x, c), me.at(yu, x, other), me.at(yd, x, other), me.at(yo, x, other)]
    for peer in peers:
        pl.semaphore_signal(barrier, inc=1, device_id=peer, device_id_type=pl.DeviceIdType.MESH)

    depth = ROW_DEVICES * HEAD_DIM
    own_f, own_b = CORES * x + c, CORES * y + c

    def rows_at(position):
        return pl.ds(pl.multiple_of(position * rows_y, rows_y), rows_y)

    def columns_at(block):
        return pl.ds(pl.multiple_of(block * width, width), width)

    def head_at(head):
        return pl.ds(pl.multiple_of(head * HEAD_DIM, HEAD_DIM), HEAD_DIM)

    per_slot = rows_y // HEAD_DIM

    def stage(which, j):
        return part.at[2 * which + j // per_slot, pl.ds(j % per_slot * HEAD_DIM, HEAD_DIM)]

    copies = [(w_hbm.at[which, j], stage(which, j)) for which in (0, 1) for j in range(ROW_DEVICES)]
    copies += [(w.at[columns_at(own_b), head_at(2 * j + x // 2)], w_kv.at[s, j])
               for s, w in enumerate((w_key_hbm, w_value_hbm)) for j in range(RING)]
    copies += [
        (heads_hbm, gath_f.at[own_f, pl.ds(0, RING)]), (grad_q_hbm, gath_b.at[own_b, pl.ds(0, RING)]),
        (kv_hbm.at[0], kvp.at[:, 0]), (kv_hbm.at[1], kvp.at[:, 1]),
        (x_hbm.at[rows_at(y), columns_at(own_f)], x_ref.at[0]), (x_hbm.at[rows_at(x), columns_at(own_b)], x_ref.at[1]),
        (dout_hbm.at[rows_at(x), columns_at(own_b)], dout_ref), (inv_hbm.at[rows_at(x)], inv_ref)]
    loads = [pltpu.make_async_copy(src, dst, loc_sem.at[n]) for n, (src, dst) in enumerate(copies)]
    keep_sem = len(loads)
    for copy in loads:
        copy.start()
    first_rest = (chunks - spreads[1]) * r
    rest_ref[pl.ds(first_rest, 8), :] = jnp.zeros((8, width), jnp.float32)
    for copy in loads:
        copy.wait()
    for which, weights in enumerate((wb_f, wb_b)):
        for j in range(ROW_DEVICES):
            weights[pl.ds(j * HEAD_DIM, HEAD_DIM), :] = stage(which, j)[...].astype(jnp.bfloat16)
    for j in range(RING):
        for s in (0, 1):
            weights = jnp.transpose(w_kv[s, j].astype(jnp.float32)).astype(jnp.bfloat16)
            wb_b[pl.ds(depth + (2 * j + s) * HEAD_DIM, HEAD_DIM), :] = weights
    pl.semaphore_wait(barrier, len(peers))

    transfers = []

    def transfer(link, peer, src, dst, came_from=None, came_to=None):
        n = len(transfers)

        def copy(a, b):
            return lambda: pltpu.make_async_remote_copy(
                src_ref=a, dst_ref=b, send_sem=send_sem.at[n], recv_sem=recv_sem.at[n], device_id=peer,
                device_id_type=pl.DeviceIdType.MESH)
        made = Transfer(link, 4 * math.prod(dst.shape), copy(src, dst), copy(came_from, came_to) if came_to is not None else None)
        transfers.append(made)
        return made

    def moved(link, peer, sent, came):
        return transfer(link, peer, sent, sent, came, came)

    def gone(sent):
        for copy in sent:
            copy.outgoing().wait_send()
            copy.left = True

    p = lax.rem(x, 2)
    xn = x + 1 - 2 * p
    mine, theirs = CORES * c + p, CORES * c + 1 - p
    kv_threads, settle, settled = [], [], []
    for k in range(chunks):
        rows = pl.ds(k * r, r)
        core_copy = transfer('core', to_partner, kvp.at[pl.ds(CORES * other, CORES), :, rows], kv_core.at[:, :, rows])
        chip_copy = transfer('right', me.at(y, xn, c), kv_send.at[:, rows], kv_chip.at[:, rows])

        def add_core(rows=rows):
            kv_send[:, rows, :] = kvp[theirs, :, rows, :] + kv_core[1 - p, :, rows, :]

        def add_chip(rows=rows):
            total = kvp[mine, :, rows, :] + kv_core[p, :, rows, :] + kv_chip[:, rows, :]
            gath_b[own_b, pl.ds(RING, 2), rows, :] = total.astype(jnp.bfloat16).astype(jnp.float32)

        kv_threads.append([Step(sends=[core_copy]), Step([core_copy], add_core, [chip_copy], cost=0.1)])
        settle.append(add_chip)
        settled.append(chip_copy)

    def add_pass(backward, gath, wb, ring, fin, spread, ahead_of):
        gather_ring, sum_ring = (along_y, along_x) if backward else (along_x, along_y)
        g_plus, g_minus, g, g_up, g_down, g_far = gather_ring
        s_plus, s_minus, s, s_up, s_down, s_far = sum_ring
        own, left, right, far = [CORES * pos + c for pos in (g, g_down, g_up, g_far)]
        p_own, p_left, p_right, p_far = [CORES * pos + other for pos in (g, g_down, g_up, g_far)]
        parts = gath.shape[1]
        half = parts // 2
        threads, passed, done, ring_sums, begun = [], [], [], [], []
        x_block = x_ref.at[1 if backward else 0]

        def multiply(by, k, before=()):
            gone(before)
            d = turn(s, by)
            rows = pl.ds(k * r, r)
            pieces = [gath[j, d, rows, :] for j in range(ROW_DEVICES)]
            if backward and by % 2 == 0:
                pieces += [gath[CORES * j + d // 2, RING + n, rows, :] for j in range(RING) for n in (0, 1)]
            lhs = jnp.concatenate([piece.astype(jnp.bfloat16) for piece in pieces], axis=1)
            part[d, rows, :] = jnp.dot(lhs, wb[pl.ds(0, lhs.shape[1]), :], preferred_element_type=jnp.float32)

        def add_ring(way, step, k):
            d = turn(s, -(2 + step) if way == 0 else 2 + step)
            part[d, pl.ds(k * r + way * h, h), :] += ring[way, step, k]

        def store(k, values):
            if k < spread:
                fin[pl.ds(k * r, r), :] = values
            else:
                rest_ref[pl.ds((k - spread) * r, r), :] = values

        def finish_forward(k):
            rows = pl.ds(k * r, r)
            store(k, (x_block[rows, :].astype(jnp.float32) + part[s, rows, :]).astype(jnp.bfloat16).astype(jnp.float32))

        def row_sums(k):
            rows = pl.ds(k * r, r)
            total = part[s, rows, :]
            unit = x_block[rows, :].astype(jnp.float32) * inv_ref[rows, :]
            row_sum = jnp.sum(total * gain_ref[...] * unit, axis=1, keepdims=True)
            square = jnp.concatenate([jnp.broadcast_to(row_sum, (r, 128)), jnp.zeros((128 - r, 128), jnp.float32)], axis=0)
            rowpart[k] = jnp.transpose(square)[0:8, :]
            gain_row = jnp.sum(total * unit, axis=0, keepdims=True)
            row_id = lax.broadcasted_iota(jnp.int32, (8, width), 0)
            rest_ref[pl.ds(first_rest, 8), :] += jnp.where(row_id == 0, jnp.broadcast_to(gain_row, (8, width)), 0.0)

        def finish_backward(k):
            rows = pl.ds(k * r, r)
            sums = rowpart[k]
            for m in range(ROW_DEVICES - 1):
                sums = sums + rowall[m, k]
            mean = jnp.transpose(sums)[0:r, 0:1] * (1.0 / (width * ROW_DEVICES))
            inv = inv_ref[rows, :]
            unit = x_block[rows, :].astype(jnp.float32) * inv
            delta = inv * (part[s, rows, :] * gain_ref[...] - unit * mean)
            store(k, (dout_ref[rows, :].astype(jnp.float32) + delta).astype(jnp.bfloat16).astype(jnp.float32))

        for k in range(chunks):
            rows = pl.ds(k * r, r)

            def block(source, first=0, count=parts, rows=rows):
                return gath.at[source, pl.ds(first, count), rows]

            s_right = moved(*g_plus, block(own), block(left))
            s_left = moved(*g_minus, block(own), block(right))
            s_core = moved('core', to_partner, block(own), block(p_own))
            f_right = moved(*g_plus, block(left, 0, half), block(far, 0, half))
            f_left = moved(*g_minus, block(right, half, parts - half), block(far, half, parts - half))
            c_left = moved('core', to_partner, block(left), block(p_left))
            c_right = moved('core', to_partner, block(right), block(p_right))
            c_far = moved('core', to_partner, block(far), block(p_far))
            sums = [[transfer(link, peer, part.at[turn(s, -(1 + step) if way == 0 else 1 + step), pl.ds(k * r + way * h, h)],
                              ring.at[way, step, k]) for step in range(RING - 1)]
                    for way, (link, peer) in enumerate((s_plus, s_minus))]
            ring_sums.append(sums[0] + sums[1])
            after = [passed[k - AHEAD]] if k >= AHEAD else []
            before = ()
            if ahead_of is not None:
                after.append(ahead_of[0][k])
                before = ahead_of[1][k]
            steps = [Step([settled[k]] if backward else (), settle[k] if backward else None, [s_right, s_left, s_core], after, 0.1),
                     Step([s_right], None, [f_right, c_left]), Step([s_left], None, [f_left, c_right])]
            begun.append(steps[0])
            passed.append(steps[-1])
            cost = 0.6 * r / 96
            even = 2 * cost if backward else cost
            steps += [Step([f_right, f_left], None, [c_far]),
                      Step([s_core, c_left, c_right, c_far], functools.partial(multiply, -1, k, before), [sums[0][0]], cost=cost),
                      Step((), functools.partial(multiply, 1, k), [sums[1][0]], cost=cost),
                      Step((), functools.partial(multiply, 2, k), cost=even),
                      Step((), functools.partial(multiply, 0, k), cost=even)]
            for step in range(RING - 1):
                for way in (0, 1):
                    steps.append(Step([sums[way][step]], functools.partial(add_ring, way, step, k),
                                      [sums[way][step + 1]] if step < RING - 2 else [], cost=0.15))
            if backward:
                members = [(pos, core) for pos in (yu, yd, yo) for core in (c, other)] + [(y, other)]
                notes = [transfer('note', me.at(pos, x, core), rowpart.at[k], rowall.at[m, k])
                         for (pos, core), m in zip(members, (2, 3, 0, 1, 4, 5, 6))]
                steps.append(Step((), functools.partial(row_sums, k), notes, cost=0.4))
                steps.append(Step(notes, functools.partial(finish_backward, k), cost=0.5))
            else:
                steps.append(Step((), functools.partial(finish_forward, k), cost=0.3))
            done.append(steps[-1])
            threads.append(steps)
        return threads, done, ring_sums, begun

    def add_spread(all_hbm, fin, spread, done, first_sem, odd):
        threads = []
        for k in range(spread):
            x_first = k % 2 == odd
            ((a_plus, a_minus, a, a_up, a_down, a_far),
             (b_plus, b_minus, b, b_up, b_down, b_far)) = (along_x, along_y) if x_first else (along_y, along_x)

            def place(core, b_pos, a_pos, part_rows=None, k=k, x_first=x_first):
                spot = (k, core, b_pos, a_pos) if x_first else (k, core, a_pos, b_pos)
                return all_hbm.at[spot + (() if part_rows is None else (pl.ds(*part_rows),))]

            def bundle(core, b_pos, first=0, count=RING, k=k, x_first=x_first):
                return all_hbm.at[(k, core, b_pos, pl.ds(first, count)) if x_first else (k, core, pl.ds(first, count), b_pos)]

            source = fin.at[pl.ds(k * r, r)]
            keep = pltpu.make_async_copy(source, place(c, b, a), loc_sem.at[first_sem + k])
            top, low = (0, h), (h, h)
            a0 = transfer(*a_plus, source, place(c, b, a), source, place(c, b, a_down))
            a1 = transfer(*a_minus, source, place(c, b, a), source, place(c, b, a_up))
            h0 = moved(*a_plus, place(c, b, a_down, top), place(c, b, a_far, top))
            h1 = moved(*a_minus, place(c, b, a_up, low), place(c, b, a_far, low))
            b0 = moved(*b_plus, bundle(c, b, 0, 2), bundle(c, b_down, 0, 2))
            b1 = moved(*b_minus, bundle(c, b, 2, 2), bundle(c, b_up, 2, 2))
            b2 = moved(*b_plus, bundle(c, b, 2, 2), bundle(c, b_down, 2, 2))
            b3 = moved(*b_minus, bundle(c, b, 0, 2), bundle(c, b_up, 0, 2))
            g0 = moved(*b_plus, bundle(c, b_down, 0, 2), bundle(c, b_far, 0, 2))
            g1 = moved(*b_minus, bundle(c, b_up, 2, 2), bundle(c, b_far, 2, 2))
            cores = [moved('core', to_partner, bundle(c, pos), bundle(other, pos)) for pos in (b, b_down, b_up, b_far)]
            threads.append([
                Step((), keep.start, [a0, a1], (done[k],), 0.1, True),
                Step([a0], None, [h0], bulk=True), Step([a1], None, [h1], bulk=True),
                Step([h0, h1], keep.wait, [b0, b1, b2, b3, cores[0]], cost=0.1, bulk=True),
                Step([b0], None, [g0], bulk=True), Step([b1], None, [g1], bulk=True),
                Step([b2], None, [cores[1]]), Step([b3], None, [cores[2]]),
                Step([g0, g1], None, [cores[3]]), Step(cores)])
        return threads

    forward, done_f, sums_f, _ = add_pass(False, gath_f, wb_f, ring_f, fin_f, spreads[0], None)
    backward, done_b, _, begun = add_pass(True, gath_b, wb_b, ring_b, fin_b, spreads[1], (done_f, sums_f))
    spread_f = add_spread(out_all, fin_f, spreads[0], done_f, keep_sem, 1)
    spread_b = add_spread(grad_all, fin_b, spreads[1], done_b, keep_sem + spreads[0], 0)
    swap = transfer('right', me.at(y, xn, c), gath_b.at[own_b, pl.ds(RING, 2)], kv_far.at[c])
    swap_core = moved('core', to_partner, kv_far.at[c], kv_far.at[other])
    swaps = [[Step((), None, [swap], begun, bulk=True), Step([swap], None, [swap_core]), Step([swap_core])]]
    for step in in_order(forward + kv_threads + backward + spread_f + swaps + spread_b):
        for copy in step.waits:
            copy.incoming().wait_recv()
        if step.work is not None:
            step.work()
        for copy in step.sends:
            copy.outgoing().start()

    kv_copies = []
    for core in range(CORES):
        for src, place in ((gath_b.at[CORES * y + core, pl.ds(RING, 2)], CORES * core + p), (kv_far.at[core], CORES * core + 1 - p)):
            kv_copies.append(pltpu.make_async_copy(src, kv_out.at[:, place], loc_sem.at[len(kv_copies)]))
    for copy in kv_copies:
        copy.start()
    for copy in kv_copies:
        copy.wait()
    gone([copy for copy in transfers if not copy.left])


def exchange(heads, grad_q, kv, w_blocks, w_key, w_value, x_rows, dout_rows, inv, gain_block, spread=None):
    tokens, d_model = x_rows.shape
    rows_y, width = tokens // RING, d_model // ROW_DEVICES
    chunks = CHUNKS
    spreads = (chunks, SPREAD if spread is None else spread)
    r = rows_y // chunks
    any_spec = pl.BlockSpec(memory_space=pl.ANY)
    vmem_spec = pl.BlockSpec(memory_space=pltpu.VMEM)
    depth, n_kv = ROW_DEVICES * HEAD_DIM, w_key.shape[1]
    f32, bf16 = jnp.float32, jnp.bfloat16

    def gathered(count):
        return jax.ShapeDtypeStruct((count, CORES, RING, RING, r, width), f32)

    passes = chunks * (8 + 2 * (RING - 1))
    copies = 2 * passes + chunks * (2 + ROW_DEVICES - 1) + 14 * sum(spreads) + 2
    dma = pltpu.SemaphoreType.DMA
    sums = pltpu.VMEM((2, RING - 1, chunks, r // 2, width), f32)
    return pl.pallas_call(
        functools.partial(exchange_kernel, chunks, spreads),
        out_shape=[jax.ShapeDtypeStruct(((chunks - spreads[1]) * r + 8, width), f32), gathered(spreads[0]), gathered(spreads[1]),
                   jax.ShapeDtypeStruct((2, RING, rows_y, HEAD_DIM), f32)],
        in_specs=[any_spec] * 9 + [vmem_spec],
        out_specs=[vmem_spec, any_spec, any_spec, any_spec],
        scratch_shapes=[
            pltpu.VMEM((ROW_DEVICES, RING, rows_y, HEAD_DIM), f32),
            pltpu.VMEM((ROW_DEVICES, RING + 2, rows_y, HEAD_DIM), f32),
            pltpu.VMEM((depth, width), bf16), pltpu.VMEM((depth + n_kv, width), bf16),
            pltpu.VMEM((RING, rows_y, width), f32), sums, sums,
            pltpu.VMEM((spreads[0] * r, width), f32), pltpu.VMEM((spreads[1] * r, width), f32),
            pltpu.VMEM((2, rows_y, width), bf16), pltpu.VMEM((rows_y, width), bf16), pltpu.VMEM((rows_y, 1), f32),
            pltpu.VMEM((RING, 2, rows_y, HEAD_DIM), f32), pltpu.VMEM((CORES, 2, rows_y, HEAD_DIM), f32),
            pltpu.VMEM((2, rows_y, HEAD_DIM), f32), pltpu.VMEM((2, rows_y, HEAD_DIM), f32), pltpu.VMEM((CORES, 2, rows_y, HEAD_DIM), f32),
            pltpu.VMEM((chunks, 8, 128), f32), pltpu.VMEM((ROW_DEVICES - 1, chunks, 8, 128), f32),
            pltpu.VMEM((2, RING, width, HEAD_DIM), bf16),
            dma((copies,)), dma((copies,)), dma((3 * ROW_DEVICES + 8 + sum(spreads),))],
        compiler_params=pltpu.CompilerParams(collective_id=1, has_side_effects=True, vmem_limit_bytes=VMEM_BYTES),
        cost_estimate=pl.CostEstimate(flops=2 * tokens * (2 * depth + n_kv) * width, bytes_accessed=16 * tokens * width, transcendentals=0),
        name='exchange',
    )(heads, grad_q, kv, w_blocks, w_key, w_value, x_rows, dout_rows, inv, gain_block)


def rounded(kernel, gathered, grid, block, index_map, out_rows, place_of, rows, so_far):
    d_model = ROW_DEVICES * gathered.shape[-1]
    moved_rows = math.prod(grid) * out_rows
    return pl.pallas_call(
        kernel, grid=grid,
        in_specs=[pl.BlockSpec(block, index_map)] + ([pl.BlockSpec(memory_space=pl.ANY)] if so_far is not None else []),
        out_specs=pl.BlockSpec((out_rows, d_model), lambda *at: (place_of(*at), 0)),
        out_shape=jax.ShapeDtypeStruct((rows, d_model), jnp.bfloat16),
        input_output_aliases={1: 0} if so_far is not None else {},
        compiler_params=pltpu.CompilerParams(vmem_limit_bytes=VMEM_BYTES),
        cost_estimate=pl.CostEstimate(flops=moved_rows * d_model, bytes_accessed=6 * moved_rows * d_model, transcendentals=0),
        name='narrow',
    )(*((gathered,) if so_far is None else (gathered, so_far)))


def narrow_spread(gathered, spread, rows, by_y, so_far=None):
    r, width = gathered.shape[-2:]
    chunks = rows // RING // r
    group = max(n for n in range(1, 5) if math.gcd(spread, chunks) % n == 0)
    block = (group, CORES, 1, RING, r, width) if by_y else (group, CORES, RING, 1, r, width)

    def kernel(in_ref, *rest):
        for k in range(group):
            for n in range(ROW_DEVICES):
                at = (k, n % CORES) + ((0, n // CORES) if by_y else (n // CORES, 0))
                rest[-1][pl.ds(k * r, r), pl.ds(n * width, width)] = in_ref[at].astype(jnp.bfloat16)

    return rounded(kernel, gathered, (spread // group, RING), block,
                   lambda k, i: (k, 0, i, 0, 0, 0) if by_y else (k, 0, 0, i, 0, 0),
                   group * r, lambda k, i: i * chunks // group + k, rows, so_far)


def narrow_rest(gathered, pad, spread, r, rows, so_far):
    width = gathered.shape[-1]
    chunks = rows // RING // r
    count = chunks - spread
    blocks = gathered.reshape(RING, RING, CORES, count * r + pad, width)

    def kernel(in_ref, *rest):
        for n in range(ROW_DEVICES):
            rest[-1][:, pl.ds(n * width, width)] = in_ref[n // CORES, 0, n % CORES, pl.ds(0, count * r), :].astype(jnp.bfloat16)

    return rounded(kernel, blocks, (RING,), (RING, 1, CORES, count * r + pad, width), lambda x: (0, x, 0, 0, 0), count * r,
                   lambda x: (x * chunks + spread) // count, rows, so_far)


def solution(mesh):
    assert mesh.shape['tp'] == RING * RING * CORES

    def block_fn(hidden, grad_out, norm_gain, w_query, w_key, w_value, w_out):
        batch, seq_len, d_model = hidden.shape
        index = lax.axis_index('tp')
        column = index // ROW_DEVICES * CORES + index % CORES
        tokens, width = batch * seq_len, d_model // ROW_DEVICES
        rows_y = tokens // RING

        cos_l, sin_l = rope_lanes(seq_len)
        gain_row = norm_gain.astype(jnp.float32).reshape(1, d_model)
        grad_rows = grad_out.reshape(tokens, d_model)

        normed, inv_rms, q_rot, k_rot, v_head, grad_heads, w_blocks = project(
            hidden.reshape(tokens, d_model), grad_rows, gain_row, w_query, w_key, w_value, w_out, cos_l, sin_l)
        heads, heads_send, grad_q, grad_q_send, grad_kv_send = attend(q_rot, k_rot, v_head, grad_heads, cos_l, sin_l, seq_len)
        gain_block = lax.dynamic_slice(gain_row, (0, column * width), (1, width))
        by_rows = (RING, rows_y, HEAD_DIM)
        rest_block, out_spread, grad_spread, grad_kv = exchange(
            heads_send.reshape(by_rows), grad_q_send.reshape(by_rows), grad_kv_send.reshape((2,) + by_rows),
            w_blocks, w_key, w_value, hidden.reshape(tokens, d_model), grad_rows, inv_rms, gain_block)
        grad_rest = lax.all_gather(rest_block, 'tp', axis=0, tiled=True)
        r = rows_y // CHUNKS
        block_out = narrow_spread(out_spread, CHUNKS, tokens, True).reshape(hidden.shape)
        grad_hidden = narrow_rest(grad_rest, 8, SPREAD, r, tokens, narrow_spread(grad_spread, SPREAD, tokens, False)).reshape(hidden.shape)
        grad_gain = jnp.sum(grad_rest.reshape(RING, RING, CORES, -1, width)[:, :, :, (CHUNKS - SPREAD) * r, :], axis=1).reshape(d_model)
        grad_w_query, grad_w_key, grad_w_value, grad_w_out = weight_grads(
            normed, grad_rows, grad_q, grad_kv.reshape(2, tokens, HEAD_DIM), heads)
        return block_out, grad_hidden, grad_gain, grad_w_query, grad_w_key, grad_w_value, grad_w_out

    act_spec = P('dp', None, None)
    return jax.shard_map(
        block_fn, mesh=mesh,
        in_specs=(act_spec, act_spec, P(None), P(None, 'tp'), P(None, None), P(None, None), P('tp', None)),
        out_specs=(act_spec, act_spec, P('dp'), P('dp', 'tp'), P('dp', 'tp'), P('dp', 'tp'), P(('dp', 'tp'), None)),
        check_vma=False)
```

```python
import functools
import math
import jax
import jax.numpy as jnp
from jax import lax
from jax.experimental import pallas as pl
from jax.experimental.pallas import tpu as pltpu
from jax.sharding import PartitionSpec as P

HEAD_DIM = 128
NORM_EPS = 1.0e-5
ROPE_BASE = 10000.0
MASK_VALUE = -1.0e30
SCORE_SCALE = 1.0 / math.sqrt(HEAD_DIM)
RING = 4
CORES = 2
ROW_DEVICES = RING * CORES
CHUNKS = 9
AHEAD = 3
SPREAD = 6
X_FIRST = ((0, 0, 1, 1, 0, 1, 0, 1, 1), (1, 0, 1, 0, 0, 0))
LAG = 3
VMEM_BYTES = 62 * 1024 * 1024


def rope_lanes(seq_len):
    lane = lax.broadcasted_iota(jnp.int32, (1, HEAD_DIM), 1)
    inv_freq = ROPE_BASE ** (-(lane - lane % 2).astype(jnp.float32) / HEAD_DIM)
    angles = jnp.arange(seq_len, dtype=jnp.float32)[:, None] * inv_freq
    return jnp.cos(angles), jnp.where(lane % 2 == 0, -jnp.sin(angles), jnp.sin(angles))


def rotate(tensor, cos_l, sin_l):
    lane = lax.broadcasted_iota(jnp.int32, tensor.shape, 1)
    swapped = jnp.where(lane % 2 == 0, pltpu.roll(tensor, HEAD_DIM - 1, 1), pltpu.roll(tensor, 1, 1))
    return tensor * cos_l + swapped * sin_l


NT = (((1,), (1,)), ((), ()))
TN = (((0,), (0,)), ((), ()))


def softmax_rows(q, k, first):
    scores = lax.dot_general(q, k, NT, preferred_element_type=jnp.float32) * SCORE_SCALE
    row = lax.broadcasted_iota(jnp.int32, scores.shape, 0) + first
    col = lax.broadcasted_iota(jnp.int32, scores.shape, 1)
    scores = jnp.where(row >= col, scores, MASK_VALUE)
    weight = jnp.exp(scores - jnp.max(scores, axis=1, keepdims=True))
    return weight * (1.0 / jnp.sum(weight, axis=1, keepdims=True))


def attend(q, k, v, grad_heads, cos_l, sin_l, seq_len):
    def kernel(q_ref, k_ref, v_ref, do_ref, cos_ref, sin_ref, o_ref, o_send, dq_ref, dq_send, dkv_ref):
        rows = 256
        dk = [None] * (seq_len // rows)
        dv = [None] * (seq_len // rows)
        for first in range(0, seq_len, rows):
            here, keys = pl.ds(first, rows), pl.ds(0, first + rows)
            q_rows, k_rows, v_rows, grad = q_ref[here, :], k_ref[keys, :], v_ref[keys, :], do_ref[here, :]
            probs = softmax_rows(q_rows, k_rows, first)
            probs_bf16 = probs.astype(jnp.bfloat16)
            heads = jnp.dot(probs_bf16, v_rows, preferred_element_type=jnp.float32).astype(jnp.bfloat16)
            o_ref[here, :] = heads
            o_send[here, :] = heads.astype(jnp.float32)
            grad_probs = lax.dot_general(grad, v_rows, NT, preferred_element_type=jnp.float32)
            row_dot = jnp.sum(probs * grad_probs, axis=1, keepdims=True)
            grad_scores = (probs * (grad_probs - row_dot) * SCORE_SCALE).astype(jnp.bfloat16)
            grad_q = rotate(jnp.dot(grad_scores, k_rows, preferred_element_type=jnp.float32), cos_ref[here, :], -sin_ref[here, :])
            grad_q = grad_q.astype(jnp.bfloat16)
            dq_ref[here, :] = grad_q
            dq_send[here, :] = grad_q.astype(jnp.float32)
            for sums, term in ((dk, lax.dot_general(grad_scores, q_rows, TN, preferred_element_type=jnp.float32)),
                               (dv, lax.dot_general(probs_bf16, grad, TN, preferred_element_type=jnp.float32))):
                for n in range(first // rows + 1):
                    piece = term[n * rows:(n + 1) * rows]
                    sums[n] = piece if sums[n] is None else sums[n] + piece
        for n in range(seq_len // rows):
            here = pl.ds(n * rows, rows)
            dkv_ref[0, here, :] = rotate(dk[n], cos_ref[here, :], -sin_ref[here, :])
            dkv_ref[1, here, :] = dv[n]

    spec = pl.BlockSpec((seq_len, HEAD_DIM), lambda b: (b, 0))
    table = pl.BlockSpec((seq_len, HEAD_DIM), lambda b: (0, 0))
    tokens = q.shape[0]
    rounded, wide = jax.ShapeDtypeStruct(q.shape, jnp.bfloat16), jax.ShapeDtypeStruct(q.shape, jnp.float32)
    return pl.pallas_call(
        kernel, grid=(tokens // seq_len,), in_specs=[spec] * 4 + [table] * 2,
        out_specs=(spec, spec, spec, spec, pl.BlockSpec((2, seq_len, HEAD_DIM), lambda b: (0, b, 0))),
        out_shape=(rounded, wide, rounded, wide, jax.ShapeDtypeStruct((2,) + q.shape, jnp.float32)),
        compiler_params=pltpu.CompilerParams(vmem_limit_bytes=VMEM_BYTES),
        cost_estimate=pl.CostEstimate(flops=14 * tokens * seq_len * HEAD_DIM, bytes_accessed=28 * tokens * HEAD_DIM,
                                      transcendentals=tokens * seq_len),
        name='attend',
    )(q, k, v, grad_heads, cos_l, sin_l)


def weight_grads(normed, grad_out, grad_q, grad_kv, heads):
    tokens, d_model = normed.shape
    columns = 512

    def kernel(n_ref, dout_ref, dq_ref, dkv_ref, o_ref, wq_ref, wk_ref, wv_ref, wo_ref, left_ref):
        @pl.when(pl.program_id(0) == 0)
        def _():
            pieces = (dq_ref[...].astype(jnp.float32), dkv_ref[0], dkv_ref[1], o_ref[...].astype(jnp.float32))
            for n, piece in enumerate(pieces):
                left_ref[pl.ds(n * HEAD_DIM, HEAD_DIM), :] = jnp.transpose(piece).astype(jnp.bfloat16)

        grads = jnp.dot(left_ref[pl.ds(0, 3 * HEAD_DIM), :], n_ref[...], preferred_element_type=jnp.float32)
        for n, ref in enumerate((wq_ref, wk_ref, wv_ref)):
            ref[...] = jnp.transpose(grads[n * HEAD_DIM:(n + 1) * HEAD_DIM])
        wo_ref[...] = jnp.dot(left_ref[pl.ds(3 * HEAD_DIM, HEAD_DIM), :], dout_ref[...], preferred_element_type=jnp.float32)

    wide = pl.BlockSpec((tokens, columns), lambda i: (0, i))
    tall = pl.BlockSpec((columns, HEAD_DIM), lambda i: (i, 0))
    head = pl.BlockSpec((tokens, HEAD_DIM), lambda i: (0, 0))
    tall_out = jax.ShapeDtypeStruct((d_model, HEAD_DIM), jnp.float32)
    return pl.pallas_call(
        kernel, grid=(d_model // columns,),
        in_specs=[wide, wide, head, pl.BlockSpec((2, tokens, HEAD_DIM), lambda i: (0, 0, 0)), head],
        out_specs=(tall, tall, tall, pl.BlockSpec((HEAD_DIM, columns), lambda i: (0, i))),
        out_shape=(tall_out, tall_out, tall_out, jax.ShapeDtypeStruct((HEAD_DIM, d_model), jnp.float32)),
        scratch_shapes=[pltpu.VMEM((4 * HEAD_DIM, tokens), jnp.bfloat16)],
        compiler_params=pltpu.CompilerParams(vmem_limit_bytes=VMEM_BYTES),
        cost_estimate=pl.CostEstimate(flops=8 * tokens * d_model * HEAD_DIM, bytes_accessed=4 * tokens * d_model, transcendentals=0),
        name='weight_grads',
    )(normed, grad_out, grad_q, grad_kv, heads)


class Place:
    def __init__(self):
        index = lax.axis_index('tp')
        self.c = lax.rem(index, CORES)
        self.x = lax.rem(index // CORES, RING)
        self.y = index // ROW_DEVICES

    def at(self, y, x, c):
        return {'tp': (y * RING + x) * CORES + c}


def turn(position, by):
    return lax.rem(position + (by % RING), RING)


def project(hidden, grad_out, gain, w_query, w_key, w_value, w_out, cos_l, sin_l):
    tokens, d_model = hidden.shape
    seq_len = cos_l.shape[0]
    rows = 384
    steps = tokens // rows
    width = d_model // ROW_DEVICES
    sharers = RING * ROW_DEVICES // (w_key.shape[1] // HEAD_DIM)

    def kernel(x_ref, dout_ref, gain_ref, cos_ref, sin_ref, wq_hbm, wk_hbm, wv_hbm, wo_hbm,
               normed_ref, inv_ref, q_ref, k_ref, v_ref, do_ref, gain_out, got_hbm, w_ref, wo_ref, blocks, loc_sem, send_sem, recv_sem):
        me = Place()
        others = [(by, flip) for by in (1, 2, 3) for flip in (0, 1)] + [(0, 1)]

        def exchanges(which):
            here = me.x if which == 0 else me.y
            for n, (by, flip) in enumerate(others):
                core = 1 - me.c if flip else me.c
                there, origin = turn(here, by), turn(here, -by)
                peer = me.at(me.y, there, core) if which == 0 else me.at(there, me.x, core)

                def copy(dst, which=which, n=n, peer=peer, src=CORES * there + core):
                    return pltpu.make_async_remote_copy(
                        src_ref=blocks.at[which, src], dst_ref=got_hbm.at[which, dst], send_sem=send_sem.at[which, n],
                        recv_sem=recv_sem.at[which, n], device_id=peer, device_id_type=pl.DeviceIdType.MESH)
                yield copy(CORES * here + me.c), copy(CORES * origin + core)

        def kept(which):
            own = CORES * (me.x if which == 0 else me.y) + me.c
            return pltpu.make_async_copy(blocks.at[which, own], got_hbm.at[which, own], loc_sem.at[which])

        @pl.when(pl.program_id(0) == 0)
        def _():
            barrier = pltpu.get_barrier_semaphore()
            peers = [me.at(me.y, turn(me.x, by), 1 - me.c if flip else me.c) for by, flip in others]
            peers += [me.at(turn(me.y, by), me.x, 1 - me.c if flip else me.c) for by, flip in others[:-1]]
            for peer in peers:
                pl.semaphore_signal(barrier, inc=1, device_id=peer, device_id_type=pl.DeviceIdType.MESH)
            head = lax.axis_index('tp') // sharers
            kv_columns = pl.ds(pl.multiple_of(head * HEAD_DIM, HEAD_DIM), HEAD_DIM)
            loads = [pltpu.make_async_copy(src, dst, loc_sem.at[n]) for n, (src, dst) in enumerate((
                (wo_hbm, wo_ref), (wq_hbm, w_ref.at[:, pl.ds(0, HEAD_DIM)]),
                (wk_hbm.at[:, kv_columns], w_ref.at[:, pl.ds(HEAD_DIM, HEAD_DIM)]),
                (wv_hbm.at[:, kv_columns], w_ref.at[:, pl.ds(2 * HEAD_DIM, HEAD_DIM)])))]
            for load in loads:
                load.start()
            for load in loads:
                load.wait()
            for j in range(ROW_DEVICES):
                columns = pl.ds(j * width, width)
                blocks[0, j] = wo_ref[:, columns].astype(jnp.float32)
                blocks[1, j] = jnp.transpose(w_ref[columns, pl.ds(0, HEAD_DIM)].astype(jnp.float32))
            pl.semaphore_wait(barrier, len(peers))
            for which in (0, 1):
                for out, _ in exchanges(which):
                    out.start()
                kept(which).start()

        values = x_ref[...].astype(jnp.float32)
        inv = lax.rsqrt(jnp.mean(values * values, axis=1, keepdims=True) + NORM_EPS)
        inv_ref[...] = inv
        wide_gain = gain_ref[...].astype(jnp.float32)
        gain_out[...] = wide_gain
        normed = (values * inv * wide_gain).astype(jnp.bfloat16)
        normed_ref[...] = normed
        heads = jnp.dot(normed, w_ref[...], preferred_element_type=jnp.float32)
        q_ref[...] = rotate(heads[:, :HEAD_DIM], cos_ref[...], sin_ref[...]).astype(jnp.bfloat16)
        k_ref[...] = rotate(heads[:, HEAD_DIM:2 * HEAD_DIM], cos_ref[...], sin_ref[...]).astype(jnp.bfloat16)
        v_ref[...] = heads[:, 2 * HEAD_DIM:].astype(jnp.bfloat16)
        do_ref[...] = lax.dot_general(dout_ref[...], wo_ref[...], NT, preferred_element_type=jnp.float32).astype(jnp.bfloat16)

        @pl.when(pl.program_id(0) == steps - 1)
        def _():
            for which in (0, 1):
                for out, came in exchanges(which):
                    came.wait_recv()
                    out.wait_send()
                kept(which).wait()

    row_spec = pl.BlockSpec((rows, d_model), lambda i: (i, 0))
    head_spec = pl.BlockSpec((rows, HEAD_DIM), lambda i: (i, 0))
    table_spec = pl.BlockSpec((rows, HEAD_DIM), lambda i: (i % (seq_len // rows), 0))
    any_spec = pl.BlockSpec(memory_space=pl.ANY)
    head = jax.ShapeDtypeStruct((tokens, HEAD_DIM), jnp.bfloat16)
    blocks = (2, ROW_DEVICES, HEAD_DIM, width)
    dma = pltpu.SemaphoreType.DMA
    return pl.pallas_call(
        kernel, grid=(steps,),
        in_specs=[row_spec, row_spec, pl.BlockSpec((1, d_model), lambda i: (0, 0)), table_spec, table_spec] + [any_spec] * 4,
        out_specs=(row_spec, pl.BlockSpec((rows, 1), lambda i: (i, 0)), head_spec, head_spec, head_spec, head_spec,
                   pl.BlockSpec((1, d_model), lambda i: (0, 0)), any_spec),
        out_shape=(jax.ShapeDtypeStruct((tokens, d_model), jnp.bfloat16), jax.ShapeDtypeStruct((tokens, 1), jnp.float32),
                   head, head, head, head, jax.ShapeDtypeStruct((1, d_model), jnp.float32), jax.ShapeDtypeStruct(blocks, jnp.float32)),
        scratch_shapes=[pltpu.VMEM((d_model, 3 * HEAD_DIM), jnp.bfloat16), pltpu.VMEM((HEAD_DIM, d_model), jnp.bfloat16),
                        pltpu.VMEM(blocks, jnp.float32), dma((4,)), dma((2, 7)), dma((2, 7))],
        compiler_params=pltpu.CompilerParams(collective_id=2, has_side_effects=True, vmem_limit_bytes=VMEM_BYTES),
        cost_estimate=pl.CostEstimate(flops=8 * tokens * d_model * HEAD_DIM, bytes_accessed=6 * tokens * d_model, transcendentals=0),
        name='project',
    )(hidden, grad_out, gain, cos_l, sin_l, w_query, w_key, w_value, w_out)


class Transfer:
    def __init__(self, link, size, outgoing, incoming=None):
        self.link, self.size, self.outgoing, self.incoming = link, size, outgoing, incoming or outgoing
        self.left = False


class Step:
    def __init__(self, waits=(), work=None, sends=(), after=(), cost=0.05, bulk=False):
        self.waits, self.work, self.sends, self.after, self.cost, self.bulk = waits, work, sends, after, cost, bulk


LINK_RATE = 45e3
CORE_RATE = 300e3
HOP = 2.5
CORE_HOP = 2.0
QUEUE = 6.0
STEP = 0.1


def in_order(threads):
    now, busy, arrival, finished, order = 4.0, {}, {}, set(), []
    position = [0] * len(threads)
    while any(position[i] < len(threads[i]) for i in range(len(threads))):
        chosen, soonest = None, math.inf
        for i, steps in enumerate(threads):
            if position[i] == len(steps) or any(step not in finished for step in steps[position[i]].after):
                continue
            step = steps[position[i]]
            ready = max([arrival.get(copy, math.inf) for copy in step.waits], default=0.0)
            if step.bulk:
                ready = max([ready] + [busy.get(copy.link, 0.0) - QUEUE for copy in step.sends if copy.link != 'core'])
            if ready <= now:
                chosen = i
                break
            soonest = min(soonest, ready)
        if chosen is None:
            now = soonest
            continue
        step = threads[chosen][position[chosen]]
        position[chosen] += 1
        now += step.cost + STEP
        for copy in step.sends:
            rate, hop = (CORE_RATE, CORE_HOP) if copy.link == 'core' else (LINK_RATE, HOP)
            busy[copy.link] = max(now, busy.get(copy.link, 0.0)) + copy.size / rate
            arrival[copy] = busy[copy.link] + hop
        finished.add(step)
        order.append(step)
    return order


def exchange_kernel(chunks, spreads, *refs):
    (heads_hbm, grad_q_hbm, kv_hbm, w_hbm, w_key_hbm, w_value_hbm, x_hbm, dout_hbm, inv_hbm, gain_hbm,
     rest_ref, out_all, grad_all, kv_out,
     gath_f, gath_b, wb_f, wb_b, part, ring_f, ring_b, fin_f, fin_b, x_ref, dout_ref, inv_ref, gain_ref,
     kvp, kv_core, kv_send, kv_chip, kv_far, rowpart, rowall, w_kv, send_sem, recv_sem, loc_sem) = refs
    me = Place()
    x, y, c = me.x, me.y, me.c
    xr, xl, xo = turn(x, 1), turn(x, -1), turn(x, 2)
    yu, yd, yo = turn(y, 1), turn(y, -1), turn(y, 2)
    other = 1 - c
    rows_y, width = x_ref.shape[1:]
    r = rows_y // chunks
    h = r // 2
    to_right, to_left, to_partner = me.at(y, xr, c), me.at(y, xl, c), me.at(y, x, other)
    to_up, to_down = me.at(yu, x, c), me.at(yd, x, c)
    along_x = (('right', to_right), ('left', to_left), x, xr, xl, xo)
    along_y = (('up', to_up), ('down', to_down), y, yu, yd, yo)

    barrier = pltpu.get_barrier_semaphore()
    peers = [to_up, to_down, to_right, to_left, to_partner,
             me.at(yo, x, c), me.at(yu, x, other), me.at(yd, x, other), me.at(yo, x, other)]
    for peer in peers:
        pl.semaphore_signal(barrier, inc=1, device_id=peer, device_id_type=pl.DeviceIdType.MESH)

    depth = ROW_DEVICES * HEAD_DIM
    own_f, own_b = CORES * x + c, CORES * y + c

    def rows_at(position):
        return pl.ds(pl.multiple_of(position * rows_y, rows_y), rows_y)

    def columns_at(block):
        return pl.ds(pl.multiple_of(block * width, width), width)

    def head_at(head):
        return pl.ds(pl.multiple_of(head * HEAD_DIM, HEAD_DIM), HEAD_DIM)

    per_slot = rows_y // HEAD_DIM

    def stage(which, j):
        return part.at[2 * which + j // per_slot, pl.ds(j % per_slot * HEAD_DIM, HEAD_DIM)]

    copies = [(w_hbm.at[which, j], stage(which, j)) for which in (0, 1) for j in range(ROW_DEVICES)]
    copies += [(w.at[columns_at(own_b), head_at(2 * j + x // 2)], w_kv.at[s, j])
               for s, w in enumerate((w_key_hbm, w_value_hbm)) for j in range(RING)]
    copies += [
        (heads_hbm, gath_f.at[own_f, pl.ds(0, RING)]), (grad_q_hbm, gath_b.at[own_b, pl.ds(0, RING)]),
        (kv_hbm.at[0], kvp.at[:, 0]), (kv_hbm.at[1], kvp.at[:, 1]),
        (x_hbm.at[rows_at(y), columns_at(own_f)], x_ref.at[0]), (x_hbm.at[rows_at(x), columns_at(own_b)], x_ref.at[1]),
        (dout_hbm.at[rows_at(x), columns_at(own_b)], dout_ref), (inv_hbm.at[rows_at(x)], inv_ref), (gain_hbm.at[:, columns_at(own_b)], gain_ref)]
    loads = [pltpu.make_async_copy(src, dst, loc_sem.at[n]) for n, (src, dst) in enumerate(copies)]
    keep_sem = len(loads)
    for copy in loads:
        copy.start()
    first_rest = (chunks - spreads[1]) * r
    rest_ref[pl.ds(first_rest, 8), :] = jnp.zeros((8, width), jnp.float32)
    for copy in loads:
        copy.wait()
    for which, weights in enumerate((wb_f, wb_b)):
        for j in range(ROW_DEVICES):
            weights[pl.ds(j * HEAD_DIM, HEAD_DIM), :] = stage(which, j)[...].astype(jnp.bfloat16)
    for j in range(RING):
        for s in (0, 1):
            weights = jnp.transpose(w_kv[s, j].astype(jnp.float32)).astype(jnp.bfloat16)
            wb_b[pl.ds(depth + (2 * j + s) * HEAD_DIM, HEAD_DIM), :] = weights
    pl.semaphore_wait(barrier, len(peers))

    transfers = []

    def transfer(link, peer, src, dst, came_from=None, came_to=None):
        n = len(transfers)

        def copy(a, b):
            return lambda: pltpu.make_async_remote_copy(
                src_ref=a, dst_ref=b, send_sem=send_sem.at[n], recv_sem=recv_sem.at[n], device_id=peer,
                device_id_type=pl.DeviceIdType.MESH)
        made = Transfer(link, 4 * math.prod(dst.shape), copy(src, dst), copy(came_from, came_to) if came_to is not None else None)
        transfers.append(made)
        return made

    def moved(link, peer, sent, came):
        return transfer(link, peer, sent, sent, came, came)

    def gone(sent):
        for copy in sent:
            copy.outgoing().wait_send()
            copy.left = True

    p = lax.rem(x, 2)
    xn = x + 1 - 2 * p
    mine, theirs = CORES * c + p, CORES * c + 1 - p
    kv_threads, settle, settled = [], [], []
    for k in range(chunks):
        rows = pl.ds(k * r, r)
        core_copy = transfer('core', to_partner, kvp.at[pl.ds(CORES * other, CORES), :, rows], kv_core.at[:, :, rows])
        chip_copy = transfer('right', me.at(y, xn, c), kv_send.at[:, rows], kv_chip.at[:, rows])

        def add_core(rows=rows):
            kv_send[:, rows, :] = kvp[theirs, :, rows, :] + kv_core[1 - p, :, rows, :]

        def add_chip(rows=rows):
            total = kvp[mine, :, rows, :] + kv_core[p, :, rows, :] + kv_chip[:, rows, :]
            gath_b[own_b, pl.ds(RING, 2), rows, :] = total.astype(jnp.bfloat16).astype(jnp.float32)

        kv_threads.append([Step(sends=[core_copy]), Step([core_copy], add_core, [chip_copy], cost=0.1, bulk=True)])
        settle.append(add_chip)
        settled.append(chip_copy)

    def add_pass(backward, gath, wb, ring, fin, spread, ahead_of):
        gather_ring, sum_ring = (along_y, along_x) if backward else (along_x, along_y)
        g_plus, g_minus, g, g_up, g_down, g_far = gather_ring
        s_plus, s_minus, s, s_up, s_down, s_far = sum_ring
        own, left, right, far = [CORES * pos + c for pos in (g, g_down, g_up, g_far)]
        p_own, p_left, p_right, p_far = [CORES * pos + other for pos in (g, g_down, g_up, g_far)]
        parts = gath.shape[1]
        half = parts // 2
        threads, passed, done, ring_sums, begun = [], [], [], [], []
        x_block = x_ref.at[1 if backward else 0]

        def multiply(by, k, before=()):
            gone(before)
            d = turn(s, by)
            rows = pl.ds(k * r, r)
            pieces = [gath[j, d, rows, :] for j in range(ROW_DEVICES)]
            if backward and by % 2 == 0:
                pieces += [gath[CORES * j + d // 2, RING + n, rows, :] for j in range(RING) for n in (0, 1)]
            lhs = jnp.concatenate([piece.astype(jnp.bfloat16) for piece in pieces], axis=1)
            part[d, rows, :] = jnp.dot(lhs, wb[pl.ds(0, lhs.shape[1]), :], preferred_element_type=jnp.float32)

        def add_ring(way, step, k):
            d = turn(s, -(2 + step) if way == 0 else 2 + step)
            part[d, pl.ds(k * r + way * h, h), :] += ring[way, step, k]

        def store(k, values):
            if k < spread:
                fin[pl.ds(k * r, r), :] = values
            else:
                rest_ref[pl.ds((k - spread) * r, r), :] = values

        def finish_forward(k):
            rows = pl.ds(k * r, r)
            store(k, (x_block[rows, :].astype(jnp.float32) + part[s, rows, :]).astype(jnp.bfloat16).astype(jnp.float32))

        def row_sums(k):
            rows = pl.ds(k * r, r)
            total = part[s, rows, :]
            unit = x_block[rows, :].astype(jnp.float32) * inv_ref[rows, :]
            row_sum = jnp.sum(total * gain_ref[...] * unit, axis=1, keepdims=True)
            square = jnp.concatenate([jnp.broadcast_to(row_sum, (r, 128)), jnp.zeros((128 - r, 128), jnp.float32)], axis=0)
            rowpart[k] = jnp.transpose(square)[0:8, :]
            gain_row = jnp.sum(total * unit, axis=0, keepdims=True)
            row_id = lax.broadcasted_iota(jnp.int32, (8, width), 0)
            rest_ref[pl.ds(first_rest, 8), :] += jnp.where(row_id == 0, jnp.broadcast_to(gain_row, (8, width)), 0.0)

        def finish_backward(k):
            rows = pl.ds(k * r, r)
            sums = rowpart[k]
            for m in range(ROW_DEVICES - 1):
                sums = sums + rowall[m, k]
            mean = jnp.transpose(sums)[0:r, 0:1] * (1.0 / (width * ROW_DEVICES))
            inv = inv_ref[rows, :]
            unit = x_block[rows, :].astype(jnp.float32) * inv
            delta = inv * (part[s, rows, :] * gain_ref[...] - unit * mean)
            store(k, (dout_ref[rows, :].astype(jnp.float32) + delta).astype(jnp.bfloat16).astype(jnp.float32))

        for k in range(chunks):
            rows = pl.ds(k * r, r)

            def block(source, first=0, count=parts, rows=rows):
                return gath.at[source, pl.ds(first, count), rows]

            s_right = moved(*g_plus, block(own), block(left))
            s_left = moved(*g_minus, block(own), block(right))
            s_core = moved('core', to_partner, block(own), block(p_own))
            f_right = moved(*g_plus, block(left, 0, half), block(far, 0, half))
            f_left = moved(*g_minus, block(right, half, parts - half), block(far, half, parts - half))
            c_left = moved('core', to_partner, block(left), block(p_left))
            c_right = moved('core', to_partner, block(right), block(p_right))
            c_far = moved('core', to_partner, block(far), block(p_far))
            sums = [[transfer(link, peer, part.at[turn(s, -(1 + step) if way == 0 else 1 + step), pl.ds(k * r + way * h, h)],
                              ring.at[way, step, k]) for step in range(RING - 1)]
                    for way, (link, peer) in enumerate((s_plus, s_minus))]
            ring_sums.append(sums[0] + sums[1])
            after = [passed[k - AHEAD]] if k >= AHEAD else []
            before = ()
            if ahead_of is not None:
                after.append(ahead_of[0][k])
                before = ahead_of[1][k]
            steps = [Step([settled[k]] if backward else (), settle[k] if backward else None, [s_right, s_left, s_core], after, 0.1),
                     Step([s_right], None, [f_right, c_left]), Step([s_left], None, [f_left, c_right])]
            begun.append(steps[0])
            passed.append(steps[-1])
            cost = 1.2 * r / 96
            even = 2 * cost if backward else cost
            steps += [Step([f_right, f_left], None, [c_far]),
                      Step([s_core, c_left, c_right, c_far], functools.partial(multiply, -1, k, before), [sums[0][0]], cost=cost),
                      Step((), functools.partial(multiply, 1, k), [sums[1][0]], cost=cost),
                      Step((), functools.partial(multiply, 2, k), cost=even),
                      Step((), functools.partial(multiply, 0, k), cost=even)]
            for step in range(RING - 1):
                for way in (0, 1):
                    steps.append(Step([sums[way][step]], functools.partial(add_ring, way, step, k),
                                      [sums[way][step + 1]] if step < RING - 2 else [], cost=0.15))
            if backward:
                members = [(pos, core) for pos in (yu, yd, yo) for core in (c, other)] + [(y, other)]
                notes = [transfer('note', me.at(pos, x, core), rowpart.at[k], rowall.at[m, k])
                         for (pos, core), m in zip(members, (2, 3, 0, 1, 4, 5, 6))]
                steps.append(Step((), functools.partial(row_sums, k), notes, cost=0.4))
                steps.append(Step(notes, functools.partial(finish_backward, k), cost=0.5))
            else:
                steps.append(Step((), functools.partial(finish_forward, k), cost=0.3))
            done.append(steps[-1])
            threads.append(steps)
        return threads, done, ring_sums, begun

    def add_spread(all_hbm, fin, spread, done, first_sem, x_firsts):
        threads = []
        for k in range(spread):
            x_first = x_firsts[k]
            ((a_plus, a_minus, a, a_up, a_down, a_far),
             (b_plus, b_minus, b, b_up, b_down, b_far)) = (along_x, along_y) if x_first else (along_y, along_x)

            def place(core, b_pos, a_pos, part_rows=None, k=k, x_first=x_first):
                spot = (k, core, b_pos, a_pos) if x_first else (k, core, a_pos, b_pos)
                return all_hbm.at[spot + (() if part_rows is None else (pl.ds(*part_rows),))]

            def bundle(core, b_pos, first=0, count=RING, k=k, x_first=x_first):
                return all_hbm.at[(k, core, b_pos, pl.ds(first, count)) if x_first else (k, core, pl.ds(first, count), b_pos)]

            source = fin.at[pl.ds(k * r, r)]
            keep = pltpu.make_async_copy(source, place(c, b, a), loc_sem.at[first_sem + k])
            top, low = (0, h), (h, h)
            a0 = transfer(*a_plus, source, place(c, b, a), source, place(c, b, a_down))
            a1 = transfer(*a_minus, source, place(c, b, a), source, place(c, b, a_up))
            h0 = moved(*a_plus, place(c, b, a_down, top), place(c, b, a_far, top))
            h1 = moved(*a_minus, place(c, b, a_up, low), place(c, b, a_far, low))
            b0 = moved(*b_plus, bundle(c, b, 0, 2), bundle(c, b_down, 0, 2))
            b1 = moved(*b_minus, bundle(c, b, 2, 2), bundle(c, b_up, 2, 2))
            b2 = moved(*b_plus, bundle(c, b, 2, 2), bundle(c, b_down, 2, 2))
            b3 = moved(*b_minus, bundle(c, b, 0, 2), bundle(c, b_up, 0, 2))
            g0 = moved(*b_plus, bundle(c, b_down, 0, 2), bundle(c, b_far, 0, 2))
            g1 = moved(*b_minus, bundle(c, b_up, 2, 2), bundle(c, b_far, 2, 2))
            cores = [moved('core', to_partner, bundle(c, pos), bundle(other, pos)) for pos in (b, b_down, b_up, b_far)]
            threads.append([
                Step((), keep.start, [a0, a1], (done[k],), 0.1, True),
                Step([a0], None, [h0], bulk=True), Step([a1], None, [h1], bulk=True),
                Step([h0, h1], keep.wait, [b0, b1, b2, b3, cores[0]], cost=0.1, bulk=True),
                Step([b0], None, [g0], bulk=True), Step([b1], None, [g1], bulk=True),
                Step([b2], None, [cores[1]]), Step([b3], None, [cores[2]]),
                Step([g0, g1], None, [cores[3]]), Step(cores)])
        return threads

    forward, done_f, sums_f, _ = add_pass(False, gath_f, wb_f, ring_f, fin_f, spreads[0], None)
    backward, done_b, _, begun = add_pass(True, gath_b, wb_b, ring_b, fin_b, spreads[1], (done_f, sums_f))
    spread_f = add_spread(out_all, fin_f, spreads[0], done_f, keep_sem, X_FIRST[0])
    spread_b = add_spread(grad_all, fin_b, spreads[1], done_b, keep_sem + spreads[0], X_FIRST[1])
    swap = transfer('right', me.at(y, xn, c), gath_b.at[own_b, pl.ds(RING, 2)], kv_far.at[c])
    swap_core = moved('core', to_partner, kv_far.at[c], kv_far.at[other])
    swaps = [[Step((), None, [swap], begun, bulk=True), Step([swap], None, [swap_core]), Step([swap_core])]]
    passes = []
    for k in range(chunks + LAG):
        passes += forward[k:k + 1] + (backward[k - LAG:k - LAG + 1] if k >= LAG else [])
    for step in in_order(kv_threads + passes + spread_b + spread_f + swaps):
        for copy in step.waits:
            copy.incoming().wait_recv()
        if step.work is not None:
            step.work()
        for copy in step.sends:
            copy.outgoing().start()

    kv_copies = []
    for core in range(CORES):
        for src, place in ((gath_b.at[CORES * y + core, pl.ds(RING, 2)], CORES * core + p), (kv_far.at[core], CORES * core + 1 - p)):
            kv_copies.append(pltpu.make_async_copy(src, kv_out.at[:, place], loc_sem.at[len(kv_copies)]))
    for copy in kv_copies:
        copy.start()
    for copy in kv_copies:
        copy.wait()
    gone([copy for copy in transfers if not copy.left])


def exchange(heads, grad_q, kv, w_blocks, w_key, w_value, x_rows, dout_rows, inv, gain, spread=None):
    tokens, d_model = x_rows.shape
    rows_y, width = tokens // RING, d_model // ROW_DEVICES
    chunks = CHUNKS
    spreads = (chunks, SPREAD if spread is None else spread)
    r = rows_y // chunks
    any_spec = pl.BlockSpec(memory_space=pl.ANY)
    vmem_spec = pl.BlockSpec(memory_space=pltpu.VMEM)
    depth, n_kv = ROW_DEVICES * HEAD_DIM, w_key.shape[1]
    f32, bf16 = jnp.float32, jnp.bfloat16

    def gathered(count):
        return jax.ShapeDtypeStruct((count, CORES, RING, RING, r, width), f32)

    passes = chunks * (8 + 2 * (RING - 1))
    copies = 2 * passes + chunks * (2 + ROW_DEVICES - 1) + 14 * sum(spreads) + 2
    dma = pltpu.SemaphoreType.DMA
    sums = pltpu.VMEM((2, RING - 1, chunks, r // 2, width), f32)
    return pl.pallas_call(
        functools.partial(exchange_kernel, chunks, spreads),
        out_shape=[jax.ShapeDtypeStruct(((chunks - spreads[1]) * r + 8, width), f32), gathered(spreads[0]), gathered(spreads[1]),
                   jax.ShapeDtypeStruct((2, RING, rows_y, HEAD_DIM), f32)],
        in_specs=[any_spec] * 10,
        out_specs=[vmem_spec, any_spec, any_spec, any_spec],
        scratch_shapes=[
            pltpu.VMEM((ROW_DEVICES, RING, rows_y, HEAD_DIM), f32),
            pltpu.VMEM((ROW_DEVICES, RING + 2, rows_y, HEAD_DIM), f32),
            pltpu.VMEM((depth, width), bf16), pltpu.VMEM((depth + n_kv, width), bf16),
            pltpu.VMEM((RING, rows_y, width), f32), sums, sums,
            pltpu.VMEM((spreads[0] * r, width), f32), pltpu.VMEM((spreads[1] * r, width), f32),
            pltpu.VMEM((2, rows_y, width), bf16), pltpu.VMEM((rows_y, width), bf16), pltpu.VMEM((rows_y, 1), f32), pltpu.VMEM((1, width), f32),
            pltpu.VMEM((RING, 2, rows_y, HEAD_DIM), f32), pltpu.VMEM((CORES, 2, rows_y, HEAD_DIM), f32),
            pltpu.VMEM((2, rows_y, HEAD_DIM), f32), pltpu.VMEM((2, rows_y, HEAD_DIM), f32), pltpu.VMEM((CORES, 2, rows_y, HEAD_DIM), f32),
            pltpu.VMEM((chunks, 8, 128), f32), pltpu.VMEM((ROW_DEVICES - 1, chunks, 8, 128), f32),
            pltpu.VMEM((2, RING, width, HEAD_DIM), bf16),
            dma((copies,)), dma((copies,)), dma((3 * ROW_DEVICES + 9 + sum(spreads),))],
        compiler_params=pltpu.CompilerParams(collective_id=1, has_side_effects=True, vmem_limit_bytes=VMEM_BYTES),
        cost_estimate=pl.CostEstimate(flops=2 * tokens * (2 * depth + n_kv) * width, bytes_accessed=16 * tokens * width, transcendentals=0),
        name='exchange',
    )(heads, grad_q, kv, w_blocks, w_key, w_value, x_rows, dout_rows, inv, gain)


def rounded(kernel, gathered, grid, block, index_map, out_rows, place_of, rows, so_far):
    d_model = ROW_DEVICES * gathered.shape[-1]
    moved_rows = math.prod(grid) * out_rows
    return pl.pallas_call(
        kernel, grid=grid,
        in_specs=[pl.BlockSpec(block, index_map)] + ([pl.BlockSpec(memory_space=pl.ANY)] if so_far is not None else []),
        out_specs=pl.BlockSpec((out_rows, d_model), lambda *at: (place_of(*at), 0)),
        out_shape=jax.ShapeDtypeStruct((rows, d_model), jnp.bfloat16),
        input_output_aliases={1: 0} if so_far is not None else {},
        compiler_params=pltpu.CompilerParams(vmem_limit_bytes=VMEM_BYTES),
        cost_estimate=pl.CostEstimate(flops=moved_rows * d_model, bytes_accessed=6 * moved_rows * d_model, transcendentals=0),
        name='narrow',
    )(*((gathered,) if so_far is None else (gathered, so_far)))


def narrow_spread(gathered, spread, rows, by_y, so_far=None):
    r, width = gathered.shape[-2:]
    chunks = rows // RING // r
    group = max(n for n in range(1, 5) if math.gcd(spread, chunks) % n == 0)
    block = (group, CORES, 1, RING, r, width) if by_y else (group, CORES, RING, 1, r, width)

    def kernel(in_ref, *rest):
        for k in range(group):
            for n in range(ROW_DEVICES):
                at = (k, n % CORES) + ((0, n // CORES) if by_y else (n // CORES, 0))
                rest[-1][pl.ds(k * r, r), pl.ds(n * width, width)] = in_ref[at].astype(jnp.bfloat16)

    return rounded(kernel, gathered, (spread // group, RING), block,
                   lambda k, i: (k, 0, i, 0, 0, 0) if by_y else (k, 0, 0, i, 0, 0),
                   group * r, lambda k, i: i * chunks // group + k, rows, so_far)


def narrow_rest(gathered, pad, spread, r, rows, so_far):
    width = gathered.shape[-1]
    chunks = rows // RING // r
    count = chunks - spread
    blocks = gathered.reshape(RING, RING, CORES, count * r + pad, width)

    def kernel(in_ref, *rest):
        for n in range(ROW_DEVICES):
            rest[-1][:, pl.ds(n * width, width)] = in_ref[n // CORES, 0, n % CORES, pl.ds(0, count * r), :].astype(jnp.bfloat16)

    return rounded(kernel, blocks, (RING,), (RING, 1, CORES, count * r + pad, width), lambda x: (0, x, 0, 0, 0), count * r,
                   lambda x: (x * chunks + spread) // count, rows, so_far)


def solution(mesh):
    assert mesh.shape['tp'] == RING * RING * CORES

    def block_fn(hidden, grad_out, norm_gain, w_query, w_key, w_value, w_out):
        batch, seq_len, d_model = hidden.shape
        tokens, width = batch * seq_len, d_model // ROW_DEVICES
        rows_y = tokens // RING

        cos_l, sin_l = rope_lanes(seq_len)
        grad_rows = grad_out.reshape(tokens, d_model)

        normed, inv_rms, q_rot, k_rot, v_head, grad_heads, gain, w_blocks = project(
            hidden.reshape(tokens, d_model), grad_rows, norm_gain.reshape(1, d_model), w_query, w_key, w_value, w_out, cos_l, sin_l)
        heads, heads_send, grad_q, grad_q_send, grad_kv_send = attend(q_rot, k_rot, v_head, grad_heads, cos_l, sin_l, seq_len)
        by_rows = (RING, rows_y, HEAD_DIM)
        rest_block, out_spread, grad_spread, grad_kv = exchange(
            heads_send.reshape(by_rows), grad_q_send.reshape(by_rows), grad_kv_send.reshape((2,) + by_rows),
            w_blocks, w_key, w_value, hidden.reshape(tokens, d_model), grad_rows, inv_rms, gain)
        grad_rest = lax.all_gather(rest_block, 'tp', axis=0, tiled=True)
        r = rows_y // CHUNKS
        block_out = narrow_spread(out_spread, CHUNKS, tokens, True).reshape(hidden.shape)
        grad_hidden = narrow_rest(grad_rest, 8, SPREAD, r, tokens, narrow_spread(grad_spread, SPREAD, tokens, False)).reshape(hidden.shape)
        grad_gain = jnp.sum(grad_rest.reshape(RING, RING, CORES, -1, width)[:, :, :, (CHUNKS - SPREAD) * r, :], axis=1).reshape(d_model)
        grad_w_query, grad_w_key, grad_w_value, grad_w_out = weight_grads(
            normed, grad_rows, grad_q, grad_kv.reshape(2, tokens, HEAD_DIM), heads)
        return block_out, grad_hidden, grad_gain, grad_w_query, grad_w_key, grad_w_value, grad_w_out

    act_spec = P('dp', None, None)
    return jax.shard_map(
        block_fn, mesh=mesh,
        in_specs=(act_spec, act_spec, P(None), P(None, 'tp'), P(None, None), P(None, None), P('tp', None)),
        out_specs=(act_spec, act_spec, P('dp'), P('dp', 'tp'), P('dp', 'tp'), P('dp', 'tp'), P(('dp', 'tp'), None)),
        check_vma=False)
```

```python
import functools
import math
import jax
import jax.numpy as jnp
from jax import lax
from jax.experimental import pallas as pl
from jax.experimental.pallas import tpu as pltpu
from jax.sharding import PartitionSpec as P

HEAD_DIM = 128
NORM_EPS = 1.0e-5
ROPE_BASE = 10000.0
MASK_VALUE = -1.0e30
SCORE_SCALE = 1.0 / math.sqrt(HEAD_DIM)
RING = 4
CORES = 2
ROW_DEVICES = RING * CORES
CHUNKS = 9
AHEAD = 3
SPREAD = 6
X_FIRST = ((0, 1, 0, 1, 1, 0, 0, 1, 1), (0, 0, 0, 0, 1, 1))
LAG = 4
VMEM_BYTES = 62 * 1024 * 1024


def rope_lanes(seq_len):
    lane = lax.broadcasted_iota(jnp.int32, (1, HEAD_DIM), 1)
    inv_freq = ROPE_BASE ** (-(lane - lane % 2).astype(jnp.float32) / HEAD_DIM)
    angles = jnp.arange(seq_len, dtype=jnp.float32)[:, None] * inv_freq
    return jnp.cos(angles), jnp.where(lane % 2 == 0, -jnp.sin(angles), jnp.sin(angles))


def rotate(tensor, cos_l, sin_l):
    lane = lax.broadcasted_iota(jnp.int32, tensor.shape, 1)
    swapped = jnp.where(lane % 2 == 0, pltpu.roll(tensor, HEAD_DIM - 1, 1), pltpu.roll(tensor, 1, 1))
    return tensor * cos_l + swapped * sin_l


NT = (((1,), (1,)), ((), ()))
TN = (((0,), (0,)), ((), ()))


def softmax_rows(q, k, first):
    scores = lax.dot_general(q, k, NT, preferred_element_type=jnp.float32) * SCORE_SCALE
    row = lax.broadcasted_iota(jnp.int32, scores.shape, 0) + first
    col = lax.broadcasted_iota(jnp.int32, scores.shape, 1)
    scores = jnp.where(row >= col, scores, MASK_VALUE)
    weight = jnp.exp(scores - jnp.max(scores, axis=1, keepdims=True))
    return weight * (1.0 / jnp.sum(weight, axis=1, keepdims=True))


def attend(q, k, v, seq_len):
    def kernel(q_ref, k_ref, v_ref, o_ref, send_ref):
        probs = softmax_rows(q_ref[...], k_ref[...], 0).astype(jnp.bfloat16)
        heads = jnp.dot(probs, v_ref[...], preferred_element_type=jnp.float32).astype(jnp.bfloat16)
        o_ref[...] = heads
        send_ref[...] = heads.astype(jnp.float32)

    spec = pl.BlockSpec((seq_len, HEAD_DIM), lambda b: (b, 0))
    tokens = q.shape[0]
    return pl.pallas_call(
        kernel, grid=(tokens // seq_len,), in_specs=[spec] * 3, out_specs=(spec, spec),
        out_shape=(jax.ShapeDtypeStruct(q.shape, jnp.bfloat16), jax.ShapeDtypeStruct(q.shape, jnp.float32)),
        compiler_params=pltpu.CompilerParams(vmem_limit_bytes=VMEM_BYTES),
        cost_estimate=pl.CostEstimate(flops=4 * tokens * seq_len * HEAD_DIM, bytes_accessed=10 * tokens * HEAD_DIM,
                                      transcendentals=tokens * seq_len),
        name='attend',
    )(q, k, v)


def weight_grads(normed, grad_out, grad_q, grad_kv, heads):
    tokens, d_model = normed.shape
    columns = 512

    def kernel(n_ref, dout_ref, dq_ref, dkv_ref, o_ref, wq_ref, wk_ref, wv_ref, wo_ref, left_ref):
        @pl.when(pl.program_id(0) == 0)
        def _():
            pieces = (dq_ref[...].astype(jnp.float32), dkv_ref[0], dkv_ref[1], o_ref[...].astype(jnp.float32))
            for n, piece in enumerate(pieces):
                left_ref[pl.ds(n * HEAD_DIM, HEAD_DIM), :] = jnp.transpose(piece).astype(jnp.bfloat16)

        grads = jnp.dot(left_ref[pl.ds(0, 3 * HEAD_DIM), :], n_ref[...], preferred_element_type=jnp.float32)
        for n, ref in enumerate((wq_ref, wk_ref, wv_ref)):
            ref[...] = jnp.transpose(grads[n * HEAD_DIM:(n + 1) * HEAD_DIM])
        wo_ref[...] = jnp.dot(left_ref[pl.ds(3 * HEAD_DIM, HEAD_DIM), :], dout_ref[...], preferred_element_type=jnp.float32)

    wide = pl.BlockSpec((tokens, columns), lambda i: (0, i))
    tall = pl.BlockSpec((columns, HEAD_DIM), lambda i: (i, 0))
    head = pl.BlockSpec((tokens, HEAD_DIM), lambda i: (0, 0))
    tall_out = jax.ShapeDtypeStruct((d_model, HEAD_DIM), jnp.float32)
    return pl.pallas_call(
        kernel, grid=(d_model // columns,),
        in_specs=[wide, wide, head, pl.BlockSpec((2, tokens, HEAD_DIM), lambda i: (0, 0, 0)), head],
        out_specs=(tall, tall, tall, pl.BlockSpec((HEAD_DIM, columns), lambda i: (0, i))),
        out_shape=(tall_out, tall_out, tall_out, jax.ShapeDtypeStruct((HEAD_DIM, d_model), jnp.float32)),
        scratch_shapes=[pltpu.VMEM((4 * HEAD_DIM, tokens), jnp.bfloat16)],
        compiler_params=pltpu.CompilerParams(vmem_limit_bytes=VMEM_BYTES),
        cost_estimate=pl.CostEstimate(flops=8 * tokens * d_model * HEAD_DIM, bytes_accessed=4 * tokens * d_model, transcendentals=0),
        name='weight_grads',
    )(normed, grad_out, grad_q, grad_kv, heads)


class Place:
    def __init__(self):
        index = lax.axis_index('tp')
        self.c = lax.rem(index, CORES)
        self.x = lax.rem(index // CORES, RING)
        self.y = index // ROW_DEVICES

    def at(self, y, x, c):
        return {'tp': (y * RING + x) * CORES + c}


def turn(position, by):
    return lax.rem(position + (by % RING), RING)


def project(hidden, grad_out, gain, w_query, w_key, w_value, w_out, cos_l, sin_l):
    tokens, d_model = hidden.shape
    seq_len = cos_l.shape[0]
    rows = 384
    steps = tokens // rows
    width = d_model // ROW_DEVICES
    sharers = RING * ROW_DEVICES // (w_key.shape[1] // HEAD_DIM)

    def kernel(x_ref, dout_ref, gain_ref, cos_ref, sin_ref, wq_hbm, wk_hbm, wv_hbm, wo_hbm,
               normed_ref, inv_ref, q_ref, k_ref, v_ref, do_ref, gain_out, got_hbm, w_ref, wo_ref, blocks, held, loc_sem, send_sem, recv_sem):
        me = Place()
        now, last = pl.program_id(0) % 2, (pl.program_id(0) + 1) % 2
        others = [(by, flip) for by in (1, 2, 3) for flip in (0, 1)] + [(0, 1)]

        def exchanges(which):
            here = me.x if which == 0 else me.y
            for n, (by, flip) in enumerate(others):
                core = 1 - me.c if flip else me.c
                there, origin = turn(here, by), turn(here, -by)
                peer = me.at(me.y, there, core) if which == 0 else me.at(there, me.x, core)

                def copy(dst, which=which, n=n, peer=peer, src=CORES * there + core):
                    return pltpu.make_async_remote_copy(
                        src_ref=blocks.at[which, src], dst_ref=got_hbm.at[which, dst], send_sem=send_sem.at[which, n],
                        recv_sem=recv_sem.at[which, n], device_id=peer, device_id_type=pl.DeviceIdType.MESH)
                yield copy(CORES * here + me.c), copy(CORES * origin + core)

        def kept(which):
            own = CORES * (me.x if which == 0 else me.y) + me.c
            return pltpu.make_async_copy(blocks.at[which, own], got_hbm.at[which, own], loc_sem.at[which])

        @pl.when(pl.program_id(0) == 0)
        def _():
            barrier = pltpu.get_barrier_semaphore()
            peers = [me.at(me.y, turn(me.x, by), 1 - me.c if flip else me.c) for by, flip in others]
            peers += [me.at(turn(me.y, by), me.x, 1 - me.c if flip else me.c) for by, flip in others[:-1]]
            for peer in peers:
                pl.semaphore_signal(barrier, inc=1, device_id=peer, device_id_type=pl.DeviceIdType.MESH)
            head = lax.axis_index('tp') // sharers
            kv_columns = pl.ds(pl.multiple_of(head * HEAD_DIM, HEAD_DIM), HEAD_DIM)
            loads = [pltpu.make_async_copy(src, dst, loc_sem.at[n]) for n, (src, dst) in enumerate((
                (wo_hbm, wo_ref), (wq_hbm, w_ref.at[:, pl.ds(0, HEAD_DIM)]),
                (wk_hbm.at[:, kv_columns], w_ref.at[:, pl.ds(HEAD_DIM, HEAD_DIM)]),
                (wv_hbm.at[:, kv_columns], w_ref.at[:, pl.ds(2 * HEAD_DIM, HEAD_DIM)])))]
            for load in loads:
                load.start()
            for load in loads:
                load.wait()
            for j in range(ROW_DEVICES):
                columns = pl.ds(j * width, width)
                blocks[0, j] = wo_ref[:, columns].astype(jnp.float32)
                blocks[1, j] = jnp.transpose(w_ref[columns, pl.ds(0, HEAD_DIM)].astype(jnp.float32))
            pl.semaphore_wait(barrier, len(peers))
            for which in (0, 1):
                for out, _ in exchanges(which):
                    out.start()
                kept(which).start()

        values = x_ref[...].astype(jnp.float32)
        inv = lax.rsqrt(jnp.mean(values * values, axis=1, keepdims=True) + NORM_EPS)
        inv_ref[...] = inv
        wide_gain = gain_ref[...].astype(jnp.float32)
        gain_out[...] = wide_gain
        normed = (values * inv * wide_gain).astype(jnp.bfloat16)
        normed_ref[...] = normed
        held[now] = normed
        heads = jnp.dot(held[last], w_ref[...], preferred_element_type=jnp.float32)
        q_ref[...] = rotate(heads[:, :HEAD_DIM], cos_ref[...], sin_ref[...]).astype(jnp.bfloat16)
        k_ref[...] = rotate(heads[:, HEAD_DIM:2 * HEAD_DIM], cos_ref[...], sin_ref[...]).astype(jnp.bfloat16)
        v_ref[...] = heads[:, 2 * HEAD_DIM:].astype(jnp.bfloat16)
        do_ref[...] = lax.dot_general(dout_ref[...], wo_ref[...], NT, preferred_element_type=jnp.float32).astype(jnp.bfloat16)

        @pl.when(pl.program_id(0) == steps)
        def _():
            for which in (0, 1):
                for out, came in exchanges(which):
                    came.wait_recv()
                    out.wait_send()
                kept(which).wait()

    def this(i):
        return i - i // steps

    def before(i):
        return i - 1 + (steps - i) // steps

    row_spec = pl.BlockSpec((rows, d_model), lambda i: (this(i), 0))
    row_before = pl.BlockSpec((rows, d_model), lambda i: (before(i), 0))
    head_spec = pl.BlockSpec((rows, HEAD_DIM), lambda i: (before(i), 0))
    table_spec = pl.BlockSpec((rows, HEAD_DIM), lambda i: (before(i) % (seq_len // rows), 0))
    any_spec = pl.BlockSpec(memory_space=pl.ANY)
    head = jax.ShapeDtypeStruct((tokens, HEAD_DIM), jnp.bfloat16)
    blocks = (2, ROW_DEVICES, HEAD_DIM, width)
    dma = pltpu.SemaphoreType.DMA
    return pl.pallas_call(
        kernel, grid=(steps + 1,),
        in_specs=[row_spec, row_before, pl.BlockSpec((1, d_model), lambda i: (0, 0)), table_spec, table_spec] + [any_spec] * 4,
        out_specs=(row_spec, pl.BlockSpec((rows, 1), lambda i: (this(i), 0)), head_spec, head_spec, head_spec, head_spec,
                   pl.BlockSpec((1, d_model), lambda i: (0, 0)), any_spec),
        out_shape=(jax.ShapeDtypeStruct((tokens, d_model), jnp.bfloat16), jax.ShapeDtypeStruct((tokens, 1), jnp.float32),
                   head, head, head, head, jax.ShapeDtypeStruct((1, d_model), jnp.float32), jax.ShapeDtypeStruct(blocks, jnp.float32)),
        scratch_shapes=[pltpu.VMEM((d_model, 3 * HEAD_DIM), jnp.bfloat16), pltpu.VMEM((HEAD_DIM, d_model), jnp.bfloat16),
                        pltpu.VMEM(blocks, jnp.float32), pltpu.VMEM((2, rows, d_model), jnp.bfloat16),
                        dma((4,)), dma((2, 7)), dma((2, 7))],
        compiler_params=pltpu.CompilerParams(collective_id=2, has_side_effects=True, vmem_limit_bytes=VMEM_BYTES),
        cost_estimate=pl.CostEstimate(flops=8 * tokens * d_model * HEAD_DIM, bytes_accessed=6 * tokens * d_model, transcendentals=0),
        name='project',
    )(hidden, grad_out, gain, cos_l, sin_l, w_query, w_key, w_value, w_out)


class Transfer:
    def __init__(self, link, size, outgoing, incoming=None):
        self.link, self.size, self.outgoing, self.incoming = link, size, outgoing, incoming or outgoing
        self.left = False


class Step:
    def __init__(self, waits=(), work=None, sends=(), after=(), cost=0.05, bulk=False):
        self.waits, self.work, self.sends, self.after, self.cost, self.bulk = waits, work, sends, after, cost, bulk


LINK_RATE = 45e3
CORE_RATE = 300e3
HOP = 2.5
CORE_HOP = 2.0
QUEUE = 12.0
STEP = 0.1


def in_order(threads):
    now, busy, arrival, finished, order = 4.0, {}, {}, set(), []
    position = [0] * len(threads)
    while any(position[i] < len(threads[i]) for i in range(len(threads))):
        chosen, soonest = None, math.inf
        for i, steps in enumerate(threads):
            if position[i] == len(steps) or any(step not in finished for step in steps[position[i]].after):
                continue
            step = steps[position[i]]
            ready = max([arrival.get(copy, math.inf) for copy in step.waits], default=0.0)
            if step.bulk:
                ready = max([ready] + [busy.get(copy.link, 0.0) - QUEUE for copy in step.sends if copy.link != 'core'])
            if ready <= now:
                chosen = i
                break
            soonest = min(soonest, ready)
        if chosen is None:
            now = soonest
            continue
        step = threads[chosen][position[chosen]]
        position[chosen] += 1
        now += step.cost + STEP
        for copy in step.sends:
            rate, hop = (CORE_RATE, CORE_HOP) if copy.link == 'core' else (LINK_RATE, HOP)
            busy[copy.link] = max(now, busy.get(copy.link, 0.0)) + copy.size / rate
            arrival[copy] = busy[copy.link] + hop
        finished.add(step)
        order.append(step)
    return order


def exchange_kernel(chunks, spreads, *refs):
    (heads_hbm, q_hbm, k_hbm, v_hbm, do_hbm, cos_hbm, sin_hbm, w_hbm, w_key_hbm, w_value_hbm, x_hbm, dout_hbm, inv_hbm, gain_hbm,
     rest_ref, out_all, grad_all, kv_out, grad_q_out,
     gath_f, gath_b, wb_f, wb_b, part, ring_f, ring_b, fin_f, fin_b, x_ref, dout_ref, inv_ref, gain_ref,
     q_ref, k_ref, v_ref, do_ref, cos_ref, sin_ref, grad_q_ref, kvp, kv_core, kv_send, kv_chip, kv_far, rowpart, rowall, w_kv, send_sem, recv_sem, loc_sem) = refs
    me = Place()
    x, y, c = me.x, me.y, me.c
    xr, xl, xo = turn(x, 1), turn(x, -1), turn(x, 2)
    yu, yd, yo = turn(y, 1), turn(y, -1), turn(y, 2)
    other = 1 - c
    rows_y, width = x_ref.shape[1:]
    r = rows_y // chunks
    h = r // 2
    to_right, to_left, to_partner = me.at(y, xr, c), me.at(y, xl, c), me.at(y, x, other)
    to_up, to_down = me.at(yu, x, c), me.at(yd, x, c)
    along_x = (('right', to_right), ('left', to_left), x, xr, xl, xo)
    along_y = (('up', to_up), ('down', to_down), y, yu, yd, yo)

    barrier = pltpu.get_barrier_semaphore()
    peers = [to_up, to_down, to_right, to_left, to_partner,
             me.at(yo, x, c), me.at(yu, x, other), me.at(yd, x, other), me.at(yo, x, other)]
    for peer in peers:
        pl.semaphore_signal(barrier, inc=1, device_id=peer, device_id_type=pl.DeviceIdType.MESH)

    depth = ROW_DEVICES * HEAD_DIM
    own_f, own_b = CORES * x + c, CORES * y + c

    def rows_at(position):
        return pl.ds(pl.multiple_of(position * rows_y, rows_y), rows_y)

    def columns_at(block):
        return pl.ds(pl.multiple_of(block * width, width), width)

    def head_at(head):
        return pl.ds(pl.multiple_of(head * HEAD_DIM, HEAD_DIM), HEAD_DIM)

    per_slot = rows_y // HEAD_DIM

    def stage(which, j):
        return part.at[2 * which + j // per_slot, pl.ds(j % per_slot * HEAD_DIM, HEAD_DIM)]

    copies = [(w_hbm.at[which, j], stage(which, j)) for which in (0, 1) for j in range(ROW_DEVICES)]
    copies += [(w.at[columns_at(own_b), head_at(2 * j + x // 2)], w_kv.at[s, j])
               for s, w in enumerate((w_key_hbm, w_value_hbm)) for j in range(RING)]
    copies += [
        (heads_hbm, gath_f.at[own_f, pl.ds(0, RING)]), (q_hbm, q_ref), (k_hbm, k_ref), (v_hbm, v_ref),
        (do_hbm, do_ref), (cos_hbm, cos_ref), (sin_hbm, sin_ref),
        (x_hbm.at[rows_at(y), columns_at(own_f)], x_ref.at[0]), (x_hbm.at[rows_at(x), columns_at(own_b)], x_ref.at[1]),
        (dout_hbm.at[rows_at(x), columns_at(own_b)], dout_ref), (inv_hbm.at[rows_at(x)], inv_ref), (gain_hbm.at[:, columns_at(own_b)], gain_ref)]
    loads = [pltpu.make_async_copy(src, dst, loc_sem.at[n]) for n, (src, dst) in enumerate(copies)]
    keep_sem = len(loads)
    for copy in loads:
        copy.start()
    first_rest = (chunks - spreads[1]) * r
    rest_ref[pl.ds(first_rest, 8), :] = jnp.zeros((8, width), jnp.float32)
    for copy in loads:
        copy.wait()
    for which, weights in enumerate((wb_f, wb_b)):
        for j in range(ROW_DEVICES):
            weights[pl.ds(j * HEAD_DIM, HEAD_DIM), :] = stage(which, j)[...].astype(jnp.bfloat16)
    for j in range(RING):
        for s in (0, 1):
            weights = jnp.transpose(w_kv[s, j].astype(jnp.float32)).astype(jnp.bfloat16)
            wb_b[pl.ds(depth + (2 * j + s) * HEAD_DIM, HEAD_DIM), :] = weights
    pl.semaphore_wait(barrier, len(peers))

    transfers = []

    def transfer(link, peer, src, dst, came_from=None, came_to=None):
        n = len(transfers)

        def copy(a, b):
            return lambda: pltpu.make_async_remote_copy(
                src_ref=a, dst_ref=b, send_sem=send_sem.at[n], recv_sem=recv_sem.at[n], device_id=peer,
                device_id_type=pl.DeviceIdType.MESH)
        made = Transfer(link, 4 * math.prod(dst.shape), copy(src, dst), copy(came_from, came_to) if came_to is not None else None)
        transfers.append(made)
        return made

    def moved(link, peer, sent, came):
        return transfer(link, peer, sent, sent, came, came)

    def gone(sent):
        for copy in sent:
            copy.outgoing().wait_send()
            copy.left = True

    seq_len = cos_ref.shape[0]
    run = seq_len // RING

    def spot(first):
        return first // rows_y, pl.ds(first % rows_y, run)

    def attend_back(base, first):
        here, keys = pl.ds(base + first, run), pl.ds(base, first + run)
        q_rows, k_rows, v_rows, grad = q_ref[here, :], k_ref[keys, :], v_ref[keys, :], do_ref[here, :]
        probs = softmax_rows(q_rows, k_rows, first)
        grad_probs = lax.dot_general(grad, v_rows, NT, preferred_element_type=jnp.float32)
        row_dot = jnp.sum(probs * grad_probs, axis=1, keepdims=True)
        grad_scores = (probs * (grad_probs - row_dot) * SCORE_SCALE).astype(jnp.bfloat16)
        at = pl.ds(first, run)
        grad_q = rotate(jnp.dot(grad_scores, k_rows, preferred_element_type=jnp.float32), cos_ref[at, :], -sin_ref[at, :])
        grad_q = grad_q.astype(jnp.bfloat16)
        grad_q_ref[here, :] = grad_q
        d, rows = spot(base + first)
        gath_b[own_b, d, rows, :] = grad_q.astype(jnp.float32)
        terms = (lax.dot_general(grad_scores, q_rows, TN, preferred_element_type=jnp.float32),
                 lax.dot_general(probs.astype(jnp.bfloat16), grad, TN, preferred_element_type=jnp.float32))
        for n, term in enumerate(terms):
            for key in range(0, first + run, run):
                d, rows = spot(base + key)
                piece = term[key:key + run]
                kvp[d, n, rows, :] = piece if key == first else kvp[d, n, rows, :] + piece

    def rotate_keys(base):
        for first in range(0, seq_len, run):
            d, rows = spot(base + first)
            at = pl.ds(first, run)
            kvp[d, 0, rows, :] = rotate(kvp[d, 0, rows, :], cos_ref[at, :], -sin_ref[at, :])

    attention = []
    for base in range(0, RING * rows_y, seq_len):
        attention += [Step((), functools.partial(attend_back, base, first), cost=0.8) for first in range(0, seq_len, run)]
        attention.append(Step((), functools.partial(rotate_keys, base), cost=0.3))

    p = lax.rem(x, 2)
    xn = x + 1 - 2 * p
    mine, theirs = CORES * c + p, CORES * c + 1 - p
    kv_threads, settle, settled = [], [], []
    for k in range(chunks):
        rows = pl.ds(k * r, r)
        core_copy = transfer('core', to_partner, kvp.at[pl.ds(CORES * other, CORES), :, rows], kv_core.at[:, :, rows])
        chip_copy = transfer('right', me.at(y, xn, c), kv_send.at[:, rows], kv_chip.at[:, rows])

        def add_core(rows=rows):
            kv_send[:, rows, :] = kvp[theirs, :, rows, :] + kv_core[1 - p, :, rows, :]

        def add_chip(rows=rows):
            total = kvp[mine, :, rows, :] + kv_core[p, :, rows, :] + kv_chip[:, rows, :]
            gath_b[own_b, pl.ds(RING, 2), rows, :] = total.astype(jnp.bfloat16).astype(jnp.float32)

        kv_threads.append([Step(sends=[core_copy], after=attention[-1:]), Step([core_copy], add_core, [chip_copy], cost=0.1, bulk=True)])
        settle.append(add_chip)
        settled.append(chip_copy)

    def add_pass(backward, gath, wb, ring, fin, spread, ahead_of):
        gather_ring, sum_ring = (along_y, along_x) if backward else (along_x, along_y)
        g_plus, g_minus, g, g_up, g_down, g_far = gather_ring
        s_plus, s_minus, s, s_up, s_down, s_far = sum_ring
        own, left, right, far = [CORES * pos + c for pos in (g, g_down, g_up, g_far)]
        p_own, p_left, p_right, p_far = [CORES * pos + other for pos in (g, g_down, g_up, g_far)]
        parts = gath.shape[1]
        half = parts // 2
        threads, passed, done, ring_sums, begun = [], [], [], [], []
        x_block = x_ref.at[1 if backward else 0]

        def multiply(by, k, before=()):
            gone(before)
            d = turn(s, by)
            rows = pl.ds(k * r, r)
            pieces = [gath[j, d, rows, :] for j in range(ROW_DEVICES)]
            if backward and by % 2 == 0:
                pieces += [gath[CORES * j + d // 2, RING + n, rows, :] for j in range(RING) for n in (0, 1)]
            lhs = jnp.concatenate([piece.astype(jnp.bfloat16) for piece in pieces], axis=1)
            part[d, rows, :] = jnp.dot(lhs, wb[pl.ds(0, lhs.shape[1]), :], preferred_element_type=jnp.float32)

        def add_ring(way, step, k):
            d = turn(s, -(2 + step) if way == 0 else 2 + step)
            part[d, pl.ds(k * r + way * h, h), :] += ring[way, step, k]

        def store(k, values):
            if k < spread:
                fin[pl.ds(k * r, r), :] = values
            else:
                rest_ref[pl.ds((k - spread) * r, r), :] = values

        def finish_forward(k):
            rows = pl.ds(k * r, r)
            store(k, (x_block[rows, :].astype(jnp.float32) + part[s, rows, :]).astype(jnp.bfloat16).astype(jnp.float32))

        def row_sums(k):
            rows = pl.ds(k * r, r)
            total = part[s, rows, :]
            unit = x_block[rows, :].astype(jnp.float32) * inv_ref[rows, :]
            row_sum = jnp.sum(total * gain_ref[...] * unit, axis=1, keepdims=True)
            square = jnp.concatenate([jnp.broadcast_to(row_sum, (r, 128)), jnp.zeros((128 - r, 128), jnp.float32)], axis=0)
            rowpart[k] = jnp.transpose(square)[0:8, :]
            gain_row = jnp.sum(total * unit, axis=0, keepdims=True)
            row_id = lax.broadcasted_iota(jnp.int32, (8, width), 0)
            rest_ref[pl.ds(first_rest, 8), :] += jnp.where(row_id == 0, jnp.broadcast_to(gain_row, (8, width)), 0.0)

        def finish_backward(k):
            rows = pl.ds(k * r, r)
            sums = rowpart[k]
            for m in range(ROW_DEVICES - 1):
                sums = sums + rowall[m, k]
            mean = jnp.transpose(sums)[0:r, 0:1] * (1.0 / (width * ROW_DEVICES))
            inv = inv_ref[rows, :]
            unit = x_block[rows, :].astype(jnp.float32) * inv
            delta = inv * (part[s, rows, :] * gain_ref[...] - unit * mean)
            store(k, (dout_ref[rows, :].astype(jnp.float32) + delta).astype(jnp.bfloat16).astype(jnp.float32))

        for k in range(chunks):
            rows = pl.ds(k * r, r)

            def block(source, first=0, count=parts, rows=rows):
                return gath.at[source, pl.ds(first, count), rows]

            s_right = moved(*g_plus, block(own), block(left))
            s_left = moved(*g_minus, block(own), block(right))
            s_core = moved('core', to_partner, block(own), block(p_own))
            f_right = moved(*g_plus, block(left, 0, half), block(far, 0, half))
            f_left = moved(*g_minus, block(right, half, parts - half), block(far, half, parts - half))
            c_left = moved('core', to_partner, block(left), block(p_left))
            c_right = moved('core', to_partner, block(right), block(p_right))
            c_far = moved('core', to_partner, block(far), block(p_far))
            sums = [[transfer(link, peer, part.at[turn(s, -(1 + step) if way == 0 else 1 + step), pl.ds(k * r + way * h, h)],
                              ring.at[way, step, k]) for step in range(RING - 1)]
                    for way, (link, peer) in enumerate((s_plus, s_minus))]
            ring_sums.append(sums[0] + sums[1])
            after = [passed[k - AHEAD]] if k >= AHEAD else []
            before = ()
            if ahead_of is not None:
                after += [ahead_of[0][k], attention[-1]]
                before = ahead_of[1][k]
            steps = [Step([settled[k]] if backward else (), settle[k] if backward else None, [s_right, s_left, s_core], after, 0.1),
                     Step([s_right], None, [f_right, c_left]), Step([s_left], None, [f_left, c_right])]
            begun.append(steps[0])
            passed.append(steps[-1])
            cost = 1.2 * r / 96
            even = 2 * cost if backward else cost
            steps += [Step([f_right, f_left], None, [c_far]),
                      Step([s_core, c_left, c_right, c_far], functools.partial(multiply, -1, k, before), [sums[0][0]], cost=cost),
                      Step((), functools.partial(multiply, 1, k), [sums[1][0]], cost=cost),
                      Step((), functools.partial(multiply, 2, k), cost=even),
                      Step((), functools.partial(multiply, 0, k), cost=even)]
            for step in range(RING - 1):
                for way in (0, 1):
                    steps.append(Step([sums[way][step]], functools.partial(add_ring, way, step, k),
                                      [sums[way][step + 1]] if step < RING - 2 else [], cost=0.15))
            if backward:
                members = [(pos, core) for pos in (yu, yd, yo) for core in (c, other)] + [(y, other)]
                notes = [transfer('note', me.at(pos, x, core), rowpart.at[k], rowall.at[m, k])
                         for (pos, core), m in zip(members, (2, 3, 0, 1, 4, 5, 6))]
                steps.append(Step((), functools.partial(row_sums, k), notes, cost=0.4))
                steps.append(Step(notes, functools.partial(finish_backward, k), cost=0.5))
            else:
                steps.append(Step((), functools.partial(finish_forward, k), cost=0.3))
            done.append(steps[-1])
            threads.append(steps)
        return threads, done, ring_sums, begun

    def add_spread(all_hbm, fin, spread, done, first_sem, x_firsts):
        threads = []
        for k in range(spread):
            x_first = x_firsts[k]
            ((a_plus, a_minus, a, a_up, a_down, a_far),
             (b_plus, b_minus, b, b_up, b_down, b_far)) = (along_x, along_y) if x_first else (along_y, along_x)

            def place(core, b_pos, a_pos, part_rows=None, k=k, x_first=x_first):
                spot = (k, core, b_pos, a_pos) if x_first else (k, core, a_pos, b_pos)
                return all_hbm.at[spot + (() if part_rows is None else (pl.ds(*part_rows),))]

            def bundle(core, b_pos, first=0, count=RING, k=k, x_first=x_first):
                return all_hbm.at[(k, core, b_pos, pl.ds(first, count)) if x_first else (k, core, pl.ds(first, count), b_pos)]

            source = fin.at[pl.ds(k * r, r)]
            keep = pltpu.make_async_copy(source, place(c, b, a), loc_sem.at[first_sem + k])
            top, low = (0, h), (h, h)
            a0 = transfer(*a_plus, source, place(c, b, a), source, place(c, b, a_down))
            a1 = transfer(*a_minus, source, place(c, b, a), source, place(c, b, a_up))
            h0 = moved(*a_plus, place(c, b, a_down, top), place(c, b, a_far, top))
            h1 = moved(*a_minus, place(c, b, a_up, low), place(c, b, a_far, low))
            b0 = moved(*b_plus, bundle(c, b, 0, 2), bundle(c, b_down, 0, 2))
            b1 = moved(*b_minus, bundle(c, b, 2, 2), bundle(c, b_up, 2, 2))
            b2 = moved(*b_plus, bundle(c, b, 2, 2), bundle(c, b_down, 2, 2))
            b3 = moved(*b_minus, bundle(c, b, 0, 2), bundle(c, b_up, 0, 2))
            g0 = moved(*b_plus, bundle(c, b_down, 0, 2), bundle(c, b_far, 0, 2))
            g1 = moved(*b_minus, bundle(c, b_up, 2, 2), bundle(c, b_far, 2, 2))
            cores = [moved('core', to_partner, bundle(c, pos), bundle(other, pos)) for pos in (b, b_down, b_up, b_far)]
            threads.append([
                Step((), keep.start, [a0, a1], (done[k],), 0.1, True),
                Step([a0], None, [h0], bulk=True), Step([a1], None, [h1], bulk=True),
                Step([h0, h1], keep.wait, [b0, b1, b2, b3, cores[0]], cost=0.1, bulk=True),
                Step([b0], None, [g0], bulk=True), Step([b1], None, [g1], bulk=True),
                Step([b2], None, [cores[1]]), Step([b3], None, [cores[2]]),
                Step([g0, g1], None, [cores[3]]), Step(cores)])
        return threads

    forward, done_f, sums_f, _ = add_pass(False, gath_f, wb_f, ring_f, fin_f, spreads[0], None)
    backward, done_b, _, begun = add_pass(True, gath_b, wb_b, ring_b, fin_b, spreads[1], (done_f, sums_f))
    spread_f = add_spread(out_all, fin_f, spreads[0], done_f, keep_sem, X_FIRST[0])
    spread_b = add_spread(grad_all, fin_b, spreads[1], done_b, keep_sem + spreads[0], X_FIRST[1])
    swap = transfer('right', me.at(y, xn, c), gath_b.at[own_b, pl.ds(RING, 2)], kv_far.at[c])
    swap_core = moved('core', to_partner, kv_far.at[c], kv_far.at[other])
    swaps = [[Step((), None, [swap], begun, bulk=True), Step([swap], None, [swap_core]), Step([swap_core])]]
    passes = []
    for k in range(chunks + LAG):
        passes += forward[k:k + 1] + (backward[k - LAG:k - LAG + 1] if k >= LAG else [])
    for step in in_order(kv_threads + passes + [attention] + spread_b + spread_f + swaps):
        for copy in step.waits:
            copy.incoming().wait_recv()
        if step.work is not None:
            step.work()
        for copy in step.sends:
            copy.outgoing().start()

    kv_copies = []
    for core in range(CORES):
        for src, place in ((gath_b.at[CORES * y + core, pl.ds(RING, 2)], CORES * core + p), (kv_far.at[core], CORES * core + 1 - p)):
            kv_copies.append(pltpu.make_async_copy(src, kv_out.at[:, place], loc_sem.at[len(kv_copies)]))
    kv_copies.append(pltpu.make_async_copy(grad_q_ref, grad_q_out, loc_sem.at[len(kv_copies)]))
    for copy in kv_copies:
        copy.start()
    for copy in kv_copies:
        copy.wait()
    gone([copy for copy in transfers if not copy.left])


def exchange(heads, q, k, v, grad_heads, cos_l, sin_l, w_blocks, w_key, w_value, x_rows, dout_rows, inv, gain, spread=None):
    tokens, d_model = x_rows.shape
    rows_y, width = tokens // RING, d_model // ROW_DEVICES
    chunks = CHUNKS
    spreads = (chunks, SPREAD if spread is None else spread)
    r = rows_y // chunks
    any_spec = pl.BlockSpec(memory_space=pl.ANY)
    vmem_spec = pl.BlockSpec(memory_space=pltpu.VMEM)
    depth, n_kv = ROW_DEVICES * HEAD_DIM, w_key.shape[1]
    f32, bf16 = jnp.float32, jnp.bfloat16

    def gathered(count):
        return jax.ShapeDtypeStruct((count, CORES, RING, RING, r, width), f32)

    passes = chunks * (8 + 2 * (RING - 1))
    copies = 2 * passes + chunks * (2 + ROW_DEVICES - 1) + 14 * sum(spreads) + 2
    dma = pltpu.SemaphoreType.DMA
    sums = pltpu.VMEM((2, RING - 1, chunks, r // 2, width), f32)
    return pl.pallas_call(
        functools.partial(exchange_kernel, chunks, spreads),
        out_shape=[jax.ShapeDtypeStruct(((chunks - spreads[1]) * r + 8, width), f32), gathered(spreads[0]), gathered(spreads[1]),
                   jax.ShapeDtypeStruct((2, RING, rows_y, HEAD_DIM), f32), jax.ShapeDtypeStruct(q.shape, bf16)],
        in_specs=[any_spec] * 14,
        out_specs=[vmem_spec, any_spec, any_spec, any_spec, any_spec],
        scratch_shapes=[
            pltpu.VMEM((ROW_DEVICES, RING, rows_y, HEAD_DIM), f32),
            pltpu.VMEM((ROW_DEVICES, RING + 2, rows_y, HEAD_DIM), f32),
            pltpu.VMEM((depth, width), bf16), pltpu.VMEM((depth + n_kv, width), bf16),
            pltpu.VMEM((RING, rows_y, width), f32), sums, sums,
            pltpu.VMEM((spreads[0] * r, width), f32), pltpu.VMEM((spreads[1] * r, width), f32),
            pltpu.VMEM((2, rows_y, width), bf16), pltpu.VMEM((rows_y, width), bf16), pltpu.VMEM((rows_y, 1), f32), pltpu.VMEM((1, width), f32),
            pltpu.VMEM(q.shape, bf16), pltpu.VMEM(q.shape, bf16), pltpu.VMEM(q.shape, bf16), pltpu.VMEM(q.shape, bf16),
            pltpu.VMEM(cos_l.shape, f32), pltpu.VMEM(cos_l.shape, f32), pltpu.VMEM(q.shape, bf16),
            pltpu.VMEM((RING, 2, rows_y, HEAD_DIM), f32), pltpu.VMEM((CORES, 2, rows_y, HEAD_DIM), f32),
            pltpu.VMEM((2, rows_y, HEAD_DIM), f32), pltpu.VMEM((2, rows_y, HEAD_DIM), f32), pltpu.VMEM((CORES, 2, rows_y, HEAD_DIM), f32),
            pltpu.VMEM((chunks, 8, 128), f32), pltpu.VMEM((ROW_DEVICES - 1, chunks, 8, 128), f32),
            pltpu.VMEM((2, RING, width, HEAD_DIM), bf16),
            dma((copies,)), dma((copies,)), dma((3 * ROW_DEVICES + 12 + sum(spreads),))],
        compiler_params=pltpu.CompilerParams(collective_id=1, has_side_effects=True, vmem_limit_bytes=VMEM_BYTES),
        cost_estimate=pl.CostEstimate(flops=2 * tokens * (2 * depth + n_kv) * width, bytes_accessed=16 * tokens * width, transcendentals=0),
        name='exchange',
    )(heads, q, k, v, grad_heads, cos_l, sin_l, w_blocks, w_key, w_value, x_rows, dout_rows, inv, gain)


def rounded(kernel, gathered, grid, block, index_map, out_rows, place_of, rows, so_far):
    d_model = ROW_DEVICES * gathered.shape[-1]
    moved_rows = math.prod(grid) * out_rows
    return pl.pallas_call(
        kernel, grid=grid,
        in_specs=[pl.BlockSpec(block, index_map)] + ([pl.BlockSpec(memory_space=pl.ANY)] if so_far is not None else []),
        out_specs=pl.BlockSpec((out_rows, d_model), lambda *at: (place_of(*at), 0)),
        out_shape=jax.ShapeDtypeStruct((rows, d_model), jnp.bfloat16),
        input_output_aliases={1: 0} if so_far is not None else {},
        compiler_params=pltpu.CompilerParams(vmem_limit_bytes=VMEM_BYTES),
        cost_estimate=pl.CostEstimate(flops=moved_rows * d_model, bytes_accessed=6 * moved_rows * d_model, transcendentals=0),
        name='narrow',
    )(*((gathered,) if so_far is None else (gathered, so_far)))


def narrow_spread(gathered, spread, rows, by_y, so_far=None):
    r, width = gathered.shape[-2:]
    chunks = rows // RING // r
    group = max(n for n in range(1, 5) if math.gcd(spread, chunks) % n == 0)
    block = (group, CORES, 1, RING, r, width) if by_y else (group, CORES, RING, 1, r, width)

    def kernel(in_ref, *rest):
        for k in range(group):
            for n in range(ROW_DEVICES):
                at = (k, n % CORES) + ((0, n // CORES) if by_y else (n // CORES, 0))
                rest[-1][pl.ds(k * r, r), pl.ds(n * width, width)] = in_ref[at].astype(jnp.bfloat16)

    return rounded(kernel, gathered, (spread // group, RING), block,
                   lambda k, i: (k, 0, i, 0, 0, 0) if by_y else (k, 0, 0, i, 0, 0),
                   group * r, lambda k, i: i * chunks // group + k, rows, so_far)


def narrow_rest(gathered, spread, r, rows, so_far):
    width = gathered.shape[-1]
    count = rows // RING // r - spread
    blocks = gathered.reshape(RING, RING, CORES, count * r + 8, width)
    places = rows // RING // (count * r)

    def kernel(in_ref, so_far_ref, out_ref, gain_ref):
        @pl.when(pl.program_id(0) == 0)
        def _():
            gain_ref[...] = jnp.zeros_like(gain_ref)

        for n in range(ROW_DEVICES):
            columns = pl.ds(n * width, width)
            out_ref[:, columns] = in_ref[n // CORES, 0, n % CORES, pl.ds(0, count * r), :].astype(jnp.bfloat16)
            gain_ref[:, columns] += in_ref[n // CORES, 0, n % CORES, pl.ds(count * r, 8), :]

    d_model = ROW_DEVICES * width
    return pl.pallas_call(
        kernel, grid=(RING,),
        in_specs=[pl.BlockSpec((RING, 1, CORES, count * r + 8, width), lambda x: (0, x, 0, 0, 0)), pl.BlockSpec(memory_space=pl.ANY)],
        out_specs=(pl.BlockSpec((count * r, d_model), lambda x: (x * places + spread // count, 0)), pl.BlockSpec((8, d_model), lambda x: (0, 0))),
        out_shape=(jax.ShapeDtypeStruct((rows, d_model), jnp.bfloat16), jax.ShapeDtypeStruct((8, d_model), jnp.float32)),
        input_output_aliases={1: 0}, compiler_params=pltpu.CompilerParams(vmem_limit_bytes=VMEM_BYTES),
        cost_estimate=pl.CostEstimate(flops=RING * count * r * d_model, bytes_accessed=6 * RING * count * r * d_model, transcendentals=0),
        name='narrow',
    )(blocks, so_far)


def solution(mesh):
    assert mesh.shape['tp'] == RING * RING * CORES

    def block_fn(hidden, grad_out, norm_gain, w_query, w_key, w_value, w_out):
        batch, seq_len, d_model = hidden.shape
        tokens, width = batch * seq_len, d_model // ROW_DEVICES
        rows_y = tokens // RING

        cos_l, sin_l = rope_lanes(seq_len)
        grad_rows = grad_out.reshape(tokens, d_model)

        normed, inv_rms, q_rot, k_rot, v_head, grad_heads, gain, w_blocks = project(
            hidden.reshape(tokens, d_model), grad_rows, norm_gain.reshape(1, d_model), w_query, w_key, w_value, w_out, cos_l, sin_l)
        heads, heads_send = attend(q_rot, k_rot, v_head, seq_len)
        rest_block, out_spread, grad_spread, grad_kv, grad_q = exchange(
            heads_send.reshape(RING, rows_y, HEAD_DIM), q_rot, k_rot, v_head, grad_heads, cos_l, sin_l,
            w_blocks, w_key, w_value, hidden.reshape(tokens, d_model), grad_rows, inv_rms, gain)
        grad_rest = lax.all_gather(rest_block, 'tp', axis=0, tiled=True)
        r = rows_y // CHUNKS
        block_out = narrow_spread(out_spread, CHUNKS, tokens, True).reshape(hidden.shape)
        grad_hidden, gain_rows = narrow_rest(grad_rest, SPREAD, r, tokens, narrow_spread(grad_spread, SPREAD, tokens, False))
        grad_hidden, grad_gain = grad_hidden.reshape(hidden.shape), gain_rows[0]
        grad_w_query, grad_w_key, grad_w_value, grad_w_out = weight_grads(
            normed, grad_rows, grad_q, grad_kv.reshape(2, tokens, HEAD_DIM), heads)
        return block_out, grad_hidden, grad_gain, grad_w_query, grad_w_key, grad_w_value, grad_w_out

    act_spec = P('dp', None, None)
    return jax.shard_map(
        block_fn, mesh=mesh,
        in_specs=(act_spec, act_spec, P(None), P(None, 'tp'), P(None, None), P(None, None), P('tp', None)),
        out_specs=(act_spec, act_spec, P('dp'), P('dp', 'tp'), P('dp', 'tp'), P('dp', 'tp'), P(('dp', 'tp'), None)),
        check_vma=False)
```

```python
import functools
import math
import jax
import jax.numpy as jnp
from jax import lax
from jax.experimental import pallas as pl
from jax.experimental.pallas import tpu as pltpu
from jax.sharding import PartitionSpec as P

HEAD_DIM = 128
NORM_EPS = 1.0e-5
ROPE_BASE = 10000.0
MASK_VALUE = -1.0e30
SCORE_SCALE = 1.0 / math.sqrt(HEAD_DIM)
RING = 4
CORES = 2
ROW_DEVICES = RING * CORES
CHUNKS = 9
AHEAD = 3
SPREAD = 6
X_FIRST = ('010110011', '000011')
LAG = 4
VMEM_BYTES = 62 * 1024 * 1024


def rope_lanes(seq_len):
    lane = lax.broadcasted_iota(jnp.int32, (1, HEAD_DIM), 1)
    inv_freq = ROPE_BASE ** (-(lane - lane % 2).astype(jnp.float32) / HEAD_DIM)
    angles = jnp.arange(seq_len, dtype=jnp.float32)[:, None] * inv_freq
    return jnp.cos(angles), jnp.where(lane % 2 == 0, -jnp.sin(angles), jnp.sin(angles))


def rotate(tensor, cos_l, sin_l):
    lane = lax.broadcasted_iota(jnp.int32, tensor.shape, 1)
    swapped = jnp.where(lane % 2 == 0, pltpu.roll(tensor, HEAD_DIM - 1, 1), pltpu.roll(tensor, 1, 1))
    return tensor * cos_l + swapped * sin_l


NT = (((1,), (1,)), ((), ()))
TN = (((0,), (0,)), ((), ()))


def weight_grads(hidden, inv, gain, grad_out, grad_q, grad_kv, heads):
    tokens, d_model = hidden.shape
    columns = 512

    def kernel(x_ref, inv_ref, gain_ref, dout_ref, dq_ref, dkv_ref, o_ref, wq_ref, wk_ref, wv_ref, wo_ref, left_ref):
        @pl.when(pl.program_id(0) == 0)
        def _():
            pieces = (dq_ref[...].astype(jnp.float32), dkv_ref[0], dkv_ref[1], o_ref[...].astype(jnp.float32))
            for n, piece in enumerate(pieces):
                left_ref[pl.ds(n * HEAD_DIM, HEAD_DIM), :] = jnp.transpose(piece).astype(jnp.bfloat16)

        normed = (x_ref[...].astype(jnp.float32) * inv_ref[...] * gain_ref[...]).astype(jnp.bfloat16)
        grads = jnp.dot(left_ref[pl.ds(0, 3 * HEAD_DIM), :], normed, preferred_element_type=jnp.float32)
        for n, ref in enumerate((wq_ref, wk_ref, wv_ref)):
            ref[...] = jnp.transpose(grads[n * HEAD_DIM:(n + 1) * HEAD_DIM])
        wo_ref[...] = jnp.dot(left_ref[pl.ds(3 * HEAD_DIM, HEAD_DIM), :], dout_ref[...], preferred_element_type=jnp.float32)

    wide = pl.BlockSpec((tokens, columns), lambda i: (0, i))
    tall = pl.BlockSpec((columns, HEAD_DIM), lambda i: (i, 0))
    head = pl.BlockSpec((tokens, HEAD_DIM), lambda i: (0, 0))
    tall_out = jax.ShapeDtypeStruct((d_model, HEAD_DIM), jnp.float32)
    return pl.pallas_call(
        kernel, grid=(d_model // columns,),
        in_specs=[wide, pl.BlockSpec((tokens, 1), lambda i: (0, 0)), pl.BlockSpec((1, columns), lambda i: (0, i)), wide, head,
                  pl.BlockSpec((2, tokens, HEAD_DIM), lambda i: (0, 0, 0)), head],
        out_specs=(tall, tall, tall, pl.BlockSpec((HEAD_DIM, columns), lambda i: (0, i))),
        out_shape=(tall_out, tall_out, tall_out, jax.ShapeDtypeStruct((HEAD_DIM, d_model), jnp.float32)),
        scratch_shapes=[pltpu.VMEM((4 * HEAD_DIM, tokens), jnp.bfloat16)],
        compiler_params=pltpu.CompilerParams(vmem_limit_bytes=VMEM_BYTES),
        cost_estimate=pl.CostEstimate(flops=8 * tokens * d_model * HEAD_DIM, bytes_accessed=4 * tokens * d_model, transcendentals=0),
        name='weight_grads',
    )(hidden, inv, gain, grad_out, grad_q, grad_kv, heads)


class Place:
    def __init__(self):
        index = lax.axis_index('tp')
        self.c = lax.rem(index, CORES)
        self.x = lax.rem(index // CORES, RING)
        self.y = index // ROW_DEVICES

    def at(self, y, x, c):
        return {'tp': (y * RING + x) * CORES + c}


def turn(position, by):
    return lax.rem(position + (by % RING), RING)


def softmax_rows(q, k, first):
    scores = lax.dot_general(q, k, NT, preferred_element_type=jnp.float32) * SCORE_SCALE
    row = lax.broadcasted_iota(jnp.int32, scores.shape, 0) + first
    col = lax.broadcasted_iota(jnp.int32, scores.shape, 1)
    scores = jnp.where(row >= col, scores, MASK_VALUE)
    weight = jnp.exp(scores - jnp.max(scores, axis=1, keepdims=True))
    return weight * (1.0 / jnp.sum(weight, axis=1, keepdims=True))


def project(hidden, grad_out, gain, w_query, w_key, w_value, w_out, cos_l, sin_l):
    tokens, d_model = hidden.shape
    seq_len = cos_l.shape[0]
    rows = 384
    steps = tokens // rows
    width = d_model // ROW_DEVICES
    sharers = RING * ROW_DEVICES // (w_key.shape[1] // HEAD_DIM)

    def kernel(x_ref, dout_ref, gain_ref, cos_ref, sin_ref, wq_hbm, wk_hbm, wv_hbm, wo_hbm,
               inv_ref, q_ref, k_ref, v_ref, do_ref, o_ref, o_send, gain_out, got_hbm, w_ref, wo_ref, blocks, loc_sem, send_sem, recv_sem):
        me = Place()
        here = pl.ds(pl.multiple_of(pl.program_id(0) * rows, rows), rows)
        others = [(by, flip) for by in (1, 2, 3) for flip in (0, 1)] + [(0, 1)]

        def exchanges(which):
            here = me.x if which == 0 else me.y
            for n, (by, flip) in enumerate(others):
                core = 1 - me.c if flip else me.c
                there, origin = turn(here, by), turn(here, -by)
                peer = me.at(me.y, there, core) if which == 0 else me.at(there, me.x, core)

                def copy(dst, which=which, n=n, peer=peer, src=CORES * there + core):
                    return pltpu.make_async_remote_copy(
                        src_ref=blocks.at[which, src], dst_ref=got_hbm.at[which, dst], send_sem=send_sem.at[which, n],
                        recv_sem=recv_sem.at[which, n], device_id=peer, device_id_type=pl.DeviceIdType.MESH)
                yield copy(CORES * here + me.c), copy(CORES * origin + core)

        def kept(which):
            own = CORES * (me.x if which == 0 else me.y) + me.c
            return pltpu.make_async_copy(blocks.at[which, own], got_hbm.at[which, own], loc_sem.at[which])

        @pl.when(pl.program_id(0) == 0)
        def _():
            barrier = pltpu.get_barrier_semaphore()
            peers = [me.at(me.y, turn(me.x, by), 1 - me.c if flip else me.c) for by, flip in others]
            peers += [me.at(turn(me.y, by), me.x, 1 - me.c if flip else me.c) for by, flip in others[:-1]]
            for peer in peers:
                pl.semaphore_signal(barrier, inc=1, device_id=peer, device_id_type=pl.DeviceIdType.MESH)
            head = lax.axis_index('tp') // sharers
            kv_columns = pl.ds(pl.multiple_of(head * HEAD_DIM, HEAD_DIM), HEAD_DIM)
            loads = [pltpu.make_async_copy(src, dst, loc_sem.at[n]) for n, (src, dst) in enumerate((
                (wo_hbm, wo_ref), (wq_hbm, w_ref.at[:, pl.ds(0, HEAD_DIM)]),
                (wk_hbm.at[:, kv_columns], w_ref.at[:, pl.ds(HEAD_DIM, HEAD_DIM)]),
                (wv_hbm.at[:, kv_columns], w_ref.at[:, pl.ds(2 * HEAD_DIM, HEAD_DIM)])))]
            for load in loads:
                load.start()
            for load in loads:
                load.wait()
            for j in range(ROW_DEVICES):
                columns = pl.ds(j * width, width)
                blocks[0, j] = wo_ref[:, columns].astype(jnp.float32)
                blocks[1, j] = jnp.transpose(w_ref[columns, pl.ds(0, HEAD_DIM)].astype(jnp.float32))
            pl.semaphore_wait(barrier, len(peers))
            for which in (0, 1):
                for out, _ in exchanges(which):
                    out.start()
                kept(which).start()

        values = x_ref[...].astype(jnp.float32)
        inv = lax.rsqrt(jnp.mean(values * values, axis=1, keepdims=True) + NORM_EPS)
        inv_ref[...] = inv
        wide_gain = gain_ref[...].astype(jnp.float32)
        gain_out[...] = wide_gain
        normed = (values * inv * wide_gain).astype(jnp.bfloat16)
        heads = jnp.dot(normed, w_ref[...], preferred_element_type=jnp.float32)
        q_ref[here, :] = rotate(heads[:, :HEAD_DIM], cos_ref[...], sin_ref[...]).astype(jnp.bfloat16)
        k_ref[here, :] = rotate(heads[:, HEAD_DIM:2 * HEAD_DIM], cos_ref[...], sin_ref[...]).astype(jnp.bfloat16)
        v_ref[here, :] = heads[:, 2 * HEAD_DIM:].astype(jnp.bfloat16)
        do_ref[...] = lax.dot_general(dout_ref[...], wo_ref[...], NT, preferred_element_type=jnp.float32).astype(jnp.bfloat16)

        @pl.when(pl.program_id(0) == steps - 1)
        def _():
            for base in range(0, tokens, seq_len):
                rows_of = pl.ds(base, seq_len)
                probs = softmax_rows(q_ref[rows_of, :], k_ref[rows_of, :], 0).astype(jnp.bfloat16)
                attended = jnp.dot(probs, v_ref[rows_of, :], preferred_element_type=jnp.float32).astype(jnp.bfloat16)
                o_ref[rows_of, :] = attended
                o_send[rows_of, :] = attended.astype(jnp.float32)
            for which in (0, 1):
                for out, came in exchanges(which):
                    came.wait_recv()
                    out.wait_send()
                kept(which).wait()

    row_spec = pl.BlockSpec((rows, d_model), lambda i: (i, 0))
    head_spec = pl.BlockSpec((rows, HEAD_DIM), lambda i: (i, 0))
    table_spec = pl.BlockSpec((rows, HEAD_DIM), lambda i: (i % (seq_len // rows), 0))
    all_rows = pl.BlockSpec((tokens, HEAD_DIM), lambda i: (0, 0))
    any_spec = pl.BlockSpec(memory_space=pl.ANY)
    head = jax.ShapeDtypeStruct((tokens, HEAD_DIM), jnp.bfloat16)
    blocks = (2, ROW_DEVICES, HEAD_DIM, width)
    dma = pltpu.SemaphoreType.DMA
    return pl.pallas_call(
        kernel, grid=(steps,),
        in_specs=[row_spec, row_spec, pl.BlockSpec((1, d_model), lambda i: (0, 0)), table_spec, table_spec] + [any_spec] * 4,
        out_specs=(pl.BlockSpec((rows, 1), lambda i: (i, 0)), all_rows, all_rows, all_rows, head_spec, all_rows, all_rows,
                   pl.BlockSpec((1, d_model), lambda i: (0, 0)), any_spec),
        out_shape=(jax.ShapeDtypeStruct((tokens, 1), jnp.float32), head, head, head, head, head,
                   jax.ShapeDtypeStruct((tokens, HEAD_DIM), jnp.float32), jax.ShapeDtypeStruct((1, d_model), jnp.float32),
                   jax.ShapeDtypeStruct(blocks, jnp.float32)),
        scratch_shapes=[pltpu.VMEM((d_model, 3 * HEAD_DIM), jnp.bfloat16), pltpu.VMEM((HEAD_DIM, d_model), jnp.bfloat16),
                        pltpu.VMEM(blocks, jnp.float32), dma((4,)), dma((2, 7)), dma((2, 7))],
        compiler_params=pltpu.CompilerParams(collective_id=2, has_side_effects=True, vmem_limit_bytes=VMEM_BYTES),
        cost_estimate=pl.CostEstimate(flops=8 * tokens * d_model * HEAD_DIM, bytes_accessed=6 * tokens * d_model, transcendentals=0),
        name='project',
    )(hidden, grad_out, gain, cos_l, sin_l, w_query, w_key, w_value, w_out)


class Transfer:
    def __init__(self, link, size, outgoing, incoming=None):
        self.link, self.size, self.outgoing, self.incoming = link, size, outgoing, incoming or outgoing
        self.left = False


class Step:
    def __init__(self, waits=(), work=None, sends=(), after=(), cost=0.05, bulk=False):
        self.waits, self.work, self.sends, self.after, self.cost, self.bulk = waits, work, sends, after, cost, bulk


LINK_RATE = 45e3
CORE_RATE = 300e3
HOP = 2.5
CORE_HOP = 2.0
QUEUE = 12.0
STEP = 0.1


def in_order(threads):
    now, busy, arrival, finished, order = 4.0, {}, {}, set(), []
    position = [0] * len(threads)
    while any(position[i] < len(threads[i]) for i in range(len(threads))):
        chosen, soonest = None, math.inf
        for i, steps in enumerate(threads):
            if position[i] == len(steps) or any(step not in finished for step in steps[position[i]].after):
                continue
            step = steps[position[i]]
            ready = max([arrival.get(copy, math.inf) for copy in step.waits], default=0.0)
            if step.bulk:
                ready = max([ready] + [busy.get(copy.link, 0.0) - QUEUE for copy in step.sends if copy.link != 'core'])
            if ready <= now:
                chosen = i
                break
            soonest = min(soonest, ready)
        if chosen is None:
            now = soonest
            continue
        step = threads[chosen][position[chosen]]
        position[chosen] += 1
        now += step.cost + STEP
        for copy in step.sends:
            rate, hop = (CORE_RATE, CORE_HOP) if copy.link == 'core' else (LINK_RATE, HOP)
            busy[copy.link] = max(now, busy.get(copy.link, 0.0)) + copy.size / rate
            arrival[copy] = busy[copy.link] + hop
        finished.add(step)
        order.append(step)
    return order


def exchange_kernel(chunks, spreads, *refs):
    (heads_hbm, q_hbm, k_hbm, v_hbm, do_hbm, cos_hbm, sin_hbm, w_hbm, w_key_hbm, w_value_hbm, x_hbm, dout_hbm, inv_hbm, gain_hbm,
     rest_ref, out_all, grad_all, kv_out, grad_q_out,
     gath_f, gath_b, wb_f, wb_b, part, ring_f, ring_b, fin_f, fin_b, x_ref, dout_ref, inv_ref, gain_ref,
     q_ref, k_ref, v_ref, do_ref, cos_ref, sin_ref, grad_q_ref, kvp, kv_core, kv_send, kv_chip, kv_far, rowpart, rowall, w_kv, send_sem, recv_sem, loc_sem) = refs
    me = Place()
    x, y, c = me.x, me.y, me.c
    xr, xl, xo = turn(x, 1), turn(x, -1), turn(x, 2)
    yu, yd, yo = turn(y, 1), turn(y, -1), turn(y, 2)
    other = 1 - c
    rows_y, width = x_ref.shape[1:]
    r = rows_y // chunks
    h = r // 2
    to_right, to_left, to_partner = me.at(y, xr, c), me.at(y, xl, c), me.at(y, x, other)
    to_up, to_down = me.at(yu, x, c), me.at(yd, x, c)
    along_x = (('right', to_right), ('left', to_left), x, xr, xl, xo)
    along_y = (('up', to_up), ('down', to_down), y, yu, yd, yo)

    barrier = pltpu.get_barrier_semaphore()
    peers = [to_up, to_down, to_right, to_left, to_partner,
             me.at(yo, x, c), me.at(yu, x, other), me.at(yd, x, other), me.at(yo, x, other)]
    for peer in peers:
        pl.semaphore_signal(barrier, inc=1, device_id=peer, device_id_type=pl.DeviceIdType.MESH)

    depth = ROW_DEVICES * HEAD_DIM
    own_f, own_b = CORES * x + c, CORES * y + c

    def rows_at(position):
        return pl.ds(pl.multiple_of(position * rows_y, rows_y), rows_y)

    def columns_at(block):
        return pl.ds(pl.multiple_of(block * width, width), width)

    def head_at(head):
        return pl.ds(pl.multiple_of(head * HEAD_DIM, HEAD_DIM), HEAD_DIM)

    per_slot = rows_y // HEAD_DIM

    def stage(which, j):
        return part.at[2 * which + j // per_slot, pl.ds(j % per_slot * HEAD_DIM, HEAD_DIM)]

    copies = [(w_hbm.at[which, j], stage(which, j)) for which in (0, 1) for j in range(ROW_DEVICES)]
    copies += [(w.at[columns_at(own_b), head_at(2 * j + x // 2)], w_kv.at[s, j])
               for s, w in enumerate((w_key_hbm, w_value_hbm)) for j in range(RING)]
    copies += [
        (heads_hbm, gath_f.at[own_f, pl.ds(0, RING)]), (q_hbm, q_ref), (k_hbm, k_ref), (v_hbm, v_ref),
        (do_hbm, do_ref), (cos_hbm, cos_ref), (sin_hbm, sin_ref),
        (x_hbm.at[rows_at(y), columns_at(own_f)], x_ref.at[0]), (x_hbm.at[rows_at(x), columns_at(own_b)], x_ref.at[1]),
        (dout_hbm.at[rows_at(x), columns_at(own_b)], dout_ref), (inv_hbm.at[rows_at(x)], inv_ref), (gain_hbm.at[:, columns_at(own_b)], gain_ref)]
    loads = [pltpu.make_async_copy(src, dst, loc_sem.at[n]) for n, (src, dst) in enumerate(copies)]
    keep_sem = len(loads)
    for copy in loads:
        copy.start()
    first_rest = (chunks - spreads[1]) * r
    rest_ref[pl.ds(first_rest, 8), :] = jnp.zeros((8, width), jnp.float32)
    for copy in loads:
        copy.wait()
    for which, weights in enumerate((wb_f, wb_b)):
        for j in range(ROW_DEVICES):
            weights[pl.ds(j * HEAD_DIM, HEAD_DIM), :] = stage(which, j)[...].astype(jnp.bfloat16)
    for j in range(RING):
        for s in (0, 1):
            weights = jnp.transpose(w_kv[s, j].astype(jnp.float32)).astype(jnp.bfloat16)
            wb_b[pl.ds(depth + (2 * j + s) * HEAD_DIM, HEAD_DIM), :] = weights
    pl.semaphore_wait(barrier, len(peers))

    transfers = []

    def transfer(link, peer, src, dst, came_from=None, came_to=None):
        n = len(transfers)

        def copy(a, b):
            return lambda: pltpu.make_async_remote_copy(
                src_ref=a, dst_ref=b, send_sem=send_sem.at[n], recv_sem=recv_sem.at[n], device_id=peer,
                device_id_type=pl.DeviceIdType.MESH)
        made = Transfer(link, 4 * math.prod(dst.shape), copy(src, dst), copy(came_from, came_to) if came_to is not None else None)
        transfers.append(made)
        return made

    def moved(link, peer, sent, came):
        return transfer(link, peer, sent, sent, came, came)

    def gone(sent):
        for copy in sent:
            copy.outgoing().wait_send()
            copy.left = True

    seq_len = cos_ref.shape[0]
    run = seq_len // RING

    def spot(first):
        return first // rows_y, pl.ds(first % rows_y, run)

    def attend_back(base, first):
        here, keys = pl.ds(base + first, run), pl.ds(base, first + run)
        q_rows, k_rows, v_rows, grad = q_ref[here, :], k_ref[keys, :], v_ref[keys, :], do_ref[here, :]
        probs = softmax_rows(q_rows, k_rows, first)
        grad_probs = lax.dot_general(grad, v_rows, NT, preferred_element_type=jnp.float32)
        row_dot = jnp.sum(probs * grad_probs, axis=1, keepdims=True)
        grad_scores = (probs * (grad_probs - row_dot) * SCORE_SCALE).astype(jnp.bfloat16)
        at = pl.ds(first, run)
        grad_q = rotate(jnp.dot(grad_scores, k_rows, preferred_element_type=jnp.float32), cos_ref[at, :], -sin_ref[at, :])
        grad_q = grad_q.astype(jnp.bfloat16)
        grad_q_ref[here, :] = grad_q
        d, rows = spot(base + first)
        gath_b[own_b, d, rows, :] = grad_q.astype(jnp.float32)
        terms = (lax.dot_general(grad_scores, q_rows, TN, preferred_element_type=jnp.float32),
                 lax.dot_general(probs.astype(jnp.bfloat16), grad, TN, preferred_element_type=jnp.float32))
        for n, term in enumerate(terms):
            for key in range(0, first + run, run):
                d, rows = spot(base + key)
                piece = term[key:key + run]
                kvp[d, n, rows, :] = piece if key == first else kvp[d, n, rows, :] + piece

    def rotate_keys(base):
        for first in range(0, seq_len, run):
            d, rows = spot(base + first)
            at = pl.ds(first, run)
            kvp[d, 0, rows, :] = rotate(kvp[d, 0, rows, :], cos_ref[at, :], -sin_ref[at, :])

    attention = []
    for base in range(0, RING * rows_y, seq_len):
        attention += [Step((), functools.partial(attend_back, base, first), cost=0.8) for first in range(0, seq_len, run)]
        attention.append(Step((), functools.partial(rotate_keys, base), cost=0.3))

    p = lax.rem(x, 2)
    xn = x + 1 - 2 * p
    mine, theirs = CORES * c + p, CORES * c + 1 - p
    kv_threads, settle, settled = [], [], []
    for k in range(chunks):
        rows = pl.ds(k * r, r)
        core_copy = transfer('core', to_partner, kvp.at[pl.ds(CORES * other, CORES), :, rows], kv_core.at[:, :, rows])
        chip_copy = transfer('right', me.at(y, xn, c), kv_send.at[:, rows], kv_chip.at[:, rows])

        def add_core(rows=rows):
            kv_send[:, rows, :] = kvp[theirs, :, rows, :] + kv_core[1 - p, :, rows, :]

        def add_chip(rows=rows):
            total = kvp[mine, :, rows, :] + kv_core[p, :, rows, :] + kv_chip[:, rows, :]
            gath_b[own_b, pl.ds(RING, 2), rows, :] = total.astype(jnp.bfloat16).astype(jnp.float32)

        kv_threads.append([Step(sends=[core_copy], after=attention[-1:]), Step([core_copy], add_core, [chip_copy], cost=0.1, bulk=True)])
        settle.append(add_chip)
        settled.append(chip_copy)

    def add_pass(backward, gath, wb, ring, fin, spread, ahead_of):
        gather_ring, sum_ring = (along_y, along_x) if backward else (along_x, along_y)
        g_plus, g_minus, g, g_up, g_down, g_far = gather_ring
        s_plus, s_minus, s, s_up, s_down, s_far = sum_ring
        own, left, right, far = [CORES * pos + c for pos in (g, g_down, g_up, g_far)]
        p_own, p_left, p_right, p_far = [CORES * pos + other for pos in (g, g_down, g_up, g_far)]
        parts = gath.shape[1]
        half = parts // 2
        threads, passed, done, ring_sums, begun = [], [], [], [], []
        x_block = x_ref.at[1 if backward else 0]

        def multiply(by, k, before=()):
            gone(before)
            d = turn(s, by)
            rows = pl.ds(k * r, r)
            pieces = [gath[j, d, rows, :] for j in range(ROW_DEVICES)]
            if backward and by % 2 == 0:
                pieces += [gath[CORES * j + d // 2, RING + n, rows, :] for j in range(RING) for n in (0, 1)]
            lhs = jnp.concatenate([piece.astype(jnp.bfloat16) for piece in pieces], axis=1)
            part[d, rows, :] = jnp.dot(lhs, wb[pl.ds(0, lhs.shape[1]), :], preferred_element_type=jnp.float32)

        def add_ring(way, step, k):
            d = turn(s, -(2 + step) if way == 0 else 2 + step)
            part[d, pl.ds(k * r + way * h, h), :] += ring[way, step, k]

        def store(k, values):
            if k < spread:
                fin[pl.ds(k * r, r), :] = values
            else:
                rest_ref[pl.ds((k - spread) * r, r), :] = values

        def finish_forward(k):
            rows = pl.ds(k * r, r)
            store(k, (x_block[rows, :].astype(jnp.float32) + part[s, rows, :]).astype(jnp.bfloat16).astype(jnp.float32))

        def row_sums(k):
            rows = pl.ds(k * r, r)
            total = part[s, rows, :]
            unit = x_block[rows, :].astype(jnp.float32) * inv_ref[rows, :]
            row_sum = jnp.sum(total * gain_ref[...] * unit, axis=1, keepdims=True)
            square = jnp.concatenate([jnp.broadcast_to(row_sum, (r, 128)), jnp.zeros((128 - r, 128), jnp.float32)], axis=0)
            rowpart[k] = jnp.transpose(square)[0:8, :]
            gain_row = jnp.sum(total * unit, axis=0, keepdims=True)
            row_id = lax.broadcasted_iota(jnp.int32, (8, width), 0)
            rest_ref[pl.ds(first_rest, 8), :] += jnp.where(row_id == 0, jnp.broadcast_to(gain_row, (8, width)), 0.0)

        def finish_backward(k):
            rows = pl.ds(k * r, r)
            sums = rowpart[k]
            for m in range(ROW_DEVICES - 1):
                sums = sums + rowall[m, k]
            mean = jnp.transpose(sums)[0:r, 0:1] * (1.0 / (width * ROW_DEVICES))
            inv = inv_ref[rows, :]
            unit = x_block[rows, :].astype(jnp.float32) * inv
            delta = inv * (part[s, rows, :] * gain_ref[...] - unit * mean)
            store(k, (dout_ref[rows, :].astype(jnp.float32) + delta).astype(jnp.bfloat16).astype(jnp.float32))

        for k in range(chunks):
            rows = pl.ds(k * r, r)

            def block(source, first=0, count=parts, rows=rows):
                return gath.at[source, pl.ds(first, count), rows]

            s_right = moved(*g_plus, block(own), block(left))
            s_left = moved(*g_minus, block(own), block(right))
            s_core = moved('core', to_partner, block(own), block(p_own))
            f_right = moved(*g_plus, block(left, 0, half), block(far, 0, half))
            f_left = moved(*g_minus, block(right, half, parts - half), block(far, half, parts - half))
            c_left = moved('core', to_partner, block(left), block(p_left))
            c_right = moved('core', to_partner, block(right), block(p_right))
            c_far = moved('core', to_partner, block(far), block(p_far))
            sums = [[transfer(link, peer, part.at[turn(s, -(1 + step) if way == 0 else 1 + step), pl.ds(k * r + way * h, h)],
                              ring.at[way, step, k]) for step in range(RING - 1)]
                    for way, (link, peer) in enumerate((s_plus, s_minus))]
            ring_sums.append(sums[0] + sums[1])
            after = [passed[k - AHEAD]] if k >= AHEAD else []
            before = ()
            if ahead_of is not None:
                after += [ahead_of[0][k], attention[-1]]
                before = ahead_of[1][k]
            steps = [Step([settled[k]] if backward else (), settle[k] if backward else None, [s_right, s_left, s_core], after, 0.1),
                     Step([s_right], None, [f_right, c_left]), Step([s_left], None, [f_left, c_right])]
            begun.append(steps[0])
            passed.append(steps[-1])
            cost = 1.2 * r / 96
            even = 2 * cost if backward else cost
            steps += [Step([f_right, f_left], None, [c_far]),
                      Step([s_core, c_left, c_right, c_far], functools.partial(multiply, -1, k, before), [sums[0][0]], cost=cost),
                      Step((), functools.partial(multiply, 1, k), [sums[1][0]], cost=cost),
                      Step((), functools.partial(multiply, 2, k), cost=even),
                      Step((), functools.partial(multiply, 0, k), cost=even)]
            for step in range(RING - 1):
                for way in (0, 1):
                    steps.append(Step([sums[way][step]], functools.partial(add_ring, way, step, k),
                                      [sums[way][step + 1]] if step < RING - 2 else [], cost=0.15))
            if backward:
                members = [(pos, core) for pos in (yu, yd, yo) for core in (c, other)] + [(y, other)]
                notes = [transfer('note', me.at(pos, x, core), rowpart.at[k], rowall.at[m, k])
                         for (pos, core), m in zip(members, (2, 3, 0, 1, 4, 5, 6))]
                steps.append(Step((), functools.partial(row_sums, k), notes, cost=0.4))
                steps.append(Step(notes, functools.partial(finish_backward, k), cost=0.5))
            else:
                steps.append(Step((), functools.partial(finish_forward, k), cost=0.3))
            done.append(steps[-1])
            threads.append(steps)
        return threads, done, ring_sums, begun

    def add_spread(all_hbm, fin, spread, done, first_sem, x_firsts):
        threads = []
        for k in range(spread):
            x_first = x_firsts[k] == '1'
            ((a_plus, a_minus, a, a_up, a_down, a_far),
             (b_plus, b_minus, b, b_up, b_down, b_far)) = (along_x, along_y) if x_first else (along_y, along_x)

            def place(core, b_pos, a_pos, part_rows=None, k=k, x_first=x_first):
                spot = (k, core, b_pos, a_pos) if x_first else (k, core, a_pos, b_pos)
                return all_hbm.at[spot + (() if part_rows is None else (pl.ds(*part_rows),))]

            def bundle(core, b_pos, first=0, count=RING, k=k, x_first=x_first):
                return all_hbm.at[(k, core, b_pos, pl.ds(first, count)) if x_first else (k, core, pl.ds(first, count), b_pos)]

            source = fin.at[pl.ds(k * r, r)]
            keep = pltpu.make_async_copy(source, place(c, b, a), loc_sem.at[first_sem + k])
            top, low = (0, h), (h, h)
            a0 = transfer(*a_plus, source, place(c, b, a), source, place(c, b, a_down))
            a1 = transfer(*a_minus, source, place(c, b, a), source, place(c, b, a_up))
            h0 = moved(*a_plus, place(c, b, a_down, top), place(c, b, a_far, top))
            h1 = moved(*a_minus, place(c, b, a_up, low), place(c, b, a_far, low))
            b0 = moved(*b_plus, bundle(c, b, 0, 2), bundle(c, b_down, 0, 2))
            b1 = moved(*b_minus, bundle(c, b, 2, 2), bundle(c, b_up, 2, 2))
            b2 = moved(*b_plus, bundle(c, b, 2, 2), bundle(c, b_down, 2, 2))
            b3 = moved(*b_minus, bundle(c, b, 0, 2), bundle(c, b_up, 0, 2))
            g0 = moved(*b_plus, bundle(c, b_down, 0, 2), bundle(c, b_far, 0, 2))
            g1 = moved(*b_minus, bundle(c, b_up, 2, 2), bundle(c, b_far, 2, 2))
            cores = [moved('core', to_partner, bundle(c, pos), bundle(other, pos)) for pos in (b, b_down, b_up, b_far)]
            threads.append([
                Step((), keep.start, [a0, a1], (done[k],), 0.1, True),
                Step([a0], None, [h0], bulk=True), Step([a1], None, [h1], bulk=True),
                Step([h0, h1], keep.wait, [b0, b1, b2, b3, cores[0]], cost=0.1, bulk=True),
                Step([b0], None, [g0], bulk=True), Step([b1], None, [g1], bulk=True),
                Step([b2], None, [cores[1]]), Step([b3], None, [cores[2]]),
                Step([g0, g1], None, [cores[3]]), Step(cores)])
        return threads

    forward, done_f, sums_f, _ = add_pass(False, gath_f, wb_f, ring_f, fin_f, spreads[0], None)
    backward, done_b, _, begun = add_pass(True, gath_b, wb_b, ring_b, fin_b, spreads[1], (done_f, sums_f))
    spread_f = add_spread(out_all, fin_f, spreads[0], done_f, keep_sem, X_FIRST[0])
    spread_b = add_spread(grad_all, fin_b, spreads[1], done_b, keep_sem + spreads[0], X_FIRST[1])
    swap = transfer('right', me.at(y, xn, c), gath_b.at[own_b, pl.ds(RING, 2)], kv_far.at[c])
    swap_core = moved('core', to_partner, kv_far.at[c], kv_far.at[other])
    swaps = [[Step((), None, [swap], begun, bulk=True), Step([swap], None, [swap_core]), Step([swap_core])]]
    passes = []
    for k in range(chunks + LAG):
        passes += forward[k:k + 1] + (backward[k - LAG:k - LAG + 1] if k >= LAG else [])
    for step in in_order(kv_threads + passes + [attention] + spread_b + spread_f + swaps):
        for copy in step.waits:
            copy.incoming().wait_recv()
        if step.work is not None:
            step.work()
        for copy in step.sends:
            copy.outgoing().start()

    kv_copies = []
    for core in range(CORES):
        for src, place in ((gath_b.at[CORES * y + core, pl.ds(RING, 2)], CORES * core + p), (kv_far.at[core], CORES * core + 1 - p)):
            kv_copies.append(pltpu.make_async_copy(src, kv_out.at[:, place], loc_sem.at[len(kv_copies)]))
    kv_copies.append(pltpu.make_async_copy(grad_q_ref, grad_q_out, loc_sem.at[len(kv_copies)]))
    for copy in kv_copies:
        copy.start()
    for copy in kv_copies:
        copy.wait()
    gone([copy for copy in transfers if not copy.left])


def exchange(heads, q, k, v, grad_heads, cos_l, sin_l, w_blocks, w_key, w_value, x_rows, dout_rows, inv, gain, spread=None):
    tokens, d_model = x_rows.shape
    rows_y, width = tokens // RING, d_model // ROW_DEVICES
    chunks = CHUNKS
    spreads = (chunks, SPREAD if spread is None else spread)
    r = rows_y // chunks
    any_spec = pl.BlockSpec(memory_space=pl.ANY)
    vmem_spec = pl.BlockSpec(memory_space=pltpu.VMEM)
    depth, n_kv = ROW_DEVICES * HEAD_DIM, w_key.shape[1]
    f32, bf16 = jnp.float32, jnp.bfloat16

    def gathered(count):
        return jax.ShapeDtypeStruct((count, CORES, RING, RING, r, width), f32)

    passes = chunks * (8 + 2 * (RING - 1))
    copies = 2 * passes + chunks * (2 + ROW_DEVICES - 1) + 14 * sum(spreads) + 2
    dma = pltpu.SemaphoreType.DMA
    sums = pltpu.VMEM((2, RING - 1, chunks, r // 2, width), f32)
    return pl.pallas_call(
        functools.partial(exchange_kernel, chunks, spreads),
        out_shape=[jax.ShapeDtypeStruct(((chunks - spreads[1]) * r + 8, width), f32), gathered(spreads[0]), gathered(spreads[1]),
                   jax.ShapeDtypeStruct((2, RING, rows_y, HEAD_DIM), f32), jax.ShapeDtypeStruct(q.shape, bf16)],
        in_specs=[any_spec] * 14,
        out_specs=[vmem_spec, any_spec, any_spec, any_spec, any_spec],
        scratch_shapes=[
            pltpu.VMEM((ROW_DEVICES, RING, rows_y, HEAD_DIM), f32),
            pltpu.VMEM((ROW_DEVICES, RING + 2, rows_y, HEAD_DIM), f32),
            pltpu.VMEM((depth, width), bf16), pltpu.VMEM((depth + n_kv, width), bf16),
            pltpu.VMEM((RING, rows_y, width), f32), sums, sums,
            pltpu.VMEM((spreads[0] * r, width), f32), pltpu.VMEM((spreads[1] * r, width), f32),
            pltpu.VMEM((2, rows_y, width), bf16), pltpu.VMEM((rows_y, width), bf16), pltpu.VMEM((rows_y, 1), f32), pltpu.VMEM((1, width), f32),
            pltpu.VMEM(q.shape, bf16), pltpu.VMEM(q.shape, bf16), pltpu.VMEM(q.shape, bf16), pltpu.VMEM(q.shape, bf16),
            pltpu.VMEM(cos_l.shape, f32), pltpu.VMEM(cos_l.shape, f32), pltpu.VMEM(q.shape, bf16),
            pltpu.VMEM((RING, 2, rows_y, HEAD_DIM), f32), pltpu.VMEM((CORES, 2, rows_y, HEAD_DIM), f32),
            pltpu.VMEM((2, rows_y, HEAD_DIM), f32), pltpu.VMEM((2, rows_y, HEAD_DIM), f32), pltpu.VMEM((CORES, 2, rows_y, HEAD_DIM), f32),
            pltpu.VMEM((chunks, 8, 128), f32), pltpu.VMEM((ROW_DEVICES - 1, chunks, 8, 128), f32),
            pltpu.VMEM((2, RING, width, HEAD_DIM), bf16),
            dma((copies,)), dma((copies,)), dma((3 * ROW_DEVICES + 12 + sum(spreads),))],
        compiler_params=pltpu.CompilerParams(collective_id=1, has_side_effects=True, vmem_limit_bytes=VMEM_BYTES),
        cost_estimate=pl.CostEstimate(flops=2 * tokens * (2 * depth + n_kv) * width, bytes_accessed=16 * tokens * width, transcendentals=0),
        name='exchange',
    )(heads, q, k, v, grad_heads, cos_l, sin_l, w_blocks, w_key, w_value, x_rows, dout_rows, inv, gain)


def rounded(kernel, gathered, grid, block, index_map, out_rows, place_of, rows, so_far):
    d_model = ROW_DEVICES * gathered.shape[-1]
    moved_rows = math.prod(grid) * out_rows
    return pl.pallas_call(
        kernel, grid=grid,
        in_specs=[pl.BlockSpec(block, index_map)] + ([pl.BlockSpec(memory_space=pl.ANY)] if so_far is not None else []),
        out_specs=pl.BlockSpec((out_rows, d_model), lambda *at: (place_of(*at), 0)),
        out_shape=jax.ShapeDtypeStruct((rows, d_model), jnp.bfloat16),
        input_output_aliases={1: 0} if so_far is not None else {},
        compiler_params=pltpu.CompilerParams(vmem_limit_bytes=VMEM_BYTES),
        cost_estimate=pl.CostEstimate(flops=moved_rows * d_model, bytes_accessed=6 * moved_rows * d_model, transcendentals=0),
        name='narrow',
    )(*((gathered,) if so_far is None else (gathered, so_far)))


def narrow_spread(gathered, spread, rows, by_y, so_far=None):
    r, width = gathered.shape[-2:]
    chunks = rows // RING // r
    group = max(n for n in range(1, 5) if math.gcd(spread, chunks) % n == 0)
    block = (group, CORES, 1, RING, r, width) if by_y else (group, CORES, RING, 1, r, width)

    def kernel(in_ref, *rest):
        for k in range(group):
            for n in range(ROW_DEVICES):
                at = (k, n % CORES) + ((0, n // CORES) if by_y else (n // CORES, 0))
                rest[-1][pl.ds(k * r, r), pl.ds(n * width, width)] = in_ref[at].astype(jnp.bfloat16)

    return rounded(kernel, gathered, (spread // group, RING), block,
                   lambda k, i: (k, 0, i, 0, 0, 0) if by_y else (k, 0, 0, i, 0, 0),
                   group * r, lambda k, i: i * chunks // group + k, rows, so_far)


def narrow_rest(gathered, spread, r, rows, so_far):
    width = gathered.shape[-1]
    count = rows // RING // r - spread
    blocks = gathered.reshape(RING, RING, CORES, count * r + 8, width)
    places = rows // RING // (count * r)

    def kernel(in_ref, so_far_ref, out_ref, gain_ref):
        @pl.when(pl.program_id(0) == 0)
        def _():
            gain_ref[...] = jnp.zeros_like(gain_ref)

        for n in range(ROW_DEVICES):
            columns = pl.ds(n * width, width)
            out_ref[:, columns] = in_ref[n // CORES, 0, n % CORES, pl.ds(0, count * r), :].astype(jnp.bfloat16)
            gain_ref[:, columns] += in_ref[n // CORES, 0, n % CORES, pl.ds(count * r, 1), :]

    d_model = ROW_DEVICES * width
    return pl.pallas_call(
        kernel, grid=(RING,),
        in_specs=[pl.BlockSpec((RING, 1, CORES, count * r + 8, width), lambda x: (0, x, 0, 0, 0)), pl.BlockSpec(memory_space=pl.ANY)],
        out_specs=(pl.BlockSpec((count * r, d_model), lambda x: (x * places + spread // count, 0)), pl.BlockSpec((1, d_model), lambda x: (0, 0))),
        out_shape=(jax.ShapeDtypeStruct((rows, d_model), jnp.bfloat16), jax.ShapeDtypeStruct((1, d_model), jnp.float32)),
        input_output_aliases={1: 0}, compiler_params=pltpu.CompilerParams(vmem_limit_bytes=VMEM_BYTES),
        cost_estimate=pl.CostEstimate(flops=RING * count * r * d_model, bytes_accessed=6 * RING * count * r * d_model, transcendentals=0),
        name='narrow',
    )(blocks, so_far)


def solution(mesh):
    assert mesh.shape['tp'] == RING * RING * CORES

    def block_fn(hidden, grad_out, norm_gain, w_query, w_key, w_value, w_out):
        batch, seq_len, d_model = hidden.shape
        tokens, width = batch * seq_len, d_model // ROW_DEVICES
        rows_y = tokens // RING

        cos_l, sin_l = rope_lanes(seq_len)
        grad_rows = grad_out.reshape(tokens, d_model)

        inv_rms, q_rot, k_rot, v_head, grad_heads, heads, heads_send, gain, w_blocks = project(
            hidden.reshape(tokens, d_model), grad_rows, norm_gain.reshape(1, d_model), w_query, w_key, w_value, w_out, cos_l, sin_l)
        rest_block, out_spread, grad_spread, grad_kv, grad_q = exchange(
            heads_send.reshape(RING, rows_y, HEAD_DIM), q_rot, k_rot, v_head, grad_heads, cos_l, sin_l,
            w_blocks, w_key, w_value, hidden.reshape(tokens, d_model), grad_rows, inv_rms, gain)
        grad_rest = lax.all_gather(rest_block, 'tp', axis=0, tiled=True)
        r = rows_y // CHUNKS
        block_out = narrow_spread(out_spread, CHUNKS, tokens, True).reshape(hidden.shape)
        grad_hidden, gain_rows = narrow_rest(grad_rest, SPREAD, r, tokens, narrow_spread(grad_spread, SPREAD, tokens, False))
        grad_hidden, grad_gain = grad_hidden.reshape(hidden.shape), gain_rows.reshape(d_model)
        grad_w_query, grad_w_key, grad_w_value, grad_w_out = weight_grads(
            hidden.reshape(tokens, d_model), inv_rms, gain, grad_rows, grad_q, grad_kv.reshape(2, tokens, HEAD_DIM), heads)
        return block_out, grad_hidden, grad_gain, grad_w_query, grad_w_key, grad_w_value, grad_w_out

    act_spec = P('dp', None, None)
    return jax.shard_map(
        block_fn, mesh=mesh,
        in_specs=(act_spec, act_spec, P(None), P(None, 'tp'), P(None, None), P(None, None), P('tp', None)),
        out_specs=(act_spec, act_spec, P('dp'), P('dp', 'tp'), P('dp', 'tp'), P('dp', 'tp'), P(('dp', 'tp'), None)),
        check_vma=False)
```

```python
import functools
import math
import jax
import jax.numpy as jnp
from jax import lax
from jax.experimental import pallas as pl
from jax.experimental.pallas import tpu as pltpu
from jax.sharding import PartitionSpec as P

HEAD_DIM = 128
NORM_EPS = 1.0e-5
ROPE_BASE = 10000.0
MASK_VALUE = -1.0e30
SCORE_SCALE = 1.0 / math.sqrt(HEAD_DIM)
RING = 4
CORES = 2
ROW_DEVICES = RING * CORES
CHUNKS = 9
AHEAD = 3
SPREAD = 6
X_FIRST = ('001211101', '100010')
LAG = 4
VMEM_BYTES = 62 * 1024 * 1024


def rope_lanes(seq_len):
    lane = lax.broadcasted_iota(jnp.int32, (1, HEAD_DIM), 1)
    inv_freq = ROPE_BASE ** (-(lane - lane % 2).astype(jnp.float32) / HEAD_DIM)
    angles = jnp.arange(seq_len, dtype=jnp.float32)[:, None] * inv_freq
    return jnp.cos(angles), jnp.where(lane % 2 == 0, -jnp.sin(angles), jnp.sin(angles))


def rotate(tensor, cos_l, sin_l):
    lane = lax.broadcasted_iota(jnp.int32, tensor.shape, 1)
    swapped = jnp.where(lane % 2 == 0, pltpu.roll(tensor, HEAD_DIM - 1, 1), pltpu.roll(tensor, 1, 1))
    return tensor * cos_l + swapped * sin_l


NT = (((1,), (1,)), ((), ()))
TN = (((0,), (0,)), ((), ()))


def weight_grads(hidden, inv, gain, grad_out, grad_q, grad_kv, heads):
    tokens, d_model = hidden.shape
    columns = 512

    def kernel(x_ref, inv_ref, gain_ref, dout_ref, dq_ref, dkv_ref, o_ref, wq_ref, wk_ref, wv_ref, wo_ref, left_ref):
        @pl.when(pl.program_id(0) == 0)
        def _():
            pieces = (dq_ref[...].astype(jnp.float32), dkv_ref[0], dkv_ref[1], o_ref[...].astype(jnp.float32))
            for n, piece in enumerate(pieces):
                left_ref[pl.ds(n * HEAD_DIM, HEAD_DIM), :] = jnp.transpose(piece).astype(jnp.bfloat16)

        normed = (x_ref[...].astype(jnp.float32) * inv_ref[...] * gain_ref[...]).astype(jnp.bfloat16)
        grads = jnp.dot(left_ref[pl.ds(0, 3 * HEAD_DIM), :], normed, preferred_element_type=jnp.float32)
        for n, ref in enumerate((wq_ref, wk_ref, wv_ref)):
            ref[...] = jnp.transpose(grads[n * HEAD_DIM:(n + 1) * HEAD_DIM])
        wo_ref[...] = jnp.dot(left_ref[pl.ds(3 * HEAD_DIM, HEAD_DIM), :], dout_ref[...], preferred_element_type=jnp.float32)

    wide = pl.BlockSpec((tokens, columns), lambda i: (0, i))
    tall = pl.BlockSpec((columns, HEAD_DIM), lambda i: (i, 0))
    head = pl.BlockSpec((tokens, HEAD_DIM), lambda i: (0, 0))
    tall_out = jax.ShapeDtypeStruct((d_model, HEAD_DIM), jnp.float32)
    return pl.pallas_call(
        kernel, grid=(d_model // columns,),
        in_specs=[wide, pl.BlockSpec((tokens, 1), lambda i: (0, 0)), pl.BlockSpec((1, columns), lambda i: (0, i)), wide, head,
                  pl.BlockSpec((2, tokens, HEAD_DIM), lambda i: (0, 0, 0)), head],
        out_specs=(tall, tall, tall, pl.BlockSpec((HEAD_DIM, columns), lambda i: (0, i))),
        out_shape=(tall_out, tall_out, tall_out, jax.ShapeDtypeStruct((HEAD_DIM, d_model), jnp.float32)),
        scratch_shapes=[pltpu.VMEM((4 * HEAD_DIM, tokens), jnp.bfloat16)],
        compiler_params=pltpu.CompilerParams(vmem_limit_bytes=VMEM_BYTES),
        cost_estimate=pl.CostEstimate(flops=8 * tokens * d_model * HEAD_DIM, bytes_accessed=4 * tokens * d_model, transcendentals=0),
        name='weight_grads',
    )(hidden, inv, gain, grad_out, grad_q, grad_kv, heads)


class Place:
    def __init__(self):
        index = lax.axis_index('tp')
        self.c = lax.rem(index, CORES)
        self.x = lax.rem(index // CORES, RING)
        self.y = index // ROW_DEVICES

    def at(self, y, x, c):
        return {'tp': (y * RING + x) * CORES + c}


def turn(position, by):
    return lax.rem(position + (by % RING), RING)


def softmax_rows(q, k, first):
    scores = lax.dot_general(q, k, NT, preferred_element_type=jnp.float32) * SCORE_SCALE
    row = lax.broadcasted_iota(jnp.int32, scores.shape, 0) + first
    col = lax.broadcasted_iota(jnp.int32, scores.shape, 1)
    scores = jnp.where(row >= col, scores, MASK_VALUE)
    weight = jnp.exp(scores - jnp.max(scores, axis=1, keepdims=True))
    return weight * (1.0 / jnp.sum(weight, axis=1, keepdims=True))


def project(hidden, grad_out, gain, w_query, w_key, w_value, w_out, cos_l, sin_l):
    tokens, d_model = hidden.shape
    seq_len = cos_l.shape[0]
    rows = 192
    steps = tokens // rows
    width = d_model // ROW_DEVICES
    sharers = RING * ROW_DEVICES // (w_key.shape[1] // HEAD_DIM)

    def kernel(x_ref, dout_ref, gain_ref, cos_ref, sin_ref, wq_hbm, wk_hbm, wv_hbm, wo_hbm,
               inv_ref, q_ref, k_ref, v_ref, do_ref, o_ref, o_send, gain_out, got_hbm, w_ref, wo_ref, blocks, loc_sem, send_sem, recv_sem):
        me = Place()
        here = pl.ds(pl.multiple_of(pl.program_id(0) * rows, rows), rows)
        others = [(by, flip) for by in (2, 1, 3) for flip in (0, 1)] + [(0, 1)]

        def exchanges(which):
            here = me.x if which == 0 else me.y
            for n, (by, flip) in enumerate(others):
                core = 1 - me.c if flip else me.c
                there, origin = turn(here, by), turn(here, -by)
                peer = me.at(me.y, there, core) if which == 0 else me.at(there, me.x, core)

                def copy(dst, which=which, n=n, peer=peer, src=CORES * there + core):
                    return pltpu.make_async_remote_copy(
                        src_ref=blocks.at[which, src], dst_ref=got_hbm.at[which, dst], send_sem=send_sem.at[which, n],
                        recv_sem=recv_sem.at[which, n], device_id=peer, device_id_type=pl.DeviceIdType.MESH)
                yield copy(CORES * here + me.c), copy(CORES * origin + core)

        def kept(which):
            own = CORES * (me.x if which == 0 else me.y) + me.c
            return pltpu.make_async_copy(blocks.at[which, own], got_hbm.at[which, own], loc_sem.at[which])

        @pl.when(pl.program_id(0) == 0)
        def _():
            barrier = pltpu.get_barrier_semaphore()
            peers = [me.at(me.y, turn(me.x, by), 1 - me.c if flip else me.c) for by, flip in others]
            peers += [me.at(turn(me.y, by), me.x, 1 - me.c if flip else me.c) for by, flip in others[:-1]]
            for peer in peers:
                pl.semaphore_signal(barrier, inc=1, device_id=peer, device_id_type=pl.DeviceIdType.MESH)
            head = lax.axis_index('tp') // sharers
            kv_columns = pl.ds(pl.multiple_of(head * HEAD_DIM, HEAD_DIM), HEAD_DIM)
            loads = [pltpu.make_async_copy(src, dst, loc_sem.at[n]) for n, (src, dst) in enumerate((
                (wo_hbm, wo_ref), (wq_hbm, w_ref.at[:, pl.ds(0, HEAD_DIM)]),
                (wk_hbm.at[:, kv_columns], w_ref.at[:, pl.ds(HEAD_DIM, HEAD_DIM)]),
                (wv_hbm.at[:, kv_columns], w_ref.at[:, pl.ds(2 * HEAD_DIM, HEAD_DIM)])))]
            for load in loads:
                load.start()
            for load in loads:
                load.wait()
            for j in range(ROW_DEVICES):
                columns = pl.ds(j * width, width)
                blocks[0, j] = wo_ref[:, columns].astype(jnp.float32)
                blocks[1, j] = jnp.transpose(w_ref[columns, pl.ds(0, HEAD_DIM)].astype(jnp.float32))
            pl.semaphore_wait(barrier, len(peers))
            for which in (0, 1):
                for out, _ in exchanges(which):
                    out.start()
                kept(which).start()

        values = x_ref[...].astype(jnp.float32)
        inv = lax.rsqrt(jnp.mean(values * values, axis=1, keepdims=True) + NORM_EPS)
        inv_ref[...] = inv
        wide_gain = gain_ref[...].astype(jnp.float32)
        gain_out[...] = wide_gain
        normed = (values * inv * wide_gain).astype(jnp.bfloat16)
        heads = jnp.dot(normed, w_ref[...], preferred_element_type=jnp.float32)
        q_ref[here, :] = rotate(heads[:, :HEAD_DIM], cos_ref[...], sin_ref[...]).astype(jnp.bfloat16)
        k_ref[here, :] = rotate(heads[:, HEAD_DIM:2 * HEAD_DIM], cos_ref[...], sin_ref[...]).astype(jnp.bfloat16)
        v_ref[here, :] = heads[:, 2 * HEAD_DIM:].astype(jnp.bfloat16)
        do_ref[...] = lax.dot_general(dout_ref[...], wo_ref[...], NT, preferred_element_type=jnp.float32).astype(jnp.bfloat16)

        @pl.when(pl.program_id(0) == steps - 1)
        def _():
            for base in range(0, tokens, seq_len):
                rows_of = pl.ds(base, seq_len)
                probs = softmax_rows(q_ref[rows_of, :], k_ref[rows_of, :], 0).astype(jnp.bfloat16)
                attended = jnp.dot(probs, v_ref[rows_of, :], preferred_element_type=jnp.float32).astype(jnp.bfloat16)
                o_ref[rows_of, :] = attended
                o_send[rows_of, :] = attended.astype(jnp.float32)
            for which in (0, 1):
                for out, came in exchanges(which):
                    came.wait_recv()
                    out.wait_send()
                kept(which).wait()

    row_spec = pl.BlockSpec((rows, d_model), lambda i: (i, 0))
    head_spec = pl.BlockSpec((rows, HEAD_DIM), lambda i: (i, 0))
    table_spec = pl.BlockSpec((rows, HEAD_DIM), lambda i: (i % (seq_len // rows), 0))
    all_rows = pl.BlockSpec((tokens, HEAD_DIM), lambda i: (0, 0))
    any_spec = pl.BlockSpec(memory_space=pl.ANY)
    head = jax.ShapeDtypeStruct((tokens, HEAD_DIM), jnp.bfloat16)
    blocks = (2, ROW_DEVICES, HEAD_DIM, width)
    dma = pltpu.SemaphoreType.DMA
    return pl.pallas_call(
        kernel, grid=(steps,),
        in_specs=[row_spec, row_spec, pl.BlockSpec((1, d_model), lambda i: (0, 0)), table_spec, table_spec] + [any_spec] * 4,
        out_specs=(pl.BlockSpec((rows, 1), lambda i: (i, 0)), all_rows, all_rows, all_rows, head_spec, all_rows, all_rows,
                   pl.BlockSpec((1, d_model), lambda i: (0, 0)), any_spec),
        out_shape=(jax.ShapeDtypeStruct((tokens, 1), jnp.float32), head, head, head, head, head,
                   jax.ShapeDtypeStruct((tokens, HEAD_DIM), jnp.float32), jax.ShapeDtypeStruct((1, d_model), jnp.float32),
                   jax.ShapeDtypeStruct(blocks, jnp.float32)),
        scratch_shapes=[pltpu.VMEM((d_model, 3 * HEAD_DIM), jnp.bfloat16), pltpu.VMEM((HEAD_DIM, d_model), jnp.bfloat16),
                        pltpu.VMEM(blocks, jnp.float32), dma((4,)), dma((2, 7)), dma((2, 7))],
        compiler_params=pltpu.CompilerParams(collective_id=2, has_side_effects=True, vmem_limit_bytes=VMEM_BYTES),
        cost_estimate=pl.CostEstimate(flops=8 * tokens * d_model * HEAD_DIM, bytes_accessed=6 * tokens * d_model, transcendentals=0),
        name='project',
    )(hidden, grad_out, gain, cos_l, sin_l, w_query, w_key, w_value, w_out)


class Transfer:
    def __init__(self, link, size, outgoing, incoming=None):
        self.link, self.size, self.outgoing, self.incoming = link, size, outgoing, incoming or outgoing
        self.left = False


class Step:
    def __init__(self, waits=(), work=None, sends=(), after=(), cost=0.05, bulk=False):
        self.waits, self.work, self.sends, self.after, self.cost, self.bulk = waits, work, sends, after, cost, bulk


LINK_RATE = 45e3
CORE_RATE = 300e3
HOP = 2.5
CORE_HOP = 2.0
QUEUE = 15.0
STEP = 0.1


def in_order(threads):
    now, busy, arrival, finished, order = 4.0, {}, {}, set(), []
    position = [0] * len(threads)
    while any(position[i] < len(threads[i]) for i in range(len(threads))):
        chosen, soonest = None, math.inf
        for i, steps in enumerate(threads):
            if position[i] == len(steps) or any(step not in finished for step in steps[position[i]].after):
                continue
            step = steps[position[i]]
            ready = max([arrival.get(copy, math.inf) for copy in step.waits], default=0.0)
            if step.bulk:
                ready = max([ready] + [busy.get(copy.link, 0.0) - QUEUE for copy in step.sends if copy.link != 'core'])
            if ready <= now:
                chosen = i
                break
            soonest = min(soonest, ready)
        if chosen is None:
            now = soonest
            continue
        step = threads[chosen][position[chosen]]
        position[chosen] += 1
        now += step.cost + STEP
        for copy in step.sends:
            rate, hop = (CORE_RATE, CORE_HOP) if copy.link == 'core' else (LINK_RATE, HOP)
            busy[copy.link] = max(now, busy.get(copy.link, 0.0)) + copy.size / rate
            arrival[copy] = busy[copy.link] + hop
        finished.add(step)
        order.append(step)
    return order


def exchange_kernel(chunks, spreads, *refs):
    (heads_hbm, q_hbm, k_hbm, v_hbm, do_hbm, cos_hbm, sin_hbm, w_hbm, w_key_hbm, w_value_hbm, x_hbm, dout_hbm, inv_hbm, gain_hbm,
     rest_ref, out_all, grad_all, kv_out, grad_q_out,
     gath_f, gath_b, wb_f, wb_b, part, ring_f, ring_b, fin_f, fin_b, x_ref, dout_ref, inv_ref, gain_ref,
     q_ref, k_ref, v_ref, do_ref, cos_ref, sin_ref, grad_q_ref, kvp, kv_core, kv_send, kv_chip, kv_far, rowpart, rowall, w_kv, send_sem, recv_sem, loc_sem) = refs
    me = Place()
    x, y, c = me.x, me.y, me.c
    xr, xl, xo = turn(x, 1), turn(x, -1), turn(x, 2)
    yu, yd, yo = turn(y, 1), turn(y, -1), turn(y, 2)
    other = 1 - c
    rows_y, width = x_ref.shape[1:]
    r = rows_y // chunks
    h = r // 2
    to_right, to_left, to_partner = me.at(y, xr, c), me.at(y, xl, c), me.at(y, x, other)
    to_up, to_down = me.at(yu, x, c), me.at(yd, x, c)
    along_x = (('right', to_right), ('left', to_left), x, xr, xl, xo)
    along_y = (('up', to_up), ('down', to_down), y, yu, yd, yo)

    barrier = pltpu.get_barrier_semaphore()
    peers = [to_up, to_down, to_right, to_left, to_partner,
             me.at(yo, x, c), me.at(yu, x, other), me.at(yd, x, other), me.at(yo, x, other)]
    for peer in peers:
        pl.semaphore_signal(barrier, inc=1, device_id=peer, device_id_type=pl.DeviceIdType.MESH)

    depth = ROW_DEVICES * HEAD_DIM
    own_f, own_b = CORES * x + c, CORES * y + c

    def rows_at(position):
        return pl.ds(pl.multiple_of(position * rows_y, rows_y), rows_y)

    def columns_at(block):
        return pl.ds(pl.multiple_of(block * width, width), width)

    def head_at(head):
        return pl.ds(pl.multiple_of(head * HEAD_DIM, HEAD_DIM), HEAD_DIM)

    per_slot = rows_y // HEAD_DIM

    def stage(which, j):
        return part.at[2 * which + j // per_slot, pl.ds(j % per_slot * HEAD_DIM, HEAD_DIM)]

    copies = [(w_hbm.at[which, j], stage(which, j)) for which in (0, 1) for j in range(ROW_DEVICES)]
    copies += [(w.at[columns_at(own_b), head_at(2 * j + x // 2)], w_kv.at[s, j])
               for s, w in enumerate((w_key_hbm, w_value_hbm)) for j in range(RING)]
    copies += [
        (heads_hbm, gath_f.at[own_f, pl.ds(0, RING)]), (q_hbm, q_ref), (k_hbm, k_ref), (v_hbm, v_ref),
        (do_hbm, do_ref), (cos_hbm, cos_ref), (sin_hbm, sin_ref),
        (x_hbm.at[rows_at(y), columns_at(own_f)], x_ref.at[0]), (x_hbm.at[rows_at(x), columns_at(own_b)], x_ref.at[1]),
        (dout_hbm.at[rows_at(x), columns_at(own_b)], dout_ref), (inv_hbm.at[rows_at(x)], inv_ref), (gain_hbm.at[:, columns_at(own_b)], gain_ref)]
    loads = [pltpu.make_async_copy(src, dst, loc_sem.at[n]) for n, (src, dst) in enumerate(copies)]
    keep_sem = len(loads)
    for copy in loads:
        copy.start()
    first_rest = (chunks - spreads[1]) * r
    rest_ref[pl.ds(first_rest, 8), :] = jnp.zeros((8, width), jnp.float32)
    for copy in loads:
        copy.wait()
    for which, weights in enumerate((wb_f, wb_b)):
        for j in range(ROW_DEVICES):
            weights[pl.ds(j * HEAD_DIM, HEAD_DIM), :] = stage(which, j)[...].astype(jnp.bfloat16)
    for j in range(RING):
        for s in (0, 1):
            weights = jnp.transpose(w_kv[s, j].astype(jnp.float32)).astype(jnp.bfloat16)
            wb_b[pl.ds(depth + (2 * j + s) * HEAD_DIM, HEAD_DIM), :] = weights
    pl.semaphore_wait(barrier, len(peers))

    transfers = []

    def transfer(link, peer, src, dst, came_from=None, came_to=None):
        n = len(transfers)

        def copy(a, b):
            return lambda: pltpu.make_async_remote_copy(
                src_ref=a, dst_ref=b, send_sem=send_sem.at[n], recv_sem=recv_sem.at[n], device_id=peer,
                device_id_type=pl.DeviceIdType.MESH)
        made = Transfer(link, 4 * math.prod(dst.shape), copy(src, dst), copy(came_from, came_to) if came_to is not None else None)
        transfers.append(made)
        return made

    def moved(link, peer, sent, came):
        return transfer(link, peer, sent, sent, came, came)

    def gone(sent):
        for copy in sent:
            copy.outgoing().wait_send()
            copy.left = True

    seq_len = cos_ref.shape[0]
    run = seq_len // RING

    def spot(first):
        return first // rows_y, pl.ds(first % rows_y, run)

    def attend_back(base, first):
        here, keys = pl.ds(base + first, run), pl.ds(base, first + run)
        q_rows, k_rows, v_rows, grad = q_ref[here, :], k_ref[keys, :], v_ref[keys, :], do_ref[here, :]
        probs = softmax_rows(q_rows, k_rows, first)
        grad_probs = lax.dot_general(grad, v_rows, NT, preferred_element_type=jnp.float32)
        row_dot = jnp.sum(probs * grad_probs, axis=1, keepdims=True)
        grad_scores = (probs * (grad_probs - row_dot) * SCORE_SCALE).astype(jnp.bfloat16)
        at = pl.ds(first, run)
        grad_q = rotate(jnp.dot(grad_scores, k_rows, preferred_element_type=jnp.float32), cos_ref[at, :], -sin_ref[at, :])
        grad_q = grad_q.astype(jnp.bfloat16)
        grad_q_ref[here, :] = grad_q
        d, rows = spot(base + first)
        gath_b[own_b, d, rows, :] = grad_q.astype(jnp.float32)
        terms = (lax.dot_general(grad_scores, q_rows, TN, preferred_element_type=jnp.float32),
                 lax.dot_general(probs.astype(jnp.bfloat16), grad, TN, preferred_element_type=jnp.float32))
        for n, term in enumerate(terms):
            for key in range(0, first + run, run):
                d, rows = spot(base + key)
                piece = term[key:key + run]
                kvp[d, n, rows, :] = piece if key == first else kvp[d, n, rows, :] + piece

    def rotate_keys(base):
        for first in range(0, seq_len, run):
            d, rows = spot(base + first)
            at = pl.ds(first, run)
            kvp[d, 0, rows, :] = rotate(kvp[d, 0, rows, :], cos_ref[at, :], -sin_ref[at, :])

    attention = []
    for base in range(0, RING * rows_y, seq_len):
        attention += [Step((), functools.partial(attend_back, base, first), cost=0.8) for first in range(0, seq_len, run)]
        attention.append(Step((), functools.partial(rotate_keys, base), cost=0.3))

    p = lax.rem(x, 2)
    xn = x + 1 - 2 * p
    mine, theirs = CORES * c + p, CORES * c + 1 - p
    kv_threads, settle, settled = [], [], []
    for k in range(chunks):
        rows = pl.ds(k * r, r)
        core_copy = transfer('core', to_partner, kvp.at[pl.ds(CORES * other, CORES), :, rows], kv_core.at[:, :, rows])
        chip_copy = transfer('right', me.at(y, xn, c), kv_send.at[:, rows], kv_chip.at[:, rows])

        def add_core(rows=rows):
            kv_send[:, rows, :] = kvp[theirs, :, rows, :] + kv_core[1 - p, :, rows, :]

        def add_chip(rows=rows):
            total = kvp[mine, :, rows, :] + kv_core[p, :, rows, :] + kv_chip[:, rows, :]
            gath_b[own_b, pl.ds(RING, 2), rows, :] = total.astype(jnp.bfloat16).astype(jnp.float32)

        kv_threads.append([Step(sends=[core_copy], after=attention[-1:]), Step([core_copy], add_core, [chip_copy], cost=0.1, bulk=True)])
        settle.append(add_chip)
        settled.append(chip_copy)

    def add_pass(backward, gath, wb, ring, fin, spread, ahead_of):
        gather_ring, sum_ring = (along_y, along_x) if backward else (along_x, along_y)
        g_plus, g_minus, g, g_up, g_down, g_far = gather_ring
        s_plus, s_minus, s, s_up, s_down, s_far = sum_ring
        own, left, right, far = [CORES * pos + c for pos in (g, g_down, g_up, g_far)]
        p_own, p_left, p_right, p_far = [CORES * pos + other for pos in (g, g_down, g_up, g_far)]
        parts = gath.shape[1]
        half = parts // 2
        threads, passed, done, ring_sums, begun = [], [], [], [], []
        x_block = x_ref.at[1 if backward else 0]

        def multiply(by, k, before=()):
            gone(before)
            d = turn(s, by)
            rows = pl.ds(k * r, r)
            pieces = [gath[j, d, rows, :] for j in range(ROW_DEVICES)]
            if backward and by % 2 == 0:
                pieces += [gath[CORES * j + d // 2, RING + n, rows, :] for j in range(RING) for n in (0, 1)]
            lhs = jnp.concatenate([piece.astype(jnp.bfloat16) for piece in pieces], axis=1)
            part[d, rows, :] = jnp.dot(lhs, wb[pl.ds(0, lhs.shape[1]), :], preferred_element_type=jnp.float32)

        def add_ring(way, step, k):
            d = turn(s, -(2 + step) if way == 0 else 2 + step)
            part[d, pl.ds(k * r + way * h, h), :] += ring[way, step, k]

        def store(k, values):
            if k < spread:
                fin[pl.ds(k * r, r), :] = values
            else:
                rest_ref[pl.ds((k - spread) * r, r), :] = values

        def finish_forward(k):
            rows = pl.ds(k * r, r)
            store(k, (x_block[rows, :].astype(jnp.float32) + part[s, rows, :]).astype(jnp.bfloat16).astype(jnp.float32))

        def row_sums(k):
            rows = pl.ds(k * r, r)
            total = part[s, rows, :]
            unit = x_block[rows, :].astype(jnp.float32) * inv_ref[rows, :]
            row_sum = jnp.sum(total * gain_ref[...] * unit, axis=1, keepdims=True)
            square = jnp.concatenate([jnp.broadcast_to(row_sum, (r, 128)), jnp.zeros((128 - r, 128), jnp.float32)], axis=0)
            rowpart[k] = jnp.transpose(square)[0:8, :]
            gain_row = jnp.sum(total * unit, axis=0, keepdims=True)
            row_id = lax.broadcasted_iota(jnp.int32, (8, width), 0)
            rest_ref[pl.ds(first_rest, 8), :] += jnp.where(row_id == 0, jnp.broadcast_to(gain_row, (8, width)), 0.0)

        def finish_backward(k):
            rows = pl.ds(k * r, r)
            sums = rowpart[k]
            for m in range(ROW_DEVICES - 1):
                sums = sums + rowall[m, k]
            mean = jnp.transpose(sums)[0:r, 0:1] * (1.0 / (width * ROW_DEVICES))
            inv = inv_ref[rows, :]
            unit = x_block[rows, :].astype(jnp.float32) * inv
            delta = inv * (part[s, rows, :] * gain_ref[...] - unit * mean)
            store(k, (dout_ref[rows, :].astype(jnp.float32) + delta).astype(jnp.bfloat16).astype(jnp.float32))

        for k in range(chunks):
            rows = pl.ds(k * r, r)

            def block(source, first=0, count=parts, rows=rows):
                return gath.at[source, pl.ds(first, count), rows]

            s_right = moved(*g_plus, block(own), block(left))
            s_left = moved(*g_minus, block(own), block(right))
            s_core = moved('core', to_partner, block(own), block(p_own))
            f_right = moved(*g_plus, block(left, 0, half), block(far, 0, half))
            f_left = moved(*g_minus, block(right, half, parts - half), block(far, half, parts - half))
            c_left = moved('core', to_partner, block(left), block(p_left))
            c_right = moved('core', to_partner, block(right), block(p_right))
            c_far = moved('core', to_partner, block(far), block(p_far))
            sums = [[transfer(link, peer, part.at[turn(s, -(1 + step) if way == 0 else 1 + step), pl.ds(k * r + way * h, h)],
                              ring.at[way, step, k]) for step in range(RING - 1)]
                    for way, (link, peer) in enumerate((s_plus, s_minus))]
            ring_sums.append(sums[0] + sums[1])
            after = [passed[k - AHEAD]] if k >= AHEAD else []
            before = ()
            if ahead_of is not None:
                after += [ahead_of[0][k], attention[-1]]
                before = ahead_of[1][k]
            steps = [Step([settled[k]] if backward else (), settle[k] if backward else None, [s_right, s_left, s_core], after, 0.1),
                     Step([s_right], None, [f_right, c_left]), Step([s_left], None, [f_left, c_right])]
            begun.append(steps[0])
            passed.append(steps[-1])
            cost = 1.2 * r / 96
            even = 2 * cost if backward else cost
            steps += [Step([f_right, f_left], None, [c_far]),
                      Step([s_core, c_left, c_right, c_far], functools.partial(multiply, -1, k, before), [sums[0][0]], cost=cost),
                      Step((), functools.partial(multiply, 1, k), [sums[1][0]], cost=cost),
                      Step((), functools.partial(multiply, 2, k), cost=even),
                      Step((), functools.partial(multiply, 0, k), cost=even)]
            for step in range(RING - 1):
                for way in (0, 1):
                    steps.append(Step([sums[way][step]], functools.partial(add_ring, way, step, k),
                                      [sums[way][step + 1]] if step < RING - 2 else [], cost=0.15))
            if backward:
                members = [(pos, core) for pos in (yu, yd, yo) for core in (c, other)] + [(y, other)]
                notes = [transfer('note', me.at(pos, x, core), rowpart.at[k], rowall.at[m, k])
                         for (pos, core), m in zip(members, (2, 3, 0, 1, 4, 5, 6))]
                steps.append(Step((), functools.partial(row_sums, k), notes, cost=0.4))
                steps.append(Step(notes, functools.partial(finish_backward, k), cost=0.5))
            else:
                steps.append(Step((), functools.partial(finish_forward, k), cost=0.3))
            done.append(steps[-1])
            threads.append(steps)
        return threads, done, ring_sums, begun

    def add_spread(all_hbm, fin, spread, done, first_sem, x_firsts):
        threads = []
        for k in range(spread):
            x_first, one_side = x_firsts[k] == '1', x_firsts[k] == '2'
            ((a_plus, a_minus, a, a_up, a_down, a_far),
             (b_plus, b_minus, b, b_up, b_down, b_far)) = (along_x, along_y) if x_first else (along_y, along_x)

            def place(core, b_pos, a_pos, part_rows=None, k=k, x_first=x_first):
                spot = (k, core, b_pos, a_pos) if x_first else (k, core, a_pos, b_pos)
                return all_hbm.at[spot + (() if part_rows is None else (pl.ds(*part_rows),))]

            def bundle(core, b_pos, first=0, count=RING, k=k, x_first=x_first):
                return all_hbm.at[(k, core, b_pos, pl.ds(first, count)) if x_first else (k, core, pl.ds(first, count), b_pos)]

            source = fin.at[pl.ds(k * r, r)]
            keep = pltpu.make_async_copy(source, place(c, b, a), loc_sem.at[first_sem + k])
            top, low = (0, h), (h, h)
            a0 = transfer(*a_plus, source, place(c, b, a), source, place(c, b, a_down))
            a1 = transfer(*a_minus, source, place(c, b, a), source, place(c, b, a_up))
            h0 = moved(*a_plus, place(c, b, a_down, top), place(c, b, a_far, top))
            h1 = moved(*a_minus, place(c, b, a_up, low), place(c, b, a_far, low))
            b0 = moved(*b_plus, bundle(c, b, 0, 2), bundle(c, b_down, 0, 2))
            b1 = moved(*b_minus, bundle(c, b, 2, 2), bundle(c, b_up, 2, 2))
            b2 = moved(*b_plus, bundle(c, b, 2, 2), bundle(c, b_down, 2, 2))
            b3 = moved(*b_minus, bundle(c, b, 0, 2), bundle(c, b_up, 0, 2))
            if one_side:
                far = [moved('left', me.at(y, turn(x + 2 * p, -1), c), bundle(c, xn), bundle(c, b_far))]
                forwards = [Step([b0, b1, b2, b3], None, far, bulk=True)]
            else:
                far = [moved(*b_plus, bundle(c, b_down, 0, 2), bundle(c, b_far, 0, 2)),
                       moved(*b_minus, bundle(c, b_up, 2, 2), bundle(c, b_far, 2, 2))]
                forwards = [Step([b0], None, far[:1], bulk=True), Step([b1], None, far[1:], bulk=True), Step([b2, b3])]
            cores = [moved('core', to_partner, bundle(c, pos), bundle(other, pos)) for pos in (b, b_down, b_up, b_far)]
            threads.append([
                Step((), keep.start, [a0, a1], (done[k],), 0.1, True),
                Step([a0], None, [h0], bulk=True), Step([a1], None, [h1], bulk=True),
                Step([h0, h1], keep.wait, [b0, b1, b2, b3, cores[0]], cost=0.1, bulk=True),
                *forwards, Step((), None, cores[1:3]), Step(far, None, cores[3:]), Step(cores)])
        return threads

    forward, done_f, sums_f, _ = add_pass(False, gath_f, wb_f, ring_f, fin_f, spreads[0], None)
    backward, done_b, _, begun = add_pass(True, gath_b, wb_b, ring_b, fin_b, spreads[1], (done_f, sums_f))
    spread_f = add_spread(out_all, fin_f, spreads[0], done_f, keep_sem, X_FIRST[0])
    spread_b = add_spread(grad_all, fin_b, spreads[1], done_b, keep_sem + spreads[0], X_FIRST[1])
    swap = transfer('right', me.at(y, xn, c), gath_b.at[own_b, pl.ds(RING, 2)], kv_far.at[c])
    swap_core = moved('core', to_partner, kv_far.at[c], kv_far.at[other])
    swaps = [[Step((), None, [swap], begun, bulk=True), Step([swap], None, [swap_core]), Step([swap_core])]]
    passes = []
    for k in range(chunks + LAG):
        passes += forward[k:k + 1] + (backward[k - LAG:k - LAG + 1] if k >= LAG else [])
    for step in in_order(kv_threads + passes + [attention] + spread_b + spread_f + swaps):
        for copy in step.waits:
            copy.incoming().wait_recv()
        if step.work is not None:
            step.work()
        for copy in step.sends:
            copy.outgoing().start()

    kv_copies = []
    for core in range(CORES):
        for src, place in ((gath_b.at[CORES * y + core, pl.ds(RING, 2)], CORES * core + p), (kv_far.at[core], CORES * core + 1 - p)):
            kv_copies.append(pltpu.make_async_copy(src, kv_out.at[:, place], loc_sem.at[len(kv_copies)]))
    kv_copies.append(pltpu.make_async_copy(grad_q_ref, grad_q_out, loc_sem.at[len(kv_copies)]))
    for copy in kv_copies:
        copy.start()
    for copy in kv_copies:
        copy.wait()
    gone([copy for copy in transfers if not copy.left])


def exchange(heads, q, k, v, grad_heads, cos_l, sin_l, w_blocks, w_key, w_value, x_rows, dout_rows, inv, gain, spread=None):
    tokens, d_model = x_rows.shape
    rows_y, width = tokens // RING, d_model // ROW_DEVICES
    chunks = CHUNKS
    spreads = (chunks, SPREAD if spread is None else spread)
    r = rows_y // chunks
    any_spec = pl.BlockSpec(memory_space=pl.ANY)
    vmem_spec = pl.BlockSpec(memory_space=pltpu.VMEM)
    depth, n_kv = ROW_DEVICES * HEAD_DIM, w_key.shape[1]
    f32, bf16 = jnp.float32, jnp.bfloat16

    def gathered(count):
        return jax.ShapeDtypeStruct((count, CORES, RING, RING, r, width), f32)

    passes = chunks * (8 + 2 * (RING - 1))
    copies = 2 * passes + chunks * (2 + ROW_DEVICES - 1) + 14 * sum(spreads) + 2
    dma = pltpu.SemaphoreType.DMA
    sums = pltpu.VMEM((2, RING - 1, chunks, r // 2, width), f32)
    return pl.pallas_call(
        functools.partial(exchange_kernel, chunks, spreads),
        out_shape=[jax.ShapeDtypeStruct(((chunks - spreads[1]) * r + 8, width), f32), gathered(spreads[0]), gathered(spreads[1]),
                   jax.ShapeDtypeStruct((2, RING, rows_y, HEAD_DIM), f32), jax.ShapeDtypeStruct(q.shape, bf16)],
        in_specs=[any_spec] * 14,
        out_specs=[vmem_spec, any_spec, any_spec, any_spec, any_spec],
        scratch_shapes=[
            pltpu.VMEM((ROW_DEVICES, RING, rows_y, HEAD_DIM), f32),
            pltpu.VMEM((ROW_DEVICES, RING + 2, rows_y, HEAD_DIM), f32),
            pltpu.VMEM((depth, width), bf16), pltpu.VMEM((depth + n_kv, width), bf16),
            pltpu.VMEM((RING, rows_y, width), f32), sums, sums,
            pltpu.VMEM((spreads[0] * r, width), f32), pltpu.VMEM((spreads[1] * r, width), f32),
            pltpu.VMEM((2, rows_y, width), bf16), pltpu.VMEM((rows_y, width), bf16), pltpu.VMEM((rows_y, 1), f32), pltpu.VMEM((1, width), f32),
            pltpu.VMEM(q.shape, bf16), pltpu.VMEM(q.shape, bf16), pltpu.VMEM(q.shape, bf16), pltpu.VMEM(q.shape, bf16),
            pltpu.VMEM(cos_l.shape, f32), pltpu.VMEM(cos_l.shape, f32), pltpu.VMEM(q.shape, bf16),
            pltpu.VMEM((RING, 2, rows_y, HEAD_DIM), f32), pltpu.VMEM((CORES, 2, rows_y, HEAD_DIM), f32),
            pltpu.VMEM((2, rows_y, HEAD_DIM), f32), pltpu.VMEM((2, rows_y, HEAD_DIM), f32), pltpu.VMEM((CORES, 2, rows_y, HEAD_DIM), f32),
            pltpu.VMEM((chunks, 8, 128), f32), pltpu.VMEM((ROW_DEVICES - 1, chunks, 8, 128), f32),
            pltpu.VMEM((2, RING, width, HEAD_DIM), bf16),
            dma((copies,)), dma((copies,)), dma((3 * ROW_DEVICES + 12 + sum(spreads),))],
        compiler_params=pltpu.CompilerParams(collective_id=1, has_side_effects=True, vmem_limit_bytes=VMEM_BYTES),
        cost_estimate=pl.CostEstimate(flops=2 * tokens * (2 * depth + n_kv) * width, bytes_accessed=16 * tokens * width, transcendentals=0),
        name='exchange',
    )(heads, q, k, v, grad_heads, cos_l, sin_l, w_blocks, w_key, w_value, x_rows, dout_rows, inv, gain)


def rounded(kernel, gathered, grid, block, index_map, out_rows, place_of, rows, so_far):
    d_model = ROW_DEVICES * gathered.shape[-1]
    moved_rows = math.prod(grid) * out_rows
    return pl.pallas_call(
        kernel, grid=grid,
        in_specs=[pl.BlockSpec(block, index_map)] + ([pl.BlockSpec(memory_space=pl.ANY)] if so_far is not None else []),
        out_specs=pl.BlockSpec((out_rows, d_model), lambda *at: (place_of(*at), 0)),
        out_shape=jax.ShapeDtypeStruct((rows, d_model), jnp.bfloat16),
        input_output_aliases={1: 0} if so_far is not None else {},
        compiler_params=pltpu.CompilerParams(vmem_limit_bytes=VMEM_BYTES),
        cost_estimate=pl.CostEstimate(flops=moved_rows * d_model, bytes_accessed=6 * moved_rows * d_model, transcendentals=0),
        name='narrow',
    )(*((gathered,) if so_far is None else (gathered, so_far)))


def narrow_spread(gathered, spread, rows, by_y, so_far=None):
    r, width = gathered.shape[-2:]
    chunks = rows // RING // r
    group = max(n for n in range(1, 5) if math.gcd(spread, chunks) % n == 0)
    block = (group, CORES, 1, RING, r, width) if by_y else (group, CORES, RING, 1, r, width)

    def kernel(in_ref, *rest):
        for k in range(group):
            for n in range(ROW_DEVICES):
                at = (k, n % CORES) + ((0, n // CORES) if by_y else (n // CORES, 0))
                rest[-1][pl.ds(k * r, r), pl.ds(n * width, width)] = in_ref[at].astype(jnp.bfloat16)

    return rounded(kernel, gathered, (spread // group, RING), block,
                   lambda k, i: (k, 0, i, 0, 0, 0) if by_y else (k, 0, 0, i, 0, 0),
                   group * r, lambda k, i: i * chunks // group + k, rows, so_far)


def narrow_rest(gathered, spread, r, rows, so_far):
    width = gathered.shape[-1]
    count = rows // RING // r - spread
    blocks = gathered.reshape(RING, RING, CORES, count * r + 8, width)
    places = rows // RING // (count * r)

    def kernel(in_ref, so_far_ref, out_ref, gain_ref):
        @pl.when(pl.program_id(0) == 0)
        def _():
            gain_ref[...] = jnp.zeros_like(gain_ref)

        for n in range(ROW_DEVICES):
            columns = pl.ds(n * width, width)
            out_ref[:, columns] = in_ref[n // CORES, 0, n % CORES, pl.ds(0, count * r), :].astype(jnp.bfloat16)
            gain_ref[:, columns] += in_ref[n // CORES, 0, n % CORES, pl.ds(count * r, 1), :]

    d_model = ROW_DEVICES * width
    return pl.pallas_call(
        kernel, grid=(RING,),
        in_specs=[pl.BlockSpec((RING, 1, CORES, count * r + 8, width), lambda x: (0, x, 0, 0, 0)), pl.BlockSpec(memory_space=pl.ANY)],
        out_specs=(pl.BlockSpec((count * r, d_model), lambda x: (x * places + spread // count, 0)), pl.BlockSpec((1, d_model), lambda x: (0, 0))),
        out_shape=(jax.ShapeDtypeStruct((rows, d_model), jnp.bfloat16), jax.ShapeDtypeStruct((1, d_model), jnp.float32)),
        input_output_aliases={1: 0}, compiler_params=pltpu.CompilerParams(vmem_limit_bytes=VMEM_BYTES),
        cost_estimate=pl.CostEstimate(flops=RING * count * r * d_model, bytes_accessed=6 * RING * count * r * d_model, transcendentals=0),
        name='narrow',
    )(blocks, so_far)


def solution(mesh):
    assert mesh.shape['tp'] == RING * RING * CORES

    def block_fn(hidden, grad_out, norm_gain, w_query, w_key, w_value, w_out):
        batch, seq_len, d_model = hidden.shape
        tokens, width = batch * seq_len, d_model // ROW_DEVICES
        rows_y = tokens // RING

        cos_l, sin_l = rope_lanes(seq_len)
        grad_rows = grad_out.reshape(tokens, d_model)

        inv_rms, q_rot, k_rot, v_head, grad_heads, heads, heads_send, gain, w_blocks = project(
            hidden.reshape(tokens, d_model), grad_rows, norm_gain.reshape(1, d_model), w_query, w_key, w_value, w_out, cos_l, sin_l)
        rest_block, out_spread, grad_spread, grad_kv, grad_q = exchange(
            heads_send.reshape(RING, rows_y, HEAD_DIM), q_rot, k_rot, v_head, grad_heads, cos_l, sin_l,
            w_blocks, w_key, w_value, hidden.reshape(tokens, d_model), grad_rows, inv_rms, gain)
        grad_rest = lax.all_gather(rest_block, 'tp', axis=0, tiled=True)
        r = rows_y // CHUNKS
        block_out = narrow_spread(out_spread, CHUNKS, tokens, True).reshape(hidden.shape)
        grad_hidden, gain_rows = narrow_rest(grad_rest, SPREAD, r, tokens, narrow_spread(grad_spread, SPREAD, tokens, False))
        grad_hidden, grad_gain = grad_hidden.reshape(hidden.shape), gain_rows.reshape(d_model)
        grad_w_query, grad_w_key, grad_w_value, grad_w_out = weight_grads(
            hidden.reshape(tokens, d_model), inv_rms, gain, grad_rows, grad_q, grad_kv.reshape(2, tokens, HEAD_DIM), heads)
        return block_out, grad_hidden, grad_gain, grad_w_query, grad_w_key, grad_w_value, grad_w_out

    act_spec = P('dp', None, None)
    return jax.shard_map(
        block_fn, mesh=mesh,
        in_specs=(act_spec, act_spec, P(None), P(None, 'tp'), P(None, None), P(None, None), P('tp', None)),
        out_specs=(act_spec, act_spec, P('dp'), P('dp', 'tp'), P('dp', 'tp'), P('dp', 'tp'), P(('dp', 'tp'), None)),
        check_vma=False)
```

```python
import functools
import math
import jax
import jax.numpy as jnp
from jax import lax
from jax.experimental import pallas as pl
from jax.experimental.pallas import tpu as pltpu
from jax.sharding import PartitionSpec as P

HEAD_DIM = 128
NORM_EPS = 1.0e-5
ROPE_BASE = 10000.0
MASK_VALUE = -1.0e30
SCORE_SCALE = 1.0 / math.sqrt(HEAD_DIM)
RING = 4
CORES = 2
ROW_DEVICES = RING * CORES
CHUNKS = 9
AHEAD = 3
SPREAD = 6
X_FIRST = ('010110011', '000011')
LAG = 4
VMEM_BYTES = 62 * 1024 * 1024


def rope_lanes(seq_len):
    lane = lax.broadcasted_iota(jnp.int32, (1, HEAD_DIM), 1)
    inv_freq = ROPE_BASE ** (-(lane - lane % 2).astype(jnp.float32) / HEAD_DIM)
    angles = jnp.arange(seq_len, dtype=jnp.float32)[:, None] * inv_freq
    return jnp.cos(angles), jnp.where(lane % 2 == 0, -jnp.sin(angles), jnp.sin(angles))


def rotate(tensor, cos_l, sin_l):
    lane = lax.broadcasted_iota(jnp.int32, tensor.shape, 1)
    swapped = jnp.where(lane % 2 == 0, pltpu.roll(tensor, HEAD_DIM - 1, 1), pltpu.roll(tensor, 1, 1))
    return tensor * cos_l + swapped * sin_l


NT = (((1,), (1,)), ((), ()))
TN = (((0,), (0,)), ((), ()))


def weight_grads(hidden, inv, gain, grad_out, grad_q, grad_kv, heads):
    tokens, d_model = hidden.shape
    columns = 512

    def kernel(x_ref, inv_ref, gain_ref, dout_ref, dq_ref, dkv_ref, o_ref, wq_ref, wk_ref, wv_ref, wo_ref, left_ref):
        @pl.when(pl.program_id(0) == 0)
        def _():
            pieces = (dq_ref[...].astype(jnp.float32), dkv_ref[0], dkv_ref[1], o_ref[...].astype(jnp.float32))
            for n, piece in enumerate(pieces):
                left_ref[pl.ds(n * HEAD_DIM, HEAD_DIM), :] = jnp.transpose(piece).astype(jnp.bfloat16)

        normed = (x_ref[...].astype(jnp.float32) * inv_ref[...] * gain_ref[...]).astype(jnp.bfloat16)
        grads = jnp.dot(left_ref[pl.ds(0, 3 * HEAD_DIM), :], normed, preferred_element_type=jnp.float32)
        for n, ref in enumerate((wq_ref, wk_ref, wv_ref)):
            ref[...] = jnp.transpose(grads[n * HEAD_DIM:(n + 1) * HEAD_DIM])
        wo_ref[...] = jnp.dot(left_ref[pl.ds(3 * HEAD_DIM, HEAD_DIM), :], dout_ref[...], preferred_element_type=jnp.float32)

    wide = pl.BlockSpec((tokens, columns), lambda i: (0, i))
    tall = pl.BlockSpec((columns, HEAD_DIM), lambda i: (i, 0))
    head = pl.BlockSpec((tokens, HEAD_DIM), lambda i: (0, 0))
    tall_out = jax.ShapeDtypeStruct((d_model, HEAD_DIM), jnp.float32)
    return pl.pallas_call(
        kernel, grid=(d_model // columns,),
        in_specs=[wide, pl.BlockSpec((tokens, 1), lambda i: (0, 0)), pl.BlockSpec((1, columns), lambda i: (0, i)), wide, head,
                  pl.BlockSpec((2, tokens, HEAD_DIM), lambda i: (0, 0, 0)), head],
        out_specs=(tall, tall, tall, pl.BlockSpec((HEAD_DIM, columns), lambda i: (0, i))),
        out_shape=(tall_out, tall_out, tall_out, jax.ShapeDtypeStruct((HEAD_DIM, d_model), jnp.float32)),
        scratch_shapes=[pltpu.VMEM((4 * HEAD_DIM, tokens), jnp.bfloat16)],
        compiler_params=pltpu.CompilerParams(vmem_limit_bytes=VMEM_BYTES),
        cost_estimate=pl.CostEstimate(flops=8 * tokens * d_model * HEAD_DIM, bytes_accessed=4 * tokens * d_model, transcendentals=0),
        name='weight_grads',
    )(hidden, inv, gain, grad_out, grad_q, grad_kv, heads)


class Place:
    def __init__(self):
        index = lax.axis_index('tp')
        self.c = lax.rem(index, CORES)
        self.x = lax.rem(index // CORES, RING)
        self.y = index // ROW_DEVICES

    def at(self, y, x, c):
        return {'tp': (y * RING + x) * CORES + c}


def turn(position, by):
    return lax.rem(position + (by % RING), RING)


def softmax_rows(q, k, first):
    scores = lax.dot_general(q, k, NT, preferred_element_type=jnp.float32) * SCORE_SCALE
    row = lax.broadcasted_iota(jnp.int32, scores.shape, 0) + first
    col = lax.broadcasted_iota(jnp.int32, scores.shape, 1)
    scores = jnp.where(row >= col, scores, MASK_VALUE)
    weight = jnp.exp(scores - jnp.max(scores, axis=1, keepdims=True))
    return weight * (1.0 / jnp.sum(weight, axis=1, keepdims=True))


def project(hidden, grad_out, gain, w_query, w_key, w_value, w_out, cos_l, sin_l):
    tokens, d_model = hidden.shape
    seq_len = cos_l.shape[0]
    rows = 128
    steps = tokens // rows
    width = d_model // ROW_DEVICES
    sharers = RING * ROW_DEVICES // (w_key.shape[1] // HEAD_DIM)

    def kernel(x_ref, dout_ref, gain_ref, cos_ref, sin_ref, wq_hbm, wk_hbm, wv_hbm, wo_hbm,
               inv_ref, q_ref, k_ref, v_ref, do_ref, o_ref, o_send, gain_out, got_hbm, w_ref, wo_ref, blocks, loc_sem, send_sem, recv_sem):
        me = Place()
        here = pl.ds(pl.multiple_of(pl.program_id(0) * rows, rows), rows)
        others = [(by, flip) for by in (2, 1, 3) for flip in (0, 1)] + [(0, 1)]

        def exchanges(which):
            here = me.x if which == 0 else me.y
            for n, (by, flip) in enumerate(others):
                core = 1 - me.c if flip else me.c
                there, origin = turn(here, by), turn(here, -by)
                peer = me.at(me.y, there, core) if which == 0 else me.at(there, me.x, core)

                def copy(dst, which=which, n=n, peer=peer, src=CORES * there + core):
                    return pltpu.make_async_remote_copy(
                        src_ref=blocks.at[which, src], dst_ref=got_hbm.at[which, dst], send_sem=send_sem.at[which, n],
                        recv_sem=recv_sem.at[which, n], device_id=peer, device_id_type=pl.DeviceIdType.MESH)
                yield copy(CORES * here + me.c), copy(CORES * origin + core)

        def kept(which):
            own = CORES * (me.x if which == 0 else me.y) + me.c
            return pltpu.make_async_copy(blocks.at[which, own], got_hbm.at[which, own], loc_sem.at[which])

        @pl.when(pl.program_id(0) == 0)
        def _():
            barrier = pltpu.get_barrier_semaphore()
            peers = [me.at(me.y, turn(me.x, by), 1 - me.c if flip else me.c) for by, flip in others]
            peers += [me.at(turn(me.y, by), me.x, 1 - me.c if flip else me.c) for by, flip in others[:-1]]
            for peer in peers:
                pl.semaphore_signal(barrier, inc=1, device_id=peer, device_id_type=pl.DeviceIdType.MESH)
            head = lax.axis_index('tp') // sharers
            kv_columns = pl.ds(pl.multiple_of(head * HEAD_DIM, HEAD_DIM), HEAD_DIM)
            loads = [pltpu.make_async_copy(src, dst, loc_sem.at[n]) for n, (src, dst) in enumerate((
                (wo_hbm, wo_ref), (wq_hbm, w_ref.at[:, pl.ds(0, HEAD_DIM)]),
                (wk_hbm.at[:, kv_columns], w_ref.at[:, pl.ds(HEAD_DIM, HEAD_DIM)]),
                (wv_hbm.at[:, kv_columns], w_ref.at[:, pl.ds(2 * HEAD_DIM, HEAD_DIM)])))]
            for load in loads:
                load.start()
            for load in loads:
                load.wait()
            for j in range(ROW_DEVICES):
                columns = pl.ds(j * width, width)
                blocks[0, j] = wo_ref[:, columns].astype(jnp.float32)
                blocks[1, j] = jnp.transpose(w_ref[columns, pl.ds(0, HEAD_DIM)].astype(jnp.float32))
            pl.semaphore_wait(barrier, len(peers))
            for which in (0, 1):
                for out, _ in exchanges(which):
                    out.start()
                kept(which).start()

        values = x_ref[...].astype(jnp.float32)
        inv = lax.rsqrt(jnp.mean(values * values, axis=1, keepdims=True) + NORM_EPS)
        inv_ref[...] = inv
        wide_gain = gain_ref[...].astype(jnp.float32)
        gain_out[...] = wide_gain
        normed = (values * inv * wide_gain).astype(jnp.bfloat16)
        heads = jnp.dot(normed, w_ref[...], preferred_element_type=jnp.float32)
        q_ref[here, :] = rotate(heads[:, :HEAD_DIM], cos_ref[...], sin_ref[...]).astype(jnp.bfloat16)
        k_ref[here, :] = rotate(heads[:, HEAD_DIM:2 * HEAD_DIM], cos_ref[...], sin_ref[...]).astype(jnp.bfloat16)
        v_ref[here, :] = heads[:, 2 * HEAD_DIM:].astype(jnp.bfloat16)
        do_ref[...] = lax.dot_general(dout_ref[...], wo_ref[...], NT, preferred_element_type=jnp.float32).astype(jnp.bfloat16)

        @pl.when(pl.program_id(0) == steps - 1)
        def _():
            for base in range(0, tokens, seq_len):
                rows_of = pl.ds(base, seq_len)
                probs = softmax_rows(q_ref[rows_of, :], k_ref[rows_of, :], 0).astype(jnp.bfloat16)
                attended = jnp.dot(probs, v_ref[rows_of, :], preferred_element_type=jnp.float32).astype(jnp.bfloat16)
                o_ref[rows_of, :] = attended
                o_send[rows_of, :] = attended.astype(jnp.float32)
            for which in (0, 1):
                for out, came in exchanges(which):
                    came.wait_recv()
                    out.wait_send()
                kept(which).wait()

    row_spec = pl.BlockSpec((rows, d_model), lambda i: (i, 0))
    head_spec = pl.BlockSpec((rows, HEAD_DIM), lambda i: (i, 0))
    table_spec = pl.BlockSpec((rows, HEAD_DIM), lambda i: (i % (seq_len // rows), 0))
    all_rows = pl.BlockSpec((tokens, HEAD_DIM), lambda i: (0, 0))
    any_spec = pl.BlockSpec(memory_space=pl.ANY)
    head = jax.ShapeDtypeStruct((tokens, HEAD_DIM), jnp.bfloat16)
    blocks = (2, ROW_DEVICES, HEAD_DIM, width)
    dma = pltpu.SemaphoreType.DMA
    return pl.pallas_call(
        kernel, grid=(steps,),
        in_specs=[row_spec, row_spec, pl.BlockSpec((1, d_model), lambda i: (0, 0)), table_spec, table_spec] + [any_spec] * 4,
        out_specs=(pl.BlockSpec((rows, 1), lambda i: (i, 0)), all_rows, all_rows, all_rows, head_spec, all_rows, all_rows,
                   pl.BlockSpec((1, d_model), lambda i: (0, 0)), any_spec),
        out_shape=(jax.ShapeDtypeStruct((tokens, 1), jnp.float32), head, head, head, head, head,
                   jax.ShapeDtypeStruct((tokens, HEAD_DIM), jnp.float32), jax.ShapeDtypeStruct((1, d_model), jnp.float32),
                   jax.ShapeDtypeStruct(blocks, jnp.float32)),
        scratch_shapes=[pltpu.VMEM((d_model, 3 * HEAD_DIM), jnp.bfloat16), pltpu.VMEM((HEAD_DIM, d_model), jnp.bfloat16),
                        pltpu.VMEM(blocks, jnp.float32), dma((4,)), dma((2, 7)), dma((2, 7))],
        compiler_params=pltpu.CompilerParams(collective_id=2, has_side_effects=True, vmem_limit_bytes=VMEM_BYTES),
        cost_estimate=pl.CostEstimate(flops=8 * tokens * d_model * HEAD_DIM, bytes_accessed=6 * tokens * d_model, transcendentals=0),
        name='project',
    )(hidden, grad_out, gain, cos_l, sin_l, w_query, w_key, w_value, w_out)


class Transfer:
    def __init__(self, link, size, outgoing, incoming=None):
        self.link, self.size, self.outgoing, self.incoming = link, size, outgoing, incoming or outgoing
        self.left = False


class Step:
    def __init__(self, waits=(), work=None, sends=(), after=(), cost=0.05, bulk=False):
        self.waits, self.work, self.sends, self.after, self.cost, self.bulk = waits, work, sends, after, cost, bulk


LINK_RATE = 45e3
CORE_RATE = 300e3
HOP = 2.5
CORE_HOP = 2.0
QUEUE = 12.0
STEP = 0.1


def in_order(threads):
    now, busy, arrival, finished, order = 4.0, {}, {}, set(), []
    position = [0] * len(threads)
    while any(position[i] < len(threads[i]) for i in range(len(threads))):
        chosen, soonest = None, math.inf
        for i, steps in enumerate(threads):
            if position[i] == len(steps) or any(step not in finished for step in steps[position[i]].after):
                continue
            step = steps[position[i]]
            ready = max([arrival.get(copy, math.inf) for copy in step.waits], default=0.0)
            if step.bulk:
                ready = max([ready] + [busy.get(copy.link, 0.0) - QUEUE for copy in step.sends if copy.link != 'core'])
            if ready <= now:
                chosen = i
                break
            soonest = min(soonest, ready)
        if chosen is None:
            now = soonest
            continue
        step = threads[chosen][position[chosen]]
        position[chosen] += 1
        now += step.cost + STEP
        for copy in step.sends:
            rate, hop = (CORE_RATE, CORE_HOP) if copy.link == 'core' else (LINK_RATE, HOP)
            busy[copy.link] = max(now, busy.get(copy.link, 0.0)) + copy.size / rate
            arrival[copy] = busy[copy.link] + hop
        finished.add(step)
        order.append(step)
    return order


def exchange_kernel(chunks, spreads, *refs):
    (heads_hbm, q_hbm, k_hbm, v_hbm, do_hbm, cos_hbm, sin_hbm, w_hbm, w_key_hbm, w_value_hbm, x_hbm, dout_hbm, inv_hbm, gain_hbm,
     rest_ref, out_all, grad_all, kv_out, grad_q_out,
     gath_f, gath_b, wb_f, wb_b, part, ring_f, ring_b, fin_f, fin_b, x_ref, dout_ref, inv_ref, gain_ref,
     q_ref, k_ref, v_ref, do_ref, cos_ref, sin_ref, grad_q_ref, kvp, kv_core, kv_send, kv_chip, kv_far, rowpart, rowall, w_kv, send_sem, recv_sem, loc_sem) = refs
    me = Place()
    x, y, c = me.x, me.y, me.c
    xr, xl, xo = turn(x, 1), turn(x, -1), turn(x, 2)
    yu, yd, yo = turn(y, 1), turn(y, -1), turn(y, 2)
    other = 1 - c
    rows_y, width = x_ref.shape[1:]
    r = rows_y // chunks
    h = r // 2
    to_right, to_left, to_partner = me.at(y, xr, c), me.at(y, xl, c), me.at(y, x, other)
    to_up, to_down = me.at(yu, x, c), me.at(yd, x, c)
    along_x = (('right', to_right), ('left', to_left), x, xr, xl, xo)
    along_y = (('up', to_up), ('down', to_down), y, yu, yd, yo)

    barrier = pltpu.get_barrier_semaphore()
    peers = [to_up, to_down, to_right, to_left, to_partner,
             me.at(yo, x, c), me.at(yu, x, other), me.at(yd, x, other), me.at(yo, x, other)]
    for peer in peers:
        pl.semaphore_signal(barrier, inc=1, device_id=peer, device_id_type=pl.DeviceIdType.MESH)

    depth = ROW_DEVICES * HEAD_DIM
    own_f, own_b = CORES * x + c, CORES * y + c

    def rows_at(position):
        return pl.ds(pl.multiple_of(position * rows_y, rows_y), rows_y)

    def columns_at(block):
        return pl.ds(pl.multiple_of(block * width, width), width)

    def head_at(head):
        return pl.ds(pl.multiple_of(head * HEAD_DIM, HEAD_DIM), HEAD_DIM)

    per_slot = rows_y // HEAD_DIM

    def stage(which, j):
        return part.at[2 * which + j // per_slot, pl.ds(j % per_slot * HEAD_DIM, HEAD_DIM)]

    copies = [(w_hbm.at[which, j], stage(which, j)) for which in (0, 1) for j in range(ROW_DEVICES)]
    copies += [(w.at[columns_at(own_b), head_at(2 * j + x // 2)], w_kv.at[s, j])
               for s, w in enumerate((w_key_hbm, w_value_hbm)) for j in range(RING)]
    copies += [
        (heads_hbm, gath_f.at[own_f, pl.ds(0, RING)]), (q_hbm, q_ref), (k_hbm, k_ref), (v_hbm, v_ref),
        (do_hbm, do_ref), (cos_hbm, cos_ref), (sin_hbm, sin_ref),
        (x_hbm.at[rows_at(y), columns_at(own_f)], x_ref.at[0]), (x_hbm.at[rows_at(x), columns_at(own_b)], x_ref.at[1]),
        (dout_hbm.at[rows_at(x), columns_at(own_b)], dout_ref), (inv_hbm.at[rows_at(x)], inv_ref), (gain_hbm.at[:, columns_at(own_b)], gain_ref)]
    loads = [pltpu.make_async_copy(src, dst, loc_sem.at[n]) for n, (src, dst) in enumerate(copies)]
    keep_sem = len(loads)
    for copy in loads:
        copy.start()
    first_rest = (chunks - spreads[1]) * r
    rest_ref[pl.ds(first_rest, 8), :] = jnp.zeros((8, width), jnp.float32)
    for copy in loads:
        copy.wait()
    for which, weights in enumerate((wb_f, wb_b)):
        for j in range(ROW_DEVICES):
            weights[pl.ds(j * HEAD_DIM, HEAD_DIM), :] = stage(which, j)[...].astype(jnp.bfloat16)
    for j in range(RING):
        for s in (0, 1):
            weights = jnp.transpose(w_kv[s, j].astype(jnp.float32)).astype(jnp.bfloat16)
            wb_b[pl.ds(depth + (2 * j + s) * HEAD_DIM, HEAD_DIM), :] = weights
    pl.semaphore_wait(barrier, len(peers))

    transfers = []

    def transfer(link, peer, src, dst, came_from=None, came_to=None):
        n = len(transfers)

        def copy(a, b):
            return lambda: pltpu.make_async_remote_copy(
                src_ref=a, dst_ref=b, send_sem=send_sem.at[n], recv_sem=recv_sem.at[n], device_id=peer,
                device_id_type=pl.DeviceIdType.MESH)
        made = Transfer(link, 4 * math.prod(dst.shape), copy(src, dst), copy(came_from, came_to) if came_to is not None else None)
        transfers.append(made)
        return made

    def moved(link, peer, sent, came):
        return transfer(link, peer, sent, sent, came, came)

    def gone(sent):
        for copy in sent:
            copy.outgoing().wait_send()
            copy.left = True

    seq_len = cos_ref.shape[0]
    run = seq_len // RING

    def spot(first):
        return first // rows_y, pl.ds(first % rows_y, run)

    def attend_back(base, first):
        here, keys = pl.ds(base + first, run), pl.ds(base, first + run)
        q_rows, k_rows, v_rows, grad = q_ref[here, :], k_ref[keys, :], v_ref[keys, :], do_ref[here, :]
        probs = softmax_rows(q_rows, k_rows, first)
        grad_probs = lax.dot_general(grad, v_rows, NT, preferred_element_type=jnp.float32)
        row_dot = jnp.sum(probs * grad_probs, axis=1, keepdims=True)
        grad_scores = (probs * (grad_probs - row_dot) * SCORE_SCALE).astype(jnp.bfloat16)
        at = pl.ds(first, run)
        grad_q = rotate(jnp.dot(grad_scores, k_rows, preferred_element_type=jnp.float32), cos_ref[at, :], -sin_ref[at, :])
        grad_q = grad_q.astype(jnp.bfloat16)
        grad_q_ref[here, :] = grad_q
        d, rows = spot(base + first)
        gath_b[own_b, d, rows, :] = grad_q.astype(jnp.float32)
        terms = (lax.dot_general(grad_scores, q_rows, TN, preferred_element_type=jnp.float32),
                 lax.dot_general(probs.astype(jnp.bfloat16), grad, TN, preferred_element_type=jnp.float32))
        for n, term in enumerate(terms):
            for key in range(0, first + run, run):
                d, rows = spot(base + key)
                piece = term[key:key + run]
                kvp[d, n, rows, :] = piece if key == first else kvp[d, n, rows, :] + piece

    def rotate_keys(base):
        for first in range(0, seq_len, run):
            d, rows = spot(base + first)
            at = pl.ds(first, run)
            kvp[d, 0, rows, :] = rotate(kvp[d, 0, rows, :], cos_ref[at, :], -sin_ref[at, :])

    attention = []
    for base in range(0, RING * rows_y, seq_len):
        attention += [Step((), functools.partial(attend_back, base, first), cost=0.8) for first in range(0, seq_len, run)]
        attention.append(Step((), functools.partial(rotate_keys, base), cost=0.3))

    p = lax.rem(x, 2)
    xn = x + 1 - 2 * p
    mine, theirs = CORES * c + p, CORES * c + 1 - p
    kv_threads, settle, settled = [], [], []
    for k in range(chunks):
        rows = pl.ds(k * r, r)
        core_copy = transfer('core', to_partner, kvp.at[pl.ds(CORES * other, CORES), :, rows], kv_core.at[:, :, rows])
        chip_copy = transfer('right', me.at(y, xn, c), kv_send.at[:, rows], kv_chip.at[:, rows])

        def add_core(rows=rows):
            kv_send[:, rows, :] = kvp[theirs, :, rows, :] + kv_core[1 - p, :, rows, :]

        def add_chip(rows=rows):
            total = kvp[mine, :, rows, :] + kv_core[p, :, rows, :] + kv_chip[:, rows, :]
            gath_b[own_b, pl.ds(RING, 2), rows, :] = total.astype(jnp.bfloat16).astype(jnp.float32)

        kv_threads.append([Step(sends=[core_copy], after=attention[-1:]), Step([core_copy], add_core, [chip_copy], cost=0.1, bulk=True)])
        settle.append(add_chip)
        settled.append(chip_copy)

    def add_pass(backward, gath, wb, ring, fin, spread, ahead_of):
        gather_ring, sum_ring = (along_y, along_x) if backward else (along_x, along_y)
        g_plus, g_minus, g, g_up, g_down, g_far = gather_ring
        s_plus, s_minus, s, s_up, s_down, s_far = sum_ring
        own, left, right, far = [CORES * pos + c for pos in (g, g_down, g_up, g_far)]
        p_own, p_left, p_right, p_far = [CORES * pos + other for pos in (g, g_down, g_up, g_far)]
        parts = gath.shape[1]
        half = parts // 2
        threads, passed, done, ring_sums, begun = [], [], [], [], []
        x_block = x_ref.at[1 if backward else 0]

        def multiply(by, k, before=()):
            gone(before)
            d = turn(s, by)
            rows = pl.ds(k * r, r)
            pieces = [gath[j, d, rows, :] for j in range(ROW_DEVICES)]
            if backward and by % 2 == 0:
                pieces += [gath[CORES * j + d // 2, RING + n, rows, :] for j in range(RING) for n in (0, 1)]
            lhs = jnp.concatenate([piece.astype(jnp.bfloat16) for piece in pieces], axis=1)
            part[d, rows, :] = jnp.dot(lhs, wb[pl.ds(0, lhs.shape[1]), :], preferred_element_type=jnp.float32)

        def add_ring(way, step, k):
            d = turn(s, -(2 + step) if way == 0 else 2 + step)
            part[d, pl.ds(k * r + way * h, h), :] += ring[way, step, k]

        def store(k, values):
            if k < spread:
                fin[pl.ds(k * r, r), :] = values
            else:
                rest_ref[pl.ds((k - spread) * r, r), :] = values

        def finish_forward(k):
            rows = pl.ds(k * r, r)
            store(k, (x_block[rows, :].astype(jnp.float32) + part[s, rows, :]).astype(jnp.bfloat16).astype(jnp.float32))

        def row_sums(k):
            rows = pl.ds(k * r, r)
            total = part[s, rows, :]
            unit = x_block[rows, :].astype(jnp.float32) * inv_ref[rows, :]
            row_sum = jnp.sum(total * gain_ref[...] * unit, axis=1, keepdims=True)
            square = jnp.concatenate([jnp.broadcast_to(row_sum, (r, 128)), jnp.zeros((128 - r, 128), jnp.float32)], axis=0)
            rowpart[k] = jnp.transpose(square)[0:8, :]
            gain_row = jnp.sum(total * unit, axis=0, keepdims=True)
            row_id = lax.broadcasted_iota(jnp.int32, (8, width), 0)
            rest_ref[pl.ds(first_rest, 8), :] += jnp.where(row_id == 0, jnp.broadcast_to(gain_row, (8, width)), 0.0)

        def finish_backward(k):
            rows = pl.ds(k * r, r)
            sums = rowpart[k]
            for m in range(ROW_DEVICES - 1):
                sums = sums + rowall[m, k]
            mean = jnp.transpose(sums)[0:r, 0:1] * (1.0 / (width * ROW_DEVICES))
            inv = inv_ref[rows, :]
            unit = x_block[rows, :].astype(jnp.float32) * inv
            delta = inv * (part[s, rows, :] * gain_ref[...] - unit * mean)
            store(k, (dout_ref[rows, :].astype(jnp.float32) + delta).astype(jnp.bfloat16).astype(jnp.float32))

        for k in range(chunks):
            rows = pl.ds(k * r, r)

            def block(source, first=0, count=parts, rows=rows):
                return gath.at[source, pl.ds(first, count), rows]

            s_right = moved(*g_plus, block(own), block(left))
            s_left = moved(*g_minus, block(own), block(right))
            s_core = moved('core', to_partner, block(own), block(p_own))
            f_right = moved(*g_plus, block(left, 0, half), block(far, 0, half))
            f_left = moved(*g_minus, block(right, half, parts - half), block(far, half, parts - half))
            c_left = moved('core', to_partner, block(left), block(p_left))
            c_right = moved('core', to_partner, block(right), block(p_right))
            c_far = moved('core', to_partner, block(far), block(p_far))
            sums = [[transfer(link, peer, part.at[turn(s, -(1 + step) if way == 0 else 1 + step), pl.ds(k * r + way * h, h)],
                              ring.at[way, step, k]) for step in range(RING - 1)]
                    for way, (link, peer) in enumerate((s_plus, s_minus))]
            ring_sums.append(sums[0] + sums[1])
            after = [passed[k - AHEAD]] if k >= AHEAD else []
            before = ()
            if ahead_of is not None:
                after += [ahead_of[0][k], attention[-1]]
                before = ahead_of[1][k]
            steps = [Step([settled[k]] if backward else (), settle[k] if backward else None, [s_right, s_left, s_core], after, 0.1),
                     Step([s_right], None, [f_right, c_left]), Step([s_left], None, [f_left, c_right])]
            begun.append(steps[0])
            passed.append(steps[-1])
            cost = 1.2 * r / 96
            even = 2 * cost if backward else cost
            steps += [Step([f_right, f_left], None, [c_far]),
                      Step([s_core, c_left, c_right, c_far], functools.partial(multiply, -1, k, before), [sums[0][0]], cost=cost),
                      Step((), functools.partial(multiply, 1, k), [sums[1][0]], cost=cost),
                      Step((), functools.partial(multiply, 2, k), cost=even),
                      Step((), functools.partial(multiply, 0, k), cost=even)]
            for step in range(RING - 1):
                for way in (0, 1):
                    steps.append(Step([sums[way][step]], functools.partial(add_ring, way, step, k),
                                      [sums[way][step + 1]] if step < RING - 2 else [], cost=0.15))
            if backward:
                members = [(pos, core) for pos in (yu, yd, yo) for core in (c, other)] + [(y, other)]
                notes = [transfer('note', me.at(pos, x, core), rowpart.at[k], rowall.at[m, k])
                         for (pos, core), m in zip(members, (2, 3, 0, 1, 4, 5, 6))]
                steps.append(Step((), functools.partial(row_sums, k), notes, cost=0.4))
                steps.append(Step(notes, functools.partial(finish_backward, k), cost=0.5))
            else:
                steps.append(Step((), functools.partial(finish_forward, k), cost=0.3))
            done.append(steps[-1])
            threads.append(steps)
        return threads, done, ring_sums, begun

    def add_spread(all_hbm, fin, spread, done, first_sem, x_firsts):
        threads = []
        for k in range(spread):
            x_first = x_firsts[k] == '1'
            ((a_plus, a_minus, a, a_up, a_down, a_far),
             (b_plus, b_minus, b, b_up, b_down, b_far)) = (along_x, along_y) if x_first else (along_y, along_x)

            def place(core, b_pos, a_pos, part_rows=None, k=k, x_first=x_first):
                spot = (k, core, b_pos, a_pos) if x_first else (k, core, a_pos, b_pos)
                return all_hbm.at[spot + (() if part_rows is None else (pl.ds(*part_rows),))]

            def bundle(core, b_pos, first=0, count=RING, k=k, x_first=x_first):
                return all_hbm.at[(k, core, b_pos, pl.ds(first, count)) if x_first else (k, core, pl.ds(first, count), b_pos)]

            source = fin.at[pl.ds(k * r, r)]
            keep = pltpu.make_async_copy(source, place(c, b, a), loc_sem.at[first_sem + k])
            top, low = (0, h), (h, h)
            a0 = transfer(*a_plus, source, place(c, b, a), source, place(c, b, a_down))
            a1 = transfer(*a_minus, source, place(c, b, a), source, place(c, b, a_up))
            h0 = moved(*a_plus, place(c, b, a_down, top), place(c, b, a_far, top))
            h1 = moved(*a_minus, place(c, b, a_up, low), place(c, b, a_far, low))
            b0 = moved(*b_plus, bundle(c, b, 0, 2), bundle(c, b_down, 0, 2))
            b1 = moved(*b_minus, bundle(c, b, 2, 2), bundle(c, b_up, 2, 2))
            b2 = moved(*b_plus, bundle(c, b, 2, 2), bundle(c, b_down, 2, 2))
            b3 = moved(*b_minus, bundle(c, b, 0, 2), bundle(c, b_up, 0, 2))
            g0 = moved(*b_plus, bundle(c, b_down, 0, 2), bundle(c, b_far, 0, 2))
            g1 = moved(*b_minus, bundle(c, b_up, 2, 2), bundle(c, b_far, 2, 2))
            cores = [moved('core', to_partner, bundle(c, pos), bundle(other, pos)) for pos in (b, b_down, b_up, b_far)]
            threads.append([
                Step((), keep.start, [a0, a1], (done[k],), 0.1, True),
                Step([a0], None, [h0], bulk=True), Step([a1], None, [h1], bulk=True),
                Step([h0, h1], keep.wait, [b0, b1, b2, b3, cores[0]], cost=0.1, bulk=True),
                Step([b0], None, [g0], bulk=True), Step([b1], None, [g1], bulk=True),
                Step([b2], None, [cores[1]]), Step([b3], None, [cores[2]]),
                Step([g0, g1], None, [cores[3]]), Step(cores)])
        return threads

    forward, done_f, sums_f, _ = add_pass(False, gath_f, wb_f, ring_f, fin_f, spreads[0], None)
    backward, done_b, _, begun = add_pass(True, gath_b, wb_b, ring_b, fin_b, spreads[1], (done_f, sums_f))
    spread_f = add_spread(out_all, fin_f, spreads[0], done_f, keep_sem, X_FIRST[0])
    spread_b = add_spread(grad_all, fin_b, spreads[1], done_b, keep_sem + spreads[0], X_FIRST[1])
    swap = transfer('right', me.at(y, xn, c), gath_b.at[own_b, pl.ds(RING, 2)], kv_far.at[c])
    swap_core = moved('core', to_partner, kv_far.at[c], kv_far.at[other])
    swaps = [[Step((), None, [swap], begun, bulk=True), Step([swap], None, [swap_core]), Step([swap_core])]]
    passes = []
    for k in range(chunks + LAG):
        passes += forward[k:k + 1] + (backward[k - LAG:k - LAG + 1] if k >= LAG else [])
    for step in in_order(kv_threads + passes + [attention] + spread_b + spread_f + swaps):
        for copy in step.waits:
            copy.incoming().wait_recv()
        if step.work is not None:
            step.work()
        for copy in step.sends:
            copy.outgoing().start()

    kv_copies = []
    for core in range(CORES):
        for src, place in ((gath_b.at[CORES * y + core, pl.ds(RING, 2)], CORES * core + p), (kv_far.at[core], CORES * core + 1 - p)):
            kv_copies.append(pltpu.make_async_copy(src, kv_out.at[:, place], loc_sem.at[len(kv_copies)]))
    kv_copies.append(pltpu.make_async_copy(grad_q_ref, grad_q_out, loc_sem.at[len(kv_copies)]))
    for copy in kv_copies:
        copy.start()
    for copy in kv_copies:
        copy.wait()
    gone([copy for copy in transfers if not copy.left])


def exchange(heads, q, k, v, grad_heads, cos_l, sin_l, w_blocks, w_key, w_value, x_rows, dout_rows, inv, gain, spread=None):
    tokens, d_model = x_rows.shape
    rows_y, width = tokens // RING, d_model // ROW_DEVICES
    chunks = CHUNKS
    spreads = (chunks, SPREAD if spread is None else spread)
    r = rows_y // chunks
    any_spec = pl.BlockSpec(memory_space=pl.ANY)
    vmem_spec = pl.BlockSpec(memory_space=pltpu.VMEM)
    depth, n_kv = ROW_DEVICES * HEAD_DIM, w_key.shape[1]
    f32, bf16 = jnp.float32, jnp.bfloat16

    def gathered(count):
        return jax.ShapeDtypeStruct((count, CORES, RING, RING, r, width), f32)

    passes = chunks * (8 + 2 * (RING - 1))
    copies = 2 * passes + chunks * (2 + ROW_DEVICES - 1) + 14 * sum(spreads) + 2
    dma = pltpu.SemaphoreType.DMA
    sums = pltpu.VMEM((2, RING - 1, chunks, r // 2, width), f32)
    return pl.pallas_call(
        functools.partial(exchange_kernel, chunks, spreads),
        out_shape=[jax.ShapeDtypeStruct(((chunks - spreads[1]) * r + 8, width), f32), gathered(spreads[0]), gathered(spreads[1]),
                   jax.ShapeDtypeStruct((2, RING, rows_y, HEAD_DIM), f32), jax.ShapeDtypeStruct(q.shape, bf16)],
        in_specs=[any_spec] * 14,
        out_specs=[vmem_spec, any_spec, any_spec, any_spec, any_spec],
        scratch_shapes=[
            pltpu.VMEM((ROW_DEVICES, RING, rows_y, HEAD_DIM), f32),
            pltpu.VMEM((ROW_DEVICES, RING + 2, rows_y, HEAD_DIM), f32),
            pltpu.VMEM((depth, width), bf16), pltpu.VMEM((depth + n_kv, width), bf16),
            pltpu.VMEM((RING, rows_y, width), f32), sums, sums,
            pltpu.VMEM((spreads[0] * r, width), f32), pltpu.VMEM((spreads[1] * r, width), f32),
            pltpu.VMEM((2, rows_y, width), bf16), pltpu.VMEM((rows_y, width), bf16), pltpu.VMEM((rows_y, 1), f32), pltpu.VMEM((1, width), f32),
            pltpu.VMEM(q.shape, bf16), pltpu.VMEM(q.shape, bf16), pltpu.VMEM(q.shape, bf16), pltpu.VMEM(q.shape, bf16),
            pltpu.VMEM(cos_l.shape, f32), pltpu.VMEM(cos_l.shape, f32), pltpu.VMEM(q.shape, bf16),
            pltpu.VMEM((RING, 2, rows_y, HEAD_DIM), f32), pltpu.VMEM((CORES, 2, rows_y, HEAD_DIM), f32),
            pltpu.VMEM((2, rows_y, HEAD_DIM), f32), pltpu.VMEM((2, rows_y, HEAD_DIM), f32), pltpu.VMEM((CORES, 2, rows_y, HEAD_DIM), f32),
            pltpu.VMEM((chunks, 8, 128), f32), pltpu.VMEM((ROW_DEVICES - 1, chunks, 8, 128), f32),
            pltpu.VMEM((2, RING, width, HEAD_DIM), bf16),
            dma((copies,)), dma((copies,)), dma((3 * ROW_DEVICES + 12 + sum(spreads),))],
        compiler_params=pltpu.CompilerParams(collective_id=1, has_side_effects=True, vmem_limit_bytes=VMEM_BYTES),
        cost_estimate=pl.CostEstimate(flops=2 * tokens * (2 * depth + n_kv) * width, bytes_accessed=16 * tokens * width, transcendentals=0),
        name='exchange',
    )(heads, q, k, v, grad_heads, cos_l, sin_l, w_blocks, w_key, w_value, x_rows, dout_rows, inv, gain)


def rounded(kernel, gathered, grid, block, index_map, out_rows, place_of, rows, so_far):
    d_model = ROW_DEVICES * gathered.shape[-1]
    moved_rows = math.prod(grid) * out_rows
    return pl.pallas_call(
        kernel, grid=grid,
        in_specs=[pl.BlockSpec(block, index_map)] + ([pl.BlockSpec(memory_space=pl.ANY)] if so_far is not None else []),
        out_specs=pl.BlockSpec((out_rows, d_model), lambda *at: (place_of(*at), 0)),
        out_shape=jax.ShapeDtypeStruct((rows, d_model), jnp.bfloat16),
        input_output_aliases={1: 0} if so_far is not None else {},
        compiler_params=pltpu.CompilerParams(vmem_limit_bytes=VMEM_BYTES),
        cost_estimate=pl.CostEstimate(flops=moved_rows * d_model, bytes_accessed=6 * moved_rows * d_model, transcendentals=0),
        name='narrow',
    )(*((gathered,) if so_far is None else (gathered, so_far)))


def narrow_spread(gathered, spread, rows, by_y, so_far=None):
    r, width = gathered.shape[-2:]
    chunks = rows // RING // r
    group = max(n for n in range(1, 5) if math.gcd(spread, chunks) % n == 0)
    block = (group, CORES, 1, RING, r, width) if by_y else (group, CORES, RING, 1, r, width)

    def kernel(in_ref, *rest):
        for k in range(group):
            for n in range(ROW_DEVICES):
                at = (k, n % CORES) + ((0, n // CORES) if by_y else (n // CORES, 0))
                rest[-1][pl.ds(k * r, r), pl.ds(n * width, width)] = in_ref[at].astype(jnp.bfloat16)

    return rounded(kernel, gathered, (spread // group, RING), block,
                   lambda k, i: (k, 0, i, 0, 0, 0) if by_y else (k, 0, 0, i, 0, 0),
                   group * r, lambda k, i: i * chunks // group + k, rows, so_far)


def narrow_rest(gathered, spread, r, rows, so_far):
    width = gathered.shape[-1]
    count = rows // RING // r - spread
    blocks = gathered.reshape(RING, RING, CORES, count * r + 8, width)
    places = rows // RING // (count * r)

    d_model = ROW_DEVICES * width
    wide = d_model // 2

    def kernel(in_ref, so_far_ref, out_ref, gain_ref):
        @pl.when(pl.program_id(1) == 0)
        def _():
            gain_ref[...] = jnp.zeros_like(gain_ref)

        for n in range(ROW_DEVICES // 2):
            columns = pl.ds(n * width, width)
            out_ref[:, columns] = in_ref[n // CORES, 0, n % CORES, pl.ds(0, count * r), :].astype(jnp.bfloat16)
            gain_ref[:, columns] += in_ref[n // CORES, 0, n % CORES, pl.ds(count * r, 1), :]

    return pl.pallas_call(
        kernel, grid=(2, RING),
        in_specs=[pl.BlockSpec((RING // 2, 1, CORES, count * r + 8, width), lambda side, x: (side, x, 0, 0, 0)),
                  pl.BlockSpec(memory_space=pl.ANY)],
        out_specs=(pl.BlockSpec((count * r, wide), lambda side, x: (x * places + spread // count, side)),
                   pl.BlockSpec((1, wide), lambda side, x: (0, side))),
        out_shape=(jax.ShapeDtypeStruct((rows, d_model), jnp.bfloat16), jax.ShapeDtypeStruct((1, d_model), jnp.float32)),
        input_output_aliases={1: 0}, compiler_params=pltpu.CompilerParams(vmem_limit_bytes=VMEM_BYTES),
        cost_estimate=pl.CostEstimate(flops=RING * count * r * d_model, bytes_accessed=6 * RING * count * r * d_model, transcendentals=0),
        name='narrow',
    )(blocks, so_far)


def solution(mesh):
    assert mesh.shape['tp'] == RING * RING * CORES

    def block_fn(hidden, grad_out, norm_gain, w_query, w_key, w_value, w_out):
        batch, seq_len, d_model = hidden.shape
        tokens, width = batch * seq_len, d_model // ROW_DEVICES
        rows_y = tokens // RING

        cos_l, sin_l = rope_lanes(seq_len)
        grad_rows = grad_out.reshape(tokens, d_model)

        inv_rms, q_rot, k_rot, v_head, grad_heads, heads, heads_send, gain, w_blocks = project(
            hidden.reshape(tokens, d_model), grad_rows, norm_gain.reshape(1, d_model), w_query, w_key, w_value, w_out, cos_l, sin_l)
        rest_block, out_spread, grad_spread, grad_kv, grad_q = exchange(
            heads_send.reshape(RING, rows_y, HEAD_DIM), q_rot, k_rot, v_head, grad_heads, cos_l, sin_l,
            w_blocks, w_key, w_value, hidden.reshape(tokens, d_model), grad_rows, inv_rms, gain)
        grad_rest = lax.all_gather(rest_block, 'tp', axis=0, tiled=True)
        r = rows_y // CHUNKS
        block_out = narrow_spread(out_spread, CHUNKS, tokens, True).reshape(hidden.shape)
        grad_hidden, gain_rows = narrow_rest(grad_rest, SPREAD, r, tokens, narrow_spread(grad_spread, SPREAD, tokens, False))
        grad_hidden, grad_gain = grad_hidden.reshape(hidden.shape), gain_rows.reshape(d_model)
        grad_w_query, grad_w_key, grad_w_value, grad_w_out = weight_grads(
            hidden.reshape(tokens, d_model), inv_rms, gain, grad_rows, grad_q, grad_kv.reshape(2, tokens, HEAD_DIM), heads)
        return block_out, grad_hidden, grad_gain, grad_w_query, grad_w_key, grad_w_value, grad_w_out

    act_spec = P('dp', None, None)
    return jax.shard_map(
        block_fn, mesh=mesh,
        in_specs=(act_spec, act_spec, P(None), P(None, 'tp'), P(None, None), P(None, None), P('tp', None)),
        out_specs=(act_spec, act_spec, P('dp'), P('dp', 'tp'), P('dp', 'tp'), P('dp', 'tp'), P(('dp', 'tp'), None)),
        check_vma=False)
```

```python
import functools
import math
import jax
import jax.numpy as jnp
from jax import lax
from jax.experimental import pallas as pl
from jax.experimental.pallas import tpu as pltpu
from jax.sharding import PartitionSpec as P

HEAD_DIM = 128
NORM_EPS = 1.0e-5
ROPE_BASE = 10000.0
MASK_VALUE = -1.0e30
SCORE_SCALE = 1.0 / math.sqrt(HEAD_DIM)
RING = 4
CORES = 2
ROW_DEVICES = RING * CORES
CHUNKS = 9
AHEAD = 3
SPREAD = 6
X_FIRST = ('010110011', '000011')
LAG = 4
VMEM_BYTES = 62 * 1024 * 1024


def rope_lanes(seq_len):
    lane = lax.broadcasted_iota(jnp.int32, (1, HEAD_DIM), 1)
    inv_freq = ROPE_BASE ** (-(lane - lane % 2).astype(jnp.float32) / HEAD_DIM)
    angles = jnp.arange(seq_len, dtype=jnp.float32)[:, None] * inv_freq
    return jnp.cos(angles), jnp.where(lane % 2 == 0, -jnp.sin(angles), jnp.sin(angles))


def rotate(tensor, cos_l, sin_l):
    lane = lax.broadcasted_iota(jnp.int32, tensor.shape, 1)
    swapped = jnp.where(lane % 2 == 0, pltpu.roll(tensor, HEAD_DIM - 1, 1), pltpu.roll(tensor, 1, 1))
    return tensor * cos_l + swapped * sin_l


NT = (((1,), (1,)), ((), ()))
TN = (((0,), (0,)), ((), ()))


def weight_grads(hidden, inv, gain, grad_out, grad_q, grad_kv, heads):
    tokens, d_model = hidden.shape
    columns = 512

    def kernel(x_ref, inv_ref, gain_ref, dout_ref, dq_ref, dkv_ref, o_ref, wq_ref, wk_ref, wv_ref, wo_ref, left_ref):
        @pl.when(pl.program_id(0) == 0)
        def _():
            pieces = (dq_ref[...].astype(jnp.float32), dkv_ref[0], dkv_ref[1], o_ref[...].astype(jnp.float32))
            for n, piece in enumerate(pieces):
                left_ref[pl.ds(n * HEAD_DIM, HEAD_DIM), :] = jnp.transpose(piece).astype(jnp.bfloat16)

        normed = (x_ref[...].astype(jnp.float32) * inv_ref[...] * gain_ref[...]).astype(jnp.bfloat16)
        grads = jnp.dot(left_ref[pl.ds(0, 3 * HEAD_DIM), :], normed, preferred_element_type=jnp.float32)
        for n, ref in enumerate((wq_ref, wk_ref, wv_ref)):
            ref[...] = jnp.transpose(grads[n * HEAD_DIM:(n + 1) * HEAD_DIM])
        wo_ref[...] = jnp.dot(left_ref[pl.ds(3 * HEAD_DIM, HEAD_DIM), :], dout_ref[...], preferred_element_type=jnp.float32)

    wide = pl.BlockSpec((tokens, columns), lambda i: (0, i))
    tall = pl.BlockSpec((columns, HEAD_DIM), lambda i: (i, 0))
    head = pl.BlockSpec((tokens, HEAD_DIM), lambda i: (0, 0))
    tall_out = jax.ShapeDtypeStruct((d_model, HEAD_DIM), jnp.float32)
    return pl.pallas_call(
        kernel, grid=(d_model // columns,),
        in_specs=[wide, pl.BlockSpec((tokens, 1), lambda i: (0, 0)), pl.BlockSpec((1, columns), lambda i: (0, i)), wide, head,
                  pl.BlockSpec((2, tokens, HEAD_DIM), lambda i: (0, 0, 0)), head],
        out_specs=(tall, tall, tall, pl.BlockSpec((HEAD_DIM, columns), lambda i: (0, i))),
        out_shape=(tall_out, tall_out, tall_out, jax.ShapeDtypeStruct((HEAD_DIM, d_model), jnp.float32)),
        scratch_shapes=[pltpu.VMEM((4 * HEAD_DIM, tokens), jnp.bfloat16)],
        compiler_params=pltpu.CompilerParams(vmem_limit_bytes=VMEM_BYTES),
        cost_estimate=pl.CostEstimate(flops=8 * tokens * d_model * HEAD_DIM, bytes_accessed=4 * tokens * d_model, transcendentals=0),
        name='weight_grads',
    )(hidden, inv, gain, grad_out, grad_q, grad_kv, heads)


class Place:
    def __init__(self):
        index = lax.axis_index('tp')
        self.c = lax.rem(index, CORES)
        self.x = lax.rem(index // CORES, RING)
        self.y = index // ROW_DEVICES

    def at(self, y, x, c):
        return {'tp': (y * RING + x) * CORES + c}


def turn(position, by):
    return lax.rem(position + (by % RING), RING)


def softmax_rows(q, k, first):
    scores = lax.dot_general(q, k, NT, preferred_element_type=jnp.float32) * SCORE_SCALE
    row = lax.broadcasted_iota(jnp.int32, scores.shape, 0) + first
    col = lax.broadcasted_iota(jnp.int32, scores.shape, 1)
    scores = jnp.where(row >= col, scores, MASK_VALUE)
    weight = jnp.exp(scores - jnp.max(scores, axis=1, keepdims=True))
    return weight * (1.0 / jnp.sum(weight, axis=1, keepdims=True))


def project(hidden, grad_out, gain, w_query, w_key, w_value, w_out, cos_l, sin_l):
    tokens, d_model = hidden.shape
    seq_len = cos_l.shape[0]
    rows = 128
    steps = tokens // rows
    width = d_model // ROW_DEVICES
    sharers = RING * ROW_DEVICES // (w_key.shape[1] // HEAD_DIM)

    def kernel(x_ref, dout_ref, gain_ref, cos_ref, sin_ref, wq_hbm, wk_hbm, wv_hbm, wo_hbm,
               inv_ref, q_ref, k_ref, v_ref, do_ref, o_ref, o_send, gain_out, got_hbm, w_ref, wo_ref, blocks, loc_sem, send_sem, recv_sem):
        me = Place()
        here = pl.ds(pl.multiple_of(pl.program_id(0) * rows, rows), rows)
        others = [(by, flip) for by in (2, 1, 3) for flip in (0, 1)] + [(0, 1)]

        def exchanges(which):
            here = me.x if which == 0 else me.y
            for n, (by, flip) in enumerate(others):
                core = 1 - me.c if flip else me.c
                there, origin = turn(here, by), turn(here, -by)
                peer = me.at(me.y, there, core) if which == 0 else me.at(there, me.x, core)

                def copy(dst, which=which, n=n, peer=peer, src=CORES * there + core):
                    return pltpu.make_async_remote_copy(
                        src_ref=blocks.at[which, src], dst_ref=got_hbm.at[which, dst], send_sem=send_sem.at[which, n],
                        recv_sem=recv_sem.at[which, n], device_id=peer, device_id_type=pl.DeviceIdType.MESH)
                yield copy(CORES * here + me.c), copy(CORES * origin + core)

        def kept(which):
            own = CORES * (me.x if which == 0 else me.y) + me.c
            return pltpu.make_async_copy(blocks.at[which, own], got_hbm.at[which, own], loc_sem.at[which])

        @pl.when(pl.program_id(0) == 0)
        def _():
            barrier = pltpu.get_barrier_semaphore()
            peers = [me.at(me.y, turn(me.x, by), 1 - me.c if flip else me.c) for by, flip in others]
            peers += [me.at(turn(me.y, by), me.x, 1 - me.c if flip else me.c) for by, flip in others[:-1]]
            for peer in peers:
                pl.semaphore_signal(barrier, inc=1, device_id=peer, device_id_type=pl.DeviceIdType.MESH)
            head = lax.axis_index('tp') // sharers
            kv_columns = pl.ds(pl.multiple_of(head * HEAD_DIM, HEAD_DIM), HEAD_DIM)
            loads = [pltpu.make_async_copy(src, dst, loc_sem.at[n]) for n, (src, dst) in enumerate((
                (wo_hbm, wo_ref), (wq_hbm, w_ref.at[:, pl.ds(0, HEAD_DIM)]),
                (wk_hbm.at[:, kv_columns], w_ref.at[:, pl.ds(HEAD_DIM, HEAD_DIM)]),
                (wv_hbm.at[:, kv_columns], w_ref.at[:, pl.ds(2 * HEAD_DIM, HEAD_DIM)])))]
            for load in loads:
                load.start()
            for load in loads:
                load.wait()
            for j in range(ROW_DEVICES):
                columns = pl.ds(j * width, width)
                blocks[0, j] = wo_ref[:, columns].astype(jnp.float32)
                blocks[1, j] = jnp.transpose(w_ref[columns, pl.ds(0, HEAD_DIM)].astype(jnp.float32))
            pl.semaphore_wait(barrier, len(peers))
            for which in (0, 1):
                for out, _ in exchanges(which):
                    out.start()
                kept(which).start()

        values = x_ref[...].astype(jnp.float32)
        inv = lax.rsqrt(jnp.mean(values * values, axis=1, keepdims=True) + NORM_EPS)
        inv_ref[...] = inv
        wide_gain = gain_ref[...].astype(jnp.float32)
        gain_out[...] = wide_gain
        normed = (values * inv * wide_gain).astype(jnp.bfloat16)
        heads = jnp.dot(normed, w_ref[...], preferred_element_type=jnp.float32)
        q_ref[here, :] = rotate(heads[:, :HEAD_DIM], cos_ref[...], sin_ref[...]).astype(jnp.bfloat16)
        k_ref[here, :] = rotate(heads[:, HEAD_DIM:2 * HEAD_DIM], cos_ref[...], sin_ref[...]).astype(jnp.bfloat16)
        v_ref[here, :] = heads[:, 2 * HEAD_DIM:].astype(jnp.bfloat16)
        do_ref[...] = lax.dot_general(dout_ref[...], wo_ref[...], NT, preferred_element_type=jnp.float32).astype(jnp.bfloat16)

        @pl.when(pl.program_id(0) == steps - 1)
        def _():
            for base in range(0, tokens, seq_len):
                rows_of = pl.ds(base, seq_len)
                probs = softmax_rows(q_ref[rows_of, :], k_ref[rows_of, :], 0).astype(jnp.bfloat16)
                attended = jnp.dot(probs, v_ref[rows_of, :], preferred_element_type=jnp.float32).astype(jnp.bfloat16)
                o_ref[rows_of, :] = attended
                o_send[rows_of, :] = attended.astype(jnp.float32)
            for which in (0, 1):
                for out, came in exchanges(which):
                    came.wait_recv()
                    out.wait_send()
                kept(which).wait()

    row_spec = pl.BlockSpec((rows, d_model), lambda i: (i, 0))
    head_spec = pl.BlockSpec((rows, HEAD_DIM), lambda i: (i, 0))
    table_spec = pl.BlockSpec((rows, HEAD_DIM), lambda i: (i % (seq_len // rows), 0))
    all_rows = pl.BlockSpec((tokens, HEAD_DIM), lambda i: (0, 0))
    any_spec = pl.BlockSpec(memory_space=pl.ANY)
    head = jax.ShapeDtypeStruct((tokens, HEAD_DIM), jnp.bfloat16)
    blocks = (2, ROW_DEVICES, HEAD_DIM, width)
    dma = pltpu.SemaphoreType.DMA
    return pl.pallas_call(
        kernel, grid=(steps,),
        in_specs=[row_spec, row_spec, pl.BlockSpec((1, d_model), lambda i: (0, 0)), table_spec, table_spec] + [any_spec] * 4,
        out_specs=(pl.BlockSpec((rows, 1), lambda i: (i, 0)), all_rows, all_rows, all_rows, head_spec, all_rows, all_rows,
                   pl.BlockSpec((1, d_model), lambda i: (0, 0)), any_spec),
        out_shape=(jax.ShapeDtypeStruct((tokens, 1), jnp.float32), head, head, head, head, head,
                   jax.ShapeDtypeStruct((tokens, HEAD_DIM), jnp.float32), jax.ShapeDtypeStruct((1, d_model), jnp.float32),
                   jax.ShapeDtypeStruct(blocks, jnp.float32)),
        scratch_shapes=[pltpu.VMEM((d_model, 3 * HEAD_DIM), jnp.bfloat16), pltpu.VMEM((HEAD_DIM, d_model), jnp.bfloat16),
                        pltpu.VMEM(blocks, jnp.float32), dma((4,)), dma((2, 7)), dma((2, 7))],
        compiler_params=pltpu.CompilerParams(collective_id=2, has_side_effects=True, vmem_limit_bytes=VMEM_BYTES),
        cost_estimate=pl.CostEstimate(flops=8 * tokens * d_model * HEAD_DIM, bytes_accessed=6 * tokens * d_model, transcendentals=0),
        name='project',
    )(hidden, grad_out, gain, cos_l, sin_l, w_query, w_key, w_value, w_out)


class Transfer:
    def __init__(self, link, size, outgoing, incoming=None):
        self.link, self.size, self.outgoing, self.incoming = link, size, outgoing, incoming or outgoing
        self.left = False


class Step:
    def __init__(self, waits=(), work=None, sends=(), after=(), cost=0.05, bulk=False):
        self.waits, self.work, self.sends, self.after, self.cost, self.bulk = waits, work, sends, after, cost, bulk


LINK_RATE = 45e3
CORE_RATE = 300e3
HOP = 2.5
CORE_HOP = 2.0
QUEUE = 12.0
STEP = 0.1


def in_order(threads):
    now, busy, arrival, finished, order = 4.0, {}, {}, set(), []
    position = [0] * len(threads)
    while any(position[i] < len(threads[i]) for i in range(len(threads))):
        chosen, soonest = None, math.inf
        for i, steps in enumerate(threads):
            if position[i] == len(steps) or any(step not in finished for step in steps[position[i]].after):
                continue
            step = steps[position[i]]
            ready = max([arrival.get(copy, math.inf) for copy in step.waits], default=0.0)
            if step.bulk:
                ready = max([ready] + [busy.get(copy.link, 0.0) - QUEUE for copy in step.sends if copy.link != 'core'])
            if ready <= now:
                chosen = i
                break
            soonest = min(soonest, ready)
        if chosen is None:
            now = soonest
            continue
        step = threads[chosen][position[chosen]]
        position[chosen] += 1
        now += step.cost + STEP
        for copy in step.sends:
            rate, hop = (CORE_RATE, CORE_HOP) if copy.link == 'core' else (LINK_RATE, HOP)
            busy[copy.link] = max(now, busy.get(copy.link, 0.0)) + copy.size / rate
            arrival[copy] = busy[copy.link] + hop
        finished.add(step)
        order.append(step)
    return order


def exchange_kernel(chunks, spreads, *refs):
    (heads_hbm, q_hbm, k_hbm, v_hbm, do_hbm, cos_hbm, sin_hbm, w_hbm, w_key_hbm, w_value_hbm, x_hbm, dout_hbm, inv_hbm, gain_hbm,
     rest_ref, out_all, grad_all, kv_out, grad_q_out,
     gath_f, gath_b, wb_f, wb_b, part, ring_f, ring_b, fin_f, fin_b, x_ref, dout_ref, inv_ref, gain_ref,
     q_ref, k_ref, v_ref, do_ref, cos_ref, sin_ref, grad_q_ref, kvp, kv_core, kv_send, kv_chip, kv_far, rowpart, rowall, w_kv, send_sem, recv_sem, loc_sem) = refs
    me = Place()
    x, y, c = me.x, me.y, me.c
    xr, xl, xo = turn(x, 1), turn(x, -1), turn(x, 2)
    yu, yd, yo = turn(y, 1), turn(y, -1), turn(y, 2)
    other = 1 - c
    rows_y, width = x_ref.shape[1:]
    r = rows_y // chunks
    h = r // 2
    to_right, to_left, to_partner = me.at(y, xr, c), me.at(y, xl, c), me.at(y, x, other)
    to_up, to_down = me.at(yu, x, c), me.at(yd, x, c)
    along_x = (('right', to_right), ('left', to_left), x, xr, xl, xo)
    along_y = (('up', to_up), ('down', to_down), y, yu, yd, yo)

    barrier = pltpu.get_barrier_semaphore()
    peers = [to_up, to_down, to_right, to_left, to_partner,
             me.at(yo, x, c), me.at(yu, x, other), me.at(yd, x, other), me.at(yo, x, other)]
    for peer in peers:
        pl.semaphore_signal(barrier, inc=1, device_id=peer, device_id_type=pl.DeviceIdType.MESH)

    depth = ROW_DEVICES * HEAD_DIM
    own_f, own_b = CORES * x + c, CORES * y + c

    def rows_at(position):
        return pl.ds(pl.multiple_of(position * rows_y, rows_y), rows_y)

    def columns_at(block):
        return pl.ds(pl.multiple_of(block * width, width), width)

    def head_at(head):
        return pl.ds(pl.multiple_of(head * HEAD_DIM, HEAD_DIM), HEAD_DIM)

    per_slot = rows_y // HEAD_DIM

    def stage(which, j):
        return part.at[2 * which + j // per_slot, pl.ds(j % per_slot * HEAD_DIM, HEAD_DIM)]

    copies = [(w_hbm.at[which, j], stage(which, j)) for which in (0, 1) for j in range(ROW_DEVICES)]
    copies += [(w.at[columns_at(own_b), head_at(2 * j + x // 2)], w_kv.at[s, j])
               for s, w in enumerate((w_key_hbm, w_value_hbm)) for j in range(RING)]
    copies += [
        (heads_hbm, gath_f.at[own_f, pl.ds(0, RING)]), (q_hbm, q_ref), (k_hbm, k_ref), (v_hbm, v_ref),
        (do_hbm, do_ref), (cos_hbm, cos_ref), (sin_hbm, sin_ref),
        (x_hbm.at[rows_at(y), columns_at(own_f)], x_ref.at[0]), (x_hbm.at[rows_at(x), columns_at(own_b)], x_ref.at[1]),
        (dout_hbm.at[rows_at(x), columns_at(own_b)], dout_ref), (inv_hbm.at[rows_at(x)], inv_ref), (gain_hbm.at[:, columns_at(own_b)], gain_ref)]
    loads = [pltpu.make_async_copy(src, dst, loc_sem.at[n]) for n, (src, dst) in enumerate(copies)]
    keep_sem = len(loads)
    for copy in loads:
        copy.start()
    first_rest = (chunks - spreads[1]) * r
    rest_ref[pl.ds(first_rest, 8), :] = jnp.zeros((8, width), jnp.float32)
    for copy in loads:
        copy.wait()
    for which, weights in enumerate((wb_f, wb_b)):
        for j in range(ROW_DEVICES):
            weights[pl.ds(j * HEAD_DIM, HEAD_DIM), :] = stage(which, j)[...].astype(jnp.bfloat16)
    for j in range(RING):
        for s in (0, 1):
            weights = jnp.transpose(w_kv[s, j].astype(jnp.float32)).astype(jnp.bfloat16)
            wb_b[pl.ds(depth + (2 * j + s) * HEAD_DIM, HEAD_DIM), :] = weights
    pl.semaphore_wait(barrier, len(peers))

    transfers = []

    def transfer(link, peer, src, dst, came_from=None, came_to=None):
        n = len(transfers)

        def copy(a, b):
            return lambda: pltpu.make_async_remote_copy(
                src_ref=a, dst_ref=b, send_sem=send_sem.at[n], recv_sem=recv_sem.at[n], device_id=peer,
                device_id_type=pl.DeviceIdType.MESH)
        made = Transfer(link, 4 * math.prod(dst.shape), copy(src, dst), copy(came_from, came_to) if came_to is not None else None)
        transfers.append(made)
        return made

    def moved(link, peer, sent, came):
        return transfer(link, peer, sent, sent, came, came)

    def gone(sent):
        for copy in sent:
            copy.outgoing().wait_send()
            copy.left = True

    seq_len = cos_ref.shape[0]
    run = seq_len // RING

    def spot(first):
        return first // rows_y, pl.ds(first % rows_y, run)

    def attend_back(base, first):
        here, keys = pl.ds(base + first, run), pl.ds(base, first + run)
        q_rows, k_rows, v_rows, grad = q_ref[here, :], k_ref[keys, :], v_ref[keys, :], do_ref[here, :]
        probs = softmax_rows(q_rows, k_rows, first)
        grad_probs = lax.dot_general(grad, v_rows, NT, preferred_element_type=jnp.float32)
        row_dot = jnp.sum(probs * grad_probs, axis=1, keepdims=True)
        grad_scores = (probs * (grad_probs - row_dot) * SCORE_SCALE).astype(jnp.bfloat16)
        at = pl.ds(first, run)
        grad_q = rotate(jnp.dot(grad_scores, k_rows, preferred_element_type=jnp.float32), cos_ref[at, :], -sin_ref[at, :])
        grad_q = grad_q.astype(jnp.bfloat16)
        grad_q_ref[here, :] = grad_q
        d, rows = spot(base + first)
        gath_b[own_b, d, rows, :] = grad_q.astype(jnp.float32)
        terms = (lax.dot_general(grad_scores, q_rows, TN, preferred_element_type=jnp.float32),
                 lax.dot_general(probs.astype(jnp.bfloat16), grad, TN, preferred_element_type=jnp.float32))
        for n, term in enumerate(terms):
            for key in range(0, first + run, run):
                d, rows = spot(base + key)
                piece = term[key:key + run]
                kvp[d, n, rows, :] = piece if key == first else kvp[d, n, rows, :] + piece

    def rotate_keys(base):
        for first in range(0, seq_len, run):
            d, rows = spot(base + first)
            at = pl.ds(first, run)
            kvp[d, 0, rows, :] = rotate(kvp[d, 0, rows, :], cos_ref[at, :], -sin_ref[at, :])

    attention = []
    for base in range(0, RING * rows_y, seq_len):
        attention += [Step((), functools.partial(attend_back, base, first), cost=0.8) for first in range(0, seq_len, run)]
        attention.append(Step((), functools.partial(rotate_keys, base), cost=0.3))

    p = lax.rem(x, 2)
    xn = x + 1 - 2 * p
    mine, theirs = CORES * c + p, CORES * c + 1 - p
    kv_threads, settle, settled = [], [], []
    for k in range(chunks):
        rows = pl.ds(k * r, r)
        core_copy = transfer('core', to_partner, kvp.at[pl.ds(CORES * other, CORES), :, rows], kv_core.at[:, :, rows])
        chip_copy = transfer('right', me.at(y, xn, c), kv_send.at[:, rows], kv_chip.at[:, rows])

        def add_core(rows=rows):
            kv_send[:, rows, :] = kvp[theirs, :, rows, :] + kv_core[1 - p, :, rows, :]

        def add_chip(rows=rows):
            total = kvp[mine, :, rows, :] + kv_core[p, :, rows, :] + kv_chip[:, rows, :]
            gath_b[own_b, pl.ds(RING, 2), rows, :] = total.astype(jnp.bfloat16).astype(jnp.float32)

        kv_threads.append([Step(sends=[core_copy], after=attention[-1:]), Step([core_copy], add_core, [chip_copy], cost=0.1, bulk=True)])
        settle.append(add_chip)
        settled.append(chip_copy)

    def add_pass(backward, gath, wb, ring, fin, spread, ahead_of):
        gather_ring, sum_ring = (along_y, along_x) if backward else (along_x, along_y)
        g_plus, g_minus, g, g_up, g_down, g_far = gather_ring
        s_plus, s_minus, s, s_up, s_down, s_far = sum_ring
        own, left, right, far = [CORES * pos + c for pos in (g, g_down, g_up, g_far)]
        p_own, p_left, p_right, p_far = [CORES * pos + other for pos in (g, g_down, g_up, g_far)]
        parts = gath.shape[1]
        half = parts // 2
        threads, passed, done, ring_sums, begun = [], [], [], [], []
        x_block = x_ref.at[1 if backward else 0]

        def multiply(by, k, before=()):
            gone(before)
            d = turn(s, by)
            rows = pl.ds(k * r, r)
            pieces = [gath[j, d, rows, :] for j in range(ROW_DEVICES)]
            if backward and by % 2 == 0:
                pieces += [gath[CORES * j + d // 2, RING + n, rows, :] for j in range(RING) for n in (0, 1)]
            lhs = jnp.concatenate([piece.astype(jnp.bfloat16) for piece in pieces], axis=1)
            part[d, rows, :] = jnp.dot(lhs, wb[pl.ds(0, lhs.shape[1]), :], preferred_element_type=jnp.float32)

        def add_ring(way, step, k):
            d = turn(s, -(2 + step) if way == 0 else 2 + step)
            part[d, pl.ds(k * r + way * h, h), :] += ring[way, step, k]

        def store(k, values):
            if k < spread:
                fin[pl.ds(k * r, r), :] = values
            else:
                rest_ref[pl.ds((k - spread) * r, r), :] = values

        def finish_forward(k):
            rows = pl.ds(k * r, r)
            store(k, (x_block[rows, :].astype(jnp.float32) + part[s, rows, :]).astype(jnp.bfloat16).astype(jnp.float32))

        def row_sums(k):
            rows = pl.ds(k * r, r)
            total = part[s, rows, :]
            unit = x_block[rows, :].astype(jnp.float32) * inv_ref[rows, :]
            row_sum = jnp.sum(total * gain_ref[...] * unit, axis=1, keepdims=True)
            square = jnp.concatenate([jnp.broadcast_to(row_sum, (r, 128)), jnp.zeros((128 - r, 128), jnp.float32)], axis=0)
            rowpart[k] = jnp.transpose(square)[0:8, :]
            gain_row = jnp.sum(total * unit, axis=0, keepdims=True)
            row_id = lax.broadcasted_iota(jnp.int32, (8, width), 0)
            rest_ref[pl.ds(first_rest, 8), :] += jnp.where(row_id == 0, jnp.broadcast_to(gain_row, (8, width)), 0.0)

        def finish_backward(k):
            rows = pl.ds(k * r, r)
            sums = rowpart[k]
            for m in range(ROW_DEVICES - 1):
                sums = sums + rowall[m, k]
            mean = jnp.transpose(sums)[0:r, 0:1] * (1.0 / (width * ROW_DEVICES))
            inv = inv_ref[rows, :]
            unit = x_block[rows, :].astype(jnp.float32) * inv
            delta = inv * (part[s, rows, :] * gain_ref[...] - unit * mean)
            store(k, (dout_ref[rows, :].astype(jnp.float32) + delta).astype(jnp.bfloat16).astype(jnp.float32))

        for k in range(chunks):
            rows = pl.ds(k * r, r)

            def block(source, first=0, count=parts, rows=rows):
                return gath.at[source, pl.ds(first, count), rows]

            s_right = moved(*g_plus, block(own), block(left))
            s_left = moved(*g_minus, block(own), block(right))
            s_core = moved('core', to_partner, block(own), block(p_own))
            f_right = moved(*g_plus, block(left, 0, half), block(far, 0, half))
            f_left = moved(*g_minus, block(right, half, parts - half), block(far, half, parts - half))
            c_left = moved('core', to_partner, block(left), block(p_left))
            c_right = moved('core', to_partner, block(right), block(p_right))
            c_far = moved('core', to_partner, block(far), block(p_far))
            sums = [[transfer(link, peer, part.at[turn(s, -(1 + step) if way == 0 else 1 + step), pl.ds(k * r + way * h, h)],
                              ring.at[way, step, k]) for step in range(RING - 1)]
                    for way, (link, peer) in enumerate((s_plus, s_minus))]
            ring_sums.append(sums[0] + sums[1])
            after = [passed[k - AHEAD]] if k >= AHEAD else []
            before = ()
            if ahead_of is not None:
                after += [ahead_of[0][k], attention[-1]]
                before = ahead_of[1][k]
            steps = [Step([settled[k]] if backward else (), settle[k] if backward else None, [s_right, s_left, s_core], after, 0.1),
                     Step([s_right], None, [f_right, c_left]), Step([s_left], None, [f_left, c_right])]
            begun.append(steps[0])
            passed.append(steps[-1])
            cost = 1.2 * r / 96
            even = 2 * cost if backward else cost
            steps += [Step([f_right, f_left], None, [c_far]),
                      Step([s_core, c_left, c_right, c_far], functools.partial(multiply, -1, k, before), [sums[0][0]], cost=cost),
                      Step((), functools.partial(multiply, 1, k), [sums[1][0]], cost=cost),
                      Step((), functools.partial(multiply, 2, k), cost=even),
                      Step((), functools.partial(multiply, 0, k), cost=even)]
            for step in range(RING - 1):
                for way in (0, 1):
                    steps.append(Step([sums[way][step]], functools.partial(add_ring, way, step, k),
                                      [sums[way][step + 1]] if step < RING - 2 else [], cost=0.15))
            if backward:
                members = [(pos, core) for pos in (yu, yd, yo) for core in (c, other)] + [(y, other)]
                notes = [transfer('note', me.at(pos, x, core), rowpart.at[k], rowall.at[m, k])
                         for (pos, core), m in zip(members, (2, 3, 0, 1, 4, 5, 6))]
                steps.append(Step((), functools.partial(row_sums, k), notes, cost=0.4))
                steps.append(Step(notes, functools.partial(finish_backward, k), cost=0.5))
            else:
                steps.append(Step((), functools.partial(finish_forward, k), cost=0.3))
            done.append(steps[-1])
            threads.append(steps)
        return threads, done, ring_sums, begun

    def add_spread(all_hbm, fin, spread, done, first_sem, x_firsts):
        threads = []
        for k in range(spread):
            x_first = x_firsts[k] == '1'
            ((a_plus, a_minus, a, a_up, a_down, a_far),
             (b_plus, b_minus, b, b_up, b_down, b_far)) = (along_x, along_y) if x_first else (along_y, along_x)

            def place(core, b_pos, a_pos, part_rows=None, k=k, x_first=x_first):
                spot = (k, core, b_pos, a_pos) if x_first else (k, core, a_pos, b_pos)
                return all_hbm.at[spot + (() if part_rows is None else (pl.ds(*part_rows),))]

            def bundle(core, b_pos, first=0, count=RING, k=k, x_first=x_first):
                return all_hbm.at[(k, core, b_pos, pl.ds(first, count)) if x_first else (k, core, pl.ds(first, count), b_pos)]

            source = fin.at[pl.ds(k * r, r)]
            keep = pltpu.make_async_copy(source, place(c, b, a), loc_sem.at[first_sem + k])
            top, low = (0, h), (h, h)
            a0 = transfer(*a_plus, source, place(c, b, a), source, place(c, b, a_down))
            a1 = transfer(*a_minus, source, place(c, b, a), source, place(c, b, a_up))
            h0 = moved(*a_plus, place(c, b, a_down, top), place(c, b, a_far, top))
            h1 = moved(*a_minus, place(c, b, a_up, low), place(c, b, a_far, low))
            b0 = moved(*b_plus, bundle(c, b, 0, 2), bundle(c, b_down, 0, 2))
            b1 = moved(*b_minus, bundle(c, b, 2, 2), bundle(c, b_up, 2, 2))
            b2 = moved(*b_plus, bundle(c, b, 2, 2), bundle(c, b_down, 2, 2))
            b3 = moved(*b_minus, bundle(c, b, 0, 2), bundle(c, b_up, 0, 2))
            g0 = moved(*b_plus, bundle(c, b_down, 0, 2), bundle(c, b_far, 0, 2))
            g1 = moved(*b_minus, bundle(c, b_up, 2, 2), bundle(c, b_far, 2, 2))
            cores = [moved('core', to_partner, bundle(c, pos), bundle(other, pos)) for pos in (b, b_down, b_up, b_far)]
            threads.append([
                Step((), keep.start, [a0, a1], (done[k],), 0.1, True),
                Step([a0], None, [h0], bulk=True), Step([a1], None, [h1], bulk=True),
                Step([h0, h1], keep.wait, [b0, b1, b2, b3, cores[0]], cost=0.1, bulk=True),
                Step([b0], None, [g0], bulk=True), Step([b1], None, [g1], bulk=True),
                Step([b2], None, [cores[1]]), Step([b3], None, [cores[2]]),
                Step([g0, g1], None, [cores[3]]), Step(cores)])
        return threads

    forward, done_f, sums_f, _ = add_pass(False, gath_f, wb_f, ring_f, fin_f, spreads[0], None)
    backward, done_b, _, begun = add_pass(True, gath_b, wb_b, ring_b, fin_b, spreads[1], (done_f, sums_f))
    spread_f = add_spread(out_all, fin_f, spreads[0], done_f, keep_sem, X_FIRST[0])
    spread_b = add_spread(grad_all, fin_b, spreads[1], done_b, keep_sem + spreads[0], X_FIRST[1])
    swap = transfer('right', me.at(y, xn, c), gath_b.at[own_b, pl.ds(RING, 2)], kv_far.at[c])
    swap_core = moved('core', to_partner, kv_far.at[c], kv_far.at[other])
    swaps = [[Step((), None, [swap], begun, bulk=True), Step([swap], None, [swap_core]), Step([swap_core])]]
    passes = []
    for k in range(chunks + LAG):
        passes += forward[k:k + 1] + (backward[k - LAG:k - LAG + 1] if k >= LAG else [])
    for step in in_order(kv_threads + passes + [attention] + spread_b + spread_f + swaps):
        for copy in step.waits:
            copy.incoming().wait_recv()
        if step.work is not None:
            step.work()
        for copy in step.sends:
            copy.outgoing().start()

    kv_copies = []
    for core in range(CORES):
        for src, place in ((gath_b.at[CORES * y + core, pl.ds(RING, 2)], CORES * core + p), (kv_far.at[core], CORES * core + 1 - p)):
            kv_copies.append(pltpu.make_async_copy(src, kv_out.at[:, place], loc_sem.at[len(kv_copies)]))
    kv_copies.append(pltpu.make_async_copy(grad_q_ref, grad_q_out, loc_sem.at[len(kv_copies)]))
    for copy in kv_copies:
        copy.start()
    for copy in kv_copies:
        copy.wait()
    gone([copy for copy in transfers if not copy.left])


def exchange(heads, q, k, v, grad_heads, cos_l, sin_l, w_blocks, w_key, w_value, x_rows, dout_rows, inv, gain, spread=None):
    tokens, d_model = x_rows.shape
    rows_y, width = tokens // RING, d_model // ROW_DEVICES
    chunks = CHUNKS
    spreads = (chunks, SPREAD if spread is None else spread)
    r = rows_y // chunks
    any_spec = pl.BlockSpec(memory_space=pl.ANY)
    vmem_spec = pl.BlockSpec(memory_space=pltpu.VMEM)
    depth, n_kv = ROW_DEVICES * HEAD_DIM, w_key.shape[1]
    f32, bf16 = jnp.float32, jnp.bfloat16

    def gathered(count):
        return jax.ShapeDtypeStruct((count, CORES, RING, RING, r, width), f32)

    passes = chunks * (8 + 2 * (RING - 1))
    copies = 2 * passes + chunks * (2 + ROW_DEVICES - 1) + 14 * sum(spreads) + 2
    dma = pltpu.SemaphoreType.DMA
    sums = pltpu.VMEM((2, RING - 1, chunks, r // 2, width), f32)
    return pl.pallas_call(
        functools.partial(exchange_kernel, chunks, spreads),
        out_shape=[jax.ShapeDtypeStruct(((chunks - spreads[1]) * r + 8, width), f32), gathered(spreads[0]), gathered(spreads[1]),
                   jax.ShapeDtypeStruct((2, RING, rows_y, HEAD_DIM), f32), jax.ShapeDtypeStruct(q.shape, bf16)],
        in_specs=[any_spec] * 14,
        out_specs=[vmem_spec, any_spec, any_spec, any_spec, any_spec],
        scratch_shapes=[
            pltpu.VMEM((ROW_DEVICES, RING, rows_y, HEAD_DIM), f32),
            pltpu.VMEM((ROW_DEVICES, RING + 2, rows_y, HEAD_DIM), f32),
            pltpu.VMEM((depth, width), bf16), pltpu.VMEM((depth + n_kv, width), bf16),
            pltpu.VMEM((RING, rows_y, width), f32), sums, sums,
            pltpu.VMEM((spreads[0] * r, width), f32), pltpu.VMEM((spreads[1] * r, width), f32),
            pltpu.VMEM((2, rows_y, width), bf16), pltpu.VMEM((rows_y, width), bf16), pltpu.VMEM((rows_y, 1), f32), pltpu.VMEM((1, width), f32),
            pltpu.VMEM(q.shape, bf16), pltpu.VMEM(q.shape, bf16), pltpu.VMEM(q.shape, bf16), pltpu.VMEM(q.shape, bf16),
            pltpu.VMEM(cos_l.shape, f32), pltpu.VMEM(cos_l.shape, f32), pltpu.VMEM(q.shape, bf16),
            pltpu.VMEM((RING, 2, rows_y, HEAD_DIM), f32), pltpu.VMEM((CORES, 2, rows_y, HEAD_DIM), f32),
            pltpu.VMEM((2, rows_y, HEAD_DIM), f32), pltpu.VMEM((2, rows_y, HEAD_DIM), f32), pltpu.VMEM((CORES, 2, rows_y, HEAD_DIM), f32),
            pltpu.VMEM((chunks, 8, 128), f32), pltpu.VMEM((ROW_DEVICES - 1, chunks, 8, 128), f32),
            pltpu.VMEM((2, RING, width, HEAD_DIM), bf16),
            dma((copies,)), dma((copies,)), dma((3 * ROW_DEVICES + 12 + sum(spreads),))],
        compiler_params=pltpu.CompilerParams(collective_id=1, has_side_effects=True, vmem_limit_bytes=VMEM_BYTES),
        cost_estimate=pl.CostEstimate(flops=2 * tokens * (2 * depth + n_kv) * width, bytes_accessed=16 * tokens * width, transcendentals=0),
        name='exchange',
    )(heads, q, k, v, grad_heads, cos_l, sin_l, w_blocks, w_key, w_value, x_rows, dout_rows, inv, gain)


def rounded(kernel, gathered, grid, block, index_map, out_rows, place_of, rows, so_far):
    d_model = ROW_DEVICES * gathered.shape[-1]
    moved_rows = math.prod(grid) * out_rows
    return pl.pallas_call(
        kernel, grid=grid,
        in_specs=[pl.BlockSpec(block, index_map)] + ([pl.BlockSpec(memory_space=pl.ANY)] if so_far is not None else []),
        out_specs=pl.BlockSpec((out_rows, d_model), lambda *at: (place_of(*at), 0)),
        out_shape=jax.ShapeDtypeStruct((rows, d_model), jnp.bfloat16),
        input_output_aliases={1: 0} if so_far is not None else {},
        compiler_params=pltpu.CompilerParams(vmem_limit_bytes=VMEM_BYTES),
        cost_estimate=pl.CostEstimate(flops=moved_rows * d_model, bytes_accessed=6 * moved_rows * d_model, transcendentals=0),
        name='narrow',
    )(*((gathered,) if so_far is None else (gathered, so_far)))


def narrow_spread(gathered, spread, rows, by_y, so_far=None):
    r, width = gathered.shape[-2:]
    chunks = rows // RING // r
    group = max(n for n in range(1, 5) if math.gcd(spread, chunks) % n == 0)
    block = (group, CORES, 1, RING, r, width) if by_y else (group, CORES, RING, 1, r, width)

    def kernel(in_ref, *rest):
        for k in range(group):
            for n in range(ROW_DEVICES):
                at = (k, n % CORES) + ((0, n // CORES) if by_y else (n // CORES, 0))
                rest[-1][pl.ds(k * r, r), pl.ds(n * width, width)] = in_ref[at].astype(jnp.bfloat16)

    return rounded(kernel, gathered, (spread // group, RING), block,
                   lambda k, i: (k, 0, i, 0, 0, 0) if by_y else (k, 0, 0, i, 0, 0),
                   group * r, lambda k, i: i * chunks // group + k, rows, so_far)


def narrow_rest(gathered, spread, r, rows, so_far):
    width = gathered.shape[-1]
    count = rows // RING // r - spread
    blocks = gathered.reshape(RING, RING, CORES, count * r + 8, width)
    places = rows // RING // (count * r)

    def kernel(in_ref, so_far_ref, out_ref, gain_ref):
        @pl.when(pl.program_id(0) == 0)
        def _():
            gain_ref[...] = jnp.zeros_like(gain_ref)

        for n in range(ROW_DEVICES):
            columns = pl.ds(n * width, width)
            out_ref[:, columns] = in_ref[n // CORES, 0, n % CORES, pl.ds(0, count * r), :].astype(jnp.bfloat16)
            gain_ref[:, columns] += in_ref[n // CORES, 0, n % CORES, pl.ds(count * r, 1), :]

    d_model = ROW_DEVICES * width
    return pl.pallas_call(
        kernel, grid=(RING,),
        in_specs=[pl.BlockSpec((RING, 1, CORES, count * r + 8, width), lambda x: (0, x, 0, 0, 0)), pl.BlockSpec(memory_space=pl.ANY)],
        out_specs=(pl.BlockSpec((count * r, d_model), lambda x: (x * places + spread // count, 0)), pl.BlockSpec((1, d_model), lambda x: (0, 0))),
        out_shape=(jax.ShapeDtypeStruct((rows, d_model), jnp.bfloat16), jax.ShapeDtypeStruct((1, d_model), jnp.float32)),
        input_output_aliases={1: 0}, compiler_params=pltpu.CompilerParams(vmem_limit_bytes=VMEM_BYTES),
        cost_estimate=pl.CostEstimate(flops=RING * count * r * d_model, bytes_accessed=6 * RING * count * r * d_model, transcendentals=0),
        name='narrow',
    )(blocks, so_far)


def solution(mesh):
    assert mesh.shape['tp'] == RING * RING * CORES

    def block_fn(hidden, grad_out, norm_gain, w_query, w_key, w_value, w_out):
        batch, seq_len, d_model = hidden.shape
        tokens, width = batch * seq_len, d_model // ROW_DEVICES
        rows_y = tokens // RING

        cos_l, sin_l = rope_lanes(seq_len)
        grad_rows = grad_out.reshape(tokens, d_model)

        inv_rms, q_rot, k_rot, v_head, grad_heads, heads, heads_send, gain, w_blocks = project(
            hidden.reshape(tokens, d_model), grad_rows, norm_gain.reshape(1, d_model), w_query, w_key, w_value, w_out, cos_l, sin_l)
        rest_block, out_spread, grad_spread, grad_kv, grad_q = exchange(
            heads_send.reshape(RING, rows_y, HEAD_DIM), q_rot, k_rot, v_head, grad_heads, cos_l, sin_l,
            w_blocks, w_key, w_value, hidden.reshape(tokens, d_model), grad_rows, inv_rms, gain)
        grad_rest = lax.all_gather(rest_block, 'tp', axis=0, tiled=True)
        r = rows_y // CHUNKS
        block_out = narrow_spread(out_spread, CHUNKS, tokens, True).reshape(hidden.shape)
        grad_hidden, gain_rows = narrow_rest(grad_rest, SPREAD, r, tokens, narrow_spread(grad_spread, SPREAD, tokens, False))
        grad_hidden, grad_gain = grad_hidden.reshape(hidden.shape), gain_rows.reshape(d_model)
        grad_w_query, grad_w_key, grad_w_value, grad_w_out = weight_grads(
            hidden.reshape(tokens, d_model), inv_rms, gain, grad_rows, grad_q, grad_kv.reshape(2, tokens, HEAD_DIM), heads)
        return block_out, grad_hidden, grad_gain, grad_w_query, grad_w_key, grad_w_value, grad_w_out

    act_spec = P('dp', None, None)
    return jax.shard_map(
        block_fn, mesh=mesh,
        in_specs=(act_spec, act_spec, P(None), P(None, 'tp'), P(None, None), P(None, None), P('tp', None)),
        out_specs=(act_spec, act_spec, P('dp'), P('dp', 'tp'), P('dp', 'tp'), P('dp', 'tp'), P(('dp', 'tp'), None)),
        check_vma=False)
```
